16 devices in a mesh: dp: 2 (over y, z), tp: 8 (over x, core).
Axes of the slice: x: 4, y: 2, z: 1, core: 2. Of those that a mesh axis runs over, the one named last changes fastest.
The devices are a block of a 4x4x8 slice.
Arguments:
- x_in: bfloat16 [16, 1536, 2048], P('dp', 'tp'), parts along dimension 0
- ln_scale: bfloat16 [2048], replicated
- w_q: bfloat16 [2048, 2048], P(None, 'tp')
- w_k: bfloat16 [2048, 256], replicated
- w_v: bfloat16 [2048, 256], replicated
- w_o: bfloat16 [2048, 2048], P('tp')
- grad_y: bfloat16 [16, 1536, 2048], P('dp', 'tp'), parts along dimension 0
Outputs:
- output 1: bfloat16 [16, 1536, 2048], P('dp', 'tp'), parts along dimension 0
- output 2: bfloat16 [16, 1536, 2048], P('dp', 'tp'), parts along dimension 0
- output 3: float32 [4096], P('dp'), parts along dimension 0
- output 4: bfloat16 [4096, 2048], P('dp', 'tp'), parts along dimension 0
- output 5: float32 [4096, 256], P('dp'), parts along dimension 0
- output 6: float32 [4096, 256], P('dp'), parts along dimension 0
- output 7: bfloat16 [4096, 2048], P(('dp', 'tp')), parts along dimension 0
There are 2 independent parts. The reference program is written for one: setup_inputs(seed, part) draws one part's arguments, and reference() takes and returns one part's arrays. A program takes and returns all parts, laid end to end along the dimension named above; an argument that names none is the same for every part.
All inputs are finite; a program needn't handle non-finite values.
Results may differ from the reference program's by a relative error of at most 0.0158944.
Values are sent between devices in bfloat16 or wider.
A program may use at most 768 MiB of HBM per device.

```python
import jax
import jax.numpy as jnp
from jax import lax

BATCH_SIZE = 8
SEQ_LEN = 1536
MODEL_DIM = 2048
NUM_HEADS = 8
HEAD_DIM = 256
Q_BLOCK = 64
QBLOCK_COUNT = SEQ_LEN // Q_BLOCK
PROJ_DIM = NUM_HEADS * HEAD_DIM
LN_EPS = 1e-6
ROPE_BASE = 10000.0


def setup_inputs(seed: int = 0, part: int = 0) -> dict:
    part_key = jax.random.fold_in(jax.random.key(seed), part)
    key_x, key_dy = jax.random.split(part_key)
    key_ln, key_q, key_k, key_v, key_o = jax.random.split(jax.random.key(seed + 1), 5)
    act_shape = (BATCH_SIZE, SEQ_LEN, MODEL_DIM)
    x_in = jax.random.normal(key_x, act_shape, jnp.float32)
    grad_y = jax.random.normal(key_dy, act_shape, jnp.float32)
    ln_scale = 1.0 + 0.3 * jax.random.normal(key_ln, (MODEL_DIM,), jnp.float32)
    w_q = jax.random.normal(key_q, (MODEL_DIM, PROJ_DIM), jnp.float32) * MODEL_DIM ** -0.5
    w_k = jax.random.normal(key_k, (MODEL_DIM, HEAD_DIM), jnp.float32) * MODEL_DIM ** -0.5
    w_v = jax.random.normal(key_v, (MODEL_DIM, HEAD_DIM), jnp.float32) * MODEL_DIM ** -0.5
    w_o = jax.random.normal(key_o, (PROJ_DIM, MODEL_DIM), jnp.float32) * PROJ_DIM ** -0.5
    return {'x_in': x_in.astype(jnp.bfloat16), 'ln_scale': ln_scale.astype(jnp.bfloat16), 'w_q': w_q.astype(jnp.bfloat16), 'w_k': w_k.astype(jnp.bfloat16), 'w_v': w_v.astype(jnp.bfloat16), 'w_o': w_o.astype(jnp.bfloat16), 'grad_y': grad_y.astype(jnp.bfloat16)}


def to_bf16(vectors):
    return vectors.astype(jnp.bfloat16).astype(jnp.float32)


def rope_tables():
    half_dim = HEAD_DIM // 2
    inv_freq = ROPE_BASE ** (-2.0 * jnp.arange(half_dim, dtype=jnp.float32) / HEAD_DIM)
    angles = jnp.arange(SEQ_LEN, dtype=jnp.float32)[:, None] * inv_freq[None, :]
    return jnp.cos(angles), jnp.sin(angles)


def rotate(vectors, cos_t, sin_t):
    half_dim = vectors.shape[-1] // 2
    lo_half = vectors[..., :half_dim]
    hi_half = vectors[..., half_dim:]
    return jnp.concatenate([lo_half * cos_t - hi_half * sin_t, hi_half * cos_t + lo_half * sin_t], axis=-1)


def attend_rows(q_rows, row_start, key_rows, value_rows):
    scores = jnp.einsum('qhd,kd->hqk', q_rows, key_rows) * HEAD_DIM ** -0.5
    q_pos = row_start + jnp.arange(Q_BLOCK)
    allowed = jnp.arange(SEQ_LEN)[None, :] <= q_pos[:, None]
    scores = jnp.where(allowed[None], scores, -1e30)
    log_norm = jax.nn.logsumexp(scores, axis=-1, keepdims=True)
    prob_rows = to_bf16(jnp.exp(scores - log_norm))
    return to_bf16(jnp.einsum('hqk,kd->qhd', prob_rows, value_rows))


def attend_sequence(seq_item):
    q_seq, key_seq, value_seq = seq_item
    attend_saved = jax.checkpoint(attend_rows)

    def map_body(map_item):
        return attend_saved(map_item[0], map_item[1], key_seq, value_seq)

    q_blocks = q_seq.reshape(QBLOCK_COUNT, Q_BLOCK, NUM_HEADS, HEAD_DIM)
    starts = jnp.arange(QBLOCK_COUNT) * Q_BLOCK
    return lax.map(map_body, (q_blocks, starts)).reshape(SEQ_LEN, NUM_HEADS, HEAD_DIM)


def block_forward(x_f32, ln_gain, w_q, w_k, w_v, w_o):
    centered = x_f32 - jnp.mean(x_f32, axis=-1, keepdims=True)
    inv_std = lax.rsqrt(jnp.mean(centered * centered, axis=-1, keepdims=True) + LN_EPS)
    normed = to_bf16(centered * inv_std * ln_gain)
    flat_hn = normed.reshape(BATCH_SIZE * SEQ_LEN, MODEL_DIM)
    cos_t, sin_t = rope_tables()
    queries = jnp.dot(flat_hn, w_q).reshape(BATCH_SIZE, SEQ_LEN, NUM_HEADS, HEAD_DIM)
    queries = to_bf16(rotate(queries, cos_t[:, None, :], sin_t[:, None, :]))
    key_rows = to_bf16(rotate(jnp.dot(flat_hn, w_k).reshape(BATCH_SIZE, SEQ_LEN, HEAD_DIM), cos_t, sin_t))
    value_rows = to_bf16(jnp.dot(flat_hn, w_v).reshape(BATCH_SIZE, SEQ_LEN, HEAD_DIM))
    attn_out = lax.map(attend_sequence, (queries, key_rows, value_rows))
    proj_out = jnp.dot(attn_out.reshape(BATCH_SIZE * SEQ_LEN, PROJ_DIM), w_o)
    return x_f32 + proj_out.reshape(BATCH_SIZE, SEQ_LEN, MODEL_DIM)


def reference(x_in, ln_scale, w_q, w_k, w_v, w_o, grad_y):
    y_f32, pullback = jax.vjp(block_forward, x_in.astype(jnp.float32), ln_scale.astype(jnp.float32), w_q.astype(jnp.float32), w_k.astype(jnp.float32), w_v.astype(jnp.float32), w_o.astype(jnp.float32))
    grad_x, grad_ln, grad_wq, grad_wk, grad_wv, grad_wo = pullback(grad_y.astype(jnp.float32))
    return (y_f32.astype(jnp.bfloat16), grad_x.astype(jnp.bfloat16), grad_ln, grad_wq.astype(jnp.bfloat16), grad_wk, grad_wv, grad_wo.astype(jnp.bfloat16))
```

```python
import functools
import jax
import jax.numpy as jnp
from jax import lax
from jax.experimental import pallas as pl
from jax.experimental.pallas import tpu as pltpu
from jax.sharding import PartitionSpec as P

LN_EPS = 1e-6
ROPE_BASE = 10000.0
LOG2E = 1.4426950408889634
F32 = jnp.float32
BF16 = jnp.bfloat16


def rope_tables(positions, head_dim):
    half_dim = head_dim // 2
    inv_freq = ROPE_BASE ** (-2.0 * jnp.arange(half_dim, dtype=F32) / head_dim)
    angles = positions.astype(F32)[:, None] * inv_freq[None, :]
    return jnp.cos(angles), jnp.sin(angles)


def rotate(vectors, cos_t, sin_t):
    half_dim = vectors.shape[-1] // 2
    lo_half = vectors[..., :half_dim]
    hi_half = vectors[..., half_dim:]
    return jnp.concatenate([lo_half * cos_t - hi_half * sin_t, hi_half * cos_t + lo_half * sin_t], axis=-1)


def dot_nn(a, b):
    return lax.dot_general(a, b, (((1,), (0,)), ((), ())), preferred_element_type=F32)


def dot_nt(a, b):
    return lax.dot_general(a, b, (((1,), (1,)), ((), ())), preferred_element_type=F32)


def attn_body(n_heads, tok, seq, d, group, q_ref, do_ref, kv_ref, cos_ref, sin_ref,
              o_ref, dq_ref, dkv_ref, bias, s_buf, p_buf, ds_buf):
    scale = d ** -0.5
    rows = group * tok
    kb = 256
    half = d // 2

    @pl.when(pl.program_id(0) == 0)
    def _():
        t0 = lax.axis_index('tp') * tok
        row = lax.broadcasted_iota(jnp.int32, (tok, seq), 0) + t0
        col = lax.broadcasted_iota(jnp.int32, (tok, seq), 1)
        bias[...] = jnp.where(col <= row, F32(3.0e38), F32(-1e30))

    for g in range(n_heads // group):
        q = jnp.concatenate([q_ref[0, g * group + j] for j in range(group)], axis=0)
        do = jnp.concatenate([do_ref[0, g * group + j] for j in range(group)], axis=0)
        for c in range(seq // kb):
            cols = slice(c * kb, (c + 1) * kb)
            s_buf[:, cols] = dot_nt(q, kv_ref[0, cols, :d])
        rb = 16
        for r in range(rows // rb):
            rs = slice(r * rb, (r + 1) * rb)
            t = (r * rb) % tok
            s = jnp.minimum(s_buf[rs, :], bias[t:t + rb, :])
            m = jnp.max(s, axis=1, keepdims=True)
            e = jnp.exp2(s * (scale * LOG2E) - m * (scale * LOG2E))
            l = jnp.sum(e, axis=1, keepdims=True)
            p_buf[rs, :] = (e * (1.0 / l)).astype(BF16)
        o = dot_nn(p_buf[...], kv_ref[0, :, d:])
        dvec = jnp.sum(o * do.astype(F32), axis=1, keepdims=True)
        o16 = o.astype(BF16)
        for j in range(group):
            o_ref[0, g * group + j] = o16[j * tok:(j + 1) * tok]
        dv_t = dot_nn(do.T, p_buf[...])
        for c in range(seq // kb):
            cols = slice(c * kb, (c + 1) * kb)
            dp = dot_nt(do, kv_ref[0, cols, d:])
            ds_buf[:, cols] = (p_buf[:, cols].astype(F32) * (dp - dvec)).astype(BF16)
        dq = dot_nn(ds_buf[...], kv_ref[0, :, :d]) * scale
        dk_t = dot_nn(q.T, ds_buf[...])
        for j in range(group):
            part = dq[j * tok:(j + 1) * tok]
            lo, hi = part[:, :half], part[:, half:]
            cs, sn = cos_ref[...], sin_ref[...]
            dq_ref[0, g * group + j, :, :half] = (lo * cs + hi * sn).astype(BF16)
            dq_ref[0, g * group + j, :, half:] = (hi * cs - lo * sn).astype(BF16)
        if g == 0:
            s_buf[:d, :] = dk_t
            s_buf[d:2 * d, :] = dv_t
            dk_acc, dv_acc = dk_t, dv_t
        else:
            dk_acc = dk_acc + dk_t
            dv_acc = dv_acc + dv_t
    dkv_ref[0, :, :d] = (dk_acc * scale).T.astype(BF16)
    dkv_ref[0, :, d:] = dv_acc.T.astype(BF16)


def attention(q, do, kv, cos_t, sin_t):
    n_batch, n_heads, tok, d = q.shape
    seq = kv.shape[1]
    group = 4
    rows = group * tok
    head_spec = pl.BlockSpec((1, n_heads, tok, d), lambda b: (b, 0, 0, 0))
    kv_spec = pl.BlockSpec((1, seq, 2 * d), lambda b: (b, 0, 0))
    tab_spec = pl.BlockSpec((tok, d // 2), lambda b: (0, 0))
    return pl.pallas_call(
        functools.partial(attn_body, n_heads, tok, seq, d, group),
        grid=(n_batch,),
        in_specs=[head_spec, head_spec, kv_spec, tab_spec, tab_spec],
        out_specs=[head_spec, head_spec, kv_spec],
        out_shape=[jax.ShapeDtypeStruct(q.shape, BF16), jax.ShapeDtypeStruct(q.shape, BF16),
                   jax.ShapeDtypeStruct(kv.shape, BF16)],
        scratch_shapes=[pltpu.VMEM((tok, seq), F32), pltpu.VMEM((rows, seq), F32),
                        pltpu.VMEM((rows, seq), BF16), pltpu.VMEM((rows, seq), BF16)],
        compiler_params=pltpu.CompilerParams(dimension_semantics=("arbitrary",), vmem_limit_bytes=56 * 2**20),
        cost_estimate=pl.CostEstimate(flops=12 * n_batch * n_heads * tok * seq * d, bytes_accessed=40 * 2**20,
                                      transcendentals=n_batch * n_heads * tok * seq),
        name="attention",
    )(q, do, kv, cos_t, sin_t)


def solution(mesh):
    act_spec = P('dp', 'tp', None)

    def device_step(x_loc, ln_scale, wq_loc, w_k, w_v, wo_loc, dy_loc):
        n_batch, tok, model_dim = x_loc.shape
        d = w_k.shape[1]
        t0 = lax.axis_index('tp') * tok
        cos_t, sin_t = rope_tables(t0 + jnp.arange(tok), d)

        wq_h = lax.all_gather(wq_loc, 'tp', axis=0)
        x_f32 = x_loc.astype(F32)
        centered = x_f32 - jnp.mean(x_f32, axis=-1, keepdims=True)
        inv_std = lax.rsqrt(jnp.mean(centered * centered, axis=-1, keepdims=True) + LN_EPS)
        x_hat = centered * inv_std
        ln_gain = ln_scale.astype(F32)
        hn = (x_hat * ln_gain).astype(BF16)
        w_kv = jnp.concatenate([w_k, w_v], axis=1)
        kv_raw = jnp.einsum('bte,ed->btd', hn, w_kv, preferred_element_type=F32)
        k_loc = rotate(kv_raw[..., :d], cos_t, sin_t)
        kv_loc = jnp.concatenate([k_loc, kv_raw[..., d:]], axis=-1).astype(BF16)
        kv_full = lax.all_gather(kv_loc, 'tp', axis=1, tiled=True)
        wo_h = lax.all_gather(wo_loc, 'tp', axis=0)
        q = jnp.einsum('bte,hed->bhtd', hn, wq_h, preferred_element_type=F32)
        q = rotate(q, cos_t, sin_t).astype(BF16)
        do = jnp.einsum('bte,hde->bhtd', dy_loc, wo_h, preferred_element_type=F32).astype(BF16)

        o, dq, dkv = attention(q, do, kv_full, cos_t, sin_t)

        dkv_loc = lax.psum_scatter(dkv, 'tp', scatter_dimension=1, tiled=True)
        gwo = jnp.einsum('bhtd,bte->hde', o, dy_loc, preferred_element_type=F32)
        gwo = lax.psum_scatter(gwo, 'tp', scatter_dimension=0, tiled=True)[0].astype(BF16)
        gwq = jnp.einsum('bte,bhtd->hed', hn, dq, preferred_element_type=F32)
        gwq = lax.psum_scatter(gwq, 'tp', scatter_dimension=0, tiled=True)[0].astype(BF16)
        y = (x_f32 + jnp.einsum('bhtd,hde->bte', o, wo_h, preferred_element_type=F32)).astype(BF16)

        dk_loc = rotate(dkv_loc[..., :d].astype(F32), cos_t, -sin_t).astype(BF16)
        dkv_loc = jnp.concatenate([dk_loc, dkv_loc[..., d:]], axis=-1)
        gwkv = jnp.einsum('bte,btd->ed', hn, dkv_loc, preferred_element_type=F32)
        gwkv = lax.psum(gwkv, 'tp')
        dhn = jnp.einsum('bhtd,hed->bte', dq, wq_h, preferred_element_type=F32)
        dhn = dhn + jnp.einsum('btd,ed->bte', dkv_loc, w_kv, preferred_element_type=F32)
        d_hat = dhn * ln_gain
        grad_ln = lax.psum(jnp.sum(dhn * x_hat, axis=(0, 1)), 'tp')
        grad_x = inv_std * (d_hat - jnp.mean(d_hat, axis=-1, keepdims=True) - x_hat * jnp.mean(d_hat * x_hat, axis=-1, keepdims=True)) + dy_loc.astype(F32)
        return y, grad_x.astype(BF16), grad_ln, gwq, gwkv[:, :d], gwkv[:, d:], gwo

    return jax.shard_map(device_step, mesh=mesh, in_specs=(act_spec, P(None), P(None, 'tp'), P(None, None), P(None, None), P('tp', None), act_spec), out_specs=(act_spec, act_spec, P('dp'), P('dp', 'tp'), P('dp', None), P('dp', None), P(('dp', 'tp'), None)), check_vma=False)
```

```python
import functools
import jax
import jax.numpy as jnp
from jax import lax
from jax.experimental import pallas as pl
from jax.experimental.pallas import tpu as pltpu
from jax.sharding import PartitionSpec as P

LN_EPS = 1e-6
ROPE_BASE = 10000.0
LOG2E = 1.4426950408889634
F32 = jnp.float32
BF16 = jnp.bfloat16


def rope_tables(positions, head_dim):
    half_dim = head_dim // 2
    inv_freq = ROPE_BASE ** (-2.0 * jnp.arange(half_dim, dtype=F32) / head_dim)
    angles = positions.astype(F32)[:, None] * inv_freq[None, :]
    return jnp.cos(angles), jnp.sin(angles)


def rotate(vectors, cos_t, sin_t):
    half_dim = vectors.shape[-1] // 2
    lo_half = vectors[..., :half_dim]
    hi_half = vectors[..., half_dim:]
    return jnp.concatenate([lo_half * cos_t - hi_half * sin_t, hi_half * cos_t + lo_half * sin_t], axis=-1)


def dot_nn(a, b):
    return lax.dot_general(a, b, (((1,), (0,)), ((), ())), preferred_element_type=F32)


def dot_nt(a, b):
    return lax.dot_general(a, b, (((1,), (1,)), ((), ())), preferred_element_type=F32)


def attn_body(n_heads, tok, seq, d, group, q_ref, do_ref, kv_ref, cos_ref, sin_ref,
              o_ref, dq_ref, dkv_ref, bias, s_buf, p_buf, ds_buf):
    scale = d ** -0.5
    rows = group * tok
    kb = 256
    half = d // 2

    @pl.when(pl.program_id(0) == 0)
    def _():
        t0 = lax.axis_index('tp') * tok
        row = lax.broadcasted_iota(jnp.int32, (tok, seq), 0) + t0
        col = lax.broadcasted_iota(jnp.int32, (tok, seq), 1)
        bias[...] = jnp.where(col <= row, F32(3.0e38), F32(-1e30))

    for g in range(n_heads // group):
        q = jnp.concatenate([q_ref[0, g * group + j] for j in range(group)], axis=0)
        do = jnp.concatenate([do_ref[0, g * group + j] for j in range(group)], axis=0)
        for c in range(seq // kb):
            cols = slice(c * kb, (c + 1) * kb)
            s_buf[:, cols] = dot_nt(q, kv_ref[0, cols, :d])
        rb = 16
        for r in range(rows // rb):
            rs = slice(r * rb, (r + 1) * rb)
            t = (r * rb) % tok
            s = jnp.minimum(s_buf[rs, :], bias[t:t + rb, :])
            m = jnp.max(s, axis=1, keepdims=True)
            e = jnp.exp2(s * (scale * LOG2E) - m * (scale * LOG2E))
            l = jnp.sum(e, axis=1, keepdims=True)
            p_buf[rs, :] = (e * (1.0 / l)).astype(BF16)
        o = dot_nn(p_buf[...], kv_ref[0, :, d:])
        dvec = jnp.sum(o * do.astype(F32), axis=1, keepdims=True)
        o16 = o.astype(BF16)
        for j in range(group):
            o_ref[0, g * group + j] = o16[j * tok:(j + 1) * tok]
        dv_t = dot_nn(do.T, p_buf[...])
        for c in range(seq // kb):
            cols = slice(c * kb, (c + 1) * kb)
            dp = dot_nt(do, kv_ref[0, cols, d:])
            ds_buf[:, cols] = (p_buf[:, cols].astype(F32) * (dp - dvec)).astype(BF16)
        dq = dot_nn(ds_buf[...], kv_ref[0, :, :d]) * scale
        dk_t = dot_nn(q.T, ds_buf[...])
        for j in range(group):
            part = dq[j * tok:(j + 1) * tok]
            lo, hi = part[:, :half], part[:, half:]
            cs, sn = cos_ref[...], sin_ref[...]
            dq_ref[0, g * group + j, :, :half] = (lo * cs + hi * sn).astype(BF16)
            dq_ref[0, g * group + j, :, half:] = (hi * cs - lo * sn).astype(BF16)
        if g == 0:
            dk_acc, dv_acc = dk_t, dv_t
        else:
            dk_acc = dk_acc + dk_t
            dv_acc = dv_acc + dv_t
    dkv_ref[0, :, :d] = (dk_acc * scale).T.astype(BF16)
    dkv_ref[0, :, d:] = dv_acc.T.astype(BF16)


def attention(q, do, kv, cos_t, sin_t):
    n_batch, n_heads, tok, d = q.shape
    seq = kv.shape[1]
    group = 4
    rows = group * tok
    head_spec = pl.BlockSpec((1, n_heads, tok, d), lambda b: (b, 0, 0, 0))
    kv_spec = pl.BlockSpec((1, seq, 2 * d), lambda b: (b, 0, 0))
    tab_spec = pl.BlockSpec((tok, d // 2), lambda b: (0, 0))
    return pl.pallas_call(
        functools.partial(attn_body, n_heads, tok, seq, d, group),
        grid=(n_batch,),
        in_specs=[head_spec, head_spec, kv_spec, tab_spec, tab_spec],
        out_specs=[head_spec, head_spec, kv_spec],
        out_shape=[jax.ShapeDtypeStruct(q.shape, BF16), jax.ShapeDtypeStruct(q.shape, BF16),
                   jax.ShapeDtypeStruct(kv.shape, BF16)],
        scratch_shapes=[pltpu.VMEM((tok, seq), F32), pltpu.VMEM((rows, seq), F32),
                        pltpu.VMEM((rows, seq), BF16), pltpu.VMEM((rows, seq), BF16)],
        compiler_params=pltpu.CompilerParams(dimension_semantics=("arbitrary",), vmem_limit_bytes=56 * 2**20),
        cost_estimate=pl.CostEstimate(flops=12 * n_batch * n_heads * tok * seq * d, bytes_accessed=40 * 2**20,
                                      transcendentals=n_batch * n_heads * tok * seq),
        name="attention",
    )(q, do, kv, cos_t, sin_t)


def rdma(src, dst, send, recv, to):
    return pltpu.make_async_remote_copy(src_ref=src, dst_ref=dst, send_sem=send, recv_sem=recv,
                                        device_id={'tp': to}, device_id_type=pl.DeviceIdType.MESH)


def ring_ids():
    me = lax.axis_index('tp')
    k = lax.rem(me, 2)
    return me, k, me + 1 - 2 * k, lax.rem(me + 2, 8), lax.rem(me + 6, 8)


def enter(peers):
    barrier = pltpu.get_barrier_semaphore()
    for p in peers:
        pl.semaphore_signal(barrier, inc=1, device_id={'tp': p}, device_id_type=pl.DeviceIdType.MESH)
    pl.semaphore_wait(barrier, len(peers))


def proj_body(nb, tok, x_hbm, g_ref, wq_hbm, wkv_ref, wo_hbm, dy_hbm, cos_ref, sin_ref,
              hn_hbm, q_hbm, do_hbm, kv_hbm, wqf_hbm, wof_hbm,
              x_v, hn_v, dy_v, wq_v, wo_v, kv_v, out_v,
              send, recv, x_sem, dy_sem, own_sem, out_sem, misc_sem, w_sem):
    n_tok, e = x_hbm.shape
    d = kv_v.shape[1] // 2
    half = d // 2
    mc = 2 * tok
    me, k, mate, cw, ccw = ring_ids()
    base = 2 * (me // 2)

    def head(off, par):
        return lax.rem(base + 2 * off + 8, 8) + par
    enter((mate, cw, ccw))

    fulls = (wq_v, wo_v)
    locs = (wq_hbm, wo_hbm)

    def half_of(w, ref, j):
        n = ref.shape[0] // 2
        return ref.at[pl.ds(j * n, n)]

    sends = []

    def send_full(w, h, j, to, own=False):
        src = locs[w] if own else fulls[w].at[h]
        c = rdma(src, fulls[w].at[h], send.at[w, j], recv.at[w, j], to)
        c.start()
        sends.append(c)

    def send_half(w, h, part, j, to):
        c = rdma(half_of(w, fulls[w].at[h], part), half_of(w, fulls[w].at[h], part), send.at[w, j], recv.at[w, j], to)
        c.start()
        sends.append(c)

    def wait_full(w, h, j):
        rdma(fulls[w].at[h], fulls[w].at[h], send.at[w, j], recv.at[w, j], mate).wait_recv()

    def wait_half(w, h, part, j):
        ref = half_of(w, fulls[w].at[h], part)
        rdma(ref, ref, send.at[w, j], recv.at[w, j], mate).wait_recv()

    for w in range(2):
        send_full(w, me, 0, cw, True)
        send_full(w, me, 1, ccw, True)
        send_full(w, me, 4, mate, True)
    own = [pltpu.make_async_copy(locs[w], fulls[w].at[me], own_sem.at[w]) for w in range(2)]
    xs = [pltpu.make_async_copy(x_hbm.at[pl.ds(b * tok, tok)], x_v.at[pl.ds(b * tok, tok)], x_sem.at[b]) for b in range(nb)]
    for c in xs:
        c.start()
    for c in own:
        c.start()
    dyc = pltpu.make_async_copy(dy_hbm, dy_v, dy_sem)
    dyc.start()

    gain = g_ref[...].astype(F32)
    for b in range(nb):
        xs[b].wait()

        @pl.loop(0, tok // 16, unroll=2)
        def _(r):
            rs = pl.ds(pl.multiple_of(b * tok + r * 16, 16), 16)
            x = x_v[rs, :].astype(F32)
            c = x - jnp.mean(x, axis=1, keepdims=True)
            inv = lax.rsqrt(jnp.mean(c * c, axis=1, keepdims=True) + LN_EPS)
            hn_v[rs, :] = (c * inv * gain).astype(BF16)
    hn_out = pltpu.make_async_copy(hn_v, hn_hbm, misc_sem.at[0])
    hn_out.start()

    def rope_rows(raw):
        lo, hi = raw[:, :half], raw[:, half:d]
        cs, sn = cos_ref[...], sin_ref[...]
        return lo * cs - hi * sn, hi * cs + lo * sn

    @pl.loop(0, n_tok // mc)
    def _(i):
        rs = pl.ds(pl.multiple_of(i * mc, mc), mc)
        raw = dot_nn(hn_v[rs, :], wkv_ref[...])
        lo, hi = rope_rows(raw)
        kv_v[rs, :half] = lo.astype(BF16)
        kv_v[rs, half:d] = hi.astype(BF16)
        kv_v[rs, d:] = raw[:, d:].astype(BF16)
    kv_out = pltpu.make_async_copy(kv_v, kv_hbm, misc_sem.at[1])
    kv_out.start()

    outs = []
    saves = []

    def save(w, h):
        c = pltpu.make_async_copy(fulls[w].at[h], (wqf_hbm, wof_hbm)[w].at[h], w_sem.at[len(saves)])
        c.start()
        saves.append(c)

    def project(w, h):
        slot = len(outs) % 4
        if len(outs) >= 4:
            outs[-4].wait()

        @pl.loop(0, n_tok // mc)
        def _(i):
            rs = pl.ds(pl.multiple_of(i * mc, mc), mc)
            if w == 0:
                lo, hi = rope_rows(dot_nn(hn_v[rs, :], wq_v[h]))
                o0 = lo.reshape(2, tok, half).astype(BF16)
                o1 = hi.reshape(2, tok, half).astype(BF16)
                out_v[slot, pl.ds(2 * i, 2), :, :half] = o0
                out_v[slot, pl.ds(2 * i, 2), :, half:] = o1
            else:
                out_v[slot, pl.ds(2 * i, 2)] = dot_nt(dy_v[rs, :], wo_v[h]).reshape(2, tok, d).astype(BF16)
        c = pltpu.make_async_copy(out_v.at[slot], (q_hbm, do_hbm)[w].at[:, h], out_sem.at[slot])
        c.start()
        outs.append(c)
        save(w, h)

    other = 1 - k
    for w in range(2):
        own[w].wait()
        if w == 1:
            dyc.wait()
        project(w, me)
        wait_full(w, mate, 4)
        project(w, mate)
    for w in range(2):
        wait_full(w, head(-1, k), 0)
        send_half(w, head(-1, k), 0, 2, cw)
        wait_full(w, head(1, k), 1)
        send_half(w, head(1, k), 1, 3, ccw)
        send_full(w, head(-1, k), 5, mate)
        send_full(w, head(1, k), 6, mate)
        project(w, head(-1, k))
        project(w, head(1, k))
        wait_full(w, head(-1, other), 5)
        project(w, head(-1, other))
        wait_full(w, head(1, other), 6)
        project(w, head(1, other))
    for w in range(2):
        wait_half(w, head(2, k), 0, 2)
        send_half(w, head(2, k), 0, 7, mate)
        wait_half(w, head(2, k), 1, 3)
        send_half(w, head(2, k), 1, 8, mate)
        project(w, head(2, k))
        wait_half(w, head(2, other), 0, 7)
        wait_half(w, head(2, other), 1, 8)
        project(w, head(2, other))
    for c in outs[-4:] + saves + [hn_out, kv_out]:
        c.wait()
    for c in sends:
        c.wait_send()


def project(x, gain, wq, w_kv, wo, dy, cos_t, sin_t):
    nb, tok, e = x.shape
    d = wq.shape[1]
    n_heads = 8
    n_tok = nb * tok
    any_spec = pl.BlockSpec(memory_space=pl.ANY)
    vmem = pl.BlockSpec(memory_space=pltpu.VMEM)
    act = jax.ShapeDtypeStruct((nb, n_heads, tok, d), BF16)
    dma = pltpu.SemaphoreType.DMA
    flops = 2 * n_tok * e * (2 * n_heads + 2) * d
    cos2, sin2 = jnp.tile(cos_t, (2, 1)), jnp.tile(sin_t, (2, 1))
    hn, q, do, kv, wqf, wof = pl.pallas_call(
        functools.partial(proj_body, nb, tok),
        in_specs=[any_spec, vmem, any_spec, vmem, any_spec, any_spec, vmem, vmem],
        out_specs=[any_spec] * 6,
        out_shape=[jax.ShapeDtypeStruct((n_tok, e), BF16), act, act, jax.ShapeDtypeStruct((n_tok, 2 * d), BF16),
                   jax.ShapeDtypeStruct((n_heads, e, d), BF16), jax.ShapeDtypeStruct((n_heads, d, e), BF16)],
        scratch_shapes=[pltpu.VMEM((n_tok, e), BF16), pltpu.VMEM((n_tok, e), BF16), pltpu.VMEM((n_tok, e), BF16),
                        pltpu.VMEM((n_heads, e, d), BF16), pltpu.VMEM((n_heads, d, e), BF16),
                        pltpu.VMEM((n_tok, 2 * d), BF16), pltpu.VMEM((4, nb, tok, d), BF16),
                        dma((2, 9)), dma((2, 9)), dma((nb,)), dma(()), dma((2,)), dma((4,)), dma((2,)), dma((16,))],
        compiler_params=pltpu.CompilerParams(collective_id=0, has_side_effects=True, vmem_limit_bytes=60 * 2**20),
        cost_estimate=pl.CostEstimate(flops=flops, bytes_accessed=60 * 2**20, transcendentals=0),
        name="project",
    )(x.reshape(n_tok, e), gain.reshape(1, e), wq, w_kv, wo, dy.reshape(n_tok, e), cos2, sin2)
    return hn.reshape(nb, tok, e), q, do, kv.reshape(nb, tok, 2 * d), wqf, wof


def solution(mesh):
    act_spec = P('dp', 'tp', None)

    def device_step(x_loc, ln_scale, wq_loc, w_k, w_v, wo_loc, dy_loc):
        n_batch, tok, model_dim = x_loc.shape
        d = w_k.shape[1]
        t0 = lax.axis_index('tp') * tok
        cos_t, sin_t = rope_tables(t0 + jnp.arange(tok), d)

        w_kv = jnp.concatenate([w_k, w_v], axis=1)
        hn, q, do, kv_loc, wq_h, wo_h = project(x_loc, ln_scale, wq_loc, w_kv, wo_loc, dy_loc, cos_t, sin_t)
        kv_full = lax.all_gather(kv_loc, 'tp', axis=1, tiled=True)
        x_f32 = x_loc.astype(F32)
        centered = x_f32 - jnp.mean(x_f32, axis=-1, keepdims=True)
        inv_std = lax.rsqrt(jnp.mean(centered * centered, axis=-1, keepdims=True) + LN_EPS)
        x_hat = centered * inv_std
        ln_gain = ln_scale.astype(F32)

        o, dq, dkv = attention(q, do, kv_full, cos_t, sin_t)

        dkv_loc = lax.psum_scatter(dkv, 'tp', scatter_dimension=1, tiled=True)
        gwo = jnp.einsum('bhtd,bte->hde', o, dy_loc, preferred_element_type=F32)
        gwo = lax.psum_scatter(gwo, 'tp', scatter_dimension=0, tiled=True)[0].astype(BF16)
        gwq = jnp.einsum('bte,bhtd->hed', hn, dq, preferred_element_type=F32)
        gwq = lax.psum_scatter(gwq, 'tp', scatter_dimension=0, tiled=True)[0].astype(BF16)
        y = (x_f32 + jnp.einsum('bhtd,hde->bte', o, wo_h, preferred_element_type=F32)).astype(BF16)

        dk_loc = rotate(dkv_loc[..., :d].astype(F32), cos_t, -sin_t).astype(BF16)
        dkv_loc = jnp.concatenate([dk_loc, dkv_loc[..., d:]], axis=-1)
        gwkv = jnp.einsum('bte,btd->ed', hn, dkv_loc, preferred_element_type=F32)
        gwkv = lax.psum(gwkv, 'tp')
        dhn = jnp.einsum('bhtd,hed->bte', dq, wq_h, preferred_element_type=F32)
        dhn = dhn + jnp.einsum('btd,ed->bte', dkv_loc, w_kv, preferred_element_type=F32)
        d_hat = dhn * ln_gain
        grad_ln = lax.psum(jnp.sum(dhn * x_hat, axis=(0, 1)), 'tp')
        grad_x = inv_std * (d_hat - jnp.mean(d_hat, axis=-1, keepdims=True) - x_hat * jnp.mean(d_hat * x_hat, axis=-1, keepdims=True)) + dy_loc.astype(F32)
        return y, grad_x.astype(BF16), grad_ln, gwq, gwkv[:, :d], gwkv[:, d:], gwo

    return jax.shard_map(device_step, mesh=mesh, in_specs=(act_spec, P(None), P(None, 'tp'), P(None, None), P(None, None), P('tp', None), act_spec), out_specs=(act_spec, act_spec, P('dp'), P('dp', 'tp'), P('dp', None), P('dp', None), P(('dp', 'tp'), None)), check_vma=False)
```

```python
import functools
import jax
import jax.numpy as jnp
from jax import lax
from jax.experimental import pallas as pl
from jax.experimental.pallas import tpu as pltpu
from jax.sharding import PartitionSpec as P

LN_EPS = 1e-6
ROPE_BASE = 10000.0
LOG2E = 1.4426950408889634
F32 = jnp.float32
BF16 = jnp.bfloat16


def rope_tables(positions, head_dim):
    half_dim = head_dim // 2
    inv_freq = ROPE_BASE ** (-2.0 * jnp.arange(half_dim, dtype=F32) / head_dim)
    angles = positions.astype(F32)[:, None] * inv_freq[None, :]
    return jnp.cos(angles), jnp.sin(angles)


def rotate(vectors, cos_t, sin_t):
    half_dim = vectors.shape[-1] // 2
    lo_half = vectors[..., :half_dim]
    hi_half = vectors[..., half_dim:]
    return jnp.concatenate([lo_half * cos_t - hi_half * sin_t, hi_half * cos_t + lo_half * sin_t], axis=-1)


def dot_nn(a, b):
    return lax.dot_general(a, b, (((1,), (0,)), ((), ())), preferred_element_type=F32)


def dot_nt(a, b):
    return lax.dot_general(a, b, (((1,), (1,)), ((), ())), preferred_element_type=F32)


def rdma(src, dst, send, recv, to):
    return pltpu.make_async_remote_copy(src_ref=src, dst_ref=dst, send_sem=send, recv_sem=recv,
                                        device_id={'tp': to}, device_id_type=pl.DeviceIdType.MESH)


def ring_ids():
    me = lax.axis_index('tp')
    k = lax.rem(me, 2)
    return me, k, me + 1 - 2 * k, lax.rem(me + 2, 8), lax.rem(me + 6, 8)


def enter(peers):
    barrier = pltpu.get_barrier_semaphore()
    for p in peers:
        pl.semaphore_signal(barrier, inc=1, device_id={'tp': p}, device_id_type=pl.DeviceIdType.MESH)
    pl.semaphore_wait(barrier, len(peers))


def attn_body(nb, n_heads, tok, seq, d, group, q_hbm, do_hbm, kvl_hbm, cos_ref, sin_ref,
              o_hbm, dq_hbm, dkv_hbm,
              kv_all, q_v, do_v, o_v, dq_v, bias, s_buf, p_buf, ds_buf, mrecv, rrecv,
              kv_send, kv_recv, m_send, m_recv, r_send, r_recv, own_sem, in_sem, out_sem, fin_sem):
    scale = d ** -0.5
    rows = group * tok
    kb = 256
    half = d // 2
    me, k, mate, cw, ccw = ring_ids()
    c = me // 2

    def blk(j):
        return pl.ds(pl.multiple_of(j * tok, 16), tok)

    def kvb(b, j):
        return kv_all.at[b, blk(j)]

    def kv_copy(b, j, tag, to, src=None):
        return rdma(kvb(b, j) if src is None else src, kvb(b, j), kv_send.at[b, tag], kv_recv.at[b, tag], to)

    def own(b):
        @pl.when(c <= 2)
        def _():
            kv_copy(b, me, 0, cw, kvl_hbm.at[b]).start()

        @pl.when(c == 0)
        def _():
            kv_copy(b, me, 2, ccw, kvl_hbm.at[b]).start()
        kv_copy(b, me, 3, mate, kvl_hbm.at[b]).start()

    def service_a(b):
        @pl.when(c >= 1)
        def _():
            kv_copy(b, me - 2, 0, cw).wait_recv()

            @pl.when(c <= 2)
            def _():
                kv_copy(b, me - 2, 1, cw).start()
            kv_copy(b, me - 2, 4, mate).start()

        @pl.when(c == 3)
        def _():
            kv_copy(b, me - 6, 2, ccw).wait_recv()
            kv_copy(b, me - 6, 6, mate).start()

    def service_b(b):
        @pl.when(c >= 2)
        def _():
            kv_copy(b, me - 4, 1, cw).wait_recv()
            kv_copy(b, me - 4, 5, mate).start()

    def own_copy(b):
        return pltpu.make_async_copy(kvl_hbm.at[b], kvb(b, me), own_sem.at[b])

    def ready(b):
        own_copy(b).wait()
        kv_copy(b, mate, 3, mate).wait_recv()
        for n, tag in ((1, 4), (2, 5), (3, 6)):
            @pl.when(c >= n)
            def _():
                kv_copy(b, mate - 2 * n, tag, mate).wait_recv()

    def drain_kv(b):
        for cond, tag in ((c <= 2, 0), ((c >= 1) & (c <= 2), 1), (c == 0, 2), (c >= 0, 3), (c >= 1, 4), (c >= 2, 5), (c == 3, 6)):
            @pl.when(cond)
            def _():
                kv_copy(b, me, tag, mate).wait_send()

    def m_copy(b, n):
        return rdma(kvb(b, 2 * n + 1 - k), mrecv.at[b, n], m_send.at[b, n], m_recv.at[b, n], mate)

    def r_copy(b, n, slot, to):
        return rdma(kvb(b, 2 * n + k), rrecv.at[b, slot], r_send.at[b, slot], r_recv.at[b, slot], to)

    def add_into(b, n, other):
        v = kv_all[b, blk(2 * n + k), :].astype(F32) + other[...].astype(F32)
        kv_all[b, blk(2 * n + k), :] = v.astype(BF16)

    def fin_copy(b):
        return pltpu.make_async_copy(kvb(b, me), dkv_hbm.at[b], fin_sem.at[b])

    def to_mate(b):
        for n in range(4):
            @pl.when(c >= n)
            def _():
                m_copy(b, n).start()

    def stage1(b):
        for n in range(4):
            @pl.when(c >= n)
            def _():
                m_copy(b, n).wait()
                add_into(b, n, mrecv.at[b, n])

        @pl.when(c == 3)
        def _():
            r_copy(b, 1, 2, ccw).start()
            r_copy(b, 2, 1, ccw).start()
            r_copy(b, 0, 0, cw).start()
            fin_copy(b).start()

        @pl.when(c == 2)
        def _():
            r_copy(b, 0, 1, ccw).start()

    def stage2(b):
        @pl.when(c == 2)
        def _():
            r_copy(b, 1, 2, ccw).wait_recv()
            add_into(b, 1, rrecv.at[b, 2])
            r_copy(b, 1, 2, ccw).start()
            r_copy(b, 2, 1, ccw).wait_recv()
            add_into(b, 2, rrecv.at[b, 1])
            fin_copy(b).start()

        @pl.when(c == 1)
        def _():
            r_copy(b, 0, 1, ccw).wait_recv()
            add_into(b, 0, rrecv.at[b, 1])
            r_copy(b, 0, 1, ccw).start()

    def stage3(b):
        @pl.when(c == 0)
        def _():
            r_copy(b, 0, 0, cw).wait_recv()
            add_into(b, 0, rrecv.at[b, 0])
            r_copy(b, 0, 1, ccw).wait_recv()
            add_into(b, 0, rrecv.at[b, 1])
            fin_copy(b).start()

        @pl.when(c == 1)
        def _():
            r_copy(b, 1, 2, ccw).wait_recv()
            add_into(b, 1, rrecv.at[b, 2])
            fin_copy(b).start()

    def load(b, slot):
        return (pltpu.make_async_copy(q_hbm.at[b], q_v.at[slot], in_sem.at[0, slot]),
                pltpu.make_async_copy(do_hbm.at[b], do_v.at[slot], in_sem.at[1, slot]))

    def store(b, slot):
        return (pltpu.make_async_copy(o_v.at[slot], o_hbm.at[b], out_sem.at[0, slot]),
                pltpu.make_async_copy(dq_v.at[slot], dq_hbm.at[b], out_sem.at[1, slot]))

    enter((mate, cw, ccw))
    for b in range(nb):
        own_copy(b).start()
    for x in load(0, 0):
        x.start()
    for b in range(min(3, nb)):
        own(b)

    @pl.loop(2 * c + 2, 8)
    def _(j):
        for b in range(nb):
            kv_all[b, blk(j), :] = jnp.zeros((tok, 2 * d), BF16)
    t0 = me * tok
    row = lax.broadcasted_iota(jnp.int32, (tok, seq), 0) + t0
    col = lax.broadcasted_iota(jnp.int32, (tok, seq), 1)
    bias[...] = jnp.where(col <= row, F32(3.0e38), F32(-1e30))
    for b in range(min(2, nb)):
        service_a(b)
    service_b(0)

    @pl.loop(0, nb)
    def _(b):
        slot = lax.rem(b, 2)

        @pl.when(b + 1 < nb)
        def _():
            for x in load(b + 1, 1 - slot):
                x.start()

        @pl.when(b + 3 < nb)
        def _():
            own(b + 3)

        @pl.when(b + 2 < nb)
        def _():
            service_a(b + 2)

        @pl.when(b + 1 < nb)
        def _():
            service_b(b + 1)

        @pl.when(b >= 1)
        def _():
            stage1(b - 1)

        @pl.when(b >= 2)
        def _():
            stage2(b - 2)
            for x in store(b - 2, slot):
                x.wait()

        @pl.when(b >= 3)
        def _():
            stage3(b - 3)
        for x in load(b, slot):
            x.wait()
        ready(b)
        k_ref = kv_all.at[b, :, :d]
        v_ref = kv_all.at[b, :, d:]
        dk_acc = dv_acc = None
        for g in range(n_heads // group):
            q = jnp.concatenate([q_v[slot, g * group + j] for j in range(group)], axis=0)
            do = jnp.concatenate([do_v[slot, g * group + j] for j in range(group)], axis=0)
            for i in range(seq // kb):
                cols = slice(i * kb, (i + 1) * kb)
                s_buf[:, cols] = dot_nt(q, k_ref[cols, :])
            rb = 16
            for r in range(rows // rb):
                rs = slice(r * rb, (r + 1) * rb)
                t = (r * rb) % tok
                s = jnp.minimum(s_buf[rs, :], bias[t:t + rb, :])
                m = jnp.max(s, axis=1, keepdims=True)
                e = jnp.exp2(s * (scale * LOG2E) - m * (scale * LOG2E))
                l = jnp.sum(e, axis=1, keepdims=True)
                p_buf[rs, :] = (e * (1.0 / l)).astype(BF16)
            o = dot_nn(p_buf[...], v_ref[...])
            dvec = jnp.sum(o * do.astype(F32), axis=1, keepdims=True)
            o16 = o.astype(BF16)
            for j in range(group):
                o_v[slot, g * group + j] = o16[j * tok:(j + 1) * tok]
            dv_t = dot_nn(do.T, p_buf[...])
            for i in range(seq // kb):
                cols = slice(i * kb, (i + 1) * kb)
                dp = dot_nt(do, v_ref[cols, :])
                ds_buf[:, cols] = (p_buf[:, cols].astype(F32) * (dp - dvec)).astype(BF16)
            dq = dot_nn(ds_buf[...], k_ref[...]) * scale
            dk_t = dot_nn(q.T, ds_buf[...])
            for j in range(group):
                part = dq[j * tok:(j + 1) * tok]
                lo, hi = part[:, :half], part[:, half:]
                cs, sn = cos_ref[...], sin_ref[...]
                dq_v[slot, g * group + j, :, :half] = (lo * cs + hi * sn).astype(BF16)
                dq_v[slot, g * group + j, :, half:] = (hi * cs - lo * sn).astype(BF16)
            dk_acc = dk_t if g == 0 else dk_acc + dk_t
            dv_acc = dv_t if g == 0 else dv_acc + dv_t
        drain_kv(b)
        kv_all[b, :, :d] = (dk_acc * scale).T.astype(BF16)
        kv_all[b, :, d:] = dv_acc.T.astype(BF16)
        for x in store(b, slot):
            x.start()
        to_mate(b)

    n = nb
    stage1(n - 1)
    stage2(n - 2)
    if n >= 3:
        stage3(n - 3)
    stage2(n - 1)
    stage3(n - 2)
    stage3(n - 1)
    for b in (n - 2, n - 1):
        for x in store(b, b % 2):
            x.wait()
    for b in range(n):
        fin_copy(b).wait()
        for cond, slot in ((c == 3, 0), (c >= 1, 1), (c >= 2, 2)):
            @pl.when(cond)
            def _():
                r_copy(b, 0, slot, cw).wait_send()


def attention(q, do, kv, cos_t, sin_t):
    nb, n_heads, tok, d = q.shape
    seq = tok * 8
    group = 4
    rows = group * tok
    any_spec = pl.BlockSpec(memory_space=pl.ANY)
    vmem = pl.BlockSpec(memory_space=pltpu.VMEM)
    dma = pltpu.SemaphoreType.DMA
    slab = pltpu.VMEM((2, n_heads, tok, d), BF16)
    return pl.pallas_call(
        functools.partial(attn_body, nb, n_heads, tok, seq, d, group),
        in_specs=[any_spec, any_spec, any_spec, vmem, vmem],
        out_specs=[any_spec, any_spec, any_spec],
        out_shape=[jax.ShapeDtypeStruct(q.shape, BF16), jax.ShapeDtypeStruct(q.shape, BF16),
                   jax.ShapeDtypeStruct(kv.shape, BF16)],
        scratch_shapes=[pltpu.VMEM((nb, seq, 2 * d), BF16), slab, slab, slab, slab,
                        pltpu.VMEM((tok, seq), F32), pltpu.VMEM((rows, seq), F32),
                        pltpu.VMEM((rows, seq), BF16), pltpu.VMEM((rows, seq), BF16),
                        pltpu.VMEM((nb, 4, tok, 2 * d), BF16), pltpu.VMEM((nb, 3, tok, 2 * d), BF16),
                        dma((nb, 7)), dma((nb, 7)), dma((nb, 4)), dma((nb, 4)), dma((nb, 3)), dma((nb, 3)),
                        dma((nb,)), dma((2, 2)), dma((2, 2)), dma((nb,))],
        compiler_params=pltpu.CompilerParams(collective_id=1, has_side_effects=True, vmem_limit_bytes=63 * 2**20),
        cost_estimate=pl.CostEstimate(flops=12 * nb * n_heads * tok * seq * d, bytes_accessed=40 * 2**20,
                                      transcendentals=nb * n_heads * tok * seq),
        name="attention",
    )(q, do, kv, cos_t, sin_t)


def proj_body(nb, tok, x_hbm, g_ref, wq_hbm, wkv_ref, wo_hbm, dy_hbm, cos_ref, sin_ref,
              hn_hbm, q_hbm, do_hbm, kv_hbm, wqf_hbm, wof_hbm,
              x_v, hn_v, dy_v, wq_v, wo_v, kv_v, out_v,
              send, recv, x_sem, dy_sem, own_sem, out_sem, misc_sem, w_sem):
    n_tok, e = x_hbm.shape
    d = kv_v.shape[1] // 2
    half = d // 2
    mc = 2 * tok
    me, k, mate, cw, ccw = ring_ids()
    base = 2 * (me // 2)

    def head(off, par):
        return lax.rem(base + 2 * off + 8, 8) + par
    enter((mate, cw, ccw))

    fulls = (wq_v, wo_v)
    locs = (wq_hbm, wo_hbm)

    def half_of(w, ref, j):
        n = ref.shape[0] // 2
        return ref.at[pl.ds(j * n, n)]

    sends = []

    def send_full(w, h, j, to, own=False):
        src = locs[w] if own else fulls[w].at[h]
        c = rdma(src, fulls[w].at[h], send.at[w, j], recv.at[w, j], to)
        c.start()
        sends.append(c)

    def send_half(w, h, part, j, to):
        c = rdma(half_of(w, fulls[w].at[h], part), half_of(w, fulls[w].at[h], part), send.at[w, j], recv.at[w, j], to)
        c.start()
        sends.append(c)

    def wait_full(w, h, j):
        rdma(fulls[w].at[h], fulls[w].at[h], send.at[w, j], recv.at[w, j], mate).wait_recv()

    def wait_half(w, h, part, j):
        ref = half_of(w, fulls[w].at[h], part)
        rdma(ref, ref, send.at[w, j], recv.at[w, j], mate).wait_recv()

    for w in range(2):
        send_full(w, me, 0, cw, True)
        send_full(w, me, 1, ccw, True)
        send_full(w, me, 4, mate, True)
    own = [pltpu.make_async_copy(locs[w], fulls[w].at[me], own_sem.at[w]) for w in range(2)]
    xs = [pltpu.make_async_copy(x_hbm.at[pl.ds(b * tok, tok)], x_v.at[pl.ds(b * tok, tok)], x_sem.at[b]) for b in range(nb)]
    for c in xs:
        c.start()
    for c in own:
        c.start()
    dyc = pltpu.make_async_copy(dy_hbm, dy_v, dy_sem)
    dyc.start()

    gain = g_ref[...].astype(F32)
    for b in range(nb):
        xs[b].wait()

        @pl.loop(0, tok // 16, unroll=2)
        def _(r):
            rs = pl.ds(pl.multiple_of(b * tok + r * 16, 16), 16)
            x = x_v[rs, :].astype(F32)
            c = x - jnp.mean(x, axis=1, keepdims=True)
            inv = lax.rsqrt(jnp.mean(c * c, axis=1, keepdims=True) + LN_EPS)
            hn_v[rs, :] = (c * inv * gain).astype(BF16)
    hn_out = pltpu.make_async_copy(hn_v, hn_hbm, misc_sem.at[0])
    hn_out.start()

    def rope_rows(raw):
        lo, hi = raw[:, :half], raw[:, half:d]
        cs, sn = cos_ref[...], sin_ref[...]
        return lo * cs - hi * sn, hi * cs + lo * sn

    @pl.loop(0, n_tok // mc)
    def _(i):
        rs = pl.ds(pl.multiple_of(i * mc, mc), mc)
        raw = dot_nn(hn_v[rs, :], wkv_ref[...])
        lo, hi = rope_rows(raw)
        kv_v[rs, :half] = lo.astype(BF16)
        kv_v[rs, half:d] = hi.astype(BF16)
        kv_v[rs, d:] = raw[:, d:].astype(BF16)
    kv_out = pltpu.make_async_copy(kv_v, kv_hbm, misc_sem.at[1])
    kv_out.start()

    outs = []
    saves = []

    def save(w, h):
        c = pltpu.make_async_copy(fulls[w].at[h], (wqf_hbm, wof_hbm)[w].at[h], w_sem.at[len(saves)])
        c.start()
        saves.append(c)

    def project(w, h):
        slot = len(outs) % 4
        if len(outs) >= 4:
            outs[-4].wait()

        @pl.loop(0, n_tok // mc)
        def _(i):
            rs = pl.ds(pl.multiple_of(i * mc, mc), mc)
            if w == 0:
                lo, hi = rope_rows(dot_nn(hn_v[rs, :], wq_v[h]))
                o0 = lo.reshape(2, tok, half).astype(BF16)
                o1 = hi.reshape(2, tok, half).astype(BF16)
                out_v[slot, pl.ds(2 * i, 2), :, :half] = o0
                out_v[slot, pl.ds(2 * i, 2), :, half:] = o1
            else:
                out_v[slot, pl.ds(2 * i, 2)] = dot_nt(dy_v[rs, :], wo_v[h]).reshape(2, tok, d).astype(BF16)
        c = pltpu.make_async_copy(out_v.at[slot], (q_hbm, do_hbm)[w].at[:, h], out_sem.at[slot])
        c.start()
        outs.append(c)
        save(w, h)

    other = 1 - k
    for w in range(2):
        own[w].wait()
        if w == 1:
            dyc.wait()
        project(w, me)
        wait_full(w, mate, 4)
        project(w, mate)
    for w in range(2):
        wait_full(w, head(-1, k), 0)
        send_half(w, head(-1, k), 0, 2, cw)
        wait_full(w, head(1, k), 1)
        send_half(w, head(1, k), 1, 3, ccw)
        send_full(w, head(-1, k), 5, mate)
        send_full(w, head(1, k), 6, mate)
        project(w, head(-1, k))
        project(w, head(1, k))
        wait_full(w, head(-1, other), 5)
        project(w, head(-1, other))
        wait_full(w, head(1, other), 6)
        project(w, head(1, other))
    for w in range(2):
        wait_half(w, head(2, k), 0, 2)
        send_half(w, head(2, k), 0, 7, mate)
        wait_half(w, head(2, k), 1, 3)
        send_half(w, head(2, k), 1, 8, mate)
        project(w, head(2, k))
        wait_half(w, head(2, other), 0, 7)
        wait_half(w, head(2, other), 1, 8)
        project(w, head(2, other))
    for c in outs[-4:] + saves + [hn_out, kv_out]:
        c.wait()
    for c in sends:
        c.wait_send()


def project(x, gain, wq, w_kv, wo, dy, cos_t, sin_t):
    nb, tok, e = x.shape
    d = wq.shape[1]
    n_heads = 8
    n_tok = nb * tok
    any_spec = pl.BlockSpec(memory_space=pl.ANY)
    vmem = pl.BlockSpec(memory_space=pltpu.VMEM)
    act = jax.ShapeDtypeStruct((nb, n_heads, tok, d), BF16)
    dma = pltpu.SemaphoreType.DMA
    flops = 2 * n_tok * e * (2 * n_heads + 2) * d
    cos2, sin2 = jnp.tile(cos_t, (2, 1)), jnp.tile(sin_t, (2, 1))
    hn, q, do, kv, wqf, wof = pl.pallas_call(
        functools.partial(proj_body, nb, tok),
        in_specs=[any_spec, vmem, any_spec, vmem, any_spec, any_spec, vmem, vmem],
        out_specs=[any_spec] * 6,
        out_shape=[jax.ShapeDtypeStruct((n_tok, e), BF16), act, act, jax.ShapeDtypeStruct((n_tok, 2 * d), BF16),
                   jax.ShapeDtypeStruct((n_heads, e, d), BF16), jax.ShapeDtypeStruct((n_heads, d, e), BF16)],
        scratch_shapes=[pltpu.VMEM((n_tok, e), BF16), pltpu.VMEM((n_tok, e), BF16), pltpu.VMEM((n_tok, e), BF16),
                        pltpu.VMEM((n_heads, e, d), BF16), pltpu.VMEM((n_heads, d, e), BF16),
                        pltpu.VMEM((n_tok, 2 * d), BF16), pltpu.VMEM((4, nb, tok, d), BF16),
                        dma((2, 9)), dma((2, 9)), dma((nb,)), dma(()), dma((2,)), dma((4,)), dma((2,)), dma((16,))],
        compiler_params=pltpu.CompilerParams(collective_id=0, has_side_effects=True, vmem_limit_bytes=60 * 2**20),
        cost_estimate=pl.CostEstimate(flops=flops, bytes_accessed=60 * 2**20, transcendentals=0),
        name="project",
    )(x.reshape(n_tok, e), gain.reshape(1, e), wq, w_kv, wo, dy.reshape(n_tok, e), cos2, sin2)
    return hn.reshape(nb, tok, e), q, do, kv.reshape(nb, tok, 2 * d), wqf, wof


def solution(mesh):
    act_spec = P('dp', 'tp', None)

    def device_step(x_loc, ln_scale, wq_loc, w_k, w_v, wo_loc, dy_loc):
        n_batch, tok, model_dim = x_loc.shape
        d = w_k.shape[1]
        t0 = lax.axis_index('tp') * tok
        cos_t, sin_t = rope_tables(t0 + jnp.arange(tok), d)

        w_kv = jnp.concatenate([w_k, w_v], axis=1)
        hn, q, do, kv_loc, wq_h, wo_h = project(x_loc, ln_scale, wq_loc, w_kv, wo_loc, dy_loc, cos_t, sin_t)
        x_f32 = x_loc.astype(F32)
        centered = x_f32 - jnp.mean(x_f32, axis=-1, keepdims=True)
        inv_std = lax.rsqrt(jnp.mean(centered * centered, axis=-1, keepdims=True) + LN_EPS)
        x_hat = centered * inv_std
        ln_gain = ln_scale.astype(F32)

        o, dq, dkv_loc = attention(q, do, kv_loc, cos_t, sin_t)
        gwo = jnp.einsum('bhtd,bte->hde', o, dy_loc, preferred_element_type=F32)
        gwo = lax.psum_scatter(gwo, 'tp', scatter_dimension=0, tiled=True)[0].astype(BF16)
        gwq = jnp.einsum('bte,bhtd->hed', hn, dq, preferred_element_type=F32)
        gwq = lax.psum_scatter(gwq, 'tp', scatter_dimension=0, tiled=True)[0].astype(BF16)
        y = (x_f32 + jnp.einsum('bhtd,hde->bte', o, wo_h, preferred_element_type=F32)).astype(BF16)

        dk_loc = rotate(dkv_loc[..., :d].astype(F32), cos_t, -sin_t).astype(BF16)
        dkv_loc = jnp.concatenate([dk_loc, dkv_loc[..., d:]], axis=-1)
        gwkv = jnp.einsum('bte,btd->ed', hn, dkv_loc, preferred_element_type=F32)
        gwkv = lax.psum(gwkv, 'tp')
        dhn = jnp.einsum('bhtd,hed->bte', dq, wq_h, preferred_element_type=F32)
        dhn = dhn + jnp.einsum('btd,ed->bte', dkv_loc, w_kv, preferred_element_type=F32)
        d_hat = dhn * ln_gain
        grad_ln = lax.psum(jnp.sum(dhn * x_hat, axis=(0, 1)), 'tp')
        grad_x = inv_std * (d_hat - jnp.mean(d_hat, axis=-1, keepdims=True) - x_hat * jnp.mean(d_hat * x_hat, axis=-1, keepdims=True)) + dy_loc.astype(F32)
        return y, grad_x.astype(BF16), grad_ln, gwq, gwkv[:, :d], gwkv[:, d:], gwo

    return jax.shard_map(device_step, mesh=mesh, in_specs=(act_spec, P(None), P(None, 'tp'), P(None, None), P(None, None), P('tp', None), act_spec), out_specs=(act_spec, act_spec, P('dp'), P('dp', 'tp'), P('dp', None), P('dp', None), P(('dp', 'tp'), None)), check_vma=False)
```

```python
import functools
import jax
import jax.numpy as jnp
from jax import lax
from jax.experimental import pallas as pl
from jax.experimental.pallas import tpu as pltpu
from jax.sharding import PartitionSpec as P

LN_EPS = 1e-6
ROPE_BASE = 10000.0
LOG2E = 1.4426950408889634
F32 = jnp.float32
BF16 = jnp.bfloat16


def rope_tables(positions, head_dim):
    half_dim = head_dim // 2
    inv_freq = ROPE_BASE ** (-2.0 * jnp.arange(half_dim, dtype=F32) / head_dim)
    angles = positions.astype(F32)[:, None] * inv_freq[None, :]
    return jnp.cos(angles), jnp.sin(angles)


def rotate(vectors, cos_t, sin_t):
    half_dim = vectors.shape[-1] // 2
    lo_half = vectors[..., :half_dim]
    hi_half = vectors[..., half_dim:]
    return jnp.concatenate([lo_half * cos_t - hi_half * sin_t, hi_half * cos_t + lo_half * sin_t], axis=-1)


def dot_nn(a, b):
    return lax.dot_general(a, b, (((1,), (0,)), ((), ())), preferred_element_type=F32)


def dot_nt(a, b):
    return lax.dot_general(a, b, (((1,), (1,)), ((), ())), preferred_element_type=F32)


def rdma(src, dst, send, recv, to):
    return pltpu.make_async_remote_copy(src_ref=src, dst_ref=dst, send_sem=send, recv_sem=recv,
                                        device_id={'tp': to}, device_id_type=pl.DeviceIdType.MESH)


def ring_ids():
    me = lax.axis_index('tp')
    k = lax.rem(me, 2)
    return me, k, me + 1 - 2 * k, lax.rem(me + 2, 8), lax.rem(me + 6, 8)


def enter(peers):
    barrier = pltpu.get_barrier_semaphore()
    for p in peers:
        pl.semaphore_signal(barrier, inc=1, device_id={'tp': p}, device_id_type=pl.DeviceIdType.MESH)
    pl.semaphore_wait(barrier, len(peers))


def attn_body(nb, n_heads, tok, seq, d, group, q_hbm, do_hbm, kvl_hbm, cos_ref, sin_ref,
              o_hbm, dq_hbm, dkv_hbm, op_hbm, dqp_hbm,
              kv_all, q_v, do_v, o_v, dq_v, bias, s_buf, p_buf, ds_buf, mrecv, rrecv,
              kv_send, kv_recv, m_send, m_recv, r_send, r_recv, own_sem, in_sem, out_sem, fin_sem, p_send, p_recv):
    scale = d ** -0.5
    rows = group * tok
    kb = 256
    half = d // 2
    me, k, mate, cw, ccw = ring_ids()
    c = me // 2

    def blk(j):
        return pl.ds(pl.multiple_of(j * tok, 16), tok)

    def kvb(b, j):
        return kv_all.at[b, blk(j)]

    def kv_copy(b, j, tag, to, src=None):
        return rdma(kvb(b, j) if src is None else src, kvb(b, j), kv_send.at[b, tag], kv_recv.at[b, tag], to)

    def own(b):
        @pl.when(c <= 2)
        def _():
            kv_copy(b, me, 0, cw, kvl_hbm.at[b]).start()

        @pl.when(c == 0)
        def _():
            kv_copy(b, me, 2, ccw, kvl_hbm.at[b]).start()
        kv_copy(b, me, 3, mate, kvl_hbm.at[b]).start()

    def service_a(b):
        @pl.when(c >= 1)
        def _():
            kv_copy(b, me - 2, 0, cw).wait_recv()

            @pl.when(c <= 2)
            def _():
                kv_copy(b, me - 2, 1, cw).start()
            kv_copy(b, me - 2, 4, mate).start()

        @pl.when(c == 3)
        def _():
            kv_copy(b, me - 6, 2, ccw).wait_recv()
            kv_copy(b, me - 6, 6, mate).start()

    def service_b(b):
        @pl.when(c >= 2)
        def _():
            kv_copy(b, me - 4, 1, cw).wait_recv()
            kv_copy(b, me - 4, 5, mate).start()

    def own_copy(b):
        return pltpu.make_async_copy(kvl_hbm.at[b], kvb(b, me), own_sem.at[b])

    def ready(b):
        own_copy(b).wait()
        kv_copy(b, mate, 3, mate).wait_recv()
        for n, tag in ((1, 4), (2, 5), (3, 6)):
            @pl.when(c >= n)
            def _():
                kv_copy(b, mate - 2 * n, tag, mate).wait_recv()

    def drain_kv(b):
        for cond, tag in ((c <= 2, 0), ((c >= 1) & (c <= 2), 1), (c == 0, 2), (c >= 0, 3), (c >= 1, 4), (c >= 2, 5), (c == 3, 6)):
            @pl.when(cond)
            def _():
                kv_copy(b, me, tag, mate).wait_send()

    def m_copy(b, n):
        return rdma(kvb(b, 2 * n + 1 - k), mrecv.at[b, n], m_send.at[b, n], m_recv.at[b, n], mate)

    def r_copy(b, n, slot, to):
        return rdma(kvb(b, 2 * n + k), rrecv.at[b, slot], r_send.at[b, slot], r_recv.at[b, slot], to)

    def add_into(b, n, other):
        v = kv_all[b, blk(2 * n + k), :].astype(F32) + other[...].astype(F32)
        kv_all[b, blk(2 * n + k), :] = v.astype(BF16)

    def fin_copy(b):
        return pltpu.make_async_copy(kvb(b, me), dkv_hbm.at[b], fin_sem.at[b])

    def to_mate(b):
        for n in range(4):
            @pl.when(c >= n)
            def _():
                m_copy(b, n).start()

    def stage1(b):
        for n in range(4):
            @pl.when(c >= n)
            def _():
                m_copy(b, n).wait()
                add_into(b, n, mrecv.at[b, n])

        @pl.when(c == 3)
        def _():
            r_copy(b, 1, 2, ccw).start()
            r_copy(b, 2, 1, ccw).start()
            r_copy(b, 0, 0, cw).start()
            fin_copy(b).start()

        @pl.when(c == 2)
        def _():
            r_copy(b, 0, 1, ccw).start()

    def stage2(b):
        @pl.when(c == 2)
        def _():
            r_copy(b, 1, 2, ccw).wait_recv()
            add_into(b, 1, rrecv.at[b, 2])
            r_copy(b, 1, 2, ccw).start()
            r_copy(b, 2, 1, ccw).wait_recv()
            add_into(b, 2, rrecv.at[b, 1])
            fin_copy(b).start()

        @pl.when(c == 1)
        def _():
            r_copy(b, 0, 1, ccw).wait_recv()
            add_into(b, 0, rrecv.at[b, 1])
            r_copy(b, 0, 1, ccw).start()

    def stage3(b):
        @pl.when(c == 0)
        def _():
            r_copy(b, 0, 0, cw).wait_recv()
            add_into(b, 0, rrecv.at[b, 0])
            r_copy(b, 0, 1, ccw).wait_recv()
            add_into(b, 0, rrecv.at[b, 1])
            fin_copy(b).start()

        @pl.when(c == 1)
        def _():
            r_copy(b, 1, 2, ccw).wait_recv()
            add_into(b, 1, rrecv.at[b, 2])
            fin_copy(b).start()

    def load(b, slot):
        return (pltpu.make_async_copy(q_hbm.at[b], q_v.at[slot], in_sem.at[0, slot]),
                pltpu.make_async_copy(do_hbm.at[b], do_v.at[slot], in_sem.at[1, slot]))

    def store(b, slot):
        return (pltpu.make_async_copy(o_v.at[slot], o_hbm.at[b], out_sem.at[0, slot]),
                pltpu.make_async_copy(dq_v.at[slot], dq_hbm.at[b], out_sem.at[1, slot]))

    def hand(b, slot):
        return (rdma(o_v.at[slot, 1 - k], op_hbm.at[b], p_send.at[0, b], p_recv.at[0, b], mate),
                rdma(dq_v.at[slot, 1 - k], dqp_hbm.at[b], p_send.at[1, b], p_recv.at[1, b], mate))

    enter((mate, cw, ccw))
    for b in range(nb):
        own_copy(b).start()
    for x in load(0, 0):
        x.start()
    for b in range(min(3, nb)):
        own(b)

    @pl.loop(2 * c + 2, 8)
    def _(j):
        for b in range(nb):
            kv_all[b, blk(j), :] = jnp.zeros((tok, 2 * d), BF16)
    t0 = me * tok
    row = lax.broadcasted_iota(jnp.int32, (tok, seq), 0) + t0
    col = lax.broadcasted_iota(jnp.int32, (tok, seq), 1)
    bias[...] = jnp.where(col <= row, F32(3.0e38), F32(-1e30))
    for b in range(min(2, nb)):
        service_a(b)
    service_b(0)

    @pl.loop(0, nb)
    def _(b):
        slot = lax.rem(b, 2)

        @pl.when(b + 1 < nb)
        def _():
            for x in load(b + 1, 1 - slot):
                x.start()

        @pl.when(b + 3 < nb)
        def _():
            own(b + 3)

        @pl.when(b + 2 < nb)
        def _():
            service_a(b + 2)

        @pl.when(b + 1 < nb)
        def _():
            service_b(b + 1)

        @pl.when(b >= 1)
        def _():
            stage1(b - 1)

        @pl.when(b >= 2)
        def _():
            stage2(b - 2)
            for x in store(b - 2, slot):
                x.wait()
            for x in hand(b - 2, slot):
                x.wait_send()

        @pl.when(b >= 3)
        def _():
            stage3(b - 3)
        for x in load(b, slot):
            x.wait()
        ready(b)
        k_ref = kv_all.at[b, :, :d]
        v_ref = kv_all.at[b, :, d:]
        dk_acc = dv_acc = None
        for g in range(n_heads // group):
            q = jnp.concatenate([q_v[slot, g * group + j] for j in range(group)], axis=0)
            do = jnp.concatenate([do_v[slot, g * group + j] for j in range(group)], axis=0)
            for i in range(seq // kb):
                cols = slice(i * kb, (i + 1) * kb)
                s_buf[:, cols] = dot_nt(q, k_ref[cols, :])
            rb = 16
            for r in range(rows // rb):
                rs = slice(r * rb, (r + 1) * rb)
                t = (r * rb) % tok
                s = jnp.minimum(s_buf[rs, :], bias[t:t + rb, :])
                m = jnp.max(s, axis=1, keepdims=True)
                e = jnp.exp2(s * (scale * LOG2E) - m * (scale * LOG2E))
                l = jnp.sum(e, axis=1, keepdims=True)
                p_buf[rs, :] = (e * (1.0 / l)).astype(BF16)
            o = dot_nn(p_buf[...], v_ref[...])
            dvec = jnp.sum(o * do.astype(F32), axis=1, keepdims=True)
            o16 = o.astype(BF16)
            for j in range(group):
                o_v[slot, j % 2, (g * group + j) // 2] = o16[j * tok:(j + 1) * tok]
            dv_t = dot_nn(do.T, p_buf[...])
            for i in range(seq // kb):
                cols = slice(i * kb, (i + 1) * kb)
                dp = dot_nt(do, v_ref[cols, :])
                ds_buf[:, cols] = (p_buf[:, cols].astype(F32) * (dp - dvec)).astype(BF16)
            dq = dot_nn(ds_buf[...], k_ref[...]) * scale
            dk_t = dot_nn(q.T, ds_buf[...])
            for j in range(group):
                part = dq[j * tok:(j + 1) * tok]
                lo, hi = part[:, :half], part[:, half:]
                cs, sn = cos_ref[...], sin_ref[...]
                dq_v[slot, j % 2, (g * group + j) // 2, :, :half] = (lo * cs + hi * sn).astype(BF16)
                dq_v[slot, j % 2, (g * group + j) // 2, :, half:] = (hi * cs - lo * sn).astype(BF16)
            dk_acc = dk_t if g == 0 else dk_acc + dk_t
            dv_acc = dv_t if g == 0 else dv_acc + dv_t
        drain_kv(b)
        kv_all[b, :, :d] = (dk_acc * scale).T.astype(BF16)
        kv_all[b, :, d:] = dv_acc.T.astype(BF16)
        for x in store(b, slot) + hand(b, slot):
            x.start()
        to_mate(b)

    n = nb
    stage1(n - 1)
    stage2(n - 2)
    if n >= 3:
        stage3(n - 3)
    stage2(n - 1)
    stage3(n - 2)
    stage3(n - 1)
    for b in (n - 2, n - 1):
        for x in store(b, b % 2):
            x.wait()
        for x in hand(b, b % 2):
            x.wait_send()
    for b in range(n):
        for x in hand(b, b % 2):
            x.wait_recv()
        fin_copy(b).wait()
        for cond, slot in ((c == 3, 0), (c >= 1, 1), (c >= 2, 2)):
            @pl.when(cond)
            def _():
                r_copy(b, 0, slot, cw).wait_send()


def attention(q, do, kv, cos_t, sin_t):
    nb, n_heads, tok, d = q.shape
    seq = tok * 8
    group = 4
    rows = group * tok
    any_spec = pl.BlockSpec(memory_space=pl.ANY)
    vmem = pl.BlockSpec(memory_space=pltpu.VMEM)
    dma = pltpu.SemaphoreType.DMA
    slab = pltpu.VMEM((2, n_heads, tok, d), BF16)
    oslab = pltpu.VMEM((2, 2, n_heads // 2, tok, d), BF16)
    out = jax.ShapeDtypeStruct((nb, 2, n_heads // 2, tok, d), BF16)
    outp = jax.ShapeDtypeStruct((nb, n_heads // 2, tok, d), BF16)
    return pl.pallas_call(
        functools.partial(attn_body, nb, n_heads, tok, seq, d, group),
        in_specs=[any_spec, any_spec, any_spec, vmem, vmem],
        out_specs=[any_spec] * 5,
        out_shape=[out, out, jax.ShapeDtypeStruct(kv.shape, BF16), outp, outp],
        scratch_shapes=[pltpu.VMEM((nb, seq, 2 * d), BF16), slab, slab, oslab, oslab,
                        pltpu.VMEM((tok, seq), F32), pltpu.VMEM((rows, seq), F32),
                        pltpu.VMEM((rows, seq), BF16), pltpu.VMEM((rows, seq), BF16),
                        pltpu.VMEM((nb, 4, tok, 2 * d), BF16), pltpu.VMEM((nb, 3, tok, 2 * d), BF16),
                        dma((nb, 7)), dma((nb, 7)), dma((nb, 4)), dma((nb, 4)), dma((nb, 3)), dma((nb, 3)),
                        dma((nb,)), dma((2, 2)), dma((2, 2)), dma((nb,)), dma((2, nb)), dma((2, nb))],
        compiler_params=pltpu.CompilerParams(collective_id=1, has_side_effects=True, vmem_limit_bytes=63 * 2**20),
        cost_estimate=pl.CostEstimate(flops=12 * nb * n_heads * tok * seq * d, bytes_accessed=40 * 2**20,
                                      transcendentals=nb * n_heads * tok * seq),
        name="attention",
    )(q, do, kv, cos_t, sin_t)


def proj_body(nb, tok, x_hbm, g_ref, wq_hbm, wkv_ref, wo_hbm, dy_hbm, cos_ref, sin_ref,
              hn_hbm, q_hbm, do_hbm, kv_hbm, wqf_hbm, wof_hbm, hnp_hbm, dyp_hbm,
              x_v, hn_v, dy_v, wq_v, wo_v, kv_v, out_v,
              send, recv, x_sem, dy_sem, own_sem, out_sem, misc_sem, w_sem, p_send, p_recv):
    n_tok, e = x_hbm.shape
    d = kv_v.shape[1] // 2
    half = d // 2
    mc = 2 * tok
    me, k, mate, cw, ccw = ring_ids()
    base = 2 * (me // 2)

    def head(off, par):
        return lax.rem(base + 2 * off + 8, 8) + par
    enter((mate, cw, ccw))

    fulls = (wq_v, wo_v)
    locs = (wq_hbm, wo_hbm)

    def half_of(w, ref, j):
        n = ref.shape[0] // 2
        return ref.at[pl.ds(j * n, n)]

    sends = []

    def send_full(w, h, j, to, own=False):
        src = locs[w] if own else fulls[w].at[h]
        c = rdma(src, fulls[w].at[h], send.at[w, j], recv.at[w, j], to)
        c.start()
        sends.append(c)

    def send_half(w, h, part, j, to):
        c = rdma(half_of(w, fulls[w].at[h], part), half_of(w, fulls[w].at[h], part), send.at[w, j], recv.at[w, j], to)
        c.start()
        sends.append(c)

    def wait_full(w, h, j):
        rdma(fulls[w].at[h], fulls[w].at[h], send.at[w, j], recv.at[w, j], mate).wait_recv()

    def wait_half(w, h, part, j):
        ref = half_of(w, fulls[w].at[h], part)
        rdma(ref, ref, send.at[w, j], recv.at[w, j], mate).wait_recv()

    for w in range(2):
        send_full(w, me, 0, cw, True)
        send_full(w, me, 1, ccw, True)
        send_full(w, me, 4, mate, True)
    own = [pltpu.make_async_copy(locs[w], fulls[w].at[me], own_sem.at[w]) for w in range(2)]
    xs = [pltpu.make_async_copy(x_hbm.at[pl.ds(b * tok, tok)], x_v.at[pl.ds(b * tok, tok)], x_sem.at[b]) for b in range(nb)]
    for c in xs:
        c.start()
    for c in own:
        c.start()
    dyc = pltpu.make_async_copy(dy_hbm, dy_v, dy_sem)
    dyc.start()

    gain = g_ref[...].astype(F32)
    for b in range(nb):
        xs[b].wait()

        @pl.loop(0, tok // 16, unroll=2)
        def _(r):
            rs = pl.ds(pl.multiple_of(b * tok + r * 16, 16), 16)
            x = x_v[rs, :].astype(F32)
            c = x - jnp.mean(x, axis=1, keepdims=True)
            inv = lax.rsqrt(jnp.mean(c * c, axis=1, keepdims=True) + LN_EPS)
            hn_v[rs, :] = (c * inv * gain).astype(BF16)
    hn_out = pltpu.make_async_copy(hn_v, hn_hbm, misc_sem.at[0])
    hn_out.start()
    to_mate = [rdma(hn_v, hnp_hbm, p_send.at[0], p_recv.at[0], mate), rdma(dy_hbm, dyp_hbm, p_send.at[1], p_recv.at[1], mate)]
    for c in to_mate:
        c.start()

    def rope_rows(raw):
        lo, hi = raw[:, :half], raw[:, half:d]
        cs, sn = cos_ref[...], sin_ref[...]
        return lo * cs - hi * sn, hi * cs + lo * sn

    @pl.loop(0, n_tok // mc)
    def _(i):
        rs = pl.ds(pl.multiple_of(i * mc, mc), mc)
        raw = dot_nn(hn_v[rs, :], wkv_ref[...])
        lo, hi = rope_rows(raw)
        kv_v[rs, :half] = lo.astype(BF16)
        kv_v[rs, half:d] = hi.astype(BF16)
        kv_v[rs, d:] = raw[:, d:].astype(BF16)
    kv_out = pltpu.make_async_copy(kv_v, kv_hbm, misc_sem.at[1])
    kv_out.start()

    outs = []
    saves = []

    def save(w, h):
        c = pltpu.make_async_copy(fulls[w].at[h], (wqf_hbm, wof_hbm)[w].at[h], w_sem.at[len(saves)])
        c.start()
        saves.append(c)

    def project(w, h):
        slot = len(outs) % 4
        if len(outs) >= 4:
            outs[-4].wait()

        @pl.loop(0, n_tok // mc)
        def _(i):
            rs = pl.ds(pl.multiple_of(i * mc, mc), mc)
            if w == 0:
                lo, hi = rope_rows(dot_nn(hn_v[rs, :], wq_v[h]))
                o0 = lo.reshape(2, tok, half).astype(BF16)
                o1 = hi.reshape(2, tok, half).astype(BF16)
                out_v[slot, pl.ds(2 * i, 2), :, :half] = o0
                out_v[slot, pl.ds(2 * i, 2), :, half:] = o1
            else:
                out_v[slot, pl.ds(2 * i, 2)] = dot_nt(dy_v[rs, :], wo_v[h]).reshape(2, tok, d).astype(BF16)
        c = pltpu.make_async_copy(out_v.at[slot], (q_hbm, do_hbm)[w].at[:, h], out_sem.at[slot])
        c.start()
        outs.append(c)
        save(w, h)

    other = 1 - k
    for w in range(2):
        own[w].wait()
        if w == 1:
            dyc.wait()
        project(w, me)
        wait_full(w, mate, 4)
        project(w, mate)
    for w in range(2):
        wait_full(w, head(-1, k), 0)
        send_half(w, head(-1, k), 0, 2, cw)
        wait_full(w, head(1, k), 1)
        send_half(w, head(1, k), 1, 3, ccw)
        send_full(w, head(-1, k), 5, mate)
        send_full(w, head(1, k), 6, mate)
        project(w, head(-1, k))
        project(w, head(1, k))
        wait_full(w, head(-1, other), 5)
        project(w, head(-1, other))
        wait_full(w, head(1, other), 6)
        project(w, head(1, other))
    for w in range(2):
        wait_half(w, head(2, k), 0, 2)
        send_half(w, head(2, k), 0, 7, mate)
        wait_half(w, head(2, k), 1, 3)
        send_half(w, head(2, k), 1, 8, mate)
        project(w, head(2, k))
        wait_half(w, head(2, other), 0, 7)
        wait_half(w, head(2, other), 1, 8)
        project(w, head(2, other))
    for c in outs[-4:] + saves + [hn_out, kv_out]:
        c.wait()
    for c in sends:
        c.wait_send()
    for c in to_mate:
        c.wait()


def project(x, gain, wq, w_kv, wo, dy, cos_t, sin_t):
    nb, tok, e = x.shape
    d = wq.shape[1]
    n_heads = 8
    n_tok = nb * tok
    any_spec = pl.BlockSpec(memory_space=pl.ANY)
    vmem = pl.BlockSpec(memory_space=pltpu.VMEM)
    act = jax.ShapeDtypeStruct((nb, n_heads, tok, d), BF16)
    dma = pltpu.SemaphoreType.DMA
    flops = 2 * n_tok * e * (2 * n_heads + 2) * d
    cos2, sin2 = jnp.tile(cos_t, (2, 1)), jnp.tile(sin_t, (2, 1))
    hn, q, do, kv, wqf, wof, hn_p, dy_p = pl.pallas_call(
        functools.partial(proj_body, nb, tok),
        in_specs=[any_spec, vmem, any_spec, vmem, any_spec, any_spec, vmem, vmem],
        out_specs=[any_spec] * 8,
        out_shape=[jax.ShapeDtypeStruct((n_tok, e), BF16), act, act, jax.ShapeDtypeStruct((n_tok, 2 * d), BF16),
                   jax.ShapeDtypeStruct((n_heads, e, d), BF16), jax.ShapeDtypeStruct((n_heads, d, e), BF16),
                   jax.ShapeDtypeStruct((n_tok, e), BF16), jax.ShapeDtypeStruct((n_tok, e), BF16)],
        scratch_shapes=[pltpu.VMEM((n_tok, e), BF16), pltpu.VMEM((n_tok, e), BF16), pltpu.VMEM((n_tok, e), BF16),
                        pltpu.VMEM((n_heads, e, d), BF16), pltpu.VMEM((n_heads, d, e), BF16),
                        pltpu.VMEM((n_tok, 2 * d), BF16), pltpu.VMEM((4, nb, tok, d), BF16),
                        dma((2, 9)), dma((2, 9)), dma((nb,)), dma(()), dma((2,)), dma((4,)), dma((2,)), dma((16,)), dma((2,)), dma((2,))],
        compiler_params=pltpu.CompilerParams(collective_id=0, has_side_effects=True, vmem_limit_bytes=60 * 2**20),
        cost_estimate=pl.CostEstimate(flops=flops, bytes_accessed=60 * 2**20, transcendentals=0),
        name="project",
    )(x.reshape(n_tok, e), gain.reshape(1, e), wq, w_kv, wo, dy.reshape(n_tok, e), cos2, sin2)
    return hn, q, do, kv.reshape(nb, tok, 2 * d), wqf, wof, hn_p, dy_p


def grads_body(nb, tok, o_hbm, op_hbm, dq_hbm, dqp_hbm, hn_hbm, hnp_hbm, dy_hbm, dyp_hbm, dkv_hbm,
               wq_hbm, wo_hbm, wkv_hbm, x_hbm, g_ref, cos_ref, sin_ref,
               y_hbm, gx_hbm, gln_ref, gwo_ref, gwq_ref, gkv_hbm,
               acc, acc_kv, rbuf, rbuf_kv, kind, kp, dkv_v, fin_kv, gln_acc, gl_recv,
               rs_send, rs_recv, kv_send, kv_recv, ag_send, ag_recv, gl_send, gl_rsem, kp_sem, ld_sem, b_sem, t_sem):
    n_tok, e = x_hbm.shape
    d = wkv_hbm.shape[1] // 2
    half = d // 2
    eh, eq = e // 2, e // 4
    me, k, mate, cw, ccw = ring_ids()
    c = me // 2
    rel = [lax.rem(c + o, 4) for o in (3, 1, 2, 0)]
    enter([lax.rem(me + o, 8) for o in range(1, 8)])

    order = ((2, 1), (2, 0))

    def hop(s, dr, j):
        src = acc.at[s, dr, dr] if j == 0 else rbuf.at[s, dr, j - 1]
        return rdma(src, rbuf.at[s, dr, j], rs_send.at[s, dr, j], rs_recv.at[s, dr, j], (cw, ccw)[dr])

    def hop_kv(dr, j):
        src = acc_kv.at[dr, dr] if j == 0 else rbuf_kv.at[dr, j - 1]
        return rdma(src, rbuf_kv.at[dr, j], kv_send.at[dr, j], kv_recv.at[dr, j], (cw, ccw)[dr])

    def add(dst, term):
        @pl.loop(0, dst.shape[0] // 32)
        def _(i):
            rs = pl.ds(pl.multiple_of(i * 32, 32), 32)
            dst[rs, :] = dst[rs, :] + term[rs, :]

    def pass_on(s, j):
        for dr in range(2):
            hop(s, dr, j - 1).wait_recv()
            add(rbuf.at[s, dr, j - 1], acc.at[s, order[dr][j - 1], dr])
            hop(s, dr, j).start()

    def pass_on_kv(j):
        for dr in range(2):
            hop_kv(dr, j - 1).wait_recv()
            add(rbuf_kv.at[dr, j - 1], acc_kv.at[order[dr][j - 1], dr])
            hop_kv(dr, j).start()

    def finish(s, out):
        for dr in range(2):
            hop(s, dr, 2).wait_recv()

            @pl.loop(0, d // 32)
            def _(i):
                rs = pl.ds(pl.multiple_of(i * 32, 32), 32)
                out[rs, dr * eh:(dr + 1) * eh] = (rbuf[s, dr, 2, rs, :] + acc[s, 3, dr, rs, :]).astype(BF16)

    def piece(kk, j, lo=0, n=None):
        return gkv_hbm.at[kk, pl.ds(lo, d if n is None else n), pl.ds(pl.multiple_of(j * eq, 128), eq)]

    def ag(tag, ref, to, src=None):
        return rdma(ref if src is None else src, ref, ag_send.at[tag], ag_recv.at[tag], to)

    def ag_far(tag, to):
        return ag(tag, piece(k, rel[(0, 1)[tag - 3]], (tag - 3) * half, half), to)

    own_piece = pltpu.make_async_copy(fin_kv, piece(k, c), t_sem.at[5])

    def finish_kv():
        for dr in range(2):
            hop_kv(dr, 2).wait_recv()
            fin_kv[:, dr * (eq // 2):(dr + 1) * (eq // 2)] = rbuf_kv[dr, 2] + acc_kv[3, dr]
        ag(0, piece(k, c), cw, fin_kv).start()
        ag(1, piece(k, c), ccw, fin_kv).start()
        ag(2, piece(k, c), mate, fin_kv).start()
        own_piece.start()

    def ag_forward():
        ag(0, piece(k, rel[0]), cw).wait_recv()
        ag_far(3, cw).start()
        ag(1, piece(k, rel[1]), cw).wait_recv()
        ag_far(4, ccw).start()
        ag(5, piece(k, rel[0]), mate).start()
        ag(6, piece(k, rel[1]), mate).start()

    def ag_last():
        far = [piece(k, rel[2], i * half, half) for i in range(2)]
        for i in range(2):
            ag(3 + i, far[i], cw).wait_recv()
            ag(7 + i, far[i], mate).start()
        ag(2, piece(1 - k, c), mate).wait_recv()
        ag(5, piece(1 - k, rel[0]), mate).wait_recv()
        ag(6, piece(1 - k, rel[1]), mate).wait_recv()
        for i in range(2):
            ag(7 + i, piece(1 - k, rel[2], i * half, half), mate).wait_recv()
        for tag in range(3):
            ag(tag, piece(k, c), cw, fin_kv).wait_send()
        for tag in (3, 4, 7, 8):
            ag(tag, far[0], cw).wait_send()
        for tag in (5, 6):
            ag(tag, piece(k, c), cw).wait_send()
        own_piece.wait()

    dkv_in = pltpu.make_async_copy(dkv_hbm, dkv_v, t_sem.at[4])
    dkv_in.start()
    kp_copy = rdma(kind.at[1 - k], kp, kp_sem.at[0], kp_sem.at[1], mate)

    def products(big, a_v, at):
        def load_b(own, other):
            return (pltpu.make_async_copy(own, big.at[0], b_sem.at[0]), pltpu.make_async_copy(other, big.at[1], b_sem.at[1]))

        def load_a(i, own, other, r):
            return (pltpu.make_async_copy(own.at[:, k, rel[r]], a_v.at[i % 2, 0], ld_sem.at[i % 2, 0]),
                    pltpu.make_async_copy(other.at[:, rel[r]], a_v.at[i % 2, 1], ld_sem.at[i % 2, 1]))

        def turn(j, src):
            for i in range(nb // 2):
                at[j, :, 2 * i * tok:(2 * i + 2) * tok] = jnp.concatenate([src[2 * i], src[2 * i + 1]], axis=0).T

        def both(cols):
            return dot_nn(at[0], big[0, :, cols]) + dot_nn(at[1], big[1, :, cols])

        hn_in = load_b(hn_hbm, hnp_hbm)
        for x in hn_in:
            x.start()
        jobs = [(1, r) for r in range(4)] + [(0, r) for r in range(4)]

        def fetch(i):
            s, r = jobs[i]
            return load_a(i, (o_hbm, dq_hbm)[s], (op_hbm, dqp_hbm)[s], r)
        for i in range(2):
            for x in fetch(i):
                x.start()
        dkv_in.wait()
        for b in range(nb):
            lo, hi = dkv_v[b, :, :half].astype(F32), dkv_v[b, :, half:d].astype(F32)
            cs, sn = cos_ref[...], sin_ref[...]
            kind[0, b, :, :half] = (lo * cs + hi * sn).astype(BF16)
            kind[0, b, :, half:] = (hi * cs - lo * sn).astype(BF16)
            kind[1, b] = dkv_v[b, :, d:]
        kp_copy.start()
        turn(0, kind.at[k])
        for x in hn_in:
            x.wait()
        kp_copy.wait_recv()
        turn(1, kp)
        for r in range(4):
            for dr in range(2):
                acc_kv[r, dr] = both(pl.ds(pl.multiple_of(rel[r] * eq + dr * (eq // 2), 128), eq // 2))
        for dr in range(2):
            hop_kv(dr, 0).start()

        for i, (s, r) in enumerate(jobs):
            if i == 4:
                dy_in = load_b(dy_hbm, dyp_hbm)
                for x in dy_in:
                    x.start()
            for x in fetch(i):
                x.wait()
            turn(0, a_v.at[i % 2, 0])
            turn(1, a_v.at[i % 2, 1])
            if i + 2 < 8:
                for x in fetch(i + 2):
                    x.start()
            if i == 4:
                for x in dy_in:
                    x.wait()

            @pl.loop(0, 4)
            def _(n):
                cols = pl.ds(pl.multiple_of(n * eq, 128), eq)
                acc[s, r, n // 2, :, pl.ds(pl.multiple_of(lax.rem(n, 2) * eq, 128), eq)] = both(cols)
            if r < 2:
                hop(s, r, 0).start()
            if i == 1:
                pass_on_kv(1)
            if i == 5:
                pass_on(1, 1)
                pass_on_kv(2)

    pl.run_scoped(products, pltpu.VMEM((2, n_tok, e), BF16), pltpu.VMEM((2, 2, nb, tok, d), BF16), pltpu.VMEM((2, d, n_tok), BF16))

    mc = 2 * tok
    units = nb // 2

    def attn_out(wo_v, o_v, x_v, y_v):
        w_in = pltpu.make_async_copy(wo_hbm, wo_v, b_sem.at[0])
        w_in.start()

        def load(u):
            return (pltpu.make_async_copy(o_hbm.at[pl.ds(2 * u, 2)], o_v.at[u % 2], ld_sem.at[u % 2, 0]),
                    pltpu.make_async_copy(x_hbm.at[pl.ds(u * mc, mc)], x_v.at[u % 2], ld_sem.at[u % 2, 1]))

        def put(u):
            return pltpu.make_async_copy(y_v.at[u % 2], y_hbm.at[pl.ds(u * mc, mc)], t_sem.at[u % 2])
        for x in load(0):
            x.start()
        w_in.wait()
        for u in range(units):
            if u + 1 < units:
                for x in load(u + 1):
                    x.start()
            for x in load(u):
                x.wait()
            if u >= 2:
                put(u - 2).wait()
            sl = u % 2

            @pl.loop(0, 4)
            def _(n):
                cols = pl.ds(pl.multiple_of(n * eq, 128), eq)
                o_rows = jnp.concatenate([jnp.concatenate([o_v[sl, i, h % 2, h // 2] for h in range(8)], axis=1) for i in range(2)], axis=0)
                r = dot_nn(o_rows, wo_v[:, cols])
                y_v[sl, :, cols] = (x_v[sl, :, cols].astype(F32) + r).astype(BF16)
            put(u).start()
        for u in range(max(0, units - 2), units):
            put(u).wait()

    pl.run_scoped(attn_out, pltpu.VMEM((8 * d, e), BF16), pltpu.VMEM((2, 2, 2, 4, tok, d), BF16),
                  pltpu.VMEM((2, mc, e), BF16), pltpu.VMEM((2, mc, e), BF16))
    pass_on(0, 1)

    def hidden_grad(wq_v, wkv_v, dq_v, x_v, dy_v, dh, gx_v):
        w_in = pltpu.make_async_copy(wq_hbm, wq_v, b_sem.at[0])
        w_in.start()
        w2_in = pltpu.make_async_copy(wkv_hbm, wkv_v, b_sem.at[1])
        w2_in.start()

        def load(u):
            return (pltpu.make_async_copy(dq_hbm.at[pl.ds(2 * u, 2)], dq_v, ld_sem.at[0, 0]),
                    pltpu.make_async_copy(x_hbm.at[pl.ds(u * mc, mc)], x_v, ld_sem.at[0, 1]),
                    pltpu.make_async_copy(dy_hbm.at[pl.ds(u * mc, mc)], dy_v, ld_sem.at[1, 0]))

        def put(u):
            return pltpu.make_async_copy(gx_v, gx_hbm.at[pl.ds(u * mc, mc)], t_sem.at[0])
        gain = g_ref[...].astype(F32)
        gln_acc[...] = jnp.zeros_like(gln_acc)
        for x in load(0):
            x.start()
        w_in.wait()
        w2_in.wait()
        for u in range(units):
            for x in load(u):
                x.wait()

            @pl.loop(0, 4)
            def _(n):
                rows = pl.ds(pl.multiple_of(n * eq, 128), eq)
                t = None
                for h in range(8):
                    a = jnp.concatenate([dq_v[i, h % 2, h // 2] for i in range(2)], axis=0)
                    p = dot_nt(a, wq_v[h, rows, :])
                    t = p if t is None else t + p
                for j in range(2):
                    a = jnp.concatenate([kind[j, 2 * u + i] for i in range(2)], axis=0)
                    t = t + dot_nt(a, wkv_v[rows, j * d:(j + 1) * d])
                dh[:, rows] = t
            if u >= 1:
                put(u - 1).wait()

            @pl.loop(0, mc // 16)
            def _(r):
                rs = pl.ds(pl.multiple_of(r * 16, 16), 16)
                x = x_v[rs, :].astype(F32)
                cx = x - jnp.mean(x, axis=1, keepdims=True)
                inv = lax.rsqrt(jnp.mean(cx * cx, axis=1, keepdims=True) + LN_EPS)
                xh = cx * inv
                g = dh[rs, :]
                pr = g * xh
                gln_acc[...] += pr[:8] + pr[8:]
                gh = g * gain
                m1 = jnp.mean(gh, axis=1, keepdims=True)
                m2 = jnp.mean(gh * xh, axis=1, keepdims=True)
                gx_v[rs, :] = (inv * (gh - m1 - xh * m2) + dy_v[rs, :].astype(F32)).astype(BF16)
            put(u).start()
            if u + 1 < units:
                for x in load(u + 1):
                    x.start()
            if u == units // 2 - 1:
                pass_on(1, 2)
                finish_kv()
        put(units - 1).wait()

    pl.run_scoped(hidden_grad, pltpu.VMEM((8, e, d), BF16), pltpu.VMEM((e, 2 * d), BF16), pltpu.VMEM((2, 2, 4, tok, d), BF16),
                  pltpu.VMEM((mc, e), BF16), pltpu.VMEM((mc, e), BF16), pltpu.VMEM((mc, e), F32), pltpu.VMEM((mc, e), BF16))
    gl_recv[me] = jnp.sum(gln_acc[...], axis=0, keepdims=True)
    pass_on(0, 2)
    gl = [rdma(gl_recv.at[me], gl_recv.at[me], gl_send.at[o - 1], gl_rsem.at[o - 1], lax.rem(me + o, 8)) for o in range(1, 8)]
    for x in gl:
        x.start()
    finish(1, gwq_ref)
    ag_forward()
    for o in range(1, 8):
        src = lax.rem(me + 8 - o, 8)
        rdma(gl_recv.at[src], gl_recv.at[src], gl_send.at[o - 1], gl_rsem.at[o - 1], mate).wait_recv()
    total = gl_recv[0]
    for i in range(1, 8):
        total = total + gl_recv[i]
    gln_ref[...] = total
    finish(0, gwo_ref)
    ag_last()
    for x in gl:
        x.wait_send()
    kp_copy.wait_send()
    for dr in range(2):
        for j in range(3):
            hop_kv(dr, j).wait_send()
            for s in range(2):
                hop(s, dr, j).wait_send()


def gradients(o, o_p, dq, dq_p, hn, hn_p, dy, dy_p, dkv, wqf, wof, w_kv, x, gain, cos_t, sin_t):
    nb, tok, e = x.shape
    n_tok = nb * tok
    d = dq.shape[-1]
    any_spec = pl.BlockSpec(memory_space=pl.ANY)
    vmem = pl.BlockSpec(memory_space=pltpu.VMEM)
    dma = pltpu.SemaphoreType.DMA
    tokens = jax.ShapeDtypeStruct((n_tok, e), BF16)
    y, gx, gln, gwo, gwq_t, gkv_t = pl.pallas_call(
        functools.partial(grads_body, nb, tok),
        in_specs=[any_spec] * 13 + [vmem, vmem, vmem],
        out_specs=[any_spec, any_spec, vmem, vmem, vmem, any_spec],
        out_shape=[tokens, tokens, jax.ShapeDtypeStruct((1, e), F32), jax.ShapeDtypeStruct((d, e), BF16),
                   jax.ShapeDtypeStruct((d, e), BF16), jax.ShapeDtypeStruct((2, d, e), F32)],
        scratch_shapes=[pltpu.VMEM((2, 4, 2, d, e // 2), F32), pltpu.VMEM((4, 2, d, e // 8), F32),
                        pltpu.VMEM((2, 2, 3, d, e // 2), F32), pltpu.VMEM((2, 3, d, e // 8), F32),
                        pltpu.VMEM((2, nb, tok, d), BF16), pltpu.VMEM((nb, tok, d), BF16), pltpu.VMEM((nb, tok, 2 * d), BF16),
                        pltpu.VMEM((d, e // 4), F32), pltpu.VMEM((8, e), F32), pltpu.VMEM((8, 1, e), F32),
                        dma((2, 2, 3)), dma((2, 2, 3)), dma((2, 3)), dma((2, 3)), dma((9,)), dma((9,)), dma((7,)), dma((7,)),
                        dma((2,)), dma((2, 2)), dma((2,)), dma((6,))],
        compiler_params=pltpu.CompilerParams(collective_id=2, has_side_effects=True, vmem_limit_bytes=63 * 2**20),
        cost_estimate=pl.CostEstimate(flops=10 * n_tok * e * e, bytes_accessed=120 * 2**20, transcendentals=0),
        name="gradients",
    )(o, o_p, dq, dq_p, hn, hn_p, dy.reshape(n_tok, e), dy_p, dkv, wqf, wof.reshape(8 * d, e), w_kv, x.reshape(n_tok, e),
      gain.reshape(1, e), cos_t, sin_t)
    return y.reshape(nb, tok, e), gx.reshape(nb, tok, e), gln.reshape(e), gwq_t.T, gkv_t[0].T, gkv_t[1].T, gwo


def solution(mesh):
    act_spec = P('dp', 'tp', None)

    def device_step(x_loc, ln_scale, wq_loc, w_k, w_v, wo_loc, dy_loc):
        n_batch, tok, model_dim = x_loc.shape
        d = w_k.shape[1]
        t0 = lax.axis_index('tp') * tok
        cos_t, sin_t = rope_tables(t0 + jnp.arange(tok), d)

        w_kv = jnp.concatenate([w_k, w_v], axis=1)
        hn, q, do, kv_loc, wq_h, wo_h, hn_p, dy_p = project(x_loc, ln_scale, wq_loc, w_kv, wo_loc, dy_loc, cos_t, sin_t)
        o, dq, dkv_loc, o_p, dq_p = attention(q, do, kv_loc, cos_t, sin_t)
        return gradients(o, o_p, dq, dq_p, hn, hn_p, dy_loc, dy_p, dkv_loc, wq_h, wo_h, w_kv, x_loc, ln_scale, cos_t, sin_t)

    return jax.shard_map(device_step, mesh=mesh, in_specs=(act_spec, P(None), P(None, 'tp'), P(None, None), P(None, None), P('tp', None), act_spec), out_specs=(act_spec, act_spec, P('dp'), P('dp', 'tp'), P('dp', None), P('dp', None), P(('dp', 'tp'), None)), check_vma=False)
```

```python
import functools
import jax
import jax.numpy as jnp
from jax import lax
from jax.experimental import pallas as pl
from jax.experimental.pallas import tpu as pltpu
from jax.sharding import PartitionSpec as P

LN_EPS = 1e-6
ROPE_BASE = 10000.0
LOG2E = 1.4426950408889634
F32 = jnp.float32
BF16 = jnp.bfloat16


def rope_tables(positions, head_dim):
    half_dim = head_dim // 2
    inv_freq = ROPE_BASE ** (-2.0 * jnp.arange(half_dim, dtype=F32) / head_dim)
    angles = positions.astype(F32)[:, None] * inv_freq[None, :]
    return jnp.cos(angles), jnp.sin(angles)


def rotate(vectors, cos_t, sin_t):
    half_dim = vectors.shape[-1] // 2
    lo_half = vectors[..., :half_dim]
    hi_half = vectors[..., half_dim:]
    return jnp.concatenate([lo_half * cos_t - hi_half * sin_t, hi_half * cos_t + lo_half * sin_t], axis=-1)


def dot_nn(a, b):
    return lax.dot_general(a, b, (((1,), (0,)), ((), ())), preferred_element_type=F32)


def dot_nt(a, b):
    return lax.dot_general(a, b, (((1,), (1,)), ((), ())), preferred_element_type=F32)


def rdma(src, dst, send, recv, to):
    return pltpu.make_async_remote_copy(src_ref=src, dst_ref=dst, send_sem=send, recv_sem=recv,
                                        device_id={'tp': to}, device_id_type=pl.DeviceIdType.MESH)


def ring_ids():
    me = lax.axis_index('tp')
    k = lax.rem(me, 2)
    return me, k, me + 1 - 2 * k, lax.rem(me + 2, 8), lax.rem(me + 6, 8)


def enter(peers):
    barrier = pltpu.get_barrier_semaphore()
    for p in peers:
        pl.semaphore_signal(barrier, inc=1, device_id={'tp': p}, device_id_type=pl.DeviceIdType.MESH)
    pl.semaphore_wait(barrier, len(peers))


def attn_body(nb, tok, seq, d, q_hbm, do_hbm, kvl_hbm, cos_ref, sin_ref,
              o_hbm, dq_hbm, dkv_hbm, op_hbm, dqp_hbm,
              kv_all, q_v, do_v, o_v, dq_v, s_buf, m_buf, l_buf, p_buf, ds_buf, q_t, do_t, dk_t, dv_t, d_buf, cos4, sin4, mrecv, rrecv,
              kv_send, kv_recv, m_send, m_recv, r_send, r_recv, own_sem, in_sem, out_sem, fin_sem, p_send, p_recv):
    scale = d ** -0.5
    rows = s_buf.shape[1]
    n_blk = seq // 256
    rb = 2 * rows // n_blk
    n_rb = rows // rb
    half = d // 2
    me, k, mate, cw, ccw = ring_ids()
    c = me // 2

    def blk(j):
        return pl.ds(pl.multiple_of(j * tok, 16), tok)

    def kvb(b, j):
        return kv_all.at[b, blk(j)]

    def kv_copy(b, j, tag, to, src=None):
        return rdma(kvb(b, j) if src is None else src, kvb(b, j), kv_send.at[b, tag], kv_recv.at[b, tag], to)

    def own(b):
        @pl.when(c <= 2)
        def _():
            kv_copy(b, me, 0, cw, kvl_hbm.at[b]).start()

        @pl.when(c == 0)
        def _():
            kv_copy(b, me, 2, ccw, kvl_hbm.at[b]).start()
        kv_copy(b, me, 3, mate, kvl_hbm.at[b]).start()

    def service_a(b):
        @pl.when(c >= 1)
        def _():
            kv_copy(b, me - 2, 0, cw).wait_recv()

            @pl.when(c <= 2)
            def _():
                kv_copy(b, me - 2, 1, cw).start()
            kv_copy(b, me - 2, 4, mate).start()

        @pl.when(c == 3)
        def _():
            kv_copy(b, me - 6, 2, ccw).wait_recv()
            kv_copy(b, me - 6, 6, mate).start()

    def service_b(b):
        @pl.when(c >= 2)
        def _():
            kv_copy(b, me - 4, 1, cw).wait_recv()
            kv_copy(b, me - 4, 5, mate).start()

    def own_copy(b):
        return pltpu.make_async_copy(kvl_hbm.at[b], kvb(b, me), own_sem.at[b])

    def ready(b):
        own_copy(b).wait()
        kv_copy(b, mate, 3, mate).wait_recv()
        for n, tag in ((1, 4), (2, 5), (3, 6)):
            @pl.when(c >= n)
            def _():
                kv_copy(b, mate - 2 * n, tag, mate).wait_recv()

    def drain_kv(b):
        for cond, tag in ((c <= 2, 0), ((c >= 1) & (c <= 2), 1), (c == 0, 2), (c >= 0, 3), (c >= 1, 4), (c >= 2, 5), (c == 3, 6)):
            @pl.when(cond)
            def _():
                kv_copy(b, me, tag, mate).wait_send()

    def m_copy(b, n):
        return rdma(kvb(b, 2 * n + 1 - k), mrecv.at[b, n], m_send.at[b, n], m_recv.at[b, n], mate)

    def r_copy(b, n, slot, to):
        return rdma(kvb(b, 2 * n + k), rrecv.at[b, slot], r_send.at[b, slot], r_recv.at[b, slot], to)

    def add_into(b, n, other):
        v = kv_all[b, blk(2 * n + k), :].astype(F32) + other[...].astype(F32)
        kv_all[b, blk(2 * n + k), :] = v.astype(BF16)

    def fin_copy(b):
        return pltpu.make_async_copy(kvb(b, me), dkv_hbm.at[b], fin_sem.at[b])

    def to_mate(b):
        for n in range(4):
            @pl.when(c >= n)
            def _():
                m_copy(b, n).start()

    def stage1(b):
        for n in range(4):
            @pl.when(c >= n)
            def _():
                m_copy(b, n).wait()
                add_into(b, n, mrecv.at[b, n])

        @pl.when(c == 3)
        def _():
            r_copy(b, 1, 2, ccw).start()
            r_copy(b, 2, 1, ccw).start()
            r_copy(b, 0, 0, cw).start()
            fin_copy(b).start()

        @pl.when(c == 2)
        def _():
            r_copy(b, 0, 1, ccw).start()

    def stage2(b):
        @pl.when(c == 2)
        def _():
            r_copy(b, 1, 2, ccw).wait_recv()
            add_into(b, 1, rrecv.at[b, 2])
            r_copy(b, 1, 2, ccw).start()
            r_copy(b, 2, 1, ccw).wait_recv()
            add_into(b, 2, rrecv.at[b, 1])
            fin_copy(b).start()

        @pl.when(c == 1)
        def _():
            r_copy(b, 0, 1, ccw).wait_recv()
            add_into(b, 0, rrecv.at[b, 1])
            r_copy(b, 0, 1, ccw).start()

    def stage3(b):
        @pl.when(c == 0)
        def _():
            r_copy(b, 0, 0, cw).wait_recv()
            add_into(b, 0, rrecv.at[b, 0])
            r_copy(b, 0, 1, ccw).wait_recv()
            add_into(b, 0, rrecv.at[b, 1])
            fin_copy(b).start()

        @pl.when(c == 1)
        def _():
            r_copy(b, 1, 2, ccw).wait_recv()
            add_into(b, 1, rrecv.at[b, 2])
            fin_copy(b).start()

    def load(b, slot):
        return (pltpu.make_async_copy(q_hbm.at[b], q_v.at[slot], in_sem.at[0, slot]),
                pltpu.make_async_copy(do_hbm.at[b], do_v.at[slot], in_sem.at[1, slot]))

    def handed(dst, src, n, b, slot):
        return rdma(src.at[slot, 1 - k], dst.at[b], p_send.at[n, b], p_recv.at[n, b], mate)

    def store_o(b, slot):
        return (pltpu.make_async_copy(o_v.at[slot], o_hbm.at[b], out_sem.at[0, slot]), handed(op_hbm, o_v, 0, b, slot))

    def store_dq(b, slot):
        return (pltpu.make_async_copy(dq_v.at[slot], dq_hbm.at[b], out_sem.at[1, slot]), handed(dqp_hbm, dq_v, 1, b, slot))

    def stored(x):
        x[0].wait()
        x[1].wait_send()

    def scores(b, g, slot, i):
        cols = slice(i * 256, (i + 1) * 256)
        s = dot_nt(q_v[slot, g].reshape(rows, d), kv_all[b, cols, :d])
        col = lax.broadcasted_iota(jnp.int32, (tok, 256), 1) + i * 256
        row = lax.broadcasted_iota(jnp.int32, (tok, 256), 0) + me * tok
        s = jnp.concatenate([jnp.where(col <= row, s[j * tok:(j + 1) * tok], -1e30) for j in range(rows // tok)], axis=0)
        s_buf[g, :, cols] = s
        m = jnp.maximum(s[:, :128], s[:, 128:])
        m_buf[...] = m if i == 0 else jnp.maximum(m_buf[...], m)

    def softmax(g, i):
        n = rows // n_blk
        for r in range(i * n, (i + 1) * n, 16):
            rs = slice(r, r + 16)
            m = jnp.max(m_buf[rs, :], axis=1, keepdims=True) * (scale * LOG2E)
            l = None
            for j in range(0, seq, 128):
                e = jnp.exp2(s_buf[g, rs, j:j + 128] * (scale * LOG2E) - m)
                s_buf[g, rs, j:j + 128] = e
                l = e if l is None else l + e
            l_buf[g, rs, :] = jnp.broadcast_to(1.0 / jnp.sum(l, axis=1, keepdims=True), (16, 128))

    def turn(g, slot, i):
        rs = slice(i * rb, (i + 1) * rb)
        q_t[g, :, rs] = q_v[slot, g].reshape(rows, d)[rs].T
        do_t[g, :, rs] = do_v[slot, g].reshape(rows, d)[rs].T

    def out_rows(b, g, slot, i):
        rs = slice(i * rb, (i + 1) * rb)
        p = (s_buf[g, rs, :] * jnp.concatenate([l_buf[g, rs, :]] * (seq // 128), axis=1)).astype(BF16)
        p_buf[rs, :] = p
        o = dot_nn(p, kv_all[b, :, d:])
        dvec = jnp.sum(o * do_v[slot, g].reshape(rows, d)[rs].astype(F32), axis=1, keepdims=True)
        d_buf[rs, :] = jnp.broadcast_to(dvec, (rb, 128))
        put_rows(o_v, slot, g, i, o.astype(BF16))

    def put_rows(ref, slot, g, i, v):
        r = i * rb
        while r < (i + 1) * rb:
            n = min((i + 1) * rb - r, tok - r % tok)
            ref[slot, g, r // tok, r % tok:r % tok + n, :] = v[r - i * rb:r - i * rb + n]
            r += n

    def dq_rows(b, g, slot, i):
        rs = slice(i * rb, (i + 1) * rb)
        dq = dot_nn(ds_buf[rs, :], kv_all[b, :, :d]) * scale
        lo, hi = dq[:, :half], dq[:, half:]
        cs, sn = cos4[rs, :], sin4[rs, :]
        put_rows(dq_v, slot, g, i, jnp.concatenate([(lo * cs + hi * sn).astype(BF16), (hi * cs - lo * sn).astype(BF16)], axis=1))

    def grads(b, g, slot, i):
        cols = slice(i * 256, (i + 1) * 256)
        do = do_v[slot, g].reshape(rows, d)
        p = p_buf[:, cols]
        dp = dot_nt(do, kv_all[b, cols, d:])
        dvec = d_buf[...]
        if i > 0:
            n = rows // n_blk
            z = l_buf[1 - g, (i - 1) * n:(i - 1) * n + 8, :]
            for r in range(8, n, 8):
                z = jnp.minimum(z, l_buf[1 - g, (i - 1) * n + r:(i - 1) * n + r + 8, :])
            dvec = dvec + jnp.concatenate([jnp.minimum(z, 0.0)] * (rows // 8), axis=0)
        dd = jnp.concatenate([dvec, dvec], axis=1)
        ds = (p.astype(F32) * (dp - dd)).astype(BF16)
        ds_buf[:, cols] = ds
        dk = dot_nn(q_t[g], ds)
        dv = dot_nn(do_t[g], p)
        if g == 0:
            dk_t[:, cols] = dk
            dv_t[:, cols] = dv
        else:
            dk_t[:, cols] += dk
            dv_t[:, cols] += dv

    def close_kv(b, i):
        cols = slice(i * 256, (i + 1) * 256)
        kv_all[b, cols, :d] = (dk_t[:, cols] * scale).T.astype(BF16)
        kv_all[b, cols, d:] = dv_t[:, cols].T.astype(BF16)

    enter((mate, cw, ccw))
    for b in range(nb):
        own_copy(b).start()
    for x in load(0, 0):
        x.start()
    for b in range(min(3, nb)):
        own(b)

    @pl.loop(2 * c + 2, 8)
    def _(j):
        for b in range(nb):
            kv_all[b, blk(j), :] = jnp.zeros((tok, 2 * d), BF16)
    for j in range(rows // tok):
        cos4[j * tok:(j + 1) * tok, :] = cos_ref[...]
        sin4[j * tok:(j + 1) * tok, :] = sin_ref[...]
    ds_buf[...] = jnp.zeros_like(ds_buf)
    for b in range(min(2, nb)):
        service_a(b)
    service_b(0)
    for x in load(0, 0):
        x.wait()
    for i in range(n_rb):
        turn(0, 0, i)
    ready(0)
    for i in range(n_blk):
        scores(0, 0, 0, i)
    for i in range(n_blk):
        softmax(0, i)

    def comm_steps(b):
        for lag, stage in ((2, stage1), (3, stage2), (4, stage3)):
            @pl.when((b >= lag) & (b - lag < nb))
            def _():
                stage(b - lag)

    @pl.loop(0, nb)
    def _(b):
        slot = lax.rem(b, 2)
        nxt = jnp.minimum(b + 1, nb - 1)
        prev = jnp.maximum(b - 1, 0)

        @pl.when(b + 1 < nb)
        def _():
            for x in load(b + 1, 1 - slot):
                x.start()

        @pl.when(b + 3 < nb)
        def _():
            own(b + 3)

        @pl.when(b + 2 < nb)
        def _():
            service_a(b + 2)

        @pl.when(b + 1 < nb)
        def _():
            service_b(b + 1)
        comm_steps(b)

        @pl.when(b >= 1)
        def _():
            drain_kv(b - 1)

        @pl.when(b >= 2)
        def _():
            stored(store_o(b - 2, slot))
        spare = jnp.where(b >= 1, b - 1, nb)
        for i in range(n_blk):
            scores(b, 1, slot, i)
            if i % 2 == 1:
                out_rows(b, 0, slot, i // 2)
                dq_rows(prev, 1, 1 - slot, i // 2)
                turn(1, slot, i // 2)
        for i in range(n_blk):
            close_kv(spare, i)

        @pl.when(b >= 1)
        def _():
            for x in store_dq(b - 1, 1 - slot):
                x.start()
            to_mate(b - 1)
        for i in range(n_blk):
            grads(b, 0, slot, i)
            softmax(1, i)

        @pl.when(b + 1 < nb)
        def _():
            for x in load(b + 1, 1 - slot):
                x.wait()
            ready(b + 1)

        @pl.when(b >= 2)
        def _():
            stored(store_dq(b - 2, slot))
        nslot = lax.rem(nxt, 2)
        for i in range(n_blk):
            scores(nxt, 0, nslot, i)
            if i % 2 == 1:
                out_rows(b, 1, slot, i // 2)
                dq_rows(b, 0, slot, i // 2)
                turn(0, nslot, i // 2)
        for x in store_o(b, slot):
            x.start()
        for i in range(n_blk):
            grads(b, 1, slot, i)
            softmax(0, i)

    n = nb
    drain_kv(n - 1)
    for i in range(n_rb):
        dq_rows(n - 1, 1, (n - 1) % 2, i)
    for i in range(n_blk):
        close_kv(n - 1, i)
    for x in store_dq(n - 1, (n - 1) % 2):
        x.start()
    to_mate(n - 1)
    for b in range(n, n + 4):
        for lag, stage in ((2, stage1), (3, stage2), (4, stage3)):
            if 0 <= b - lag < n:
                stage(b - lag)
    for b in (n - 2, n - 1):
        stored(store_o(b, b % 2))
        stored(store_dq(b, b % 2))
    for b in range(n):
        handed(op_hbm, o_v, 0, b, b % 2).wait_recv()
        handed(dqp_hbm, dq_v, 1, b, b % 2).wait_recv()
        fin_copy(b).wait()
        for cond, slot in ((c == 3, 0), (c >= 1, 1), (c >= 2, 2)):
            @pl.when(cond)
            def _():
                r_copy(b, 0, slot, cw).wait_send()


def attention(q, do, kv, cos_t, sin_t):
    nb, _, hp, tok, d = q.shape
    seq = tok * 8
    rows = hp * tok
    any_spec = pl.BlockSpec(memory_space=pl.ANY)
    vmem = pl.BlockSpec(memory_space=pltpu.VMEM)
    dma = pltpu.SemaphoreType.DMA
    slab = pltpu.VMEM((2, 2, hp, tok, d), BF16)
    out = jax.ShapeDtypeStruct(q.shape, BF16)
    outp = jax.ShapeDtypeStruct((nb, hp, tok, d), BF16)
    return pl.pallas_call(
        functools.partial(attn_body, nb, tok, seq, d),
        in_specs=[any_spec, any_spec, any_spec, vmem, vmem],
        out_specs=[any_spec] * 5,
        out_shape=[out, out, jax.ShapeDtypeStruct(kv.shape, BF16), outp, outp],
        scratch_shapes=[pltpu.VMEM((nb + 1, seq, 2 * d), BF16), slab, slab, slab, slab,
                        pltpu.VMEM((2, rows, seq), F32), pltpu.VMEM((rows, 128), F32),
                        pltpu.VMEM((2, rows, 128), F32), pltpu.VMEM((rows, seq), BF16), pltpu.VMEM((rows, seq), BF16),
                        pltpu.VMEM((2, d, rows), BF16), pltpu.VMEM((2, d, rows), BF16),
                        pltpu.VMEM((d, seq), F32), pltpu.VMEM((d, seq), F32), pltpu.VMEM((rows, 128), F32),
                        pltpu.VMEM((rows, d // 2), F32), pltpu.VMEM((rows, d // 2), F32),
                        pltpu.VMEM((nb, 4, tok, 2 * d), BF16), pltpu.VMEM((nb, 3, tok, 2 * d), BF16),
                        dma((nb, 7)), dma((nb, 7)), dma((nb, 4)), dma((nb, 4)), dma((nb, 3)), dma((nb, 3)),
                        dma((nb,)), dma((2, 2)), dma((2, 2)), dma((nb,)), dma((2, nb)), dma((2, nb))],
        compiler_params=pltpu.CompilerParams(collective_id=1, has_side_effects=True, vmem_limit_bytes=63 * 2**20),
        cost_estimate=pl.CostEstimate(flops=24 * nb * rows * seq * d, bytes_accessed=40 * 2**20,
                                      transcendentals=2 * nb * rows * seq),
        name="attention",
    )(q, do, kv, cos_t, sin_t)


def proj_body(nb, tok, x_hbm, g_ref, wq_hbm, wkv_ref, wo_hbm, dy_hbm, cos_ref, sin_ref,
              hn_hbm, q_hbm, do_hbm, kv_hbm, wqf_hbm, wof_hbm, hnp_hbm, dyp_hbm,
              x_v, hn_v, dy_v, wq_v, wo_v, kv_v, out_v,
              send, recv, x_sem, dy_sem, own_sem, out_sem, misc_sem, w_sem, p_send, p_recv):
    n_tok, e = x_hbm.shape
    d = kv_v.shape[1] // 2
    half = d // 2
    mc = 2 * tok
    me, k, mate, cw, ccw = ring_ids()
    base = 2 * (me // 2)

    def head(off, par):
        return lax.rem(base + 2 * off + 8, 8) + par
    enter((mate, cw, ccw))

    fulls = (wq_v, wo_v)
    locs = (wq_hbm, wo_hbm)

    def half_of(w, ref, j):
        n = ref.shape[0] // 2
        return ref.at[pl.ds(j * n, n)]

    sends = []

    def send_full(w, h, j, to, own=False):
        src = locs[w] if own else fulls[w].at[h]
        c = rdma(src, fulls[w].at[h], send.at[w, j], recv.at[w, j], to)
        c.start()
        sends.append(c)

    def send_half(w, h, part, j, to):
        c = rdma(half_of(w, fulls[w].at[h], part), half_of(w, fulls[w].at[h], part), send.at[w, j], recv.at[w, j], to)
        c.start()
        sends.append(c)

    def wait_full(w, h, j):
        rdma(fulls[w].at[h], fulls[w].at[h], send.at[w, j], recv.at[w, j], mate).wait_recv()

    def wait_half(w, h, part, j):
        ref = half_of(w, fulls[w].at[h], part)
        rdma(ref, ref, send.at[w, j], recv.at[w, j], mate).wait_recv()

    for w in range(2):
        send_full(w, me, 0, cw, True)
        send_full(w, me, 1, ccw, True)
        send_full(w, me, 4, mate, True)
    own = [pltpu.make_async_copy(locs[w], fulls[w].at[me], own_sem.at[w]) for w in range(2)]
    xs = [pltpu.make_async_copy(x_hbm.at[pl.ds(b * tok, tok)], x_v.at[pl.ds(b * tok, tok)], x_sem.at[b]) for b in range(nb)]
    for c in xs:
        c.start()
    for c in own:
        c.start()
    dyc = pltpu.make_async_copy(dy_hbm, dy_v, dy_sem)
    dyc.start()

    gain = g_ref[...].astype(F32)
    for b in range(nb):
        xs[b].wait()

        @pl.loop(0, tok // 16, unroll=2)
        def _(r):
            rs = pl.ds(pl.multiple_of(b * tok + r * 16, 16), 16)
            x = x_v[rs, :].astype(F32)
            c = x - jnp.mean(x, axis=1, keepdims=True)
            inv = lax.rsqrt(jnp.mean(c * c, axis=1, keepdims=True) + LN_EPS)
            hn_v[rs, :] = (c * inv * gain).astype(BF16)
    hn_out = pltpu.make_async_copy(hn_v, hn_hbm, misc_sem.at[0])
    hn_out.start()
    to_mate = [rdma(hn_v, hnp_hbm, p_send.at[0], p_recv.at[0], mate), rdma(dy_hbm, dyp_hbm, p_send.at[1], p_recv.at[1], mate)]
    for c in to_mate:
        c.start()

    def rope_rows(raw):
        lo, hi = raw[:, :half], raw[:, half:d]
        cs, sn = cos_ref[...], sin_ref[...]
        return lo * cs - hi * sn, hi * cs + lo * sn

    @pl.loop(0, n_tok // mc)
    def _(i):
        rs = pl.ds(pl.multiple_of(i * mc, mc), mc)
        raw = dot_nn(hn_v[rs, :], wkv_ref[...])
        lo, hi = rope_rows(raw)
        kv_v[rs, :half] = lo.astype(BF16)
        kv_v[rs, half:d] = hi.astype(BF16)
        kv_v[rs, d:] = raw[:, d:].astype(BF16)
    kv_out = pltpu.make_async_copy(kv_v, kv_hbm, misc_sem.at[1])
    kv_out.start()

    outs = []
    saves = []

    def save(w, h):
        c = pltpu.make_async_copy(fulls[w].at[h], (wqf_hbm, wof_hbm)[w].at[h], w_sem.at[len(saves)])
        c.start()
        saves.append(c)

    def project(w, h):
        slot = len(outs) % 4
        if len(outs) >= 4:
            outs[-4].wait()

        @pl.loop(0, n_tok // mc)
        def _(i):
            rs = pl.ds(pl.multiple_of(i * mc, mc), mc)
            if w == 0:
                lo, hi = rope_rows(dot_nn(hn_v[rs, :], wq_v[h]))
                o0 = lo.reshape(2, tok, half).astype(BF16)
                o1 = hi.reshape(2, tok, half).astype(BF16)
                out_v[slot, pl.ds(2 * i, 2), :, :half] = o0
                out_v[slot, pl.ds(2 * i, 2), :, half:] = o1
            else:
                out_v[slot, pl.ds(2 * i, 2)] = dot_nt(dy_v[rs, :], wo_v[h]).reshape(2, tok, d).astype(BF16)
        c = pltpu.make_async_copy(out_v.at[slot], (q_hbm, do_hbm)[w].at[:, lax.rem(h, 2), h // 2], out_sem.at[slot])
        c.start()
        outs.append(c)
        save(w, h)

    other = 1 - k
    for w in range(2):
        own[w].wait()
        if w == 1:
            dyc.wait()
        project(w, me)
        wait_full(w, mate, 4)
        project(w, mate)
    for w in range(2):
        wait_full(w, head(-1, k), 0)
        send_half(w, head(-1, k), 0, 2, cw)
        wait_full(w, head(1, k), 1)
        send_half(w, head(1, k), 1, 3, ccw)
        send_full(w, head(-1, k), 5, mate)
        send_full(w, head(1, k), 6, mate)
        project(w, head(-1, k))
        project(w, head(1, k))
        wait_full(w, head(-1, other), 5)
        project(w, head(-1, other))
        wait_full(w, head(1, other), 6)
        project(w, head(1, other))
    for w in range(2):
        wait_half(w, head(2, k), 0, 2)
        send_half(w, head(2, k), 0, 7, mate)
        wait_half(w, head(2, k), 1, 3)
        send_half(w, head(2, k), 1, 8, mate)
        project(w, head(2, k))
        wait_half(w, head(2, other), 0, 7)
        wait_half(w, head(2, other), 1, 8)
        project(w, head(2, other))
    for c in outs[-4:] + saves + [hn_out, kv_out]:
        c.wait()
    for c in sends:
        c.wait_send()
    for c in to_mate:
        c.wait()


def project(x, gain, wq, w_kv, wo, dy, cos_t, sin_t):
    nb, tok, e = x.shape
    d = wq.shape[1]
    n_heads = 8
    n_tok = nb * tok
    any_spec = pl.BlockSpec(memory_space=pl.ANY)
    vmem = pl.BlockSpec(memory_space=pltpu.VMEM)
    act = jax.ShapeDtypeStruct((nb, 2, n_heads // 2, tok, d), BF16)
    dma = pltpu.SemaphoreType.DMA
    flops = 2 * n_tok * e * (2 * n_heads + 2) * d
    cos2, sin2 = jnp.tile(cos_t, (2, 1)), jnp.tile(sin_t, (2, 1))
    hn, q, do, kv, wqf, wof, hn_p, dy_p = pl.pallas_call(
        functools.partial(proj_body, nb, tok),
        in_specs=[any_spec, vmem, any_spec, vmem, any_spec, any_spec, vmem, vmem],
        out_specs=[any_spec] * 8,
        out_shape=[jax.ShapeDtypeStruct((n_tok, e), BF16), act, act, jax.ShapeDtypeStruct((n_tok, 2 * d), BF16),
                   jax.ShapeDtypeStruct((n_heads, e, d), BF16), jax.ShapeDtypeStruct((n_heads, d, e), BF16),
                   jax.ShapeDtypeStruct((n_tok, e), BF16), jax.ShapeDtypeStruct((n_tok, e), BF16)],
        scratch_shapes=[pltpu.VMEM((n_tok, e), BF16), pltpu.VMEM((n_tok, e), BF16), pltpu.VMEM((n_tok, e), BF16),
                        pltpu.VMEM((n_heads, e, d), BF16), pltpu.VMEM((n_heads, d, e), BF16),
                        pltpu.VMEM((n_tok, 2 * d), BF16), pltpu.VMEM((4, nb, tok, d), BF16),
                        dma((2, 9)), dma((2, 9)), dma((nb,)), dma(()), dma((2,)), dma((4,)), dma((2,)), dma((16,)), dma((2,)), dma((2,))],
        compiler_params=pltpu.CompilerParams(collective_id=0, has_side_effects=True, vmem_limit_bytes=60 * 2**20),
        cost_estimate=pl.CostEstimate(flops=flops, bytes_accessed=60 * 2**20, transcendentals=0),
        name="project",
    )(x.reshape(n_tok, e), gain.reshape(1, e), wq, w_kv, wo, dy.reshape(n_tok, e), cos2, sin2)
    return hn, q, do, kv.reshape(nb, tok, 2 * d), wqf, wof, hn_p, dy_p


def grads_body(nb, tok, o_hbm, op_hbm, dq_hbm, dqp_hbm, hn_hbm, hnp_hbm, dy_hbm, dyp_hbm, dkv_hbm,
               wq_hbm, wo_hbm, wkv_hbm, x_hbm, g_ref, cos_ref, sin_ref,
               y_hbm, gx_hbm, gln_ref, gwo_ref, gwq_ref, gkv_hbm,
               acc, acc_kv, rbuf, rbuf_kv, kind, kp, dkv_v, fin_kv, gln_acc, gl_recv,
               rs_send, rs_recv, kv_send, kv_recv, ag_send, ag_recv, gl_send, gl_rsem, kp_sem, ld_sem, b_sem, t_sem):
    n_tok, e = x_hbm.shape
    d = wkv_hbm.shape[1] // 2
    half = d // 2
    eh, eq = e // 2, e // 4
    me, k, mate, cw, ccw = ring_ids()
    c = me // 2
    rel = [lax.rem(c + o, 4) for o in (3, 1, 2, 0)]
    enter([lax.rem(me + o, 8) for o in range(1, 8)])

    order = ((2, 1), (2, 0))

    def hop(s, dr, j):
        src = acc.at[s, dr, dr] if j == 0 else rbuf.at[s, dr, j - 1]
        return rdma(src, rbuf.at[s, dr, j], rs_send.at[s, dr, j], rs_recv.at[s, dr, j], (cw, ccw)[dr])

    def hop_kv(dr, j):
        src = acc_kv.at[dr, dr] if j == 0 else rbuf_kv.at[dr, j - 1]
        return rdma(src, rbuf_kv.at[dr, j], kv_send.at[dr, j], kv_recv.at[dr, j], (cw, ccw)[dr])

    def add(dst, term):
        @pl.loop(0, dst.shape[0] // 32)
        def _(i):
            rs = pl.ds(pl.multiple_of(i * 32, 32), 32)
            dst[rs, :] = dst[rs, :] + term[rs, :]

    def pass_on(s, j):
        for dr in range(2):
            hop(s, dr, j - 1).wait_recv()
            add(rbuf.at[s, dr, j - 1], acc.at[s, order[dr][j - 1], dr])
            hop(s, dr, j).start()

    def pass_on_kv(j):
        for dr in range(2):
            hop_kv(dr, j - 1).wait_recv()
            add(rbuf_kv.at[dr, j - 1], acc_kv.at[order[dr][j - 1], dr])
            hop_kv(dr, j).start()

    def finish(s, out):
        for dr in range(2):
            hop(s, dr, 2).wait_recv()

            @pl.loop(0, d // 32)
            def _(i):
                rs = pl.ds(pl.multiple_of(i * 32, 32), 32)
                out[rs, dr * eh:(dr + 1) * eh] = (rbuf[s, dr, 2, rs, :] + acc[s, 3, dr, rs, :]).astype(BF16)

    def piece(kk, j, lo=0, n=None):
        return gkv_hbm.at[kk, pl.ds(lo, d if n is None else n), pl.ds(pl.multiple_of(j * eq, 128), eq)]

    def ag(tag, ref, to, src=None):
        return rdma(ref if src is None else src, ref, ag_send.at[tag], ag_recv.at[tag], to)

    def ag_far(tag, to):
        return ag(tag, piece(k, rel[(0, 1)[tag - 3]], (tag - 3) * half, half), to)

    own_piece = pltpu.make_async_copy(fin_kv, piece(k, c), t_sem.at[5])

    def finish_kv():
        for dr in range(2):
            hop_kv(dr, 2).wait_recv()
            fin_kv[:, dr * (eq // 2):(dr + 1) * (eq // 2)] = rbuf_kv[dr, 2] + acc_kv[3, dr]
        ag(0, piece(k, c), cw, fin_kv).start()
        ag(1, piece(k, c), ccw, fin_kv).start()
        ag(2, piece(k, c), mate, fin_kv).start()
        own_piece.start()

    def ag_forward():
        ag(0, piece(k, rel[0]), cw).wait_recv()
        ag_far(3, cw).start()
        ag(1, piece(k, rel[1]), cw).wait_recv()
        ag_far(4, ccw).start()
        ag(5, piece(k, rel[0]), mate).start()
        ag(6, piece(k, rel[1]), mate).start()

    def ag_last():
        far = [piece(k, rel[2], i * half, half) for i in range(2)]
        for i in range(2):
            ag(3 + i, far[i], cw).wait_recv()
            ag(7 + i, far[i], mate).start()
        ag(2, piece(1 - k, c), mate).wait_recv()
        ag(5, piece(1 - k, rel[0]), mate).wait_recv()
        ag(6, piece(1 - k, rel[1]), mate).wait_recv()
        for i in range(2):
            ag(7 + i, piece(1 - k, rel[2], i * half, half), mate).wait_recv()
        for tag in range(3):
            ag(tag, piece(k, c), cw, fin_kv).wait_send()
        for tag in (3, 4, 7, 8):
            ag(tag, far[0], cw).wait_send()
        for tag in (5, 6):
            ag(tag, piece(k, c), cw).wait_send()
        own_piece.wait()

    dkv_in = pltpu.make_async_copy(dkv_hbm, dkv_v, t_sem.at[4])
    dkv_in.start()
    kp_copy = rdma(kind.at[1 - k], kp, kp_sem.at[0], kp_sem.at[1], mate)

    def products(big, a_v, at):
        def load_b(own, other):
            return (pltpu.make_async_copy(own, big.at[0], b_sem.at[0]), pltpu.make_async_copy(other, big.at[1], b_sem.at[1]))

        def load_a(i, own, other, r):
            return (pltpu.make_async_copy(own.at[:, k, rel[r]], a_v.at[i % 2, 0], ld_sem.at[i % 2, 0]),
                    pltpu.make_async_copy(other.at[:, rel[r]], a_v.at[i % 2, 1], ld_sem.at[i % 2, 1]))

        def turn(j, src):
            for i in range(nb // 2):
                at[j, :, 2 * i * tok:(2 * i + 2) * tok] = jnp.concatenate([src[2 * i], src[2 * i + 1]], axis=0).T

        def both(cols):
            return dot_nn(at[0], big[0, :, cols]) + dot_nn(at[1], big[1, :, cols])

        hn_in = load_b(hn_hbm, hnp_hbm)
        for x in hn_in:
            x.start()
        jobs = [(1, r) for r in range(4)] + [(0, r) for r in range(4)]

        def fetch(i):
            s, r = jobs[i]
            return load_a(i, (o_hbm, dq_hbm)[s], (op_hbm, dqp_hbm)[s], r)
        for i in range(2):
            for x in fetch(i):
                x.start()
        dkv_in.wait()
        for b in range(nb):
            lo, hi = dkv_v[b, :, :half].astype(F32), dkv_v[b, :, half:d].astype(F32)
            cs, sn = cos_ref[...], sin_ref[...]
            kind[0, b, :, :half] = (lo * cs + hi * sn).astype(BF16)
            kind[0, b, :, half:] = (hi * cs - lo * sn).astype(BF16)
            kind[1, b] = dkv_v[b, :, d:]
        kp_copy.start()
        turn(0, kind.at[k])
        for x in hn_in:
            x.wait()
        kp_copy.wait_recv()
        turn(1, kp)
        for r in range(4):
            for dr in range(2):
                acc_kv[r, dr] = both(pl.ds(pl.multiple_of(rel[r] * eq + dr * (eq // 2), 128), eq // 2))
        for dr in range(2):
            hop_kv(dr, 0).start()

        for i, (s, r) in enumerate(jobs):
            if i == 4:
                dy_in = load_b(dy_hbm, dyp_hbm)
                for x in dy_in:
                    x.start()
            for x in fetch(i):
                x.wait()
            turn(0, a_v.at[i % 2, 0])
            turn(1, a_v.at[i % 2, 1])
            if i + 2 < 8:
                for x in fetch(i + 2):
                    x.start()
            if i == 4:
                for x in dy_in:
                    x.wait()

            @pl.loop(0, 4)
            def _(n):
                cols = pl.ds(pl.multiple_of(n * eq, 128), eq)
                acc[s, r, n // 2, :, pl.ds(pl.multiple_of(lax.rem(n, 2) * eq, 128), eq)] = both(cols)
            if r < 2:
                hop(s, r, 0).start()
            if i == 1:
                pass_on_kv(1)
            if i == 5:
                pass_on(1, 1)
                pass_on_kv(2)

    pl.run_scoped(products, pltpu.VMEM((2, n_tok, e), BF16), pltpu.VMEM((2, 2, nb, tok, d), BF16), pltpu.VMEM((2, d, n_tok), BF16))

    mc = 2 * tok
    units = nb // 2

    def attn_out(wo_v, o_v, x_v, y_v):
        w_in = pltpu.make_async_copy(wo_hbm, wo_v, b_sem.at[0])
        w_in.start()

        def load(u):
            return (pltpu.make_async_copy(o_hbm.at[pl.ds(2 * u, 2)], o_v.at[u % 2], ld_sem.at[u % 2, 0]),
                    pltpu.make_async_copy(x_hbm.at[pl.ds(u * mc, mc)], x_v.at[u % 2], ld_sem.at[u % 2, 1]))

        def put(u):
            return pltpu.make_async_copy(y_v.at[u % 2], y_hbm.at[pl.ds(u * mc, mc)], t_sem.at[u % 2])
        for x in load(0):
            x.start()
        w_in.wait()
        for u in range(units):
            if u + 1 < units:
                for x in load(u + 1):
                    x.start()
            for x in load(u):
                x.wait()
            if u >= 2:
                put(u - 2).wait()
            sl = u % 2

            @pl.loop(0, 4)
            def _(n):
                cols = pl.ds(pl.multiple_of(n * eq, 128), eq)
                o_rows = jnp.concatenate([jnp.concatenate([o_v[sl, i, h % 2, h // 2] for h in range(8)], axis=1) for i in range(2)], axis=0)
                r = dot_nn(o_rows, wo_v[:, cols])
                y_v[sl, :, cols] = (x_v[sl, :, cols].astype(F32) + r).astype(BF16)
            put(u).start()
        for u in range(max(0, units - 2), units):
            put(u).wait()

    pl.run_scoped(attn_out, pltpu.VMEM((8 * d, e), BF16), pltpu.VMEM((2, 2, 2, 4, tok, d), BF16),
                  pltpu.VMEM((2, mc, e), BF16), pltpu.VMEM((2, mc, e), BF16))
    pass_on(0, 1)

    def hidden_grad(wq_v, wkv_v, dq_v, x_v, dy_v, dh, gx_v):
        w_in = pltpu.make_async_copy(wq_hbm, wq_v, b_sem.at[0])
        w_in.start()
        w2_in = pltpu.make_async_copy(wkv_hbm, wkv_v, b_sem.at[1])
        w2_in.start()

        def load(u):
            return (pltpu.make_async_copy(dq_hbm.at[pl.ds(2 * u, 2)], dq_v, ld_sem.at[0, 0]),
                    pltpu.make_async_copy(x_hbm.at[pl.ds(u * mc, mc)], x_v, ld_sem.at[0, 1]),
                    pltpu.make_async_copy(dy_hbm.at[pl.ds(u * mc, mc)], dy_v, ld_sem.at[1, 0]))

        def put(u):
            return pltpu.make_async_copy(gx_v, gx_hbm.at[pl.ds(u * mc, mc)], t_sem.at[0])
        gain = g_ref[...].astype(F32)
        gln_acc[...] = jnp.zeros_like(gln_acc)
        for x in load(0):
            x.start()
        w_in.wait()
        w2_in.wait()
        for u in range(units):
            for x in load(u):
                x.wait()

            @pl.loop(0, 4)
            def _(n):
                rows = pl.ds(pl.multiple_of(n * eq, 128), eq)
                t = None
                for h in range(8):
                    a = jnp.concatenate([dq_v[i, h % 2, h // 2] for i in range(2)], axis=0)
                    p = dot_nt(a, wq_v[h, rows, :])
                    t = p if t is None else t + p
                for j in range(2):
                    a = jnp.concatenate([kind[j, 2 * u + i] for i in range(2)], axis=0)
                    t = t + dot_nt(a, wkv_v[rows, j * d:(j + 1) * d])
                dh[:, rows] = t
            if u >= 1:
                put(u - 1).wait()

            @pl.loop(0, mc // 16)
            def _(r):
                rs = pl.ds(pl.multiple_of(r * 16, 16), 16)
                x = x_v[rs, :].astype(F32)
                cx = x - jnp.mean(x, axis=1, keepdims=True)
                inv = lax.rsqrt(jnp.mean(cx * cx, axis=1, keepdims=True) + LN_EPS)
                xh = cx * inv
                g = dh[rs, :]
                pr = g * xh
                gln_acc[...] += pr[:8] + pr[8:]
                gh = g * gain
                m1 = jnp.mean(gh, axis=1, keepdims=True)
                m2 = jnp.mean(gh * xh, axis=1, keepdims=True)
                gx_v[rs, :] = (inv * (gh - m1 - xh * m2) + dy_v[rs, :].astype(F32)).astype(BF16)
            put(u).start()
            if u + 1 < units:
                for x in load(u + 1):
                    x.start()
            if u == units // 2 - 1:
                pass_on(1, 2)
                finish_kv()
        put(units - 1).wait()

    pl.run_scoped(hidden_grad, pltpu.VMEM((8, e, d), BF16), pltpu.VMEM((e, 2 * d), BF16), pltpu.VMEM((2, 2, 4, tok, d), BF16),
                  pltpu.VMEM((mc, e), BF16), pltpu.VMEM((mc, e), BF16), pltpu.VMEM((mc, e), F32), pltpu.VMEM((mc, e), BF16))
    gl_recv[me] = jnp.sum(gln_acc[...], axis=0, keepdims=True)
    pass_on(0, 2)
    gl = [rdma(gl_recv.at[me], gl_recv.at[me], gl_send.at[o - 1], gl_rsem.at[o - 1], lax.rem(me + o, 8)) for o in range(1, 8)]
    for x in gl:
        x.start()
    finish(1, gwq_ref)
    ag_forward()
    for o in range(1, 8):
        src = lax.rem(me + 8 - o, 8)
        rdma(gl_recv.at[src], gl_recv.at[src], gl_send.at[o - 1], gl_rsem.at[o - 1], mate).wait_recv()
    total = gl_recv[0]
    for i in range(1, 8):
        total = total + gl_recv[i]
    gln_ref[...] = total
    finish(0, gwo_ref)
    ag_last()
    for x in gl:
        x.wait_send()
    kp_copy.wait_send()
    for dr in range(2):
        for j in range(3):
            hop_kv(dr, j).wait_send()
            for s in range(2):
                hop(s, dr, j).wait_send()


def gradients(o, o_p, dq, dq_p, hn, hn_p, dy, dy_p, dkv, wqf, wof, w_kv, x, gain, cos_t, sin_t):
    nb, tok, e = x.shape
    n_tok = nb * tok
    d = dq.shape[-1]
    any_spec = pl.BlockSpec(memory_space=pl.ANY)
    vmem = pl.BlockSpec(memory_space=pltpu.VMEM)
    dma = pltpu.SemaphoreType.DMA
    tokens = jax.ShapeDtypeStruct((n_tok, e), BF16)
    y, gx, gln, gwo, gwq_t, gkv_t = pl.pallas_call(
        functools.partial(grads_body, nb, tok),
        in_specs=[any_spec] * 13 + [vmem, vmem, vmem],
        out_specs=[any_spec, any_spec, vmem, vmem, vmem, any_spec],
        out_shape=[tokens, tokens, jax.ShapeDtypeStruct((1, e), F32), jax.ShapeDtypeStruct((d, e), BF16),
                   jax.ShapeDtypeStruct((d, e), BF16), jax.ShapeDtypeStruct((2, d, e), F32)],
        scratch_shapes=[pltpu.VMEM((2, 4, 2, d, e // 2), F32), pltpu.VMEM((4, 2, d, e // 8), F32),
                        pltpu.VMEM((2, 2, 3, d, e // 2), F32), pltpu.VMEM((2, 3, d, e // 8), F32),
                        pltpu.VMEM((2, nb, tok, d), BF16), pltpu.VMEM((nb, tok, d), BF16), pltpu.VMEM((nb, tok, 2 * d), BF16),
                        pltpu.VMEM((d, e // 4), F32), pltpu.VMEM((8, e), F32), pltpu.VMEM((8, 1, e), F32),
                        dma((2, 2, 3)), dma((2, 2, 3)), dma((2, 3)), dma((2, 3)), dma((9,)), dma((9,)), dma((7,)), dma((7,)),
                        dma((2,)), dma((2, 2)), dma((2,)), dma((6,))],
        compiler_params=pltpu.CompilerParams(collective_id=2, has_side_effects=True, vmem_limit_bytes=63 * 2**20),
        cost_estimate=pl.CostEstimate(flops=10 * n_tok * e * e, bytes_accessed=120 * 2**20, transcendentals=0),
        name="gradients",
    )(o, o_p, dq, dq_p, hn, hn_p, dy.reshape(n_tok, e), dy_p, dkv, wqf, wof.reshape(8 * d, e), w_kv, x.reshape(n_tok, e),
      gain.reshape(1, e), cos_t, sin_t)
    return y.reshape(nb, tok, e), gx.reshape(nb, tok, e), gln.reshape(e), gwq_t.T, gkv_t[0].T, gkv_t[1].T, gwo


def solution(mesh):
    act_spec = P('dp', 'tp', None)

    def device_step(x_loc, ln_scale, wq_loc, w_k, w_v, wo_loc, dy_loc):
        n_batch, tok, model_dim = x_loc.shape
        d = w_k.shape[1]
        t0 = lax.axis_index('tp') * tok
        cos_t, sin_t = rope_tables(t0 + jnp.arange(tok), d)

        w_kv = jnp.concatenate([w_k, w_v], axis=1)
        hn, q, do, kv_loc, wq_h, wo_h, hn_p, dy_p = project(x_loc, ln_scale, wq_loc, w_kv, wo_loc, dy_loc, cos_t, sin_t)
        o, dq, dkv_loc, o_p, dq_p = attention(q, do, kv_loc, cos_t, sin_t)
        return gradients(o, o_p, dq, dq_p, hn, hn_p, dy_loc, dy_p, dkv_loc, wq_h, wo_h, w_kv, x_loc, ln_scale, cos_t, sin_t)

    return jax.shard_map(device_step, mesh=mesh, in_specs=(act_spec, P(None), P(None, 'tp'), P(None, None), P(None, None), P('tp', None), act_spec), out_specs=(act_spec, act_spec, P('dp'), P('dp', 'tp'), P('dp', None), P('dp', None), P(('dp', 'tp'), None)), check_vma=False)
```

```python
import functools
import jax
import jax.numpy as jnp
from jax import lax
from jax.experimental import pallas as pl
from jax.experimental.pallas import tpu as pltpu
from jax.sharding import PartitionSpec as P

LN_EPS = 1e-6
ROPE_BASE = 10000.0
LOG2E = 1.4426950408889634
F32 = jnp.float32
BF16 = jnp.bfloat16


def rope_tables(positions, head_dim):
    half_dim = head_dim // 2
    inv_freq = ROPE_BASE ** (-2.0 * jnp.arange(half_dim, dtype=F32) / head_dim)
    angles = positions.astype(F32)[:, None] * inv_freq[None, :]
    return jnp.cos(angles), jnp.sin(angles)


def rotate(vectors, cos_t, sin_t):
    half_dim = vectors.shape[-1] // 2
    lo_half = vectors[..., :half_dim]
    hi_half = vectors[..., half_dim:]
    return jnp.concatenate([lo_half * cos_t - hi_half * sin_t, hi_half * cos_t + lo_half * sin_t], axis=-1)


def dot_nn(a, b):
    return lax.dot_general(a, b, (((1,), (0,)), ((), ())), preferred_element_type=F32)


def dot_nt(a, b):
    return lax.dot_general(a, b, (((1,), (1,)), ((), ())), preferred_element_type=F32)


def rdma(src, dst, send, recv, to):
    return pltpu.make_async_remote_copy(src_ref=src, dst_ref=dst, send_sem=send, recv_sem=recv,
                                        device_id={'tp': to}, device_id_type=pl.DeviceIdType.MESH)


def ring_ids():
    me = lax.axis_index('tp')
    k = lax.rem(me, 2)
    return me, k, me + 1 - 2 * k, lax.rem(me + 2, 8), lax.rem(me + 6, 8)


def enter(peers):
    barrier = pltpu.get_barrier_semaphore()
    for p in peers:
        pl.semaphore_signal(barrier, inc=1, device_id={'tp': p}, device_id_type=pl.DeviceIdType.MESH)
    pl.semaphore_wait(barrier, len(peers))


class Gather:
    def __init__(self, ids, c, block, send, recv):
        self.me, _, self.mate, self.cw, self.ccw = ids
        self.c, self.block, self.send, self.recv = c, block, send, recv

    def copy(self, j, tag, to, src=None):
        ref = self.block(j)
        return rdma(ref if src is None else src, ref, self.send(tag), self.recv(tag), to)

    def own(self, src):
        @pl.when(self.c <= 2)
        def _():
            self.copy(self.me, 0, self.cw, src).start()

        @pl.when(self.c == 0)
        def _():
            self.copy(self.me, 2, self.ccw, src).start()
        self.copy(self.me, 3, self.mate, src).start()

    def arrived(self):
        @pl.when(self.c >= 1)
        def _():
            self.copy(self.me - 2, 0, self.cw).wait_recv()

        @pl.when(self.c == 3)
        def _():
            self.copy(self.me - 6, 2, self.ccw).wait_recv()

    def pass_on(self, src=lambda j: None):
        @pl.when(self.c >= 1)
        def _():
            @pl.when(self.c <= 2)
            def _():
                self.copy(self.me - 2, 1, self.cw, src(self.me - 2)).start()
            self.copy(self.me - 2, 4, self.mate, src(self.me - 2)).start()

        @pl.when(self.c == 3)
        def _():
            self.copy(self.me - 6, 6, self.mate, src(self.me - 6)).start()

    def forward(self):
        self.arrived()
        self.pass_on()

    def last(self):
        @pl.when(self.c >= 2)
        def _():
            self.copy(self.me - 4, 1, self.cw).wait_recv()
            self.copy(self.me - 4, 5, self.mate).start()

    def ready(self, tags=(3, 4, 5, 6)):
        if 3 in tags:
            self.copy(self.mate, 3, self.mate).wait_recv()
        for n, tag in ((1, 4), (2, 5), (3, 6)):
            if tag not in tags:
                continue

            @pl.when(self.c >= n)
            def _():
                self.copy(self.mate - 2 * n, tag, self.mate).wait_recv()

    def drain(self, tags=range(7)):
        c = self.c
        conds = (c <= 2, (c >= 1) & (c <= 2), c == 0, c >= 0, c >= 1, c >= 2, c == 3)
        for tag in tags:
            @pl.when(conds[tag])
            def _():
                self.copy(self.me, tag, self.mate).wait_send()


def attn_body(nb, tok, seq, d, q_hbm, do_hbm, kvl_hbm, kv0_hbm, cos_ref, sin_ref,
              o_hbm, dq_hbm, dkv_hbm, op_hbm, dqp_hbm,
              kv_all, q_v, do_v, o_v, dq_v, s_buf, m_buf, l_buf, p_buf, ds_buf, q_t, do_t, dk_t, dv_t, d_buf, cos4, sin4, mrecv, rrecv,
              kv_send, kv_recv, m_send, m_recv, r_send, r_recv, own_sem, in_sem, out_sem, fin_sem, p_send, p_recv, first_sem):
    scale = d ** -0.5
    rows = s_buf.shape[1]
    n_blk = seq // 256
    rb = 2 * rows // n_blk
    n_rb = rows // rb
    half = d // 2
    me, k, mate, cw, ccw = ring_ids()
    c = me // 2

    def blk(j):
        return pl.ds(pl.multiple_of(j * tok, 16), tok)

    def kvb(b, j):
        return kv_all.at[b, blk(j)]

    def gather(b):
        return Gather((me, k, mate, cw, ccw), c, lambda j: kvb(b, j), lambda t: kv_send.at[b - 1, t], lambda t: kv_recv.at[b - 1, t])

    def own(b):
        gather(b).own(kvl_hbm.at[b])

    def own_copy(b):
        return pltpu.make_async_copy(kvl_hbm.at[b], kvb(b, me), own_sem.at[b])

    def ready(b):
        own_copy(b).wait()

        @pl.when(b == 1)
        def _():
            gather(1).ready((4, 5, 6))

        @pl.when(b > 1)
        def _():
            gather(b).ready()

    def drain(b):
        @pl.when(b == 1)
        def _():
            gather(1).drain((1, 4, 5, 6))

        @pl.when(b > 1)
        def _():
            gather(b).drain()

    def m_copy(b, n):
        return rdma(kvb(b, 2 * n + 1 - k), mrecv.at[b, n], m_send.at[b, n], m_recv.at[b, n], mate)

    def r_copy(b, n, slot, to):
        return rdma(kvb(b, 2 * n + k), rrecv.at[b, slot], r_send.at[b, slot], r_recv.at[b, slot], to)

    def add_into(b, n, other):
        v = kv_all[b, blk(2 * n + k), :].astype(F32) + other[...].astype(F32)
        kv_all[b, blk(2 * n + k), :] = v.astype(BF16)

    def fin_copy(b):
        return pltpu.make_async_copy(kvb(b, me), dkv_hbm.at[b], fin_sem.at[b])

    def to_mate(b):
        for n in range(4):
            @pl.when(c >= n)
            def _():
                m_copy(b, n).start()

    def stage1(b):
        for n in range(4):
            @pl.when(c >= n)
            def _():
                m_copy(b, n).wait()
                add_into(b, n, mrecv.at[b, n])

        @pl.when(c == 3)
        def _():
            r_copy(b, 1, 2, ccw).start()
            r_copy(b, 2, 1, ccw).start()
            r_copy(b, 0, 0, cw).start()
            fin_copy(b).start()

        @pl.when(c == 2)
        def _():
            r_copy(b, 0, 1, ccw).start()

    def stage2(b):
        @pl.when(c == 2)
        def _():
            r_copy(b, 1, 2, ccw).wait_recv()
            add_into(b, 1, rrecv.at[b, 2])
            r_copy(b, 1, 2, ccw).start()
            r_copy(b, 2, 1, ccw).wait_recv()
            add_into(b, 2, rrecv.at[b, 1])
            fin_copy(b).start()

        @pl.when(c == 1)
        def _():
            r_copy(b, 0, 1, ccw).wait_recv()
            add_into(b, 0, rrecv.at[b, 1])
            r_copy(b, 0, 1, ccw).start()

    def stage3(b):
        @pl.when(c == 0)
        def _():
            r_copy(b, 0, 0, cw).wait_recv()
            add_into(b, 0, rrecv.at[b, 0])
            r_copy(b, 0, 1, ccw).wait_recv()
            add_into(b, 0, rrecv.at[b, 1])
            fin_copy(b).start()

        @pl.when(c == 1)
        def _():
            r_copy(b, 1, 2, ccw).wait_recv()
            add_into(b, 1, rrecv.at[b, 2])
            fin_copy(b).start()

    def load(b, slot):
        return (pltpu.make_async_copy(q_hbm.at[b], q_v.at[slot], in_sem.at[0, slot]),
                pltpu.make_async_copy(do_hbm.at[b], do_v.at[slot], in_sem.at[1, slot]))

    def handed(dst, src, n, b, slot):
        return rdma(src.at[slot, 1 - k], dst.at[b], p_send.at[n, b], p_recv.at[n, b], mate)

    def store_o(b, slot):
        return (pltpu.make_async_copy(o_v.at[slot], o_hbm.at[b], out_sem.at[0, slot]), handed(op_hbm, o_v, 0, b, slot))

    def store_dq(b, slot):
        return (pltpu.make_async_copy(dq_v.at[slot], dq_hbm.at[b], out_sem.at[1, slot]), handed(dqp_hbm, dq_v, 1, b, slot))

    def stored(x):
        x[0].wait()
        x[1].wait_send()

    def scores(b, g, slot, i):
        cols = slice(i * 256, (i + 1) * 256)
        s = dot_nt(q_v[slot, g].reshape(rows, d), kv_all[b, cols, :d])
        col = lax.broadcasted_iota(jnp.int32, (tok, 256), 1) + i * 256
        row = lax.broadcasted_iota(jnp.int32, (tok, 256), 0) + me * tok
        s = jnp.concatenate([jnp.where(col <= row, s[j * tok:(j + 1) * tok], -1e30) for j in range(rows // tok)], axis=0)
        s_buf[g, :, cols] = s
        m = jnp.maximum(s[:, :128], s[:, 128:])
        m_buf[...] = m if i == 0 else jnp.maximum(m_buf[...], m)

    def softmax(g, i):
        n = rows // n_blk
        for r in range(i * n, (i + 1) * n, 16):
            rs = slice(r, r + 16)
            m = jnp.max(m_buf[rs, :], axis=1, keepdims=True) * (scale * LOG2E)
            l = None
            for j in range(0, seq, 128):
                e = jnp.exp2(s_buf[g, rs, j:j + 128] * (scale * LOG2E) - m)
                s_buf[g, rs, j:j + 128] = e
                l = e if l is None else l + e
            l_buf[g, rs, :] = jnp.broadcast_to(1.0 / jnp.sum(l, axis=1, keepdims=True), (16, 128))

    def turn(g, slot, i):
        rs = slice(i * rb, (i + 1) * rb)
        q_t[g, :, rs] = q_v[slot, g].reshape(rows, d)[rs].T
        do_t[g, :, rs] = do_v[slot, g].reshape(rows, d)[rs].T

    def out_rows(b, g, slot, i):
        rs = slice(i * rb, (i + 1) * rb)
        p = (s_buf[g, rs, :] * jnp.concatenate([l_buf[g, rs, :]] * (seq // 128), axis=1)).astype(BF16)
        p_buf[rs, :] = p
        o = dot_nn(p, kv_all[b, :, d:])
        dvec = jnp.sum(o * do_v[slot, g].reshape(rows, d)[rs].astype(F32), axis=1, keepdims=True)
        d_buf[rs, :] = jnp.broadcast_to(dvec, (rb, 128))
        put_rows(o_v, slot, g, i, o.astype(BF16))

    def put_rows(ref, slot, g, i, v):
        r = i * rb
        while r < (i + 1) * rb:
            n = min((i + 1) * rb - r, tok - r % tok)
            ref[slot, g, r // tok, r % tok:r % tok + n, :] = v[r - i * rb:r - i * rb + n]
            r += n

    def dq_rows(b, g, slot, i):
        rs = slice(i * rb, (i + 1) * rb)
        dq = dot_nn(ds_buf[rs, :], kv_all[b, :, :d]) * scale
        lo, hi = dq[:, :half], dq[:, half:]
        cs, sn = cos4[rs, :], sin4[rs, :]
        put_rows(dq_v, slot, g, i, jnp.concatenate([(lo * cs + hi * sn).astype(BF16), (hi * cs - lo * sn).astype(BF16)], axis=1))

    def grads(b, g, slot, i):
        cols = slice(i * 256, (i + 1) * 256)
        do = do_v[slot, g].reshape(rows, d)
        p = p_buf[:, cols]
        dp = dot_nt(do, kv_all[b, cols, d:])
        dvec = d_buf[...]
        if i > 0:
            n = rows // n_blk
            z = l_buf[1 - g, (i - 1) * n:(i - 1) * n + 8, :]
            for r in range(8, n, 8):
                z = jnp.minimum(z, l_buf[1 - g, (i - 1) * n + r:(i - 1) * n + r + 8, :])
            dvec = dvec + jnp.concatenate([jnp.minimum(z, 0.0)] * (rows // 8), axis=0)
        dd = jnp.concatenate([dvec, dvec], axis=1)
        ds = (p.astype(F32) * (dp - dd)).astype(BF16)
        ds_buf[:, cols] = ds
        dk = dot_nn(q_t[g], ds)
        dv = dot_nn(do_t[g], p)
        if g == 0:
            dk_t[:, cols] = dk
            dv_t[:, cols] = dv
        else:
            dk_t[:, cols] += dk
            dv_t[:, cols] += dv

    def close_kv(b, i):
        cols = slice(i * 256, (i + 1) * 256)
        kv_all[b, cols, :d] = (dk_t[:, cols] * scale).T.astype(BF16)
        kv_all[b, cols, d:] = dv_t[:, cols].T.astype(BF16)

    enter((mate, cw, ccw))
    gather(1).pass_on(lambda j: kv0_hbm.at[1, blk(j)])
    if nb > 2:
        own(2)
    for x in load(0, 0):
        x.start()

    def first(j):
        return pltpu.make_async_copy(kv0_hbm.at[0, blk(j)], kvb(0, j), first_sem.at[j])

    def second(j, n):
        return pltpu.make_async_copy(kv0_hbm.at[1, blk(j)], kvb(1, j), first_sem.at[8 + n])
    arrived = ((c >= 0, mate, 0), (c >= 1, me - 2, 1), (c == 3, me - 6, 2))
    for j in range(8):
        @pl.when(j <= 2 * c + 1)
        def _():
            first(j).start()
    for b in range(1, nb):
        own_copy(b).start()
    for cond, j, i in arrived:
        @pl.when(cond)
        def _():
            second(j, i).start()

    @pl.loop(2 * c + 2, 8)
    def _(j):
        for b in range(nb):
            kv_all[b, blk(j), :] = jnp.zeros((tok, 2 * d), BF16)
    for j in range(rows // tok):
        cos4[j * tok:(j + 1) * tok, :] = cos_ref[...]
        sin4[j * tok:(j + 1) * tok, :] = sin_ref[...]
    ds_buf[...] = jnp.zeros_like(ds_buf)
    for x in load(0, 0):
        x.wait()
    for i in range(n_rb):
        turn(0, 0, i)
    for j in range(8):
        @pl.when(j <= 2 * c + 1)
        def _():
            first(j).wait()
    for cond, j, i in arrived:
        @pl.when(cond)
        def _():
            second(j, i).wait()
    for i in range(n_blk):
        scores(0, 0, 0, i)
    for i in range(n_blk):
        softmax(0, i)

    def comm_steps(b, steps):
        for lag, stage in steps:
            @pl.when(b >= lag)
            def _():
                stage(b - lag)

    @pl.loop(0, nb)
    def _(b):
        slot = lax.rem(b, 2)
        nxt = jnp.minimum(b + 1, nb - 1)
        prev = jnp.maximum(b - 1, 0)

        @pl.when(b + 1 < nb)
        def _():
            for x in load(b + 1, 1 - slot):
                x.start()

        @pl.when(b + 3 < nb)
        def _():
            own(b + 3)

        @pl.when((b >= 1) & (b + 2 < nb))
        def _():
            gather(b + 2).forward()

        @pl.when((b >= 1) & (b + 1 < nb))
        def _():
            gather(b + 1).last()
        comm_steps(b, ((2, stage1),))

        @pl.when(b >= 2)
        def _():
            drain(b - 1)

        @pl.when(b >= 2)
        def _():
            stored(store_o(b - 2, slot))
        spare = jnp.where(b >= 1, b - 1, nb)
        for i in range(n_blk):
            scores(b, 1, slot, i)
            if i % 2 == 1:
                out_rows(b, 0, slot, i // 2)
                dq_rows(prev, 1, 1 - slot, i // 2)
                turn(1, slot, i // 2)
        for i in range(n_blk):
            close_kv(spare, i)

        @pl.when(b >= 1)
        def _():
            for x in store_dq(b - 1, 1 - slot):
                x.start()
            to_mate(b - 1)

        @pl.when(b == 0)
        def _():
            gather(1).last()
        for i in range(n_blk):
            grads(b, 0, slot, i)
            softmax(1, i)

        @pl.when(b + 1 < nb)
        def _():
            for x in load(b + 1, 1 - slot):
                x.wait()
            ready(b + 1)
        if nb > 2:
            @pl.when(b == 0)
            def _():
                gather(2).forward()
        comm_steps(b, ((3, stage2), (4, stage3)))

        @pl.when(b >= 2)
        def _():
            stored(store_dq(b - 2, slot))
        nslot = lax.rem(nxt, 2)
        for i in range(n_blk):
            scores(nxt, 0, nslot, i)
            if i % 2 == 1:
                out_rows(b, 1, slot, i // 2)
                dq_rows(b, 0, slot, i // 2)
                turn(0, nslot, i // 2)
        for x in store_o(b, slot):
            x.start()
        for i in range(n_blk):
            grads(b, 1, slot, i)
            softmax(0, i)

    n = nb
    drain(n - 1)
    for i in range(n_rb):
        dq_rows(n - 1, 1, (n - 1) % 2, i)
    for i in range(n_blk):
        close_kv(n - 1, i)
    for x in store_dq(n - 1, (n - 1) % 2):
        x.start()
    to_mate(n - 1)
    for b in range(n, n + 4):
        for lag, stage in ((2, stage1), (3, stage2), (4, stage3)):
            if 0 <= b - lag < n:
                stage(b - lag)
    for b in (n - 2, n - 1):
        stored(store_o(b, b % 2))
        stored(store_dq(b, b % 2))
    for b in range(n):
        handed(op_hbm, o_v, 0, b, b % 2).wait_recv()
        handed(dqp_hbm, dq_v, 1, b, b % 2).wait_recv()
        fin_copy(b).wait()
        for cond, slot in ((c == 3, 0), (c >= 1, 1), (c >= 2, 2)):
            @pl.when(cond)
            def _():
                r_copy(b, 0, slot, cw).wait_send()


def attention(q, do, kv, kv0, cos_t, sin_t):
    nb, _, hp, tok, d = q.shape
    seq = tok * 8
    rows = hp * tok
    any_spec = pl.BlockSpec(memory_space=pl.ANY)
    vmem = pl.BlockSpec(memory_space=pltpu.VMEM)
    dma = pltpu.SemaphoreType.DMA
    slab = pltpu.VMEM((2, 2, hp, tok, d), BF16)
    out = jax.ShapeDtypeStruct(q.shape, BF16)
    outp = jax.ShapeDtypeStruct((nb, hp, tok, d), BF16)
    return pl.pallas_call(
        functools.partial(attn_body, nb, tok, seq, d),
        in_specs=[any_spec, any_spec, any_spec, any_spec, vmem, vmem],
        out_specs=[any_spec] * 5,
        out_shape=[out, out, jax.ShapeDtypeStruct(kv.shape, BF16), outp, outp],
        scratch_shapes=[pltpu.VMEM((nb + 1, seq, 2 * d), BF16), slab, slab, slab, slab,
                        pltpu.VMEM((2, rows, seq), F32), pltpu.VMEM((rows, 128), F32),
                        pltpu.VMEM((2, rows, 128), F32), pltpu.VMEM((rows, seq), BF16), pltpu.VMEM((rows, seq), BF16),
                        pltpu.VMEM((2, d, rows), BF16), pltpu.VMEM((2, d, rows), BF16),
                        pltpu.VMEM((d, seq), F32), pltpu.VMEM((d, seq), F32), pltpu.VMEM((rows, 128), F32),
                        pltpu.VMEM((rows, d // 2), F32), pltpu.VMEM((rows, d // 2), F32),
                        pltpu.VMEM((nb, 4, tok, 2 * d), BF16), pltpu.VMEM((nb, 3, tok, 2 * d), BF16),
                        dma((nb - 1, 7)), dma((nb - 1, 7)), dma((nb, 4)), dma((nb, 4)), dma((nb, 3)), dma((nb, 3)),
                        dma((nb,)), dma((2, 2)), dma((2, 2)), dma((nb,)), dma((2, nb)), dma((2, nb)), dma((11,))],
        compiler_params=pltpu.CompilerParams(collective_id=1, has_side_effects=True, vmem_limit_bytes=63 * 2**20),
        cost_estimate=pl.CostEstimate(flops=24 * nb * rows * seq * d, bytes_accessed=40 * 2**20,
                                      transcendentals=2 * nb * rows * seq),
        name="attention",
    )(q, do, kv, kv0, cos_t, sin_t)


def proj_body(nb, tok, x_hbm, g_ref, wq_hbm, wk_ref, wv_ref, wo_hbm, dy_hbm, cos_ref, sin_ref,
              kv0_hbm, hn_hbm, q_hbm, do_hbm, kv_hbm, wqf_hbm, wof_hbm, hnp_hbm, dyp_hbm,
              x_v, hn_v, dy_v, wq_v, wo_v, kv_v, out_v,
              send, recv, x_sem, dy_sem, own_sem, out_sem, misc_sem, w_sem, p_send, p_recv, kv_send, kv_recv):
    n_tok, e = x_hbm.shape
    d = kv_v.shape[1] // 2
    half = d // 2
    mc = 2 * tok
    me, k, mate, cw, ccw = ring_ids()
    base = 2 * (me // 2)

    def head(off, par):
        return lax.rem(base + 2 * off + 8, 8) + par
    enter((mate, cw, ccw))

    fulls = (wq_v, wo_v)
    locs = (wq_hbm, wo_hbm)

    def half_of(w, ref, j):
        n = ref.shape[0] // 2
        return ref.at[pl.ds(j * n, n)]

    sends = []

    def send_full(w, h, j, to, own=False):
        src = locs[w] if own else fulls[w].at[h]
        c = rdma(src, fulls[w].at[h], send.at[w, j], recv.at[w, j], to)
        c.start()
        sends.append(c)

    def send_half(w, h, part, j, to):
        c = rdma(half_of(w, fulls[w].at[h], part), half_of(w, fulls[w].at[h], part), send.at[w, j], recv.at[w, j], to)
        c.start()
        sends.append(c)

    def wait_full(w, h, j):
        rdma(fulls[w].at[h], fulls[w].at[h], send.at[w, j], recv.at[w, j], mate).wait_recv()

    def wait_half(w, h, part, j):
        ref = half_of(w, fulls[w].at[h], part)
        rdma(ref, ref, send.at[w, j], recv.at[w, j], mate).wait_recv()

    for w in range(2):
        send_full(w, me, 0, cw, True)
        send_full(w, me, 1, ccw, True)
        send_full(w, me, 4, mate, True)
    own = [pltpu.make_async_copy(locs[w], fulls[w].at[me], own_sem.at[w]) for w in range(2)]
    xs = [pltpu.make_async_copy(x_hbm.at[pl.ds(b * tok, tok)], x_v.at[pl.ds(b * tok, tok)], x_sem.at[b]) for b in range(nb)]
    for c in xs:
        c.start()
    for c in own:
        c.start()
    dyc = pltpu.make_async_copy(dy_hbm, dy_v, dy_sem)
    dyc.start()

    gain = g_ref[...].astype(F32)
    for b in range(nb):
        xs[b].wait()

        @pl.loop(0, tok // 16, unroll=2)
        def _(r):
            rs = pl.ds(pl.multiple_of(b * tok + r * 16, 16), 16)
            x = x_v[rs, :].astype(F32)
            c = x - jnp.mean(x, axis=1, keepdims=True)
            inv = lax.rsqrt(jnp.mean(c * c, axis=1, keepdims=True) + LN_EPS)
            hn_v[rs, :] = (c * inv * gain).astype(BF16)
    hn_out = pltpu.make_async_copy(hn_v, hn_hbm, misc_sem.at[0])
    hn_out.start()
    to_mate = [rdma(hn_v, hnp_hbm, p_send.at[0], p_recv.at[0], mate), rdma(dy_hbm, dyp_hbm, p_send.at[1], p_recv.at[1], mate)]
    for c in to_mate:
        c.start()

    def rope_rows(raw):
        lo, hi = raw[:, :half], raw[:, half:d]
        cs, sn = jnp.concatenate([cos_ref[...]] * 2, axis=0), jnp.concatenate([sin_ref[...]] * 2, axis=0)
        return lo * cs - hi * sn, hi * cs + lo * sn

    @pl.loop(0, n_tok // mc)
    def _(i):
        rs = pl.ds(pl.multiple_of(i * mc, mc), mc)
        lo, hi = rope_rows(dot_nn(hn_v[rs, :], wk_ref[...]))
        kv_v[rs, :half] = lo.astype(BF16)
        kv_v[rs, half:d] = hi.astype(BF16)
        kv_v[rs, d:] = dot_nn(hn_v[rs, :], wv_ref[...]).astype(BF16)
    kv_out = pltpu.make_async_copy(kv_v, kv_hbm, misc_sem.at[1])
    kv_out.start()

    outs = []
    saves = []

    def save(w, h):
        c = pltpu.make_async_copy(fulls[w].at[h], (wqf_hbm, wof_hbm)[w].at[h], w_sem.at[len(saves)])
        c.start()
        saves.append(c)

    def project(w, h):
        slot = len(outs) % 4
        if len(outs) >= 4:
            outs[-4].wait()

        @pl.loop(0, n_tok // mc)
        def _(i):
            rs = pl.ds(pl.multiple_of(i * mc, mc), mc)
            if w == 0:
                lo, hi = rope_rows(dot_nn(hn_v[rs, :], wq_v[h]))
                o0 = lo.reshape(2, tok, half).astype(BF16)
                o1 = hi.reshape(2, tok, half).astype(BF16)
                out_v[slot, pl.ds(2 * i, 2), :, :half] = o0
                out_v[slot, pl.ds(2 * i, 2), :, half:] = o1
            else:
                out_v[slot, pl.ds(2 * i, 2)] = dot_nt(dy_v[rs, :], wo_v[h]).reshape(2, tok, d).astype(BF16)
        c = pltpu.make_async_copy(out_v.at[slot], (q_hbm, do_hbm)[w].at[:, lax.rem(h, 2), h // 2], out_sem.at[slot])
        c.start()
        outs.append(c)
        save(w, h)

    other = 1 - k
    for w in range(2):
        own[w].wait()
        if w == 1:
            dyc.wait()
        project(w, me)
        wait_full(w, mate, 4)
        project(w, mate)
    for w in range(2):
        wait_full(w, head(-1, k), 0)
        send_half(w, head(-1, k), 0, 2, cw)
        wait_full(w, head(1, k), 1)
        send_half(w, head(1, k), 1, 3, ccw)
        send_full(w, head(-1, k), 5, mate)
        send_full(w, head(1, k), 6, mate)
        project(w, head(-1, k))
        project(w, head(1, k))
        wait_full(w, head(-1, other), 5)
        project(w, head(-1, other))
        wait_full(w, head(1, other), 6)
        project(w, head(1, other))

    def early(n):
        def blk(j):
            return kv0_hbm.at[n, pl.ds(pl.multiple_of(j * tok, 16), tok)]
        return Gather((me, k, mate, cw, ccw), me // 2, blk, lambda t: kv_send.at[n, t], lambda t: kv_recv.at[n, t])
    first, second = early(0), early(1)
    first.own(kv_v.at[pl.ds(0, tok)])
    own0 = pltpu.make_async_copy(kv_v.at[pl.ds(0, tok)], first.block(me), misc_sem.at[2])
    own0.start()
    for w in range(2):
        wait_half(w, head(2, k), 0, 2)
        send_half(w, head(2, k), 0, 7, mate)
        wait_half(w, head(2, k), 1, 3)
        send_half(w, head(2, k), 1, 8, mate)
        project(w, head(2, k))
        if w == 1:
            first.forward()
            second.own(kv_v.at[pl.ds(tok, tok)])
        wait_half(w, head(2, other), 0, 7)
        wait_half(w, head(2, other), 1, 8)
        project(w, head(2, other))
    first.last()
    for c in outs[-4:] + saves + [hn_out, kv_out, own0]:
        c.wait()
    first.ready()
    first.drain()
    second.arrived()
    second.ready((3,))
    second.drain((0, 2, 3))
    for c in sends:
        c.wait_send()
    for c in to_mate:
        c.wait()


def project(x, gain, wq, w_k, w_v, wo, dy, cos_t, sin_t):
    nb, tok, e = x.shape
    d = wq.shape[1]
    n_heads = 8
    n_tok = nb * tok
    any_spec = pl.BlockSpec(memory_space=pl.ANY)
    vmem = pl.BlockSpec(memory_space=pltpu.VMEM)
    act = jax.ShapeDtypeStruct((nb, 2, n_heads // 2, tok, d), BF16)
    dma = pltpu.SemaphoreType.DMA
    flops = 2 * n_tok * e * (2 * n_heads + 2) * d
    kv0, hn, q, do, kv, wqf, wof, hn_p, dy_p = pl.pallas_call(
        functools.partial(proj_body, nb, tok),
        in_specs=[any_spec, vmem, any_spec, vmem, vmem, any_spec, any_spec, vmem, vmem],
        out_specs=[any_spec] * 9,
        out_shape=[jax.ShapeDtypeStruct((2, tok * n_heads, 2 * d), BF16), jax.ShapeDtypeStruct((n_tok, e), BF16), act, act, jax.ShapeDtypeStruct((n_tok, 2 * d), BF16),
                   jax.ShapeDtypeStruct((n_heads, e, d), BF16), jax.ShapeDtypeStruct((n_heads, d, e), BF16),
                   jax.ShapeDtypeStruct((n_tok, e), BF16), jax.ShapeDtypeStruct((n_tok, e), BF16)],
        scratch_shapes=[pltpu.VMEM((n_tok, e), BF16), pltpu.VMEM((n_tok, e), BF16), pltpu.VMEM((n_tok, e), BF16),
                        pltpu.VMEM((n_heads, e, d), BF16), pltpu.VMEM((n_heads, d, e), BF16),
                        pltpu.VMEM((n_tok, 2 * d), BF16), pltpu.VMEM((4, nb, tok, d), BF16),
                        dma((2, 9)), dma((2, 9)), dma((nb,)), dma(()), dma((2,)), dma((4,)), dma((3,)), dma((16,)), dma((2,)), dma((2,)), dma((2, 7)), dma((2, 7))],
        compiler_params=pltpu.CompilerParams(collective_id=0, has_side_effects=True, vmem_limit_bytes=60 * 2**20),
        cost_estimate=pl.CostEstimate(flops=flops, bytes_accessed=60 * 2**20, transcendentals=0),
        name="project",
    )(x.reshape(n_tok, e), gain, wq, w_k, w_v, wo, dy.reshape(n_tok, e), cos_t, sin_t)
    return kv0, hn, q, do, kv.reshape(nb, tok, 2 * d), wqf, wof, hn_p, dy_p


def grads_body(nb, tok, o_hbm, op_hbm, dq_hbm, dqp_hbm, hn_hbm, hnp_hbm, dy_hbm, dyp_hbm, dkv_hbm,
               wq_hbm, wo_hbm, wk_hbm, wv_hbm, x_hbm, g_ref, cos_ref, sin_ref,
               y_hbm, gx_hbm, gln_ref, gwo_ref, gwq_ref, gkv_hbm,
               acc, acc_kv, rbuf, rbuf_kv, kind, kp, dkv_v, fin_kv, gln_acc, gl_recv,
               rs_send, rs_recv, kv_send, kv_recv, ag_send, ag_recv, gl_send, gl_rsem, kp_sem, ld_sem, b_sem, t_sem):
    n_tok, e = x_hbm.shape
    d = wk_hbm.shape[1]
    half = d // 2
    eh, eq = e // 2, e // 4
    me, k, mate, cw, ccw = ring_ids()
    c = me // 2
    rel = [lax.rem(c + o, 4) for o in (3, 1, 2, 0)]
    enter([lax.rem(me + o, 8) for o in range(1, 8)])

    order = ((2, 1), (2, 0))

    def hop(s, dr, j):
        src = acc.at[s, dr, dr] if j == 0 else rbuf.at[s, dr, j - 1]
        return rdma(src, rbuf.at[s, dr, j], rs_send.at[s, dr, j], rs_recv.at[s, dr, j], (cw, ccw)[dr])

    def hop_kv(dr, j):
        src = acc_kv.at[dr, dr] if j == 0 else rbuf_kv.at[dr, j - 1]
        return rdma(src, rbuf_kv.at[dr, j], kv_send.at[dr, j], kv_recv.at[dr, j], (cw, ccw)[dr])

    def add(dst, term):
        @pl.loop(0, dst.shape[0] // 32)
        def _(i):
            rs = pl.ds(pl.multiple_of(i * 32, 32), 32)
            dst[rs, :] = dst[rs, :] + term[rs, :]

    def pass_on(s, j):
        for dr in range(2):
            hop(s, dr, j - 1).wait_recv()
            add(rbuf.at[s, dr, j - 1], acc.at[s, order[dr][j - 1], dr])
            hop(s, dr, j).start()

    def pass_on_kv(j):
        for dr in range(2):
            hop_kv(dr, j - 1).wait_recv()
            add(rbuf_kv.at[dr, j - 1], acc_kv.at[order[dr][j - 1], dr])
            hop_kv(dr, j).start()

    def finish(s, out):
        for dr in range(2):
            hop(s, dr, 2).wait_recv()

            @pl.loop(0, d // 32)
            def _(i):
                rs = pl.ds(pl.multiple_of(i * 32, 32), 32)
                out[rs, dr * eh:(dr + 1) * eh] = (rbuf[s, dr, 2, rs, :] + acc[s, 3, dr, rs, :]).astype(BF16)

    def piece(kk, j, lo=0, n=None):
        return gkv_hbm.at[kk, pl.ds(lo, d if n is None else n), pl.ds(pl.multiple_of(j * eq, 128), eq)]

    def ag(tag, ref, to, src=None):
        return rdma(ref if src is None else src, ref, ag_send.at[tag], ag_recv.at[tag], to)

    def ag_far(tag, to):
        return ag(tag, piece(k, rel[(0, 1)[tag - 3]], (tag - 3) * half, half), to)

    own_piece = pltpu.make_async_copy(fin_kv, piece(k, c), t_sem.at[5])

    def finish_kv():
        for dr in range(2):
            hop_kv(dr, 2).wait_recv()
            fin_kv[:, dr * (eq // 2):(dr + 1) * (eq // 2)] = rbuf_kv[dr, 2] + acc_kv[3, dr]
        ag(0, piece(k, c), cw, fin_kv).start()
        ag(1, piece(k, c), ccw, fin_kv).start()
        ag(2, piece(k, c), mate, fin_kv).start()
        own_piece.start()

    def ag_forward():
        ag(0, piece(k, rel[0]), cw).wait_recv()
        ag_far(3, cw).start()
        ag(1, piece(k, rel[1]), cw).wait_recv()
        ag_far(4, ccw).start()
        ag(5, piece(k, rel[0]), mate).start()
        ag(6, piece(k, rel[1]), mate).start()

    def ag_last():
        far = [piece(k, rel[2], i * half, half) for i in range(2)]
        for i in range(2):
            ag(3 + i, far[i], cw).wait_recv()
            ag(7 + i, far[i], mate).start()
        ag(2, piece(1 - k, c), mate).wait_recv()
        ag(5, piece(1 - k, rel[0]), mate).wait_recv()
        ag(6, piece(1 - k, rel[1]), mate).wait_recv()
        for i in range(2):
            ag(7 + i, piece(1 - k, rel[2], i * half, half), mate).wait_recv()
        for tag in range(3):
            ag(tag, piece(k, c), cw, fin_kv).wait_send()
        for tag in (3, 4, 7, 8):
            ag(tag, far[0], cw).wait_send()
        for tag in (5, 6):
            ag(tag, piece(k, c), cw).wait_send()
        own_piece.wait()

    dkv_in = pltpu.make_async_copy(dkv_hbm, dkv_v, t_sem.at[4])
    dkv_in.start()
    kp_copy = rdma(kind.at[1 - k], kp, kp_sem.at[0], kp_sem.at[1], mate)

    def products(big, a_v, at):
        def load_b(own, other):
            return (pltpu.make_async_copy(own, big.at[0], b_sem.at[0]), pltpu.make_async_copy(other, big.at[1], b_sem.at[1]))

        def load_a(i, own, other, r):
            return (pltpu.make_async_copy(own.at[:, k, rel[r]], a_v.at[i % 2, 0], ld_sem.at[i % 2, 0]),
                    pltpu.make_async_copy(other.at[:, rel[r]], a_v.at[i % 2, 1], ld_sem.at[i % 2, 1]))

        def turn(j, src):
            for i in range(nb // 2):
                at[j, :, 2 * i * tok:(2 * i + 2) * tok] = jnp.concatenate([src[2 * i], src[2 * i + 1]], axis=0).T

        def both(cols):
            return dot_nn(at[0], big[0, :, cols]) + dot_nn(at[1], big[1, :, cols])

        hn_in = load_b(hn_hbm, hnp_hbm)
        for x in hn_in:
            x.start()
        jobs = [(1, r) for r in range(4)] + [(0, r) for r in range(4)]

        def fetch(i):
            s, r = jobs[i]
            return load_a(i, (o_hbm, dq_hbm)[s], (op_hbm, dqp_hbm)[s], r)
        for i in range(2):
            for x in fetch(i):
                x.start()
        dkv_in.wait()
        for b in range(nb):
            lo, hi = dkv_v[b, :, :half].astype(F32), dkv_v[b, :, half:d].astype(F32)
            cs, sn = cos_ref[...], sin_ref[...]
            kind[0, b, :, :half] = (lo * cs + hi * sn).astype(BF16)
            kind[0, b, :, half:] = (hi * cs - lo * sn).astype(BF16)
            kind[1, b] = dkv_v[b, :, d:]
        kp_copy.start()
        turn(0, kind.at[k])
        for x in hn_in:
            x.wait()
        kp_copy.wait_recv()
        turn(1, kp)
        for r in range(4):
            for dr in range(2):
                acc_kv[r, dr] = both(pl.ds(pl.multiple_of(rel[r] * eq + dr * (eq // 2), 128), eq // 2))
        for dr in range(2):
            hop_kv(dr, 0).start()

        for i, (s, r) in enumerate(jobs):
            if i == 4:
                dy_in = load_b(dy_hbm, dyp_hbm)
                for x in dy_in:
                    x.start()
            for x in fetch(i):
                x.wait()
            turn(0, a_v.at[i % 2, 0])
            turn(1, a_v.at[i % 2, 1])
            if i + 2 < 8:
                for x in fetch(i + 2):
                    x.start()
            if i == 4:
                for x in dy_in:
                    x.wait()

            @pl.loop(0, 4)
            def _(n):
                cols = pl.ds(pl.multiple_of(n * eq, 128), eq)
                acc[s, r, n // 2, :, pl.ds(pl.multiple_of(lax.rem(n, 2) * eq, 128), eq)] = both(cols)
            if r < 2:
                hop(s, r, 0).start()
            if i == 1:
                pass_on_kv(1)
            if i == 5:
                pass_on(1, 1)
                pass_on_kv(2)

    pl.run_scoped(products, pltpu.VMEM((2, n_tok, e), BF16), pltpu.VMEM((2, 2, nb, tok, d), BF16), pltpu.VMEM((2, d, n_tok), BF16))

    mc = 2 * tok
    units = nb // 2

    def attn_out(wo_v, o_v, x_v, y_v):
        w_in = pltpu.make_async_copy(wo_hbm, wo_v, b_sem.at[0])
        w_in.start()

        def load(u):
            return (pltpu.make_async_copy(o_hbm.at[pl.ds(2 * u, 2)], o_v.at[u % 2], ld_sem.at[u % 2, 0]),
                    pltpu.make_async_copy(x_hbm.at[pl.ds(u * mc, mc)], x_v.at[u % 2], ld_sem.at[u % 2, 1]))

        def put(u):
            return pltpu.make_async_copy(y_v.at[u % 2], y_hbm.at[pl.ds(u * mc, mc)], t_sem.at[u % 2])
        for x in load(0):
            x.start()
        w_in.wait()
        for u in range(units):
            if u + 1 < units:
                for x in load(u + 1):
                    x.start()
            for x in load(u):
                x.wait()
            if u >= 2:
                put(u - 2).wait()
            sl = u % 2

            @pl.loop(0, 4)
            def _(n):
                cols = pl.ds(pl.multiple_of(n * eq, 128), eq)
                o_rows = jnp.concatenate([jnp.concatenate([o_v[sl, i, h % 2, h // 2] for h in range(8)], axis=1) for i in range(2)], axis=0)
                r = dot_nn(o_rows, wo_v[:, cols])
                y_v[sl, :, cols] = (x_v[sl, :, cols].astype(F32) + r).astype(BF16)
            put(u).start()
        for u in range(max(0, units - 2), units):
            put(u).wait()

    pl.run_scoped(attn_out, pltpu.VMEM((8 * d, e), BF16), pltpu.VMEM((2, 2, 2, 4, tok, d), BF16),
                  pltpu.VMEM((2, mc, e), BF16), pltpu.VMEM((2, mc, e), BF16))
    pass_on(0, 1)

    def hidden_grad(wq_v, wk_v, wv_v, dq_v, x_v, dy_v, dh, gx_v):
        w_in = pltpu.make_async_copy(wq_hbm, wq_v, b_sem.at[0])
        w_in.start()
        w2_in = (pltpu.make_async_copy(wk_hbm, wk_v, b_sem.at[1]), pltpu.make_async_copy(wv_hbm, wv_v, ld_sem.at[1, 1]))
        for x in w2_in:
            x.start()

        def load(u):
            return (pltpu.make_async_copy(dq_hbm.at[pl.ds(2 * u, 2)], dq_v, ld_sem.at[0, 0]),
                    pltpu.make_async_copy(x_hbm.at[pl.ds(u * mc, mc)], x_v, ld_sem.at[0, 1]),
                    pltpu.make_async_copy(dy_hbm.at[pl.ds(u * mc, mc)], dy_v, ld_sem.at[1, 0]))

        def put(u):
            return pltpu.make_async_copy(gx_v, gx_hbm.at[pl.ds(u * mc, mc)], t_sem.at[0])
        gain = g_ref[...].astype(F32)
        gln_acc[...] = jnp.zeros_like(gln_acc)
        for x in load(0):
            x.start()
        w_in.wait()
        for x in w2_in:
            x.wait()
        for u in range(units):
            for x in load(u):
                x.wait()

            @pl.loop(0, 4)
            def _(n):
                rows = pl.ds(pl.multiple_of(n * eq, 128), eq)
                t = None
                for h in range(8):
                    a = jnp.concatenate([dq_v[i, h % 2, h // 2] for i in range(2)], axis=0)
                    p = dot_nt(a, wq_v[h, rows, :])
                    t = p if t is None else t + p
                for j in range(2):
                    a = jnp.concatenate([kind[j, 2 * u + i] for i in range(2)], axis=0)
                    t = t + dot_nt(a, (wk_v, wv_v)[j][rows, :])
                dh[:, rows] = t
            if u >= 1:
                put(u - 1).wait()

            @pl.loop(0, mc // 16)
            def _(r):
                rs = pl.ds(pl.multiple_of(r * 16, 16), 16)
                x = x_v[rs, :].astype(F32)
                cx = x - jnp.mean(x, axis=1, keepdims=True)
                inv = lax.rsqrt(jnp.mean(cx * cx, axis=1, keepdims=True) + LN_EPS)
                xh = cx * inv
                g = dh[rs, :]
                pr = g * xh
                gln_acc[...] += pr[:8] + pr[8:]
                gh = g * gain
                m1 = jnp.mean(gh, axis=1, keepdims=True)
                m2 = jnp.mean(gh * xh, axis=1, keepdims=True)
                gx_v[rs, :] = (inv * (gh - m1 - xh * m2) + dy_v[rs, :].astype(F32)).astype(BF16)
            put(u).start()
            if u + 1 < units:
                for x in load(u + 1):
                    x.start()
            if u == units // 2 - 1:
                pass_on(1, 2)
                finish_kv()
        put(units - 1).wait()

    pl.run_scoped(hidden_grad, pltpu.VMEM((8, e, d), BF16), pltpu.VMEM((e, d), BF16), pltpu.VMEM((e, d), BF16), pltpu.VMEM((2, 2, 4, tok, d), BF16),
                  pltpu.VMEM((mc, e), BF16), pltpu.VMEM((mc, e), BF16), pltpu.VMEM((mc, e), F32), pltpu.VMEM((mc, e), BF16))
    gl_recv[me] = jnp.sum(gln_acc[...], axis=0, keepdims=True)
    pass_on(0, 2)
    gl = [rdma(gl_recv.at[me], gl_recv.at[me], gl_send.at[o - 1], gl_rsem.at[o - 1], lax.rem(me + o, 8)) for o in range(1, 8)]
    for x in gl:
        x.start()
    finish(1, gwq_ref)
    ag_forward()
    for o in range(1, 8):
        src = lax.rem(me + 8 - o, 8)
        rdma(gl_recv.at[src], gl_recv.at[src], gl_send.at[o - 1], gl_rsem.at[o - 1], mate).wait_recv()
    total = gl_recv[0]
    for i in range(1, 8):
        total = total + gl_recv[i]
    gln_ref[...] = total
    finish(0, gwo_ref)
    ag_last()
    for x in gl:
        x.wait_send()
    kp_copy.wait_send()
    for dr in range(2):
        for j in range(3):
            hop_kv(dr, j).wait_send()
            for s in range(2):
                hop(s, dr, j).wait_send()


def gradients(o, o_p, dq, dq_p, hn, hn_p, dy, dy_p, dkv, wqf, wof, w_k, w_v, x, gain, cos_t, sin_t):
    nb, tok, e = x.shape
    n_tok = nb * tok
    d = dq.shape[-1]
    any_spec = pl.BlockSpec(memory_space=pl.ANY)
    vmem = pl.BlockSpec(memory_space=pltpu.VMEM)
    dma = pltpu.SemaphoreType.DMA
    tokens = jax.ShapeDtypeStruct((n_tok, e), BF16)
    y, gx, gln, gwo, gwq_t, gkv_t = pl.pallas_call(
        functools.partial(grads_body, nb, tok),
        in_specs=[any_spec] * 14 + [vmem, vmem, vmem],
        out_specs=[any_spec, any_spec, vmem, vmem, vmem, any_spec],
        out_shape=[tokens, tokens, jax.ShapeDtypeStruct((1, e), F32), jax.ShapeDtypeStruct((d, e), BF16),
                   jax.ShapeDtypeStruct((d, e), BF16), jax.ShapeDtypeStruct((2, d, e), F32)],
        scratch_shapes=[pltpu.VMEM((2, 4, 2, d, e // 2), F32), pltpu.VMEM((4, 2, d, e // 8), F32),
                        pltpu.VMEM((2, 2, 3, d, e // 2), F32), pltpu.VMEM((2, 3, d, e // 8), F32),
                        pltpu.VMEM((2, nb, tok, d), BF16), pltpu.VMEM((nb, tok, d), BF16), pltpu.VMEM((nb, tok, 2 * d), BF16),
                        pltpu.VMEM((d, e // 4), F32), pltpu.VMEM((8, e), F32), pltpu.VMEM((8, 1, e), F32),
                        dma((2, 2, 3)), dma((2, 2, 3)), dma((2, 3)), dma((2, 3)), dma((9,)), dma((9,)), dma((7,)), dma((7,)),
                        dma((2,)), dma((2, 2)), dma((2,)), dma((6,))],
        compiler_params=pltpu.CompilerParams(collective_id=2, has_side_effects=True, vmem_limit_bytes=63 * 2**20),
        cost_estimate=pl.CostEstimate(flops=10 * n_tok * e * e, bytes_accessed=120 * 2**20, transcendentals=0),
        name="gradients",
    )(o, o_p, dq, dq_p, hn, hn_p, dy.reshape(n_tok, e), dy_p, dkv, wqf, wof.reshape(8 * d, e), w_k, w_v, x.reshape(n_tok, e),
      gain, cos_t, sin_t)
    y, gx, gwq, gwk, gwv, gwo, gln = place(nb, y, gx, gwq_t, gkv_t, gwo, gln)
    return y.reshape(nb, tok, e), gx.reshape(nb, tok, e), gln.reshape(e), gwq, gwk, gwv, gwo


def place_body(y_in, gx_in, gq_in, gkv_in, go_in, gl_in, y, gx, gq, gk, gv, go, gl):
    y[...] = y_in[...]
    gx[...] = gx_in[...]
    gq[...] = gq_in[...].astype(F32).T.astype(BF16)
    gk[...] = gkv_in[0].T
    gv[...] = gkv_in[1].T
    go[...] = go_in[...]
    gl[...] = gl_in[...]


def place(steps, y, gx, gwq_t, gkv_t, gwo, gln):
    n_tok, e = y.shape
    d = gwo.shape[0]
    act = pl.BlockSpec((n_tok // steps, e), lambda i: (i, 0))
    cols = pl.BlockSpec((d, e // steps), lambda i: (0, i))
    turned = pl.BlockSpec((e // steps, d), lambda i: (i, 0))
    small = pl.BlockSpec((d // steps, e), lambda i: (i, 0))
    line = pl.BlockSpec((1, e), lambda i: (0, 0))
    return pl.pallas_call(
        place_body,
        grid=(steps,),
        in_specs=[act, act, cols, pl.BlockSpec((2, d, e // steps), lambda i: (0, 0, i)), small, line],
        out_specs=[act, act, turned, turned, turned, small, line],
        out_shape=[jax.ShapeDtypeStruct(y.shape, BF16), jax.ShapeDtypeStruct(y.shape, BF16), jax.ShapeDtypeStruct((e, d), BF16),
                   jax.ShapeDtypeStruct((e, d), F32), jax.ShapeDtypeStruct((e, d), F32), jax.ShapeDtypeStruct((d, e), BF16),
                   jax.ShapeDtypeStruct((1, e), F32)],
        compiler_params=pltpu.CompilerParams(dimension_semantics=("arbitrary",)),
        cost_estimate=pl.CostEstimate(flops=0, bytes_accessed=8 * y.size + 24 * gwo.size, transcendentals=0),
        name="place",
    )(y, gx, gwq_t, gkv_t, gwo, gln)


def solution(mesh):
    act_spec = P('dp', 'tp', None)

    def device_step(x_loc, ln_scale, wq_loc, w_k, w_v, wo_loc, dy_loc):
        n_batch, tok, model_dim = x_loc.shape
        d = w_k.shape[1]
        t0 = lax.axis_index('tp') * tok
        cos_t, sin_t = rope_tables(t0 + jnp.arange(tok), d)

        gain = ln_scale.reshape(1, model_dim)
        kv0, hn, q, do, kv_loc, wq_h, wo_h, hn_p, dy_p = project(x_loc, gain, wq_loc, w_k, w_v, wo_loc, dy_loc, cos_t, sin_t)
        o, dq, dkv_loc, o_p, dq_p = attention(q, do, kv_loc, kv0, cos_t, sin_t)
        return gradients(o, o_p, dq, dq_p, hn, hn_p, dy_loc, dy_p, dkv_loc, wq_h, wo_h, w_k, w_v, x_loc, gain, cos_t, sin_t)

    return jax.shard_map(device_step, mesh=mesh, in_specs=(act_spec, P(None), P(None, 'tp'), P(None, None), P(None, None), P('tp', None), act_spec), out_specs=(act_spec, act_spec, P('dp'), P('dp', 'tp'), P('dp', None), P('dp', None), P(('dp', 'tp'), None)), check_vma=False)
```

```python
import functools
import jax
import jax.numpy as jnp
from jax import lax
from jax.experimental import pallas as pl
from jax.experimental.pallas import tpu as pltpu
from jax.sharding import PartitionSpec as P

LN_EPS = 1e-6
ROPE_BASE = 10000.0
LOG2E = 1.4426950408889634
F32 = jnp.float32
BF16 = jnp.bfloat16


def rope_tables(positions, head_dim):
    half_dim = head_dim // 2
    inv_freq = ROPE_BASE ** (-2.0 * jnp.arange(half_dim, dtype=F32) / head_dim)
    angles = positions.astype(F32)[:, None] * inv_freq[None, :]
    return jnp.cos(angles), jnp.sin(angles)


def rotate(vectors, cos_t, sin_t):
    half_dim = vectors.shape[-1] // 2
    lo_half = vectors[..., :half_dim]
    hi_half = vectors[..., half_dim:]
    return jnp.concatenate([lo_half * cos_t - hi_half * sin_t, hi_half * cos_t + lo_half * sin_t], axis=-1)


def dot_nn(a, b):
    return lax.dot_general(a, b, (((1,), (0,)), ((), ())), preferred_element_type=F32)


def dot_nt(a, b):
    return lax.dot_general(a, b, (((1,), (1,)), ((), ())), preferred_element_type=F32)


def rdma(src, dst, send, recv, to):
    return pltpu.make_async_remote_copy(src_ref=src, dst_ref=dst, send_sem=send, recv_sem=recv,
                                        device_id={'tp': to}, device_id_type=pl.DeviceIdType.MESH)


def ring_ids():
    me = lax.axis_index('tp')
    k = lax.rem(me, 2)
    return me, k, me + 1 - 2 * k, lax.rem(me + 2, 8), lax.rem(me + 6, 8)


def enter(peers):
    barrier = pltpu.get_barrier_semaphore()
    for p in peers:
        pl.semaphore_signal(barrier, inc=1, device_id={'tp': p}, device_id_type=pl.DeviceIdType.MESH)
    pl.semaphore_wait(barrier, len(peers))


class Products:
    def __init__(self, big, a_v, at, ld_sem, b_sem):
        self.big, self.a_v, self.at, self.ld_sem, self.b_sem = big, a_v, at, ld_sem, b_sem
        self.nb, self.tok = a_v.shape[2], a_v.shape[3]
        self.eq = big.shape[2] // 4

    def load_b(self, own, other):
        return (pltpu.make_async_copy(own, self.big.at[0], self.b_sem.at[0]),
                pltpu.make_async_copy(other, self.big.at[1], self.b_sem.at[1]))

    def load_a(self, i, own, other):
        return (pltpu.make_async_copy(own, self.a_v.at[i % 2, 0], self.ld_sem.at[i % 2, 0]),
                pltpu.make_async_copy(other, self.a_v.at[i % 2, 1], self.ld_sem.at[i % 2, 1]))

    def turn(self, j, src):
        tok = self.tok
        for i in range(self.nb // 2):
            self.at[j, :, 2 * i * tok:(2 * i + 2) * tok] = jnp.concatenate([src[2 * i], src[2 * i + 1]], axis=0).T

    def both(self, cols):
        return dot_nn(self.at[0], self.big[0, :, cols]) + dot_nn(self.at[1], self.big[1, :, cols])

    def columns(self, dst, first, last, turned=0):
        eq = self.eq

        @pl.loop(first, last)
        def _(n):
            m = lax.rem(n + turned, 4)
            cols = pl.ds(pl.multiple_of(m * eq, 128), eq)
            dst[m // 2, :, pl.ds(pl.multiple_of(lax.rem(m, 2) * eq, 128), eq)] = self.both(cols)


class Gather:
    def __init__(self, ids, c, block, send, recv):
        self.me, _, self.mate, self.cw, self.ccw = ids
        self.c, self.block, self.send, self.recv = c, block, send, recv

    def copy(self, j, tag, to, src=None):
        ref = self.block(j)
        return rdma(ref if src is None else src, ref, self.send(tag), self.recv(tag), to)

    def own(self, src):
        @pl.when(self.c <= 2)
        def _():
            self.copy(self.me, 0, self.cw, src).start()

        @pl.when(self.c == 0)
        def _():
            self.copy(self.me, 2, self.ccw, src).start()
        self.copy(self.me, 3, self.mate, src).start()

    def arrived(self):
        @pl.when(self.c >= 1)
        def _():
            self.copy(self.me - 2, 0, self.cw).wait_recv()

        @pl.when(self.c == 3)
        def _():
            self.copy(self.me - 6, 2, self.ccw).wait_recv()

    def pass_on(self, src=lambda j: None):
        @pl.when(self.c >= 1)
        def _():
            @pl.when(self.c <= 2)
            def _():
                self.copy(self.me - 2, 1, self.cw, src(self.me - 2)).start()
            self.copy(self.me - 2, 4, self.mate, src(self.me - 2)).start()

        @pl.when(self.c == 3)
        def _():
            self.copy(self.me - 6, 6, self.mate, src(self.me - 6)).start()

    def forward(self):
        self.arrived()
        self.pass_on()

    def last(self):
        @pl.when(self.c >= 2)
        def _():
            self.copy(self.me - 4, 1, self.cw).wait_recv()
            self.copy(self.me - 4, 5, self.mate).start()

    def ready(self, tags=(3, 4, 5, 6)):
        if 3 in tags:
            self.copy(self.mate, 3, self.mate).wait_recv()
        for n, tag in ((1, 4), (2, 5), (3, 6)):
            if tag not in tags:
                continue

            @pl.when(self.c >= n)
            def _():
                self.copy(self.mate - 2 * n, tag, self.mate).wait_recv()

    def drain(self, tags=range(7)):
        c = self.c
        conds = (c <= 2, (c >= 1) & (c <= 2), c == 0, c >= 0, c >= 1, c >= 2, c == 3)
        for tag in tags:
            @pl.when(conds[tag])
            def _():
                self.copy(self.me, tag, self.mate).wait_send()


def attn_body(nb, tok, seq, d, q_hbm, do_hbm, kvl_hbm, kv0_hbm, dy_hbm, dyp_hbm, cos_ref, sin_ref,
              o_hbm, dq_hbm, dkv_hbm, op_hbm, dqp_hbm, acc_hbm, rb_hbm,
              kv_all, o_v, dq_v, mrecv, rrecv,
              kv_send, kv_recv, m_send, m_recv, r_send, r_recv, own_sem, in_sem, out_sem, fin_sem, p_send, p_recv, first_sem,
              h_send, h_recv, ld_sem, b_sem, acc_sem):
    scale = d ** -0.5
    rows = o_v.shape[2] * tok
    n_blk = seq // 256
    rb = 2 * rows // n_blk
    n_rb = rows // rb
    half = d // 2
    me, k, mate, cw, ccw = ring_ids()
    c = me // 2
    rel = [lax.rem(c + o, 4) for o in (3, 1, 2, 0)]

    def blk(j):
        return pl.ds(pl.multiple_of(j * tok, 16), tok)

    def kvb(b, j):
        return kv_all.at[b, blk(j)]

    def gather(b):
        return Gather((me, k, mate, cw, ccw), c, lambda j: kvb(b, j), lambda t: kv_send.at[b - 1, t], lambda t: kv_recv.at[b - 1, t])

    def own(b):
        gather(b).own(kvl_hbm.at[b])

    def own_copy(b):
        return pltpu.make_async_copy(kvl_hbm.at[b], kvb(b, me), own_sem.at[b])

    def ready(b):
        own_copy(b).wait()

        @pl.when(b == 1)
        def _():
            gather(1).ready((4, 5, 6))

        @pl.when(b > 1)
        def _():
            gather(b).ready()

    def drain(b):
        @pl.when(b == 1)
        def _():
            gather(1).drain((1, 4, 5, 6))

        @pl.when(b > 1)
        def _():
            gather(b).drain()

    def m_copy(b, n):
        return rdma(kvb(b, 2 * n + 1 - k), mrecv.at[b, n], m_send.at[b, n], m_recv.at[b, n], mate)

    def r_copy(b, n, slot, to):
        return rdma(kvb(b, 2 * n + k), rrecv.at[b, slot], r_send.at[b, slot], r_recv.at[b, slot], to)

    def add_into(b, n, other):
        v = kv_all[b, blk(2 * n + k), :].astype(F32) + other[...].astype(F32)
        kv_all[b, blk(2 * n + k), :] = v.astype(BF16)

    def fin_copy(b):
        return pltpu.make_async_copy(kvb(b, me), dkv_hbm.at[b], fin_sem.at[b])

    def to_mate(b):
        for n in range(4):
            @pl.when(c >= n)
            def _():
                m_copy(b, n).start()

    def stage1(b):
        for n in range(4):
            @pl.when(c >= n)
            def _():
                m_copy(b, n).wait()
                add_into(b, n, mrecv.at[b, n])

        @pl.when(c == 3)
        def _():
            r_copy(b, 1, 2, ccw).start()
            r_copy(b, 2, 1, ccw).start()
            r_copy(b, 0, 0, cw).start()
            fin_copy(b).start()

        @pl.when(c == 2)
        def _():
            r_copy(b, 0, 1, ccw).start()

    def stage2(b):
        @pl.when(c == 2)
        def _():
            r_copy(b, 1, 2, ccw).wait_recv()
            add_into(b, 1, rrecv.at[b, 2])
            r_copy(b, 1, 2, ccw).start()
            r_copy(b, 2, 1, ccw).wait_recv()
            add_into(b, 2, rrecv.at[b, 1])
            fin_copy(b).start()

        @pl.when(c == 1)
        def _():
            r_copy(b, 0, 1, ccw).wait_recv()
            add_into(b, 0, rrecv.at[b, 1])
            r_copy(b, 0, 1, ccw).start()

    def stage3(b):
        @pl.when(c == 0)
        def _():
            r_copy(b, 0, 0, cw).wait_recv()
            add_into(b, 0, rrecv.at[b, 0])
            r_copy(b, 0, 1, ccw).wait_recv()
            add_into(b, 0, rrecv.at[b, 1])
            fin_copy(b).start()

        @pl.when(c == 1)
        def _():
            r_copy(b, 1, 2, ccw).wait_recv()
            add_into(b, 1, rrecv.at[b, 2])
            fin_copy(b).start()

    def handed(dst, src, n, b, slot):
        return rdma(src.at[slot, 1 - k], dst.at[b], p_send.at[n, b], p_recv.at[n, b], mate)

    def store_o(b, slot):
        return (pltpu.make_async_copy(o_v.at[slot], o_hbm.at[b], out_sem.at[0, slot]), handed(op_hbm, o_v, 0, b, slot))

    def store_dq(b, slot):
        return (pltpu.make_async_copy(dq_v.at[slot], dq_hbm.at[b], out_sem.at[1, slot]), handed(dqp_hbm, dq_v, 1, b, slot))

    def stored(x):
        x[0].wait()
        x[1].wait_send()

    def attend(q_v, do_v, s_buf, m_buf, l_buf, p_buf, ds_buf, q_t, do_t, dk_t, dv_t, d_buf, cos4, sin4):
        def load(b, slot):
            return (pltpu.make_async_copy(q_hbm.at[b], q_v.at[slot], in_sem.at[0, slot]),
                    pltpu.make_async_copy(do_hbm.at[b], do_v.at[slot], in_sem.at[1, slot]))

        def scores(b, g, slot, i):
            cols = slice(i * 256, (i + 1) * 256)
            s = dot_nt(q_v[slot, g].reshape(rows, d), kv_all[b, cols, :d])
            col = lax.broadcasted_iota(jnp.int32, (tok, 256), 1) + i * 256
            row = lax.broadcasted_iota(jnp.int32, (tok, 256), 0) + me * tok
            s = jnp.concatenate([jnp.where(col <= row, s[j * tok:(j + 1) * tok], -1e30) for j in range(rows // tok)], axis=0)
            s_buf[g, :, cols] = s
            m = jnp.maximum(s[:, :128], s[:, 128:])
            m_buf[...] = m if i == 0 else jnp.maximum(m_buf[...], m)

        def softmax(g, i):
            n = rows // n_blk
            for r in range(i * n, (i + 1) * n, 16):
                rs = slice(r, r + 16)
                m = jnp.max(m_buf[rs, :], axis=1, keepdims=True) * (scale * LOG2E)
                l = None
                for j in range(0, seq, 128):
                    e = jnp.exp2(s_buf[g, rs, j:j + 128] * (scale * LOG2E) - m)
                    s_buf[g, rs, j:j + 128] = e
                    l = e if l is None else l + e
                l_buf[g, rs, :] = jnp.broadcast_to(1.0 / jnp.sum(l, axis=1, keepdims=True), (16, 128))

        def turn(g, slot, i):
            rs = slice(i * rb, (i + 1) * rb)
            q_t[g, :, rs] = q_v[slot, g].reshape(rows, d)[rs].T
            do_t[g, :, rs] = do_v[slot, g].reshape(rows, d)[rs].T

        def out_rows(b, g, slot, i):
            rs = slice(i * rb, (i + 1) * rb)
            p = (s_buf[g, rs, :] * jnp.concatenate([l_buf[g, rs, :]] * (seq // 128), axis=1)).astype(BF16)
            p_buf[rs, :] = p
            o = dot_nn(p, kv_all[b, :, d:])
            dvec = jnp.sum(o * do_v[slot, g].reshape(rows, d)[rs].astype(F32), axis=1, keepdims=True)
            d_buf[rs, :] = jnp.broadcast_to(dvec, (rb, 128))
            put_rows(o_v, slot, g, i, o.astype(BF16))

        def put_rows(ref, slot, g, i, v):
            r = i * rb
            while r < (i + 1) * rb:
                n = min((i + 1) * rb - r, tok - r % tok)
                ref[slot, g, r // tok, r % tok:r % tok + n, :] = v[r - i * rb:r - i * rb + n]
                r += n

        def dq_rows(b, g, slot, i):
            rs = slice(i * rb, (i + 1) * rb)
            dq = dot_nn(ds_buf[rs, :], kv_all[b, :, :d]) * scale
            lo, hi = dq[:, :half], dq[:, half:]
            cs, sn = cos4[rs, :], sin4[rs, :]
            put_rows(dq_v, slot, g, i, jnp.concatenate([(lo * cs + hi * sn).astype(BF16), (hi * cs - lo * sn).astype(BF16)], axis=1))

        def grads(b, g, slot, i):
            cols = slice(i * 256, (i + 1) * 256)
            do = do_v[slot, g].reshape(rows, d)
            p = p_buf[:, cols]
            dp = dot_nt(do, kv_all[b, cols, d:])
            dvec = d_buf[...]
            if i > 0:
                n = rows // n_blk
                z = l_buf[1 - g, (i - 1) * n:(i - 1) * n + 8, :]
                for r in range(8, n, 8):
                    z = jnp.minimum(z, l_buf[1 - g, (i - 1) * n + r:(i - 1) * n + r + 8, :])
                dvec = dvec + jnp.concatenate([jnp.minimum(z, 0.0)] * (rows // 8), axis=0)
            dd = jnp.concatenate([dvec, dvec], axis=1)
            ds = (p.astype(F32) * (dp - dd)).astype(BF16)
            ds_buf[:, cols] = ds
            dk = dot_nn(q_t[g], ds)
            dv = dot_nn(do_t[g], p)
            if g == 0:
                dk_t[:, cols] = dk
                dv_t[:, cols] = dv
            else:
                dk_t[:, cols] += dk
                dv_t[:, cols] += dv

        def close_kv(b, i):
            cols = slice(i * 256, (i + 1) * 256)
            kv_all[b, cols, :d] = (dk_t[:, cols] * scale).T.astype(BF16)
            kv_all[b, cols, d:] = dv_t[:, cols].T.astype(BF16)

        enter((mate, cw, ccw))
        gather(1).pass_on(lambda j: kv0_hbm.at[1, blk(j)])
        if nb > 2:
            own(2)
        for x in load(0, 0):
            x.start()

        def first(j):
            return pltpu.make_async_copy(kv0_hbm.at[0, blk(j)], kvb(0, j), first_sem.at[j])

        def second(j, n):
            return pltpu.make_async_copy(kv0_hbm.at[1, blk(j)], kvb(1, j), first_sem.at[8 + n])
        arrived = ((c >= 0, mate, 0), (c >= 1, me - 2, 1), (c == 3, me - 6, 2))
        for j in range(8):
            @pl.when(j <= 2 * c + 1)
            def _():
                first(j).start()
        for b in range(1, nb):
            own_copy(b).start()
        for cond, j, i in arrived:
            @pl.when(cond)
            def _():
                second(j, i).start()

        @pl.loop(2 * c + 2, 8)
        def _(j):
            for b in range(nb):
                kv_all[b, blk(j), :] = jnp.zeros((tok, 2 * d), BF16)
        for j in range(rows // tok):
            cos4[j * tok:(j + 1) * tok, :] = cos_ref[...]
            sin4[j * tok:(j + 1) * tok, :] = sin_ref[...]
        ds_buf[...] = jnp.zeros_like(ds_buf)
        for x in load(0, 0):
            x.wait()
        for i in range(n_rb):
            turn(0, 0, i)
        for j in range(8):
            @pl.when(j <= 2 * c + 1)
            def _():
                first(j).wait()
        for cond, j, i in arrived:
            @pl.when(cond)
            def _():
                second(j, i).wait()
        for i in range(n_blk):
            scores(0, 0, 0, i)
        for i in range(n_blk):
            softmax(0, i)

        def comm_steps(b, steps):
            for lag, stage in steps:
                @pl.when(b >= lag)
                def _():
                    stage(b - lag)

        @pl.loop(0, nb)
        def _(b):
            slot = lax.rem(b, 2)
            nxt = jnp.minimum(b + 1, nb - 1)
            prev = jnp.maximum(b - 1, 0)

            @pl.when(b + 1 < nb)
            def _():
                for x in load(b + 1, 1 - slot):
                    x.start()

            @pl.when(b + 3 < nb)
            def _():
                own(b + 3)

            @pl.when((b >= 1) & (b + 2 < nb))
            def _():
                gather(b + 2).forward()

            @pl.when((b >= 1) & (b + 1 < nb))
            def _():
                gather(b + 1).last()
            comm_steps(b, ((2, stage1),))

            @pl.when(b >= 2)
            def _():
                drain(b - 1)

            @pl.when(b >= 2)
            def _():
                stored(store_o(b - 2, slot))
            spare = jnp.where(b >= 1, b - 1, nb)
            for i in range(n_blk):
                scores(b, 1, slot, i)
                if i % 2 == 1:
                    out_rows(b, 0, slot, i // 2)
                    dq_rows(prev, 1, 1 - slot, i // 2)
                    turn(1, slot, i // 2)
            for i in range(n_blk):
                close_kv(spare, i)

            @pl.when(b >= 1)
            def _():
                for x in store_dq(b - 1, 1 - slot):
                    x.start()
                to_mate(b - 1)

            @pl.when(b == 0)
            def _():
                gather(1).last()
            for i in range(n_blk):
                grads(b, 0, slot, i)
                softmax(1, i)

            @pl.when(b + 1 < nb)
            def _():
                for x in load(b + 1, 1 - slot):
                    x.wait()
                ready(b + 1)
            if nb > 2:
                @pl.when(b == 0)
                def _():
                    gather(2).forward()
            comm_steps(b, ((3, stage2), (4, stage3)))

            @pl.when(b >= 2)
            def _():
                stored(store_dq(b - 2, slot))
            nslot = lax.rem(nxt, 2)
            for i in range(n_blk):
                scores(nxt, 0, nslot, i)
                if i % 2 == 1:
                    out_rows(b, 1, slot, i // 2)
                    dq_rows(b, 0, slot, i // 2)
                    turn(0, nslot, i // 2)
            for x in store_o(b, slot):
                x.start()
            for i in range(n_blk):
                grads(b, 1, slot, i)
                softmax(0, i)

        drain(nb - 1)
        for i in range(n_rb):
            dq_rows(nb - 1, 1, (nb - 1) % 2, i)
        for i in range(n_blk):
            close_kv(nb - 1, i)
        for x in store_dq(nb - 1, (nb - 1) % 2):
            x.start()
        to_mate(nb - 1)

    slab = pltpu.VMEM((2, 2, rows // tok, tok, d), BF16)
    pl.run_scoped(attend, slab, slab, pltpu.VMEM((2, rows, seq), F32), pltpu.VMEM((rows, 128), F32), pltpu.VMEM((2, rows, 128), F32),
                  pltpu.VMEM((rows, seq), BF16), pltpu.VMEM((rows, seq), BF16), pltpu.VMEM((2, d, rows), BF16),
                  pltpu.VMEM((2, d, rows), BF16), pltpu.VMEM((d, seq), F32), pltpu.VMEM((d, seq), F32),
                  pltpu.VMEM((rows, 128), F32), pltpu.VMEM((rows, half), F32), pltpu.VMEM((rows, half), F32))
    n = nb

    def first_products(big, a_v, at, acc_v):
        pr = Products(big, a_v, at, ld_sem, b_sem)
        for x in pr.load_b(dy_hbm, dyp_hbm):
            x.start()
        for b in (n - 2, n - 1):
            stored(store_o(b, b % 2))
        for b in range(n):
            handed(op_hbm, o_v, 0, b, b % 2).wait_recv()

        def fetch(r):
            return pr.load_a(r, o_hbm.at[:, k, rel[r]], op_hbm.at[:, rel[r]])

        def hop0(dr):
            return rdma(acc_v.at[dr, dr], rb_hbm.at[dr], h_send.at[dr], h_recv.at[dr], (cw, ccw)[dr])

        def save(r):
            return pltpu.make_async_copy(acc_v.at[r], acc_hbm.at[r], acc_sem.at[r])
        for r in range(2):
            for x in fetch(r):
                x.start()

        def steps(b):
            for lag, stage in ((2, stage1), (3, stage2), (4, stage3)):
                if 0 <= b - lag < n:
                    stage(b - lag)
        steps(n)
        for r in range(4):
            for x in fetch(r):
                x.wait()
            pr.turn(0, a_v.at[r % 2, 0])
            pr.turn(1, a_v.at[r % 2, 1])
            if r + 2 < 4:
                for x in fetch(r + 2):
                    x.start()
            if r == 0:
                for x in pr.load_b(dy_hbm, dyp_hbm):
                    x.wait()
            if r < 2:
                pr.columns(acc_v.at[r], 0, 2, 2 * r)
                hop0(r).start()
                pr.columns(acc_v.at[r], 2, 4, 2 * r)
            else:
                pr.columns(acc_v.at[r], 0, 4)
            save(r).start()
            if r < 3:
                steps(n + 1 + r)
        for r in range(4):
            save(r).wait()
        for dr in range(2):
            hop0(dr).wait()

    pl.run_scoped(first_products, pltpu.VMEM((2,) + dy_hbm.shape, BF16), pltpu.VMEM((2, 2, nb, tok, d), BF16),
                  pltpu.VMEM((2, d, nb * tok), BF16), pltpu.VMEM((4, 2, d, dy_hbm.shape[1] // 2), F32))
    for b in (n - 2, n - 1):
        stored(store_dq(b, b % 2))
    for b in range(n):
        handed(dqp_hbm, dq_v, 1, b, b % 2).wait_recv()
        fin_copy(b).wait()
        for cond, slot in ((c == 3, 0), (c >= 1, 1), (c >= 2, 2)):
            @pl.when(cond)
            def _():
                r_copy(b, 0, slot, cw).wait_send()


def attention(q, do, kv, kv0, dy, dy_p, cos_t, sin_t):
    nb, _, hp, tok, d = q.shape
    seq = tok * 8
    rows = hp * tok
    any_spec = pl.BlockSpec(memory_space=pl.ANY)
    vmem = pl.BlockSpec(memory_space=pltpu.VMEM)
    dma = pltpu.SemaphoreType.DMA
    slab = pltpu.VMEM((2, 2, hp, tok, d), BF16)
    out = jax.ShapeDtypeStruct(q.shape, BF16)
    outp = jax.ShapeDtypeStruct((nb, hp, tok, d), BF16)
    return pl.pallas_call(
        functools.partial(attn_body, nb, tok, seq, d),
        in_specs=[any_spec] * 6 + [vmem, vmem],
        out_specs=[any_spec] * 7,
        out_shape=[out, out, jax.ShapeDtypeStruct(kv.shape, BF16), outp, outp,
                   jax.ShapeDtypeStruct((4, 2, d, dy.shape[1] // 2), F32), jax.ShapeDtypeStruct((2, d, dy.shape[1] // 2), F32)],
        scratch_shapes=[pltpu.VMEM((nb + 1, seq, 2 * d), BF16), slab, slab,
                        pltpu.VMEM((nb, 4, tok, 2 * d), BF16), pltpu.VMEM((nb, 3, tok, 2 * d), BF16),
                        dma((nb - 1, 7)), dma((nb - 1, 7)), dma((nb, 4)), dma((nb, 4)), dma((nb, 3)), dma((nb, 3)),
                        dma((nb,)), dma((2, 2)), dma((2, 2)), dma((nb,)), dma((2, nb)), dma((2, nb)), dma((11,)),
                        dma((2,)), dma((2,)), dma((2, 2)), dma((2,)), dma((4,))],
        compiler_params=pltpu.CompilerParams(collective_id=1, has_side_effects=True, vmem_limit_bytes=63 * 2**20),
        cost_estimate=pl.CostEstimate(flops=24 * nb * rows * seq * d, bytes_accessed=40 * 2**20,
                                      transcendentals=2 * nb * rows * seq),
        name="attention",
    )(q, do, kv, kv0, dy, dy_p, cos_t, sin_t)


def proj_body(nb, tok, x_hbm, g_ref, wq_hbm, wk_ref, wv_ref, wo_hbm, dy_hbm, cos_ref, sin_ref,
              kv0_hbm, hn_hbm, q_hbm, do_hbm, kv_hbm, wqf_hbm, wof_hbm, hnp_hbm, dyp_hbm,
              x_v, hn_v, dy_v, wq_v, wo_v, kv_v, out_v,
              send, recv, x_sem, dy_sem, own_sem, out_sem, misc_sem, w_sem, p_send, p_recv, kv_send, kv_recv):
    n_tok, e = x_hbm.shape
    d = kv_v.shape[1] // 2
    half = d // 2
    mc = 2 * tok
    me, k, mate, cw, ccw = ring_ids()
    base = 2 * (me // 2)

    def head(off, par):
        return lax.rem(base + 2 * off + 8, 8) + par
    enter((mate, cw, ccw))

    fulls = (wq_v, wo_v)
    locs = (wq_hbm, wo_hbm)

    def half_of(w, ref, j):
        n = ref.shape[0] // 2
        return ref.at[pl.ds(j * n, n)]

    sends = []

    def send_full(w, h, j, to, own=False):
        src = locs[w] if own else fulls[w].at[h]
        c = rdma(src, fulls[w].at[h], send.at[w, j], recv.at[w, j], to)
        c.start()
        sends.append(c)

    def send_half(w, h, part, j, to):
        c = rdma(half_of(w, fulls[w].at[h], part), half_of(w, fulls[w].at[h], part), send.at[w, j], recv.at[w, j], to)
        c.start()
        sends.append(c)

    def wait_full(w, h, j):
        rdma(fulls[w].at[h], fulls[w].at[h], send.at[w, j], recv.at[w, j], mate).wait_recv()

    def wait_half(w, h, part, j):
        ref = half_of(w, fulls[w].at[h], part)
        rdma(ref, ref, send.at[w, j], recv.at[w, j], mate).wait_recv()

    for w in range(2):
        send_full(w, me, 0, cw, True)
        send_full(w, me, 1, ccw, True)
        send_full(w, me, 4, mate, True)
    own = [pltpu.make_async_copy(locs[w], fulls[w].at[me], own_sem.at[w]) for w in range(2)]
    xs = [pltpu.make_async_copy(x_hbm.at[pl.ds(b * tok, tok)], x_v.at[pl.ds(b * tok, tok)], x_sem.at[b]) for b in range(nb)]
    for c in xs:
        c.start()
    for c in own:
        c.start()
    dyc = pltpu.make_async_copy(dy_hbm, dy_v, dy_sem)
    dyc.start()

    gain = g_ref[...].astype(F32)
    for b in range(nb):
        xs[b].wait()

        @pl.loop(0, tok // 16, unroll=2)
        def _(r):
            rs = pl.ds(pl.multiple_of(b * tok + r * 16, 16), 16)
            x = x_v[rs, :].astype(F32)
            c = x - jnp.mean(x, axis=1, keepdims=True)
            inv = lax.rsqrt(jnp.mean(c * c, axis=1, keepdims=True) + LN_EPS)
            hn_v[rs, :] = (c * inv * gain).astype(BF16)
    hn_out = pltpu.make_async_copy(hn_v, hn_hbm, misc_sem.at[0])
    hn_out.start()
    to_mate = [rdma(hn_v, hnp_hbm, p_send.at[0], p_recv.at[0], mate), rdma(dy_hbm, dyp_hbm, p_send.at[1], p_recv.at[1], mate)]
    for c in to_mate:
        c.start()

    def rope_rows(raw):
        lo, hi = raw[:, :half], raw[:, half:d]
        cs, sn = jnp.concatenate([cos_ref[...]] * 2, axis=0), jnp.concatenate([sin_ref[...]] * 2, axis=0)
        return lo * cs - hi * sn, hi * cs + lo * sn

    @pl.loop(0, n_tok // mc)
    def _(i):
        rs = pl.ds(pl.multiple_of(i * mc, mc), mc)
        lo, hi = rope_rows(dot_nn(hn_v[rs, :], wk_ref[...]))
        kv_v[rs, :half] = lo.astype(BF16)
        kv_v[rs, half:d] = hi.astype(BF16)
        kv_v[rs, d:] = dot_nn(hn_v[rs, :], wv_ref[...]).astype(BF16)
    kv_out = pltpu.make_async_copy(kv_v, kv_hbm, misc_sem.at[1])
    kv_out.start()

    outs = []
    saves = []

    def save(w, h):
        c = pltpu.make_async_copy(fulls[w].at[h], (wqf_hbm, wof_hbm)[w].at[h], w_sem.at[len(saves)])
        c.start()
        saves.append(c)

    def project(w, h):
        slot = len(outs) % 4
        if len(outs) >= 4:
            outs[-4].wait()

        @pl.loop(0, n_tok // mc)
        def _(i):
            rs = pl.ds(pl.multiple_of(i * mc, mc), mc)
            if w == 0:
                lo, hi = rope_rows(dot_nn(hn_v[rs, :], wq_v[h]))
                o0 = lo.reshape(2, tok, half).astype(BF16)
                o1 = hi.reshape(2, tok, half).astype(BF16)
                out_v[slot, pl.ds(2 * i, 2), :, :half] = o0
                out_v[slot, pl.ds(2 * i, 2), :, half:] = o1
            else:
                out_v[slot, pl.ds(2 * i, 2)] = dot_nt(dy_v[rs, :], wo_v[h]).reshape(2, tok, d).astype(BF16)
        c = pltpu.make_async_copy(out_v.at[slot], (q_hbm, do_hbm)[w].at[:, lax.rem(h, 2), h // 2], out_sem.at[slot])
        c.start()
        outs.append(c)
        save(w, h)

    other = 1 - k
    for w in range(2):
        own[w].wait()
        if w == 1:
            dyc.wait()
        project(w, me)
        wait_full(w, mate, 4)
        project(w, mate)
    for w in range(2):
        wait_full(w, head(-1, k), 0)
        send_half(w, head(-1, k), 0, 2, cw)
        wait_full(w, head(1, k), 1)
        send_half(w, head(1, k), 1, 3, ccw)
        send_full(w, head(-1, k), 5, mate)
        send_full(w, head(1, k), 6, mate)
        project(w, head(-1, k))
        project(w, head(1, k))
        wait_full(w, head(-1, other), 5)
        project(w, head(-1, other))
        wait_full(w, head(1, other), 6)
        project(w, head(1, other))

    def early(n):
        def blk(j):
            return kv0_hbm.at[n, pl.ds(pl.multiple_of(j * tok, 16), tok)]
        return Gather((me, k, mate, cw, ccw), me // 2, blk, lambda t: kv_send.at[n, t], lambda t: kv_recv.at[n, t])
    first, second = early(0), early(1)
    first.own(kv_v.at[pl.ds(0, tok)])
    own0 = pltpu.make_async_copy(kv_v.at[pl.ds(0, tok)], first.block(me), misc_sem.at[2])
    own0.start()
    for w in range(2):
        wait_half(w, head(2, k), 0, 2)
        send_half(w, head(2, k), 0, 7, mate)
        wait_half(w, head(2, k), 1, 3)
        send_half(w, head(2, k), 1, 8, mate)
        project(w, head(2, k))
        if w == 1:
            first.forward()
            second.own(kv_v.at[pl.ds(tok, tok)])
        wait_half(w, head(2, other), 0, 7)
        wait_half(w, head(2, other), 1, 8)
        project(w, head(2, other))
    first.last()
    for c in outs[-4:] + saves + [hn_out, kv_out, own0]:
        c.wait()
    first.ready()
    first.drain()
    second.arrived()
    second.ready((3,))
    second.drain((0, 2, 3))
    for c in sends:
        c.wait_send()
    for c in to_mate:
        c.wait()


def project(x, gain, wq, w_k, w_v, wo, dy, cos_t, sin_t):
    nb, tok, e = x.shape
    d = wq.shape[1]
    n_heads = 8
    n_tok = nb * tok
    any_spec = pl.BlockSpec(memory_space=pl.ANY)
    vmem = pl.BlockSpec(memory_space=pltpu.VMEM)
    act = jax.ShapeDtypeStruct((nb, 2, n_heads // 2, tok, d), BF16)
    dma = pltpu.SemaphoreType.DMA
    flops = 2 * n_tok * e * (2 * n_heads + 2) * d
    kv0, hn, q, do, kv, wqf, wof, hn_p, dy_p = pl.pallas_call(
        functools.partial(proj_body, nb, tok),
        in_specs=[any_spec, vmem, any_spec, vmem, vmem, any_spec, any_spec, vmem, vmem],
        out_specs=[any_spec] * 9,
        out_shape=[jax.ShapeDtypeStruct((2, tok * n_heads, 2 * d), BF16), jax.ShapeDtypeStruct((n_tok, e), BF16), act, act, jax.ShapeDtypeStruct((n_tok, 2 * d), BF16),
                   jax.ShapeDtypeStruct((n_heads, e, d), BF16), jax.ShapeDtypeStruct((n_heads, d, e), BF16),
                   jax.ShapeDtypeStruct((n_tok, e), BF16), jax.ShapeDtypeStruct((n_tok, e), BF16)],
        scratch_shapes=[pltpu.VMEM((n_tok, e), BF16), pltpu.VMEM((n_tok, e), BF16), pltpu.VMEM((n_tok, e), BF16),
                        pltpu.VMEM((n_heads, e, d), BF16), pltpu.VMEM((n_heads, d, e), BF16),
                        pltpu.VMEM((n_tok, 2 * d), BF16), pltpu.VMEM((4, nb, tok, d), BF16),
                        dma((2, 9)), dma((2, 9)), dma((nb,)), dma(()), dma((2,)), dma((4,)), dma((3,)), dma((16,)), dma((2,)), dma((2,)), dma((2, 7)), dma((2, 7))],
        compiler_params=pltpu.CompilerParams(collective_id=0, has_side_effects=True, vmem_limit_bytes=60 * 2**20),
        cost_estimate=pl.CostEstimate(flops=flops, bytes_accessed=60 * 2**20, transcendentals=0),
        name="project",
    )(x.reshape(n_tok, e), gain, wq, w_k, w_v, wo, dy.reshape(n_tok, e), cos_t, sin_t)
    return kv0, hn, q, do, kv.reshape(nb, tok, 2 * d), wqf, wof, hn_p, dy_p


def grads_body(nb, tok, o_hbm, acc_hbm, rb_hbm, dq_hbm, dqp_hbm, hn_hbm, hnp_hbm, dy_hbm, dkv_hbm,
               wq_hbm, wo_hbm, wk_hbm, wv_hbm, x_hbm, g_ref, cos_ref, sin_ref,
               y_hbm, gx_hbm, gln_ref, gwo_ref, gwq_ref, gkv_hbm,
               acc, acc_kv, rbuf, rbuf_kv, kind, kp, dkv_v, fin_kv, gln_acc, gl_recv,
               rs_send, rs_recv, kv_send, kv_recv, ag_send, ag_recv, gl_send, gl_rsem, kp_sem, ld_sem, b_sem, t_sem, a_sem):
    n_tok, e = x_hbm.shape
    d = wk_hbm.shape[1]
    half = d // 2
    eh, eq = e // 2, e // 4
    me, k, mate, cw, ccw = ring_ids()
    c = me // 2
    rel = [lax.rem(c + o, 4) for o in (3, 1, 2, 0)]
    enter([lax.rem(me + o, 8) for o in range(1, 8)])

    order = ((2, 1), (2, 0))

    def hop(s, dr, j):
        src = acc.at[s, dr, dr] if j == 0 else rbuf.at[s, dr, j - 1]
        return rdma(src, rbuf.at[s, dr, j], rs_send.at[s, dr, j], rs_recv.at[s, dr, j], (cw, ccw)[dr])

    def hop_kv(dr, j):
        src = acc_kv.at[dr, dr] if j == 0 else rbuf_kv.at[dr, j - 1]
        return rdma(src, rbuf_kv.at[dr, j], kv_send.at[dr, j], kv_recv.at[dr, j], (cw, ccw)[dr])

    def add(dst, term):
        @pl.loop(0, dst.shape[0] // 32)
        def _(i):
            rs = pl.ds(pl.multiple_of(i * 32, 32), 32)
            dst[rs, :] = dst[rs, :] + term[rs, :]

    def pass_on(s, j):
        for dr in range(2):
            if (s, j) != (0, 1):
                hop(s, dr, j - 1).wait_recv()
            add(rbuf.at[s, dr, j - 1], acc.at[s, order[dr][j - 1], dr])
            hop(s, dr, j).start()

    def pass_on_kv(j):
        for dr in range(2):
            hop_kv(dr, j - 1).wait_recv()
            add(rbuf_kv.at[dr, j - 1], acc_kv.at[order[dr][j - 1], dr])
            hop_kv(dr, j).start()

    def finish(s, out):
        for dr in range(2):
            hop(s, dr, 2).wait_recv()

            @pl.loop(0, d // 32)
            def _(i):
                rs = pl.ds(pl.multiple_of(i * 32, 32), 32)
                out[rs, dr * eh:(dr + 1) * eh] = (rbuf[s, dr, 2, rs, :] + acc[s, 3, dr, rs, :]).astype(BF16)

    def piece(kk, j, lo=0, n=None):
        return gkv_hbm.at[kk, pl.ds(lo, d if n is None else n), pl.ds(pl.multiple_of(j * eq, 128), eq)]

    def ag(tag, ref, to, src=None):
        return rdma(ref if src is None else src, ref, ag_send.at[tag], ag_recv.at[tag], to)

    def ag_far(tag, to):
        return ag(tag, piece(k, rel[(0, 1)[tag - 3]], (tag - 3) * half, half), to)

    own_piece = pltpu.make_async_copy(fin_kv, piece(k, c), t_sem.at[5])

    def finish_kv():
        for dr in range(2):
            hop_kv(dr, 2).wait_recv()
            fin_kv[:, dr * (eq // 2):(dr + 1) * (eq // 2)] = rbuf_kv[dr, 2] + acc_kv[3, dr]
        ag(0, piece(k, c), cw, fin_kv).start()
        ag(1, piece(k, c), ccw, fin_kv).start()
        ag(2, piece(k, c), mate, fin_kv).start()
        own_piece.start()

    def ag_forward():
        ag(0, piece(k, rel[0]), cw).wait_recv()
        ag_far(3, cw).start()
        ag(1, piece(k, rel[1]), cw).wait_recv()
        ag_far(4, ccw).start()
        ag(5, piece(k, rel[0]), mate).start()
        ag(6, piece(k, rel[1]), mate).start()

    def ag_last():
        far = [piece(k, rel[2], i * half, half) for i in range(2)]
        for i in range(2):
            ag(3 + i, far[i], cw).wait_recv()
            ag(7 + i, far[i], mate).start()
        ag(2, piece(1 - k, c), mate).wait_recv()
        ag(5, piece(1 - k, rel[0]), mate).wait_recv()
        ag(6, piece(1 - k, rel[1]), mate).wait_recv()
        for i in range(2):
            ag(7 + i, piece(1 - k, rel[2], i * half, half), mate).wait_recv()
        for tag in range(3):
            ag(tag, piece(k, c), cw, fin_kv).wait_send()
        for tag in (3, 4, 7, 8):
            ag(tag, far[0], cw).wait_send()
        for tag in (5, 6):
            ag(tag, piece(k, c), cw).wait_send()
        own_piece.wait()

    dkv_in = pltpu.make_async_copy(dkv_hbm, dkv_v, t_sem.at[4])
    dkv_in.start()
    kp_copy = rdma(kind.at[1 - k], kp, kp_sem.at[0], kp_sem.at[1], mate)

    rb_in = pltpu.make_async_copy(rb_hbm, rbuf.at[0, :, 0], t_sem.at[2])
    rb_in.start()
    acc_in = [pltpu.make_async_copy(acc_hbm.at[r], acc.at[0, r], a_sem.at[r]) for r in range(4)]
    for r in (2, 1, 0, 3):
        acc_in[r].start()

    def products(big, a_v, at):
        pr = Products(big, a_v, at, ld_sem, b_sem)
        hn_in = pr.load_b(hn_hbm, hnp_hbm)

        def fetch(r):
            return pr.load_a(r, dq_hbm.at[:, k, rel[r]], dqp_hbm.at[:, rel[r]])
        dkv_in.wait()
        for b in range(nb):
            lo, hi = dkv_v[b, :, :half].astype(F32), dkv_v[b, :, half:d].astype(F32)
            cs, sn = cos_ref[...], sin_ref[...]
            kind[0, b, :, :half] = (lo * cs + hi * sn).astype(BF16)
            kind[0, b, :, half:] = (hi * cs - lo * sn).astype(BF16)
            kind[1, b] = dkv_v[b, :, d:]
        kp_copy.start()
        for x in hn_in:
            x.start()
        for r in range(2):
            for x in fetch(r):
                x.start()
        rb_in.wait()
        acc_in[2].wait()
        pass_on(0, 1)
        pr.turn(0, kind.at[k])
        for x in hn_in:
            x.wait()
        kp_copy.wait_recv()
        pr.turn(1, kp)
        for r in range(4):
            for dr in range(2):
                acc_kv[r, dr] = pr.both(pl.ds(pl.multiple_of(rel[r] * eq + dr * (eq // 2), 128), eq // 2))
        for dr in range(2):
            hop_kv(dr, 0).start()
        for r in range(4):
            for x in fetch(r):
                x.wait()
            pr.turn(0, a_v.at[r % 2, 0])
            pr.turn(1, a_v.at[r % 2, 1])
            if r + 2 < 4:
                for x in fetch(r + 2):
                    x.start()
            if r < 2:
                pr.columns(acc.at[1, r], 0, 2, 2 * r)
                hop(1, r, 0).start()
                pr.columns(acc.at[1, r], 2, 4, 2 * r)
            else:
                pr.columns(acc.at[1, r], 0, 4)

    pl.run_scoped(products, pltpu.VMEM((2, n_tok, e), BF16), pltpu.VMEM((2, 2, nb, tok, d), BF16), pltpu.VMEM((2, d, n_tok), BF16))
    for r in (0, 1, 3):
        acc_in[r].wait()
    pass_on(0, 2)
    pass_on_kv(1)

    mc = 2 * tok
    units = nb // 2

    def attn_out(wo_v, o_v, x_v, y_v):
        w_in = pltpu.make_async_copy(wo_hbm, wo_v, b_sem.at[0])
        w_in.start()

        def load(u):
            return (pltpu.make_async_copy(o_hbm.at[pl.ds(2 * u, 2)], o_v.at[u % 2], ld_sem.at[u % 2, 0]),
                    pltpu.make_async_copy(x_hbm.at[pl.ds(u * mc, mc)], x_v.at[u % 2], ld_sem.at[u % 2, 1]))

        def put(u):
            return pltpu.make_async_copy(y_v.at[u % 2], y_hbm.at[pl.ds(u * mc, mc)], t_sem.at[u % 2])
        for x in load(0):
            x.start()
        w_in.wait()
        for u in range(units):
            if u + 1 < units:
                for x in load(u + 1):
                    x.start()
            for x in load(u):
                x.wait()
            if u >= 2:
                put(u - 2).wait()
            sl = u % 2

            @pl.loop(0, 4)
            def _(n):
                cols = pl.ds(pl.multiple_of(n * eq, 128), eq)
                o_rows = jnp.concatenate([jnp.concatenate([o_v[sl, i, h % 2, h // 2] for h in range(8)], axis=1) for i in range(2)], axis=0)
                r = dot_nn(o_rows, wo_v[:, cols])
                y_v[sl, :, cols] = (x_v[sl, :, cols].astype(F32) + r).astype(BF16)
            put(u).start()
        for u in range(max(0, units - 2), units):
            put(u).wait()

    pl.run_scoped(attn_out, pltpu.VMEM((8 * d, e), BF16), pltpu.VMEM((2, 2, 2, 4, tok, d), BF16),
                  pltpu.VMEM((2, mc, e), BF16), pltpu.VMEM((2, mc, e), BF16))
    pass_on(1, 1)

    def hidden_grad(wq_v, wk_v, wv_v, dq_v, x_v, dy_v, dh, gx_v):
        w_in = pltpu.make_async_copy(wq_hbm, wq_v, b_sem.at[0])
        w_in.start()
        w2_in = (pltpu.make_async_copy(wk_hbm, wk_v, b_sem.at[1]), pltpu.make_async_copy(wv_hbm, wv_v, ld_sem.at[1, 1]))
        for x in w2_in:
            x.start()

        def load(u):
            return (pltpu.make_async_copy(dq_hbm.at[pl.ds(2 * u, 2)], dq_v, ld_sem.at[0, 0]),
                    pltpu.make_async_copy(x_hbm.at[pl.ds(u * mc, mc)], x_v, ld_sem.at[0, 1]),
                    pltpu.make_async_copy(dy_hbm.at[pl.ds(u * mc, mc)], dy_v, ld_sem.at[1, 0]))

        def put(u):
            return pltpu.make_async_copy(gx_v, gx_hbm.at[pl.ds(u * mc, mc)], t_sem.at[0])
        gain = g_ref[...].astype(F32)
        gln_acc[...] = jnp.zeros_like(gln_acc)
        for x in load(0):
            x.start()
        w_in.wait()
        for x in w2_in:
            x.wait()
        for u in range(units):
            for x in load(u):
                x.wait()

            @pl.loop(0, 4)
            def _(n):
                rows = pl.ds(pl.multiple_of(n * eq, 128), eq)
                t = None
                for h in range(8):
                    a = jnp.concatenate([dq_v[i, h % 2, h // 2] for i in range(2)], axis=0)
                    p = dot_nt(a, wq_v[h, rows, :])
                    t = p if t is None else t + p
                for j in range(2):
                    a = jnp.concatenate([kind[j, 2 * u + i] for i in range(2)], axis=0)
                    t = t + dot_nt(a, (wk_v, wv_v)[j][rows, :])
                dh[:, rows] = t
            if u >= 1:
                put(u - 1).wait()

            @pl.loop(0, mc // 16)
            def _(r):
                rs = pl.ds(pl.multiple_of(r * 16, 16), 16)
                x = x_v[rs, :].astype(F32)
                cx = x - jnp.mean(x, axis=1, keepdims=True)
                inv = lax.rsqrt(jnp.mean(cx * cx, axis=1, keepdims=True) + LN_EPS)
                xh = cx * inv
                g = dh[rs, :]
                pr = g * xh
                gln_acc[...] += pr[:8] + pr[8:]
                gh = g * gain
                m1 = jnp.mean(gh, axis=1, keepdims=True)
                m2 = jnp.mean(gh * xh, axis=1, keepdims=True)
                gx_v[rs, :] = (inv * (gh - m1 - xh * m2) + dy_v[rs, :].astype(F32)).astype(BF16)
            put(u).start()
            if u + 1 < units:
                for x in load(u + 1):
                    x.start()
            if u == units // 2 - 1:
                finish(0, gwo_ref)
                pass_on_kv(2)
        put(units - 1).wait()

    pl.run_scoped(hidden_grad, pltpu.VMEM((8, e, d), BF16), pltpu.VMEM((e, d), BF16), pltpu.VMEM((e, d), BF16), pltpu.VMEM((2, 2, 4, tok, d), BF16),
                  pltpu.VMEM((mc, e), BF16), pltpu.VMEM((mc, e), BF16), pltpu.VMEM((mc, e), F32), pltpu.VMEM((mc, e), BF16))
    gl_recv[me] = jnp.sum(gln_acc[...], axis=0, keepdims=True)
    pass_on(1, 2)
    finish_kv()
    gl = [rdma(gl_recv.at[me], gl_recv.at[me], gl_send.at[o - 1], gl_rsem.at[o - 1], lax.rem(me + o, 8)) for o in range(1, 8)]
    for x in gl:
        x.start()
    finish(1, gwq_ref)
    ag_forward()
    for o in range(1, 8):
        src = lax.rem(me + 8 - o, 8)
        rdma(gl_recv.at[src], gl_recv.at[src], gl_send.at[o - 1], gl_rsem.at[o - 1], mate).wait_recv()
    total = gl_recv[0]
    for i in range(1, 8):
        total = total + gl_recv[i]
    gln_ref[...] = total
    ag_last()
    for x in gl:
        x.wait_send()
    kp_copy.wait_send()
    for dr in range(2):
        for j in range(3):
            hop_kv(dr, j).wait_send()
            for s in range(2):
                if (s, j) != (0, 0):
                    hop(s, dr, j).wait_send()


def gradients(o, acc, rb, dq, dq_p, hn, hn_p, dy, dkv, wqf, wof, w_k, w_v, x, gain, cos_t, sin_t):
    nb, tok, e = x.shape
    n_tok = nb * tok
    d = dq.shape[-1]
    any_spec = pl.BlockSpec(memory_space=pl.ANY)
    vmem = pl.BlockSpec(memory_space=pltpu.VMEM)
    dma = pltpu.SemaphoreType.DMA
    tokens = jax.ShapeDtypeStruct((n_tok, e), BF16)
    y, gx, gln, gwo, gwq_t, gkv_t = pl.pallas_call(
        functools.partial(grads_body, nb, tok),
        in_specs=[any_spec] * 14 + [vmem, vmem, vmem],
        out_specs=[any_spec, any_spec, vmem, vmem, vmem, any_spec],
        out_shape=[tokens, tokens, jax.ShapeDtypeStruct((1, e), F32), jax.ShapeDtypeStruct((d, e), BF16),
                   jax.ShapeDtypeStruct((d, e), BF16), jax.ShapeDtypeStruct((2, d, e), F32)],
        scratch_shapes=[pltpu.VMEM((2, 4, 2, d, e // 2), F32), pltpu.VMEM((4, 2, d, e // 8), F32),
                        pltpu.VMEM((2, 2, 3, d, e // 2), F32), pltpu.VMEM((2, 3, d, e // 8), F32),
                        pltpu.VMEM((2, nb, tok, d), BF16), pltpu.VMEM((nb, tok, d), BF16), pltpu.VMEM((nb, tok, 2 * d), BF16),
                        pltpu.VMEM((d, e // 4), F32), pltpu.VMEM((8, e), F32), pltpu.VMEM((8, 1, e), F32),
                        dma((2, 2, 3)), dma((2, 2, 3)), dma((2, 3)), dma((2, 3)), dma((9,)), dma((9,)), dma((7,)), dma((7,)),
                        dma((2,)), dma((2, 2)), dma((2,)), dma((6,)), dma((4,))],
        compiler_params=pltpu.CompilerParams(collective_id=2, has_side_effects=True, vmem_limit_bytes=63 * 2**20),
        cost_estimate=pl.CostEstimate(flops=10 * n_tok * e * e, bytes_accessed=120 * 2**20, transcendentals=0),
        name="gradients",
    )(o, acc, rb, dq, dq_p, hn, hn_p, dy.reshape(n_tok, e), dkv, wqf, wof.reshape(8 * d, e), w_k, w_v, x.reshape(n_tok, e),
      gain, cos_t, sin_t)
    y, gx, gwq, gwk, gwv, gwo, gln = place(nb, y, gx, gwq_t, gkv_t, gwo, gln)
    return y.reshape(nb, tok, e), gx.reshape(nb, tok, e), gln.reshape(e), gwq, gwk, gwv, gwo


def place_body(y_in, gx_in, gq_in, gkv_in, go_in, gl_in, y, gx, gq, gk, gv, go, gl):
    y[...] = y_in[...]
    gx[...] = gx_in[...]
    gq[...] = gq_in[...].astype(F32).T.astype(BF16)
    gk[...] = gkv_in[0].T
    gv[...] = gkv_in[1].T
    go[...] = go_in[...]
    gl[...] = gl_in[...]


def place(steps, y, gx, gwq_t, gkv_t, gwo, gln):
    n_tok, e = y.shape
    d = gwo.shape[0]
    act = pl.BlockSpec((n_tok // steps, e), lambda i: (i, 0))
    cols = pl.BlockSpec((d, e // steps), lambda i: (0, i))
    turned = pl.BlockSpec((e // steps, d), lambda i: (i, 0))
    small = pl.BlockSpec((d // steps, e), lambda i: (i, 0))
    line = pl.BlockSpec((1, e), lambda i: (0, 0))
    return pl.pallas_call(
        place_body,
        grid=(steps,),
        in_specs=[act, act, cols, pl.BlockSpec((2, d, e // steps), lambda i: (0, 0, i)), small, line],
        out_specs=[act, act, turned, turned, turned, small, line],
        out_shape=[jax.ShapeDtypeStruct(y.shape, BF16), jax.ShapeDtypeStruct(y.shape, BF16), jax.ShapeDtypeStruct((e, d), BF16),
                   jax.ShapeDtypeStruct((e, d), F32), jax.ShapeDtypeStruct((e, d), F32), jax.ShapeDtypeStruct((d, e), BF16),
                   jax.ShapeDtypeStruct((1, e), F32)],
        compiler_params=pltpu.CompilerParams(dimension_semantics=("arbitrary",)),
        cost_estimate=pl.CostEstimate(flops=0, bytes_accessed=8 * y.size + 24 * gwo.size, transcendentals=0),
        name="place",
    )(y, gx, gwq_t, gkv_t, gwo, gln)


def solution(mesh):
    act_spec = P('dp', 'tp', None)

    def device_step(x_loc, ln_scale, wq_loc, w_k, w_v, wo_loc, dy_loc):
        n_batch, tok, model_dim = x_loc.shape
        d = w_k.shape[1]
        t0 = lax.axis_index('tp') * tok
        cos_t, sin_t = rope_tables(t0 + jnp.arange(tok), d)

        gain = ln_scale.reshape(1, model_dim)
        kv0, hn, q, do, kv_loc, wq_h, wo_h, hn_p, dy_p = project(x_loc, gain, wq_loc, w_k, w_v, wo_loc, dy_loc, cos_t, sin_t)
        o, dq, dkv_loc, o_p, dq_p, acc, rb = attention(q, do, kv_loc, kv0, dy_loc.reshape(-1, model_dim), dy_p, cos_t, sin_t)
        return gradients(o, acc, rb, dq, dq_p, hn, hn_p, dy_loc, dkv_loc, wq_h, wo_h, w_k, w_v, x_loc, gain, cos_t, sin_t)

    return jax.shard_map(device_step, mesh=mesh, in_specs=(act_spec, P(None), P(None, 'tp'), P(None, None), P(None, None), P('tp', None), act_spec), out_specs=(act_spec, act_spec, P('dp'), P('dp', 'tp'), P('dp', None), P('dp', None), P(('dp', 'tp'), None)), check_vma=False)
```

```python
import functools
import jax
import jax.numpy as jnp
from jax import lax
from jax.experimental import pallas as pl
from jax.experimental.pallas import tpu as pltpu
from jax.sharding import PartitionSpec as P

LN_EPS = 1e-6
ROPE_BASE = 10000.0
LOG2E = 1.4426950408889634
F32 = jnp.float32
BF16 = jnp.bfloat16


def rope_tables(positions, head_dim):
    half_dim = head_dim // 2
    inv_freq = ROPE_BASE ** (-2.0 * jnp.arange(half_dim, dtype=F32) / head_dim)
    angles = positions.astype(F32)[:, None] * inv_freq[None, :]
    return jnp.cos(angles), jnp.sin(angles)


def rotate(vectors, cos_t, sin_t):
    half_dim = vectors.shape[-1] // 2
    lo_half = vectors[..., :half_dim]
    hi_half = vectors[..., half_dim:]
    return jnp.concatenate([lo_half * cos_t - hi_half * sin_t, hi_half * cos_t + lo_half * sin_t], axis=-1)


def dot_nn(a, b):
    return lax.dot_general(a, b, (((1,), (0,)), ((), ())), preferred_element_type=F32)


def dot_nt(a, b):
    return lax.dot_general(a, b, (((1,), (1,)), ((), ())), preferred_element_type=F32)


def rdma(src, dst, send, recv, to):
    return pltpu.make_async_remote_copy(src_ref=src, dst_ref=dst, send_sem=send, recv_sem=recv,
                                        device_id={'tp': to}, device_id_type=pl.DeviceIdType.MESH)


def ring_ids():
    me = lax.axis_index('tp')
    k = lax.rem(me, 2)
    return me, k, me + 1 - 2 * k, lax.rem(me + 2, 8), lax.rem(me + 6, 8)


def enter(peers):
    barrier = pltpu.get_barrier_semaphore()
    for p in peers:
        pl.semaphore_signal(barrier, inc=1, device_id={'tp': p}, device_id_type=pl.DeviceIdType.MESH)
    pl.semaphore_wait(barrier, len(peers))


class Products:
    def __init__(self, big, a_v, at, ld_sem, b_sem):
        self.big, self.a_v, self.at, self.ld_sem, self.b_sem = big, a_v, at, ld_sem, b_sem
        self.nb, self.tok = a_v.shape[2], a_v.shape[3]
        self.eq = big.shape[2] // 4

    def load_b(self, own, other):
        return (pltpu.make_async_copy(own, self.big.at[0], self.b_sem.at[0]),
                pltpu.make_async_copy(other, self.big.at[1], self.b_sem.at[1]))

    def load_a(self, i, own, other):
        return (pltpu.make_async_copy(own, self.a_v.at[i % 2, 0], self.ld_sem.at[i % 2, 0]),
                pltpu.make_async_copy(other, self.a_v.at[i % 2, 1], self.ld_sem.at[i % 2, 1]))

    def turn(self, j, src):
        tok = self.tok
        for i in range(self.nb // 2):
            self.at[j, :, 2 * i * tok:(2 * i + 2) * tok] = jnp.concatenate([src[2 * i], src[2 * i + 1]], axis=0).T

    def both(self, cols):
        return dot_nn(self.at[0], self.big[0, :, cols]) + dot_nn(self.at[1], self.big[1, :, cols])

    def columns(self, dst, first, last, turned=0):
        eq = self.eq

        @pl.loop(first, last)
        def _(n):
            m = lax.rem(n + turned, 4)
            cols = pl.ds(pl.multiple_of(m * eq, 128), eq)
            dst[m // 2, :, pl.ds(pl.multiple_of(lax.rem(m, 2) * eq, 128), eq)] = self.both(cols)


class Gather:
    def __init__(self, ids, c, block, send, recv):
        self.me, _, self.mate, self.cw, self.ccw = ids
        self.c, self.block, self.send, self.recv = c, block, send, recv

    def copy(self, j, tag, to, src=None):
        ref = self.block(j)
        return rdma(ref if src is None else src, ref, self.send(tag), self.recv(tag), to)

    def own(self, src):
        @pl.when(self.c <= 2)
        def _():
            self.copy(self.me, 0, self.cw, src).start()

        @pl.when(self.c == 0)
        def _():
            self.copy(self.me, 2, self.ccw, src).start()
        self.copy(self.me, 3, self.mate, src).start()

    def arrived(self):
        @pl.when(self.c >= 1)
        def _():
            self.copy(self.me - 2, 0, self.cw).wait_recv()

        @pl.when(self.c == 3)
        def _():
            self.copy(self.me - 6, 2, self.ccw).wait_recv()

    def pass_on(self, src=lambda j: None):
        @pl.when(self.c >= 1)
        def _():
            @pl.when(self.c <= 2)
            def _():
                self.copy(self.me - 2, 1, self.cw, src(self.me - 2)).start()
            self.copy(self.me - 2, 4, self.mate, src(self.me - 2)).start()

        @pl.when(self.c == 3)
        def _():
            self.copy(self.me - 6, 6, self.mate, src(self.me - 6)).start()

    def forward(self):
        self.arrived()
        self.pass_on()

    def last(self):
        @pl.when(self.c >= 2)
        def _():
            self.copy(self.me - 4, 1, self.cw).wait_recv()
            self.copy(self.me - 4, 5, self.mate).start()

    def ready(self, tags=(3, 4, 5, 6)):
        if 3 in tags:
            self.copy(self.mate, 3, self.mate).wait_recv()
        for n, tag in ((1, 4), (2, 5), (3, 6)):
            if tag not in tags:
                continue

            @pl.when(self.c >= n)
            def _():
                self.copy(self.mate - 2 * n, tag, self.mate).wait_recv()

    def drain(self, tags=range(7)):
        c = self.c
        conds = (c <= 2, (c >= 1) & (c <= 2), c == 0, c >= 0, c >= 1, c >= 2, c == 3)
        for tag in tags:
            @pl.when(conds[tag])
            def _():
                self.copy(self.me, tag, self.mate).wait_send()


def attn_body(nb, tok, seq, d, q_hbm, do_hbm, kvl_hbm, kv0_hbm, dy_hbm, dyp_hbm, cos_ref, sin_ref,
              o_hbm, dq_hbm, dkv_hbm, op_hbm, dqp_hbm, acc_hbm,
              kv_all, o_v, dq_v, mrecv, rrecv,
              kv_send, kv_recv, m_send, m_recv, r_send, r_recv, own_sem, in_sem, out_sem, fin_sem, p_send, p_recv, first_sem,
              ld_sem, b_sem, acc_sem):
    scale = d ** -0.5
    rows = o_v.shape[2] * tok
    n_blk = seq // 256
    rb = 2 * rows // n_blk
    n_rb = rows // rb
    half = d // 2
    me, k, mate, cw, ccw = ring_ids()
    c = me // 2
    rel = [lax.rem(c + o, 4) for o in (3, 1, 2, 0)]

    def blk(j):
        return pl.ds(pl.multiple_of(j * tok, 16), tok)

    def kvb(b, j):
        return kv_all.at[b, blk(j)]

    def gather(b):
        return Gather((me, k, mate, cw, ccw), c, lambda j: kvb(b, j), lambda t: kv_send.at[b - 1, t], lambda t: kv_recv.at[b - 1, t])

    def own(b):
        gather(b).own(kvl_hbm.at[b])

    def own_copy(b):
        return pltpu.make_async_copy(kvl_hbm.at[b], kvb(b, me), own_sem.at[b])

    def ready(b):
        own_copy(b).wait()

        @pl.when(b == 1)
        def _():
            gather(1).ready((4, 5, 6))

        @pl.when(b > 1)
        def _():
            gather(b).ready()

    def drain(b):
        @pl.when(b == 1)
        def _():
            gather(1).drain((1, 4, 5, 6))

        @pl.when(b > 1)
        def _():
            gather(b).drain()

    def m_copy(b, n):
        return rdma(kvb(b, 2 * n + 1 - k), mrecv.at[b, n], m_send.at[b, n], m_recv.at[b, n], mate)

    def r_copy(b, n, slot, to):
        return rdma(kvb(b, 2 * n + k), rrecv.at[b, slot], r_send.at[b, slot], r_recv.at[b, slot], to)

    def add_into(b, n, other):
        v = kv_all[b, blk(2 * n + k), :].astype(F32) + other[...].astype(F32)
        kv_all[b, blk(2 * n + k), :] = v.astype(BF16)

    def fin_copy(b):
        return pltpu.make_async_copy(kvb(b, me), dkv_hbm.at[b], fin_sem.at[b])

    def to_mate(b):
        for n in range(4):
            @pl.when(c >= n)
            def _():
                m_copy(b, n).start()

    def stage1(b):
        for n in range(4):
            @pl.when(c >= n)
            def _():
                m_copy(b, n).wait()
                add_into(b, n, mrecv.at[b, n])

        @pl.when(c == 3)
        def _():
            r_copy(b, 1, 2, ccw).start()
            r_copy(b, 2, 1, ccw).start()
            r_copy(b, 0, 0, cw).start()
            fin_copy(b).start()

        @pl.when(c == 2)
        def _():
            r_copy(b, 0, 1, ccw).start()

    def stage2(b):
        @pl.when(c == 2)
        def _():
            r_copy(b, 1, 2, ccw).wait_recv()
            add_into(b, 1, rrecv.at[b, 2])
            r_copy(b, 1, 2, ccw).start()
            r_copy(b, 2, 1, ccw).wait_recv()
            add_into(b, 2, rrecv.at[b, 1])
            fin_copy(b).start()

        @pl.when(c == 1)
        def _():
            r_copy(b, 0, 1, ccw).wait_recv()
            add_into(b, 0, rrecv.at[b, 1])
            r_copy(b, 0, 1, ccw).start()

    def stage3(b):
        @pl.when(c == 0)
        def _():
            r_copy(b, 0, 0, cw).wait_recv()
            add_into(b, 0, rrecv.at[b, 0])
            r_copy(b, 0, 1, ccw).wait_recv()
            add_into(b, 0, rrecv.at[b, 1])
            fin_copy(b).start()

        @pl.when(c == 1)
        def _():
            r_copy(b, 1, 2, ccw).wait_recv()
            add_into(b, 1, rrecv.at[b, 2])
            fin_copy(b).start()

    def handed(dst, src, n, b, slot):
        return rdma(src.at[slot, 1 - k], dst.at[b], p_send.at[n, b], p_recv.at[n, b], mate)

    def store_o(b, slot):
        return (pltpu.make_async_copy(o_v.at[slot], o_hbm.at[b], out_sem.at[0, slot]), handed(op_hbm, o_v, 0, b, slot))

    def store_dq(b, slot):
        return (pltpu.make_async_copy(dq_v.at[slot], dq_hbm.at[b], out_sem.at[1, slot]), handed(dqp_hbm, dq_v, 1, b, slot))

    def stored(x):
        x[0].wait()
        x[1].wait_send()

    def attend(q_v, do_v, s_buf, m_buf, l_buf, p_buf, ds_buf, q_t, do_t, dk_t, dv_t, d_buf, cos4, sin4):
        def load(b, slot):
            return (pltpu.make_async_copy(q_hbm.at[b], q_v.at[slot], in_sem.at[0, slot]),
                    pltpu.make_async_copy(do_hbm.at[b], do_v.at[slot], in_sem.at[1, slot]))

        def scores(b, g, slot, i):
            w = min(512, seq)
            if (i * 256) % w:
                return
            cols = slice(i * 256, i * 256 + w)
            s = dot_nt(q_v[slot, g].reshape(rows, d), kv_all[b, cols, :d]) * (scale * LOG2E)
            col = lax.broadcasted_iota(jnp.int32, (tok, w), 1) + i * 256
            row = lax.broadcasted_iota(jnp.int32, (tok, w), 0) + me * tok
            s = jnp.concatenate([jnp.where(col <= row, s[j * tok:(j + 1) * tok], -1e30) for j in range(rows // tok)], axis=0)
            s_buf[g, :, cols] = s
            m = s[:, :128]
            for j in range(128, w, 128):
                m = jnp.maximum(m, s[:, j:j + 128])
            m_buf[...] = m if i == 0 else jnp.maximum(m_buf[...], m)

        parts = max(1, min(5, n_blk))
        part = [j * (rows // 16) // parts * 16 for j in range(parts + 1)] + [rows] * n_blk

        def softmax(g, i):
            for r in range(part[i], part[i + 1], 16):
                rs = slice(r, r + 16)
                m = jnp.max(m_buf[rs, :], axis=1, keepdims=True)
                l = None
                for j in range(0, seq, 128):
                    e = jnp.exp2(s_buf[g, rs, j:j + 128] - m)
                    s_buf[g, rs, j:j + 128] = e
                    l = e if l is None else l + e
                l_buf[g, rs, :] = jnp.broadcast_to(1.0 / jnp.sum(l, axis=1, keepdims=True), (16, 128))

        def turn(g, slot, i):
            rs = slice(i * rb, (i + 1) * rb)
            q_t[g, :, rs] = q_v[slot, g].reshape(rows, d)[rs].T
            do_t[g, :, rs] = do_v[slot, g].reshape(rows, d)[rs].T

        def out_rows(b, g, slot, i):
            rs = slice(i * rb, (i + 1) * rb)
            p = (s_buf[g, rs, :] * jnp.concatenate([l_buf[g, rs, :]] * (seq // 128), axis=1)).astype(BF16)
            p_buf[rs, :] = p
            o = dot_nn(p, kv_all[b, :, d:])
            dvec = jnp.sum(o * do_v[slot, g].reshape(rows, d)[rs].astype(F32), axis=1, keepdims=True)
            d_buf[rs, :] = jnp.broadcast_to(dvec, (rb, 128))
            put_rows(o_v, slot, g, i, o.astype(BF16))

        def put_rows(ref, slot, g, i, v):
            r = i * rb
            while r < (i + 1) * rb:
                n = min((i + 1) * rb - r, tok - r % tok)
                ref[slot, g, r // tok, r % tok:r % tok + n, :] = v[r - i * rb:r - i * rb + n]
                r += n

        def dq_rows(b, g, slot, i):
            rs = slice(i * rb, (i + 1) * rb)
            dq = dot_nn(ds_buf[rs, :], kv_all[b, :, :d]) * scale
            lo, hi = dq[:, :half], dq[:, half:]
            cs, sn = cos4[rs, :], sin4[rs, :]
            put_rows(dq_v, slot, g, i, jnp.concatenate([(lo * cs + hi * sn).astype(BF16), (hi * cs - lo * sn).astype(BF16)], axis=1))

        def grads(b, g, slot, i):
            cols = slice(i * 256, (i + 1) * 256)
            do = do_v[slot, g].reshape(rows, d)
            p = p_buf[:, cols]
            dp = dot_nt(do, kv_all[b, cols, d:])
            dvec = d_buf[...]
            if i > 0 and part[i] > part[i - 1]:
                z = None
                for r in range(part[i - 1], part[i], 8):
                    v = l_buf[1 - g, r:r + 8, :]
                    z = v if z is None else jnp.minimum(z, v)
                dvec = dvec + jnp.concatenate([jnp.minimum(z, 0.0)] * (rows // 8), axis=0)
            dd = jnp.concatenate([dvec, dvec], axis=1)
            ds = (p.astype(F32) * (dp - dd)).astype(BF16)
            ds_buf[:, cols] = ds
            dk = dot_nn(q_t[g], ds)
            dv = dot_nn(do_t[g], p)
            if g == 0:
                dk_t[:, cols] = dk
                dv_t[:, cols] = dv
            else:
                dk_t[:, cols] += dk
                dv_t[:, cols] += dv

        def close_kv(b, i):
            cols = slice(i * 256, (i + 1) * 256)
            kv_all[b, cols, :d] = (dk_t[:, cols] * scale).T.astype(BF16)
            kv_all[b, cols, d:] = dv_t[:, cols].T.astype(BF16)

        enter((mate, cw, ccw))
        gather(1).pass_on(lambda j: kv0_hbm.at[1, blk(j)])
        if nb > 2:
            own(2)
        for x in load(0, 0):
            x.start()

        def first(j):
            return pltpu.make_async_copy(kv0_hbm.at[0, blk(j)], kvb(0, j), first_sem.at[j])

        def second(j, n):
            return pltpu.make_async_copy(kv0_hbm.at[1, blk(j)], kvb(1, j), first_sem.at[8 + n])
        arrived = ((c >= 0, mate, 0), (c >= 1, me - 2, 1), (c == 3, me - 6, 2))
        for j in range(8):
            @pl.when(j <= 2 * c + 1)
            def _():
                first(j).start()
        for b in range(1, nb):
            own_copy(b).start()
        for cond, j, i in arrived:
            @pl.when(cond)
            def _():
                second(j, i).start()

        @pl.loop(2 * c + 2, 8)
        def _(j):
            for b in range(nb):
                kv_all[b, blk(j), :] = jnp.zeros((tok, 2 * d), BF16)
        for j in range(rows // tok):
            cos4[j * tok:(j + 1) * tok, :] = cos_ref[...]
            sin4[j * tok:(j + 1) * tok, :] = sin_ref[...]
        ds_buf[...] = jnp.zeros_like(ds_buf)
        for x in load(0, 0):
            x.wait()
        for i in range(n_rb):
            turn(0, 0, i)
        for j in range(8):
            @pl.when(j <= 2 * c + 1)
            def _():
                first(j).wait()
        for cond, j, i in arrived:
            @pl.when(cond)
            def _():
                second(j, i).wait()
        for i in range(n_blk):
            scores(0, 0, 0, i)
        for i in range(n_blk):
            softmax(0, i)

        def comm_steps(b, steps):
            for lag, stage in steps:
                @pl.when(b >= lag)
                def _():
                    stage(b - lag)

        @pl.loop(0, nb)
        def _(b):
            slot = lax.rem(b, 2)
            nxt = jnp.minimum(b + 1, nb - 1)
            prev = jnp.maximum(b - 1, 0)

            @pl.when(b + 1 < nb)
            def _():
                for x in load(b + 1, 1 - slot):
                    x.start()

            @pl.when(b + 3 < nb)
            def _():
                own(b + 3)

            @pl.when((b >= 1) & (b + 2 < nb))
            def _():
                gather(b + 2).forward()

            @pl.when((b >= 1) & (b + 1 < nb))
            def _():
                gather(b + 1).last()
            comm_steps(b, ((3, stage2), (4, stage3)))

            @pl.when(b >= 2)
            def _():
                drain(b - 1)

            @pl.when(b >= 2)
            def _():
                stored(store_o(b - 2, slot))
            spare = jnp.where(b >= 1, b - 1, nb)
            for i in range(n_blk):
                scores(b, 1, slot, i)
                if i % 2 == 1:
                    out_rows(b, 0, slot, i // 2)
                    dq_rows(prev, 1, 1 - slot, i // 2)
                    turn(1, slot, i // 2)
            for i in range(n_blk):
                close_kv(spare, i)

            @pl.when(b >= 1)
            def _():
                for x in store_dq(b - 1, 1 - slot):
                    x.start()
                to_mate(b - 1)

            @pl.when(b == 0)
            def _():
                gather(1).last()
            for i in range(n_blk):
                grads(b, 0, slot, i)
                softmax(1, i)

            @pl.when(b + 1 < nb)
            def _():
                for x in load(b + 1, 1 - slot):
                    x.wait()
                ready(b + 1)
            if nb > 2:
                @pl.when(b == 0)
                def _():
                    gather(2).forward()

            @pl.when(b >= 2)
            def _():
                stored(store_dq(b - 2, slot))
            nslot = lax.rem(nxt, 2)
            for i in range(n_blk):
                scores(nxt, 0, nslot, i)
                if i % 2 == 1:
                    out_rows(b, 1, slot, i // 2)
                    dq_rows(b, 0, slot, i // 2)
                    turn(0, nslot, i // 2)
            for x in store_o(b, slot):
                x.start()
            comm_steps(b, ((1, stage1),))
            for i in range(n_blk):
                grads(b, 1, slot, i)
                softmax(0, i)

        drain(nb - 1)
        for i in range(n_rb):
            dq_rows(nb - 1, 1, (nb - 1) % 2, i)
        for i in range(n_blk):
            close_kv(nb - 1, i)
        for x in store_dq(nb - 1, (nb - 1) % 2):
            x.start()
        to_mate(nb - 1)

    slab = pltpu.VMEM((2, 2, rows // tok, tok, d), BF16)
    pl.run_scoped(attend, slab, slab, pltpu.VMEM((2, rows, seq), F32), pltpu.VMEM((rows, 128), F32), pltpu.VMEM((2, rows, 128), F32),
                  pltpu.VMEM((rows, seq), BF16), pltpu.VMEM((rows, seq), BF16), pltpu.VMEM((2, d, rows), BF16),
                  pltpu.VMEM((2, d, rows), BF16), pltpu.VMEM((d, seq), F32), pltpu.VMEM((d, seq), F32),
                  pltpu.VMEM((rows, 128), F32), pltpu.VMEM((rows, half), F32), pltpu.VMEM((rows, half), F32))
    n = nb

    def first_products(big, a_v, at, acc_v):
        pr = Products(big, a_v, at, ld_sem, b_sem)
        for x in pr.load_b(dy_hbm, dyp_hbm):
            x.start()
        for b in (n - 2, n - 1):
            stored(store_o(b, b % 2))
        for b in range(n):
            handed(op_hbm, o_v, 0, b, b % 2).wait_recv()

        def fetch(r):
            return pr.load_a(r, o_hbm.at[:, k, rel[r]], op_hbm.at[:, rel[r]])

        def save(r):
            return pltpu.make_async_copy(acc_v.at[r], acc_hbm.at[r], acc_sem.at[r])
        for r in range(2):
            for x in fetch(r):
                x.start()

        todo = [((stage2, n - 3), (stage3, n - 4)), ((stage1, n - 1), (stage2, n - 2), (stage3, n - 3)),
                ((stage2, n - 1), (stage3, n - 2)), ((stage3, n - 1),)]

        def steps(i):
            for stage, b in todo[i]:
                if b >= 0:
                    stage(b)
        steps(0)
        for r in range(4):
            for x in fetch(r):
                x.wait()
            pr.turn(0, a_v.at[r % 2, 0])
            pr.turn(1, a_v.at[r % 2, 1])
            if r + 2 < 4:
                for x in fetch(r + 2):
                    x.start()
            if r == 0:
                for x in pr.load_b(dy_hbm, dyp_hbm):
                    x.wait()
            pr.columns(acc_v.at[r], 0, 4)
            save(r).start()
            if r < 3:
                steps(1 + r)
        for r in range(4):
            save(r).wait()

    pl.run_scoped(first_products, pltpu.VMEM((2,) + dy_hbm.shape, BF16), pltpu.VMEM((2, 2, nb, tok, d), BF16),
                  pltpu.VMEM((2, d, nb * tok), BF16), pltpu.VMEM((4, 2, d, dy_hbm.shape[1] // 2), F32))
    for b in (n - 2, n - 1):
        stored(store_dq(b, b % 2))
    for b in range(n):
        handed(dqp_hbm, dq_v, 1, b, b % 2).wait_recv()
        fin_copy(b).wait()
        for cond, slot in ((c == 3, 0), (c >= 1, 1), (c >= 2, 2)):
            @pl.when(cond)
            def _():
                r_copy(b, 0, slot, cw).wait_send()


def attention(q, do, kv, kv0, dy, dy_p, cos_t, sin_t):
    nb, _, hp, tok, d = q.shape
    seq = tok * 8
    rows = hp * tok
    any_spec = pl.BlockSpec(memory_space=pl.ANY)
    vmem = pl.BlockSpec(memory_space=pltpu.VMEM)
    dma = pltpu.SemaphoreType.DMA
    slab = pltpu.VMEM((2, 2, hp, tok, d), BF16)
    out = jax.ShapeDtypeStruct(q.shape, BF16)
    outp = jax.ShapeDtypeStruct((nb, hp, tok, d), BF16)
    return pl.pallas_call(
        functools.partial(attn_body, nb, tok, seq, d),
        in_specs=[any_spec] * 6 + [vmem, vmem],
        out_specs=[any_spec] * 6,
        out_shape=[out, out, jax.ShapeDtypeStruct(kv.shape, BF16), outp, outp,
                   jax.ShapeDtypeStruct((4, 2, d, dy.shape[1] // 2), F32)],
        scratch_shapes=[pltpu.VMEM((nb + 1, seq, 2 * d), BF16), slab, slab,
                        pltpu.VMEM((nb, 4, tok, 2 * d), BF16), pltpu.VMEM((nb, 3, tok, 2 * d), BF16),
                        dma((nb - 1, 7)), dma((nb - 1, 7)), dma((nb, 4)), dma((nb, 4)), dma((nb, 3)), dma((nb, 3)),
                        dma((nb,)), dma((2, 2)), dma((2, 2)), dma((nb,)), dma((2, nb)), dma((2, nb)), dma((11,)),
                        dma((2, 2)), dma((2,)), dma((4,))],
        compiler_params=pltpu.CompilerParams(collective_id=1, has_side_effects=True, vmem_limit_bytes=63 * 2**20),
        cost_estimate=pl.CostEstimate(flops=24 * nb * rows * seq * d, bytes_accessed=40 * 2**20,
                                      transcendentals=2 * nb * rows * seq),
        name="attention",
    )(q, do, kv, kv0, dy, dy_p, cos_t, sin_t)


def proj_body(nb, tok, x_hbm, g_ref, wq_hbm, wk_ref, wv_ref, wo_hbm, dy_hbm, cos_ref, sin_ref,
              kv0_hbm, hn_hbm, q_hbm, do_hbm, kv_hbm, wqf_hbm, wof_hbm, hnp_hbm, dyp_hbm,
              x_v, hn_v, dy_v, wq_v, wo_v, kv_v, out_v,
              send, recv, x_sem, dy_sem, own_sem, out_sem, misc_sem, w_sem, p_send, p_recv, kv_send, kv_recv):
    n_tok, e = x_hbm.shape
    d = kv_v.shape[1] // 2
    half = d // 2
    mc = 2 * tok
    me, k, mate, cw, ccw = ring_ids()
    base = 2 * (me // 2)

    def head(off, par):
        return lax.rem(base + 2 * off + 8, 8) + par
    enter((mate, cw, ccw))

    fulls = (wq_v, wo_v)
    locs = (wq_hbm, wo_hbm)

    def half_of(w, ref, j):
        n = ref.shape[0]
        cut = n // 2 if w == 0 else n // 4
        return ref.at[pl.ds(0, cut)] if j == 0 else ref.at[pl.ds(cut, n - cut)]

    sends = []

    def send_full(w, h, j, to, own=False):
        src = locs[w] if own else fulls[w].at[h]
        c = rdma(src, fulls[w].at[h], send.at[w, j], recv.at[w, j], to)
        c.start()
        sends.append(c)

    def send_half(w, h, part, j, to):
        c = rdma(half_of(w, fulls[w].at[h], part), half_of(w, fulls[w].at[h], part), send.at[w, j], recv.at[w, j], to)
        c.start()
        sends.append(c)

    def wait_full(w, h, j):
        rdma(fulls[w].at[h], fulls[w].at[h], send.at[w, j], recv.at[w, j], mate).wait_recv()

    def wait_half(w, h, part, j):
        ref = half_of(w, fulls[w].at[h], part)
        rdma(ref, ref, send.at[w, j], recv.at[w, j], mate).wait_recv()

    for w in range(2):
        send_full(w, me, 0, cw, True)
        send_full(w, me, 1, ccw, True)
        send_full(w, me, 4, mate, True)
    own = [pltpu.make_async_copy(locs[w], fulls[w].at[me], own_sem.at[w]) for w in range(2)]
    xs = [pltpu.make_async_copy(x_hbm.at[pl.ds(b * tok, tok)], x_v.at[pl.ds(b * tok, tok)], x_sem.at[b]) for b in range(nb)]
    for c in xs:
        c.start()
    for c in own:
        c.start()
    dyc = pltpu.make_async_copy(dy_hbm, dy_v, dy_sem)
    dyc.start()

    gain = g_ref[...].astype(F32)
    for b in range(nb):
        xs[b].wait()

        @pl.loop(0, tok // 16, unroll=2)
        def _(r):
            rs = pl.ds(pl.multiple_of(b * tok + r * 16, 16), 16)
            x = x_v[rs, :].astype(F32)
            c = x - jnp.mean(x, axis=1, keepdims=True)
            inv = lax.rsqrt(jnp.mean(c * c, axis=1, keepdims=True) + LN_EPS)
            hn_v[rs, :] = (c * inv * gain).astype(BF16)
    hn_out = pltpu.make_async_copy(hn_v, hn_hbm, misc_sem.at[0])
    hn_out.start()
    to_mate = [rdma(hn_v, hnp_hbm, p_send.at[0], p_recv.at[0], mate), rdma(dy_hbm, dyp_hbm, p_send.at[1], p_recv.at[1], mate)]
    for c in to_mate:
        c.start()

    def rope_rows(raw):
        lo, hi = raw[:, :half], raw[:, half:d]
        cs, sn = jnp.concatenate([cos_ref[...]] * 2, axis=0), jnp.concatenate([sin_ref[...]] * 2, axis=0)
        return lo * cs - hi * sn, hi * cs + lo * sn

    @pl.loop(0, n_tok // mc)
    def _(i):
        rs = pl.ds(pl.multiple_of(i * mc, mc), mc)
        lo, hi = rope_rows(dot_nn(hn_v[rs, :], wk_ref[...]))
        kv_v[rs, :half] = lo.astype(BF16)
        kv_v[rs, half:d] = hi.astype(BF16)
        kv_v[rs, d:] = dot_nn(hn_v[rs, :], wv_ref[...]).astype(BF16)
    kv_out = pltpu.make_async_copy(kv_v, kv_hbm, misc_sem.at[1])
    kv_out.start()

    outs = []
    saves = []

    def save(w, h):
        c = pltpu.make_async_copy(fulls[w].at[h], (wqf_hbm, wof_hbm)[w].at[h], w_sem.at[len(saves)])
        c.start()
        saves.append(c)

    def project(w, h):
        slot = len(outs) % 4
        if len(outs) >= 4:
            outs[-4].wait()

        @pl.loop(0, n_tok // mc)
        def _(i):
            rs = pl.ds(pl.multiple_of(i * mc, mc), mc)
            if w == 0:
                lo, hi = rope_rows(dot_nn(hn_v[rs, :], wq_v[h]))
                o0 = lo.reshape(2, tok, half).astype(BF16)
                o1 = hi.reshape(2, tok, half).astype(BF16)
                out_v[slot, pl.ds(2 * i, 2), :, :half] = o0
                out_v[slot, pl.ds(2 * i, 2), :, half:] = o1
            else:
                out_v[slot, pl.ds(2 * i, 2)] = dot_nt(dy_v[rs, :], wo_v[h]).reshape(2, tok, d).astype(BF16)
        c = pltpu.make_async_copy(out_v.at[slot], (q_hbm, do_hbm)[w].at[:, lax.rem(h, 2), h // 2], out_sem.at[slot])
        c.start()
        outs.append(c)
        save(w, h)

    other = 1 - k
    for w in range(2):
        own[w].wait()
        if w == 1:
            dyc.wait()
        project(w, me)
        wait_full(w, mate, 4)
        project(w, mate)
    for w in range(2):
        wait_full(w, head(-1, k), 0)
        send_half(w, head(-1, k), 0, 2, cw)
        wait_full(w, head(1, k), 1)
        send_half(w, head(1, k), 1, 3, ccw)
        send_full(w, head(-1, k), 5, mate)
        send_full(w, head(1, k), 6, mate)
        project(w, head(-1, k))
        project(w, head(1, k))
        wait_full(w, head(-1, other), 5)
        project(w, head(-1, other))
        wait_full(w, head(1, other), 6)
        project(w, head(1, other))

    def early(n):
        def blk(j):
            return kv0_hbm.at[n, pl.ds(pl.multiple_of(j * tok, 16), tok)]
        return Gather((me, k, mate, cw, ccw), me // 2, blk, lambda t: kv_send.at[n, t], lambda t: kv_recv.at[n, t])
    first, second = early(0), early(1)
    first.own(kv_v.at[pl.ds(0, tok)])
    own0 = pltpu.make_async_copy(kv_v.at[pl.ds(0, tok)], first.block(me), misc_sem.at[2])
    own0.start()
    for w in range(2):
        wait_half(w, head(2, k), 0, 2)
        send_half(w, head(2, k), 0, 7, mate)
        wait_half(w, head(2, k), 1, 3)
        send_half(w, head(2, k), 1, 8, mate)
        project(w, head(2, k))
        if w == 1:
            first.forward()
            second.own(kv_v.at[pl.ds(tok, tok)])
        wait_half(w, head(2, other), 0, 7)
        wait_half(w, head(2, other), 1, 8)
        project(w, head(2, other))
    first.last()
    for c in outs[-4:] + saves + [hn_out, kv_out, own0]:
        c.wait()
    first.ready()
    first.drain()
    second.arrived()
    second.ready((3,))
    second.drain((0, 2, 3))
    for c in sends:
        c.wait_send()
    for c in to_mate:
        c.wait()


def project(x, gain, wq, w_k, w_v, wo, dy, cos_t, sin_t):
    nb, tok, e = x.shape
    d = wq.shape[1]
    n_heads = 8
    n_tok = nb * tok
    any_spec = pl.BlockSpec(memory_space=pl.ANY)
    vmem = pl.BlockSpec(memory_space=pltpu.VMEM)
    act = jax.ShapeDtypeStruct((nb, 2, n_heads // 2, tok, d), BF16)
    dma = pltpu.SemaphoreType.DMA
    flops = 2 * n_tok * e * (2 * n_heads + 2) * d
    kv0, hn, q, do, kv, wqf, wof, hn_p, dy_p = pl.pallas_call(
        functools.partial(proj_body, nb, tok),
        in_specs=[any_spec, vmem, any_spec, vmem, vmem, any_spec, any_spec, vmem, vmem],
        out_specs=[any_spec] * 9,
        out_shape=[jax.ShapeDtypeStruct((2, tok * n_heads, 2 * d), BF16), jax.ShapeDtypeStruct((n_tok, e), BF16), act, act, jax.ShapeDtypeStruct((n_tok, 2 * d), BF16),
                   jax.ShapeDtypeStruct((n_heads, e, d), BF16), jax.ShapeDtypeStruct((n_heads, d, e), BF16),
                   jax.ShapeDtypeStruct((n_tok, e), BF16), jax.ShapeDtypeStruct((n_tok, e), BF16)],
        scratch_shapes=[pltpu.VMEM((n_tok, e), BF16), pltpu.VMEM((n_tok, e), BF16), pltpu.VMEM((n_tok, e), BF16),
                        pltpu.VMEM((n_heads, e, d), BF16), pltpu.VMEM((n_heads, d, e), BF16),
                        pltpu.VMEM((n_tok, 2 * d), BF16), pltpu.VMEM((4, nb, tok, d), BF16),
                        dma((2, 9)), dma((2, 9)), dma((nb,)), dma(()), dma((2,)), dma((4,)), dma((3,)), dma((16,)), dma((2,)), dma((2,)), dma((2, 7)), dma((2, 7))],
        compiler_params=pltpu.CompilerParams(collective_id=0, has_side_effects=True, vmem_limit_bytes=60 * 2**20),
        cost_estimate=pl.CostEstimate(flops=flops, bytes_accessed=60 * 2**20, transcendentals=0),
        name="project",
    )(x.reshape(n_tok, e), gain, wq, w_k, w_v, wo, dy.reshape(n_tok, e), cos_t, sin_t)
    return kv0, hn, q, do, kv.reshape(nb, tok, 2 * d), wqf, wof, hn_p, dy_p


def grads_body(nb, tok, o_hbm, acc_hbm, dq_hbm, dqp_hbm, hn_hbm, hnp_hbm, dy_hbm, dkv_hbm,
               wq_hbm, wo_hbm, wk_hbm, wv_hbm, x_hbm, g_ref, cos_ref, sin_ref,
               y_hbm, gx_hbm, gln_ref, gwo_ref, gwq_ref, gkv_hbm,
               acc, acc_kv, rbuf, rbuf_kv, kind, kp, dkv_v, fin_kv, gln_acc, gl_recv,
               rs_send, rs_recv, kv_send, kv_recv, ag_send, ag_recv, gl_send, gl_rsem, kp_sem, ld_sem, b_sem, t_sem, a_sem):
    n_tok, e = x_hbm.shape
    d = wk_hbm.shape[1]
    half = d // 2
    eh, eq = e // 2, e // 4
    me, k, mate, cw, ccw = ring_ids()
    c = me // 2
    rel = [lax.rem(c + o, 4) for o in (3, 1, 2, 0)]
    enter([lax.rem(me + o, 8) for o in range(1, 8)])

    order = ((2, 1), (2, 0))

    def hop(s, dr, j):
        first = acc_hbm.at[dr, dr] if s == 0 else acc.at[s, dr, dr]
        src = first if j == 0 else rbuf.at[s, dr, j - 1]
        return rdma(src, rbuf.at[s, dr, j], rs_send.at[s, dr, j], rs_recv.at[s, dr, j], (cw, ccw)[dr])

    def hop_kv(dr, j):
        src = acc_kv.at[dr, dr] if j == 0 else rbuf_kv.at[dr, j - 1]
        return rdma(src, rbuf_kv.at[dr, j], kv_send.at[dr, j], kv_recv.at[dr, j], (cw, ccw)[dr])

    def add(dst, term):
        @pl.loop(0, dst.shape[0] // 32)
        def _(i):
            rs = pl.ds(pl.multiple_of(i * 32, 32), 32)
            dst[rs, :] = dst[rs, :] + term[rs, :]

    def pass_on(s, j):
        for dr in range(2):
            hop(s, dr, j - 1).wait_recv()
            add(rbuf.at[s, dr, j - 1], acc.at[s, order[dr][j - 1], dr])
            hop(s, dr, j).start()

    def pass_on_kv(j):
        for dr in range(2):
            hop_kv(dr, j - 1).wait_recv()
            add(rbuf_kv.at[dr, j - 1], acc_kv.at[order[dr][j - 1], dr])
            hop_kv(dr, j).start()

    def finish(s, out):
        for dr in range(2):
            hop(s, dr, 2).wait_recv()

            @pl.loop(0, d // 32)
            def _(i):
                rs = pl.ds(pl.multiple_of(i * 32, 32), 32)
                out[rs, dr * eh:(dr + 1) * eh] = (rbuf[s, dr, 2, rs, :] + acc[s, 3, dr, rs, :]).astype(BF16)

    def piece(kk, j, lo=0, n=None):
        return gkv_hbm.at[kk, pl.ds(lo, d if n is None else n), pl.ds(pl.multiple_of(j * eq, 128), eq)]

    def ag(tag, ref, to, src=None):
        return rdma(ref if src is None else src, ref, ag_send.at[tag], ag_recv.at[tag], to)

    def ag_far(tag, to):
        return ag(tag, piece(k, rel[(0, 1)[tag - 3]], (tag - 3) * half, half), to)

    own_piece = pltpu.make_async_copy(fin_kv, piece(k, c), t_sem.at[5])

    def finish_kv():
        for dr in range(2):
            hop_kv(dr, 2).wait_recv()
            fin_kv[:, dr * (eq // 2):(dr + 1) * (eq // 2)] = rbuf_kv[dr, 2] + acc_kv[3, dr]
        ag(0, piece(k, c), cw, fin_kv).start()
        ag(1, piece(k, c), ccw, fin_kv).start()
        ag(2, piece(k, c), mate, fin_kv).start()
        own_piece.start()

    def ag_forward():
        ag(0, piece(k, rel[0]), cw).wait_recv()
        ag_far(3, cw).start()
        ag(1, piece(k, rel[1]), cw).wait_recv()
        ag_far(4, ccw).start()
        ag(5, piece(k, rel[0]), mate).start()
        ag(6, piece(k, rel[1]), mate).start()

    def ag_last():
        far = [piece(k, rel[2], i * half, half) for i in range(2)]
        for i in range(2):
            ag(3 + i, far[i], cw).wait_recv()
            ag(7 + i, far[i], mate).start()
        ag(2, piece(1 - k, c), mate).wait_recv()
        ag(5, piece(1 - k, rel[0]), mate).wait_recv()
        ag(6, piece(1 - k, rel[1]), mate).wait_recv()
        for i in range(2):
            ag(7 + i, piece(1 - k, rel[2], i * half, half), mate).wait_recv()
        for tag in range(3):
            ag(tag, piece(k, c), cw, fin_kv).wait_send()
        for tag in (3, 4, 7, 8):
            ag(tag, far[0], cw).wait_send()
        for tag in (5, 6):
            ag(tag, piece(k, c), cw).wait_send()
        own_piece.wait()

    dkv_in = pltpu.make_async_copy(dkv_hbm, dkv_v, t_sem.at[4])
    dkv_in.start()
    kp_copy = rdma(kind.at[1 - k], kp, kp_sem.at[0], kp_sem.at[1], mate)

    for dr in range(2):
        hop(0, dr, 0).start()
    acc_in = [pltpu.make_async_copy(acc_hbm.at[r], acc.at[0, r], a_sem.at[r]) for r in range(4)]
    for r in (2, 1, 0, 3):
        acc_in[r].start()

    def products(big, a_v, at):
        pr = Products(big, a_v, at, ld_sem, b_sem)
        hn_in = pr.load_b(hn_hbm, hnp_hbm)

        def fetch(r):
            return pr.load_a(r, dq_hbm.at[:, k, rel[r]], dqp_hbm.at[:, rel[r]])
        dkv_in.wait()
        for b in range(nb):
            lo, hi = dkv_v[b, :, :half].astype(F32), dkv_v[b, :, half:d].astype(F32)
            cs, sn = cos_ref[...], sin_ref[...]
            kind[0, b, :, :half] = (lo * cs + hi * sn).astype(BF16)
            kind[0, b, :, half:] = (hi * cs - lo * sn).astype(BF16)
            kind[1, b] = dkv_v[b, :, d:]
        kp_copy.start()
        for x in hn_in:
            x.start()
        for r in range(2):
            for x in fetch(r):
                x.start()
        pr.turn(0, kind.at[k])
        for x in hn_in:
            x.wait()
        kp_copy.wait_recv()
        pr.turn(1, kp)
        for r in range(4):
            for dr in range(2):
                acc_kv[r, dr] = pr.both(pl.ds(pl.multiple_of(rel[r] * eq + dr * (eq // 2), 128), eq // 2))
        for dr in range(2):
            hop_kv(dr, 0).start()
        for r in range(4):
            for x in fetch(r):
                x.wait()
            pr.turn(0, a_v.at[r % 2, 0])
            pr.turn(1, a_v.at[r % 2, 1])
            if r + 2 < 4:
                for x in fetch(r + 2):
                    x.start()
            if r < 2:
                pr.columns(acc.at[1, r], 0, 2, 2 * r)
                hop(1, r, 0).start()
                pr.columns(acc.at[1, r], 2, 4, 2 * r)
            else:
                pr.columns(acc.at[1, r], 0, 4)

    pl.run_scoped(products, pltpu.VMEM((2, n_tok, e), BF16), pltpu.VMEM((2, 2, nb, tok, d), BF16), pltpu.VMEM((2, d, n_tok), BF16))
    for r in range(4):
        acc_in[r].wait()
    pass_on(0, 1)
    pass_on_kv(1)

    mc = 2 * tok
    units = nb // 2

    def attn_out(wo_v, o_v, x_v, y_v):
        w_in = pltpu.make_async_copy(wo_hbm, wo_v, b_sem.at[0])
        w_in.start()

        def load(u):
            return (pltpu.make_async_copy(o_hbm.at[pl.ds(2 * u, 2)], o_v.at[u % 2], ld_sem.at[u % 2, 0]),
                    pltpu.make_async_copy(x_hbm.at[pl.ds(u * mc, mc)], x_v.at[u % 2], ld_sem.at[u % 2, 1]))

        def put(u):
            return pltpu.make_async_copy(y_v.at[u % 2], y_hbm.at[pl.ds(u * mc, mc)], t_sem.at[u % 2])
        for x in load(0):
            x.start()
        w_in.wait()
        for u in range(units):
            if u + 1 < units:
                for x in load(u + 1):
                    x.start()
            for x in load(u):
                x.wait()
            if u >= 2:
                put(u - 2).wait()
            sl = u % 2

            @pl.loop(0, 4)
            def _(n):
                cols = pl.ds(pl.multiple_of(n * eq, 128), eq)
                o_rows = jnp.concatenate([jnp.concatenate([o_v[sl, i, h % 2, h // 2] for h in range(8)], axis=1) for i in range(2)], axis=0)
                r = dot_nn(o_rows, wo_v[:, cols])
                y_v[sl, :, cols] = (x_v[sl, :, cols].astype(F32) + r).astype(BF16)
            put(u).start()
        for u in range(max(0, units - 2), units):
            put(u).wait()

    pl.run_scoped(attn_out, pltpu.VMEM((8 * d, e), BF16), pltpu.VMEM((2, 2, 2, 4, tok, d), BF16),
                  pltpu.VMEM((2, mc, e), BF16), pltpu.VMEM((2, mc, e), BF16))
    pass_on(1, 1)

    def hidden_grad(wq_v, wk_v, wv_v, dq_v, x_v, dy_v, dh, gx_v):
        w_in = pltpu.make_async_copy(wq_hbm, wq_v, b_sem.at[0])
        w_in.start()
        w2_in = (pltpu.make_async_copy(wk_hbm, wk_v, b_sem.at[1]), pltpu.make_async_copy(wv_hbm, wv_v, ld_sem.at[1, 1]))
        for x in w2_in:
            x.start()

        def load(u):
            return (pltpu.make_async_copy(dq_hbm.at[pl.ds(2 * u, 2)], dq_v, ld_sem.at[0, 0]),
                    pltpu.make_async_copy(x_hbm.at[pl.ds(u * mc, mc)], x_v, ld_sem.at[0, 1]),
                    pltpu.make_async_copy(dy_hbm.at[pl.ds(u * mc, mc)], dy_v, ld_sem.at[1, 0]))

        def put(u):
            return pltpu.make_async_copy(gx_v, gx_hbm.at[pl.ds(u * mc, mc)], t_sem.at[0])
        gain = g_ref[...].astype(F32)
        gln_acc[...] = jnp.zeros_like(gln_acc)
        for x in load(0):
            x.start()
        w_in.wait()
        for x in w2_in:
            x.wait()
        for u in range(units):
            for x in load(u):
                x.wait()

            @pl.loop(0, 4)
            def _(n):
                rows = pl.ds(pl.multiple_of(n * eq, 128), eq)
                t = None
                for h in range(8):
                    a = jnp.concatenate([dq_v[i, h % 2, h // 2] for i in range(2)], axis=0)
                    p = dot_nt(a, wq_v[h, rows, :])
                    t = p if t is None else t + p
                for j in range(2):
                    a = jnp.concatenate([kind[j, 2 * u + i] for i in range(2)], axis=0)
                    t = t + dot_nt(a, (wk_v, wv_v)[j][rows, :])
                dh[:, rows] = t
            if u >= 1:
                put(u - 1).wait()

            @pl.loop(0, mc // 16)
            def _(r):
                rs = pl.ds(pl.multiple_of(r * 16, 16), 16)
                x = x_v[rs, :].astype(F32)
                cx = x - jnp.mean(x, axis=1, keepdims=True)
                inv = lax.rsqrt(jnp.mean(cx * cx, axis=1, keepdims=True) + LN_EPS)
                xh = cx * inv
                g = dh[rs, :]
                pr = g * xh
                gln_acc[...] += pr[:8] + pr[8:]
                gh = g * gain
                m1 = jnp.mean(gh, axis=1, keepdims=True)
                m2 = jnp.mean(gh * xh, axis=1, keepdims=True)
                gx_v[rs, :] = (inv * (gh - m1 - xh * m2) + dy_v[rs, :].astype(F32)).astype(BF16)
            put(u).start()
            if u + 1 < units:
                for x in load(u + 1):
                    x.start()
            if u == units // 2 - 1:
                pass_on(0, 2)
                pass_on_kv(2)
        put(units - 1).wait()

    pl.run_scoped(hidden_grad, pltpu.VMEM((8, e, d), BF16), pltpu.VMEM((e, d), BF16), pltpu.VMEM((e, d), BF16), pltpu.VMEM((2, 2, 4, tok, d), BF16),
                  pltpu.VMEM((mc, e), BF16), pltpu.VMEM((mc, e), BF16), pltpu.VMEM((mc, e), F32), pltpu.VMEM((mc, e), BF16))
    gl_recv[me] = jnp.sum(gln_acc[...], axis=0, keepdims=True)
    pass_on(1, 2)
    finish(0, gwo_ref)
    finish_kv()
    gl = [rdma(gl_recv.at[me], gl_recv.at[me], gl_send.at[o - 1], gl_rsem.at[o - 1], lax.rem(me + o, 8)) for o in range(1, 8)]
    for x in gl:
        x.start()
    finish(1, gwq_ref)
    ag_forward()
    for o in range(1, 8):
        src = lax.rem(me + 8 - o, 8)
        rdma(gl_recv.at[src], gl_recv.at[src], gl_send.at[o - 1], gl_rsem.at[o - 1], mate).wait_recv()
    total = gl_recv[0]
    for i in range(1, 8):
        total = total + gl_recv[i]
    gln_ref[...] = total
    ag_last()
    for x in gl:
        x.wait_send()
    kp_copy.wait_send()
    for dr in range(2):
        for j in range(3):
            hop_kv(dr, j).wait_send()
            for s in range(2):
                hop(s, dr, j).wait_send()


def gradients(o, acc, dq, dq_p, hn, hn_p, dy, dkv, wqf, wof, w_k, w_v, x, gain, cos_t, sin_t):
    nb, tok, e = x.shape
    n_tok = nb * tok
    d = dq.shape[-1]
    any_spec = pl.BlockSpec(memory_space=pl.ANY)
    vmem = pl.BlockSpec(memory_space=pltpu.VMEM)
    dma = pltpu.SemaphoreType.DMA
    tokens = jax.ShapeDtypeStruct((n_tok, e), BF16)
    y, gx, gln, gwo, gwq_t, gkv_t = pl.pallas_call(
        functools.partial(grads_body, nb, tok),
        in_specs=[any_spec] * 13 + [vmem, vmem, vmem],
        out_specs=[any_spec, any_spec, vmem, vmem, vmem, any_spec],
        out_shape=[tokens, tokens, jax.ShapeDtypeStruct((1, e), F32), jax.ShapeDtypeStruct((d, e), BF16),
                   jax.ShapeDtypeStruct((d, e), BF16), jax.ShapeDtypeStruct((2, d, e), F32)],
        scratch_shapes=[pltpu.VMEM((2, 4, 2, d, e // 2), F32), pltpu.VMEM((4, 2, d, e // 8), F32),
                        pltpu.VMEM((2, 2, 3, d, e // 2), F32), pltpu.VMEM((2, 3, d, e // 8), F32),
                        pltpu.VMEM((2, nb, tok, d), BF16), pltpu.VMEM((nb, tok, d), BF16), pltpu.VMEM((nb, tok, 2 * d), BF16),
                        pltpu.VMEM((d, e // 4), F32), pltpu.VMEM((8, e), F32), pltpu.VMEM((8, 1, e), F32),
                        dma((2, 2, 3)), dma((2, 2, 3)), dma((2, 3)), dma((2, 3)), dma((9,)), dma((9,)), dma((7,)), dma((7,)),
                        dma((2,)), dma((2, 2)), dma((2,)), dma((6,)), dma((4,))],
        compiler_params=pltpu.CompilerParams(collective_id=2, has_side_effects=True, vmem_limit_bytes=63 * 2**20),
        cost_estimate=pl.CostEstimate(flops=10 * n_tok * e * e, bytes_accessed=120 * 2**20, transcendentals=0),
        name="gradients",
    )(o, acc, dq, dq_p, hn, hn_p, dy.reshape(n_tok, e), dkv, wqf, wof.reshape(8 * d, e), w_k, w_v, x.reshape(n_tok, e),
      gain, cos_t, sin_t)
    y, gx, gwq, gwk, gwv, gwo, gln = place(nb, y, gx, gwq_t, gkv_t, gwo, gln)
    return y.reshape(nb, tok, e), gx.reshape(nb, tok, e), gln.reshape(e), gwq, gwk, gwv, gwo


def place_body(y_in, gx_in, gq_in, gkv_in, go_in, gl_in, y, gx, gq, gk, gv, go, gl):
    y[...] = y_in[...]
    gx[...] = gx_in[...]
    gq[...] = gq_in[...].astype(F32).T.astype(BF16)
    gk[...] = gkv_in[0].T
    gv[...] = gkv_in[1].T
    go[...] = go_in[...]
    gl[...] = gl_in[...]


def place(steps, y, gx, gwq_t, gkv_t, gwo, gln):
    n_tok, e = y.shape
    d = gwo.shape[0]
    act = pl.BlockSpec((n_tok // steps, e), lambda i: (i, 0))
    cols = pl.BlockSpec((d, e // steps), lambda i: (0, i))
    turned = pl.BlockSpec((e // steps, d), lambda i: (i, 0))
    small = pl.BlockSpec((d // steps, e), lambda i: (i, 0))
    line = pl.BlockSpec((1, e), lambda i: (0, 0))
    return pl.pallas_call(
        place_body,
        grid=(steps,),
        in_specs=[act, act, cols, pl.BlockSpec((2, d, e // steps), lambda i: (0, 0, i)), small, line],
        out_specs=[act, act, turned, turned, turned, small, line],
        out_shape=[jax.ShapeDtypeStruct(y.shape, BF16), jax.ShapeDtypeStruct(y.shape, BF16), jax.ShapeDtypeStruct((e, d), BF16),
                   jax.ShapeDtypeStruct((e, d), F32), jax.ShapeDtypeStruct((e, d), F32), jax.ShapeDtypeStruct((d, e), BF16),
                   jax.ShapeDtypeStruct((1, e), F32)],
        compiler_params=pltpu.CompilerParams(dimension_semantics=("arbitrary",)),
        cost_estimate=pl.CostEstimate(flops=0, bytes_accessed=8 * y.size + 24 * gwo.size, transcendentals=0),
        name="place",
    )(y, gx, gwq_t, gkv_t, gwo, gln)


def solution(mesh):
    act_spec = P('dp', 'tp', None)

    def device_step(x_loc, ln_scale, wq_loc, w_k, w_v, wo_loc, dy_loc):
        n_batch, tok, model_dim = x_loc.shape
        d = w_k.shape[1]
        t0 = lax.axis_index('tp') * tok
        cos_t, sin_t = rope_tables(t0 + jnp.arange(tok), d)

        gain = ln_scale.reshape(1, model_dim)
        kv0, hn, q, do, kv_loc, wq_h, wo_h, hn_p, dy_p = project(x_loc, gain, wq_loc, w_k, w_v, wo_loc, dy_loc, cos_t, sin_t)
        o, dq, dkv_loc, o_p, dq_p, acc = attention(q, do, kv_loc, kv0, dy_loc.reshape(-1, model_dim), dy_p, cos_t, sin_t)
        return gradients(o, acc, dq, dq_p, hn, hn_p, dy_loc, dkv_loc, wq_h, wo_h, w_k, w_v, x_loc, gain, cos_t, sin_t)

    return jax.shard_map(device_step, mesh=mesh, in_specs=(act_spec, P(None), P(None, 'tp'), P(None, None), P(None, None), P('tp', None), act_spec), out_specs=(act_spec, act_spec, P('dp'), P('dp', 'tp'), P('dp', None), P('dp', None), P(('dp', 'tp'), None)), check_vma=False)
```

```python
import functools
import jax
import jax.numpy as jnp
from jax import lax
from jax.experimental import pallas as pl
from jax.experimental.pallas import tpu as pltpu
from jax.sharding import PartitionSpec as P

LN_EPS = 1e-6
ROPE_BASE = 10000.0
LOG2E = 1.4426950408889634
F32 = jnp.float32
BF16 = jnp.bfloat16


def rope_tables(positions, head_dim):
    half_dim = head_dim // 2
    inv_freq = ROPE_BASE ** (-2.0 * jnp.arange(half_dim, dtype=F32) / head_dim)
    angles = positions.astype(F32)[:, None] * inv_freq[None, :]
    return jnp.cos(angles), jnp.sin(angles)


def rotate(vectors, cos_t, sin_t):
    half_dim = vectors.shape[-1] // 2
    lo_half = vectors[..., :half_dim]
    hi_half = vectors[..., half_dim:]
    return jnp.concatenate([lo_half * cos_t - hi_half * sin_t, hi_half * cos_t + lo_half * sin_t], axis=-1)


def dot_nn(a, b):
    return lax.dot_general(a, b, (((1,), (0,)), ((), ())), preferred_element_type=F32)


def dot_nt(a, b):
    return lax.dot_general(a, b, (((1,), (1,)), ((), ())), preferred_element_type=F32)


def rdma(src, dst, send, recv, to):
    return pltpu.make_async_remote_copy(src_ref=src, dst_ref=dst, send_sem=send, recv_sem=recv,
                                        device_id={'tp': to}, device_id_type=pl.DeviceIdType.MESH)


def ring_ids():
    me = lax.axis_index('tp')
    k = lax.rem(me, 2)
    return me, k, me + 1 - 2 * k, lax.rem(me + 2, 8), lax.rem(me + 6, 8)


def enter(peers):
    barrier = pltpu.get_barrier_semaphore()
    for p in peers:
        pl.semaphore_signal(barrier, inc=1, device_id={'tp': p}, device_id_type=pl.DeviceIdType.MESH)
    pl.semaphore_wait(barrier, len(peers))


class Products:
    def __init__(self, big, a_v, at, ld_sem, b_sem):
        self.big, self.a_v, self.at, self.ld_sem, self.b_sem = big, a_v, at, ld_sem, b_sem
        self.nb, self.tok = a_v.shape[2], a_v.shape[3]
        self.eq = big.shape[2] // 4

    def load_b(self, own, other):
        return (pltpu.make_async_copy(own, self.big.at[0], self.b_sem.at[0]),
                pltpu.make_async_copy(other, self.big.at[1], self.b_sem.at[1]))

    def load_a(self, i, own, other):
        return (pltpu.make_async_copy(own, self.a_v.at[i % 2, 0], self.ld_sem.at[i % 2, 0]),
                pltpu.make_async_copy(other, self.a_v.at[i % 2, 1], self.ld_sem.at[i % 2, 1]))

    def turn(self, j, src):
        tok = self.tok
        for i in range(self.nb // 2):
            self.at[j, :, 2 * i * tok:(2 * i + 2) * tok] = jnp.concatenate([src[2 * i], src[2 * i + 1]], axis=0).T

    def both(self, cols):
        return dot_nn(self.at[0], self.big[0, :, cols]) + dot_nn(self.at[1], self.big[1, :, cols])

    def columns(self, dst, first, last, turned=0):
        eq = self.eq

        @pl.loop(first, last)
        def _(n):
            m = lax.rem(n + turned, 4)
            cols = pl.ds(pl.multiple_of(m * eq, 128), eq)
            dst[m // 2, :, pl.ds(pl.multiple_of(lax.rem(m, 2) * eq, 128), eq)] = self.both(cols)


class Gather:
    def __init__(self, ids, c, block, send, recv):
        self.me, _, self.mate, self.cw, self.ccw = ids
        self.c, self.block, self.send, self.recv = c, block, send, recv

    def copy(self, j, tag, to, src=None):
        ref = self.block(j)
        return rdma(ref if src is None else src, ref, self.send(tag), self.recv(tag), to)

    def own(self, src):
        @pl.when(self.c <= 2)
        def _():
            self.copy(self.me, 0, self.cw, src).start()

        @pl.when(self.c == 0)
        def _():
            self.copy(self.me, 2, self.ccw, src).start()
        self.copy(self.me, 3, self.mate, src).start()

    def arrived(self):
        @pl.when(self.c >= 1)
        def _():
            self.copy(self.me - 2, 0, self.cw).wait_recv()

        @pl.when(self.c == 3)
        def _():
            self.copy(self.me - 6, 2, self.ccw).wait_recv()

    def pass_on(self, src=lambda j: None):
        @pl.when(self.c >= 1)
        def _():
            @pl.when(self.c <= 2)
            def _():
                self.copy(self.me - 2, 1, self.cw, src(self.me - 2)).start()
            self.copy(self.me - 2, 4, self.mate, src(self.me - 2)).start()

        @pl.when(self.c == 3)
        def _():
            self.copy(self.me - 6, 6, self.mate, src(self.me - 6)).start()

    def forward(self):
        self.arrived()
        self.pass_on()

    def last(self):
        @pl.when(self.c >= 2)
        def _():
            self.copy(self.me - 4, 1, self.cw).wait_recv()
            self.copy(self.me - 4, 5, self.mate).start()

    def ready(self, tags=(3, 4, 5, 6)):
        if 3 in tags:
            self.copy(self.mate, 3, self.mate).wait_recv()
        for n, tag in ((1, 4), (2, 5), (3, 6)):
            if tag not in tags:
                continue

            @pl.when(self.c >= n)
            def _():
                self.copy(self.mate - 2 * n, tag, self.mate).wait_recv()

    def drain(self, tags=range(7)):
        c = self.c
        conds = (c <= 2, (c >= 1) & (c <= 2), c == 0, c >= 0, c >= 1, c >= 2, c == 3)
        for tag in tags:
            @pl.when(conds[tag])
            def _():
                self.copy(self.me, tag, self.mate).wait_send()


def attn_body(nb, tok, seq, d, q_hbm, do_hbm, kvl_hbm, kv0_hbm, dy_hbm, dyp_hbm, cos_ref, sin_ref,
              o_hbm, dq_hbm, dkv_hbm, op_hbm, dqp_hbm, acc_hbm,
              kv_all, o_v, dq_v, mrecv, rrecv,
              kv_send, kv_recv, m_send, m_recv, r_send, r_recv, own_sem, in_sem, out_sem, fin_sem, p_send, p_recv, first_sem,
              ld_sem, b_sem, acc_sem):
    scale = d ** -0.5
    rows = o_v.shape[2] * tok
    n_blk = seq // 256
    rb = 2 * rows // n_blk
    n_rb = rows // rb
    half = d // 2
    me, k, mate, cw, ccw = ring_ids()
    c = me // 2
    rel = [lax.rem(c + o, 4) for o in (3, 1, 2, 0)]

    def blk(j):
        return pl.ds(pl.multiple_of(j * tok, 16), tok)

    def kvb(b, j):
        return kv_all.at[b, blk(j)]

    def gather(b):
        return Gather((me, k, mate, cw, ccw), c, lambda j: kvb(b, j), lambda t: kv_send.at[b - 1, t], lambda t: kv_recv.at[b - 1, t])

    def own(b):
        gather(b).own(kvl_hbm.at[b])

    def own_copy(b):
        return pltpu.make_async_copy(kvl_hbm.at[b], kvb(b, me), own_sem.at[b])

    def ready(b):
        own_copy(b).wait()

        @pl.when(b == 1)
        def _():
            gather(1).ready((4, 5, 6))

        @pl.when(b > 1)
        def _():
            gather(b).ready()

    def drain(b):
        @pl.when(b == 1)
        def _():
            gather(1).drain((1, 4, 5, 6))

        @pl.when(b > 1)
        def _():
            gather(b).drain()

    def m_copy(b, n):
        return rdma(kvb(b, 2 * n + 1 - k), mrecv.at[b, n], m_send.at[b, n], m_recv.at[b, n], mate)

    def r_copy(b, n, slot, to):
        return rdma(kvb(b, 2 * n + k), rrecv.at[b, slot], r_send.at[b, slot], r_recv.at[b, slot], to)

    def add_into(b, n, other):
        v = kv_all[b, blk(2 * n + k), :].astype(F32) + other[...].astype(F32)
        kv_all[b, blk(2 * n + k), :] = v.astype(BF16)

    def fin_copy(b):
        return pltpu.make_async_copy(kvb(b, me), dkv_hbm.at[b], fin_sem.at[b])

    def to_mate(b):
        for n in range(4):
            @pl.when(c >= n)
            def _():
                m_copy(b, n).start()

    def stage1(b):
        for n in range(4):
            @pl.when(c >= n)
            def _():
                m_copy(b, n).wait()
                add_into(b, n, mrecv.at[b, n])

        @pl.when(c == 3)
        def _():
            r_copy(b, 1, 2, ccw).start()
            r_copy(b, 2, 1, ccw).start()
            r_copy(b, 0, 0, cw).start()
            fin_copy(b).start()

        @pl.when(c == 2)
        def _():
            r_copy(b, 0, 1, ccw).start()

    def stage2(b):
        @pl.when(c == 2)
        def _():
            r_copy(b, 1, 2, ccw).wait_recv()
            add_into(b, 1, rrecv.at[b, 2])
            r_copy(b, 1, 2, ccw).start()
            r_copy(b, 2, 1, ccw).wait_recv()
            add_into(b, 2, rrecv.at[b, 1])
            fin_copy(b).start()

        @pl.when(c == 1)
        def _():
            r_copy(b, 0, 1, ccw).wait_recv()
            add_into(b, 0, rrecv.at[b, 1])
            r_copy(b, 0, 1, ccw).start()

    def stage3(b):
        @pl.when(c == 0)
        def _():
            r_copy(b, 0, 0, cw).wait_recv()
            add_into(b, 0, rrecv.at[b, 0])
            r_copy(b, 0, 1, ccw).wait_recv()
            add_into(b, 0, rrecv.at[b, 1])
            fin_copy(b).start()

        @pl.when(c == 1)
        def _():
            r_copy(b, 1, 2, ccw).wait_recv()
            add_into(b, 1, rrecv.at[b, 2])
            fin_copy(b).start()

    def handed(dst, src, n, b, slot):
        return rdma(src.at[slot, 1 - k], dst.at[b], p_send.at[n, b], p_recv.at[n, b], mate)

    def store_o(b, slot):
        return (pltpu.make_async_copy(o_v.at[slot], o_hbm.at[b], out_sem.at[0, slot]), handed(op_hbm, o_v, 0, b, slot))

    def store_dq(b, slot):
        return (pltpu.make_async_copy(dq_v.at[slot], dq_hbm.at[b], out_sem.at[1, slot]), handed(dqp_hbm, dq_v, 1, b, slot))

    def stored(x):
        x[0].wait()
        x[1].wait_send()

    def attend(q_v, do_v, s_buf, m_buf, l_buf, p_buf, ds_buf, q_t, do_t, dk_t, dv_t, d_buf, cos4, sin4):
        def load(b, slot):
            return (pltpu.make_async_copy(q_hbm.at[b], q_v.at[slot], in_sem.at[0, slot]),
                    pltpu.make_async_copy(do_hbm.at[b], do_v.at[slot], in_sem.at[1, slot]))

        def scores(b, g, slot, i):
            w = min(512, seq)
            if (i * 256) % w:
                return
            cols = slice(i * 256, i * 256 + w)
            s = dot_nt(q_v[slot, g].reshape(rows, d), kv_all[b, cols, :d]) * (scale * LOG2E)
            col = lax.broadcasted_iota(jnp.int32, (tok, w), 1) + i * 256
            row = lax.broadcasted_iota(jnp.int32, (tok, w), 0) + me * tok
            s = jnp.concatenate([jnp.where(col <= row, s[j * tok:(j + 1) * tok], -1e30) for j in range(rows // tok)], axis=0)
            s_buf[g, :, cols] = s
            m = s[:, :128]
            for j in range(128, w, 128):
                m = jnp.maximum(m, s[:, j:j + 128])
            m_buf[...] = m if i == 0 else jnp.maximum(m_buf[...], m)

        parts = max(1, min(5, n_blk))
        part = [j * (rows // 16) // parts * 16 for j in range(parts + 1)] + [rows] * n_blk

        def softmax(g, i):
            for r in range(part[i], part[i + 1], 16):
                rs = slice(r, r + 16)
                m = jnp.max(m_buf[rs, :], axis=1, keepdims=True)
                l = None
                for j in range(0, seq, 128):
                    e = jnp.exp2(s_buf[g, rs, j:j + 128] - m)
                    s_buf[g, rs, j:j + 128] = e
                    l = e if l is None else l + e
                l_buf[g, rs, :] = jnp.broadcast_to(1.0 / jnp.sum(l, axis=1, keepdims=True), (16, 128))

        def turn(g, slot, i):
            rs = slice(i * rb, (i + 1) * rb)
            q_t[g, :, rs] = q_v[slot, g].reshape(rows, d)[rs].T
            do_t[g, :, rs] = do_v[slot, g].reshape(rows, d)[rs].T

        def out_rows(b, g, slot, i):
            rs = slice(i * rb, (i + 1) * rb)
            p = (s_buf[g, rs, :] * jnp.concatenate([l_buf[g, rs, :]] * (seq // 128), axis=1)).astype(BF16)
            p_buf[rs, :] = p
            o = dot_nn(p, kv_all[b, :, d:])
            dvec = jnp.sum(o * do_v[slot, g].reshape(rows, d)[rs].astype(F32), axis=1, keepdims=True)
            d_buf[rs, :] = jnp.broadcast_to(dvec, (rb, 128))
            put_rows(o_v, slot, g, i, o.astype(BF16))

        def put_rows(ref, slot, g, i, v):
            r = i * rb
            while r < (i + 1) * rb:
                n = min((i + 1) * rb - r, tok - r % tok)
                ref[slot, g, r // tok, r % tok:r % tok + n, :] = v[r - i * rb:r - i * rb + n]
                r += n

        def dq_rows(b, g, slot, i):
            rs = slice(i * rb, (i + 1) * rb)
            dq = dot_nn(ds_buf[rs, :], kv_all[b, :, :d]) * scale
            lo, hi = dq[:, :half], dq[:, half:]
            cs, sn = cos4[rs, :], sin4[rs, :]
            put_rows(dq_v, slot, g, i, jnp.concatenate([(lo * cs + hi * sn).astype(BF16), (hi * cs - lo * sn).astype(BF16)], axis=1))

        def grads(b, g, slot, i):
            cols = slice(i * 256, (i + 1) * 256)
            do = do_v[slot, g].reshape(rows, d)
            p = p_buf[:, cols]
            dp = dot_nt(do, kv_all[b, cols, d:])
            dvec = d_buf[...]
            if i > 0 and part[i] > part[i - 1]:
                z = None
                for r in range(part[i - 1], part[i], 8):
                    v = l_buf[1 - g, r:r + 8, :]
                    z = v if z is None else jnp.minimum(z, v)
                dvec = dvec + jnp.concatenate([jnp.minimum(z, 0.0)] * (rows // 8), axis=0)
            dd = jnp.concatenate([dvec, dvec], axis=1)
            ds = (p.astype(F32) * (dp - dd)).astype(BF16)
            ds_buf[:, cols] = ds
            dk = dot_nn(q_t[g], ds)
            dv = dot_nn(do_t[g], p)
            if g == 0:
                dk_t[:, cols] = dk
                dv_t[:, cols] = dv
            else:
                dk_t[:, cols] += dk
                dv_t[:, cols] += dv

        def close_kv(b, i):
            cols = slice(i * 256, (i + 1) * 256)
            kv_all[b, cols, :d] = (dk_t[:, cols] * scale).T.astype(BF16)
            kv_all[b, cols, d:] = dv_t[:, cols].T.astype(BF16)

        enter((mate, cw, ccw))
        gather(1).pass_on(lambda j: kv0_hbm.at[1, blk(j)])
        if nb > 2:
            own(2)
        for x in load(0, 0):
            x.start()

        def first(j):
            return pltpu.make_async_copy(kv0_hbm.at[0, blk(j)], kvb(0, j), first_sem.at[j])

        def second(j, n):
            return pltpu.make_async_copy(kv0_hbm.at[1, blk(j)], kvb(1, j), first_sem.at[8 + n])
        arrived = ((c >= 0, mate, 0), (c >= 1, me - 2, 1), (c == 3, me - 6, 2))
        for j in range(8):
            @pl.when(j <= 2 * c + 1)
            def _():
                first(j).start()
        for b in range(1, nb):
            own_copy(b).start()
        for cond, j, i in arrived:
            @pl.when(cond)
            def _():
                second(j, i).start()

        @pl.loop(2 * c + 2, 8)
        def _(j):
            for b in range(nb):
                kv_all[b, blk(j), :] = jnp.zeros((tok, 2 * d), BF16)
        for j in range(rows // tok):
            cos4[j * tok:(j + 1) * tok, :] = cos_ref[...]
            sin4[j * tok:(j + 1) * tok, :] = sin_ref[...]
        ds_buf[...] = jnp.zeros_like(ds_buf)
        for x in load(0, 0):
            x.wait()
        for i in range(n_rb):
            turn(0, 0, i)
        for j in range(8):
            @pl.when(j <= 2 * c + 1)
            def _():
                first(j).wait()
        for cond, j, i in arrived:
            @pl.when(cond)
            def _():
                second(j, i).wait()
        for i in range(n_blk):
            scores(0, 0, 0, i)
        for i in range(n_blk):
            softmax(0, i)

        def comm_steps(b, steps):
            for lag, stage in steps:
                @pl.when(b >= lag)
                def _():
                    stage(b - lag)

        @pl.loop(0, nb)
        def _(b):
            slot = lax.rem(b, 2)
            nxt = jnp.minimum(b + 1, nb - 1)
            prev = jnp.maximum(b - 1, 0)

            @pl.when(b + 1 < nb)
            def _():
                for x in load(b + 1, 1 - slot):
                    x.start()

            @pl.when(b + 3 < nb)
            def _():
                own(b + 3)

            @pl.when((b >= 1) & (b + 2 < nb))
            def _():
                gather(b + 2).forward()

            @pl.when((b >= 1) & (b + 1 < nb))
            def _():
                gather(b + 1).last()
            comm_steps(b, ((3, stage2), (4, stage3)))

            @pl.when(b >= 2)
            def _():
                drain(b - 1)

            @pl.when(b >= 2)
            def _():
                stored(store_o(b - 2, slot))
            spare = jnp.where(b >= 1, b - 1, nb)
            for i in range(n_blk):
                scores(b, 1, slot, i)
                if i % 2 == 1:
                    out_rows(b, 0, slot, i // 2)
                    dq_rows(prev, 1, 1 - slot, i // 2)
                    turn(1, slot, i // 2)
            for i in range(n_blk):
                close_kv(spare, i)

            @pl.when(b >= 1)
            def _():
                for x in store_dq(b - 1, 1 - slot):
                    x.start()
                to_mate(b - 1)

            @pl.when(b == 0)
            def _():
                gather(1).last()
            for i in range(n_blk):
                grads(b, 0, slot, i)
                softmax(1, i)

            @pl.when(b + 1 < nb)
            def _():
                for x in load(b + 1, 1 - slot):
                    x.wait()
                ready(b + 1)
            if nb > 2:
                @pl.when(b == 0)
                def _():
                    gather(2).forward()

            @pl.when(b >= 2)
            def _():
                stored(store_dq(b - 2, slot))
            nslot = lax.rem(nxt, 2)
            for i in range(n_blk):
                scores(nxt, 0, nslot, i)
                if i % 2 == 1:
                    out_rows(b, 1, slot, i // 2)
                    dq_rows(b, 0, slot, i // 2)
                    turn(0, nslot, i // 2)
            for x in store_o(b, slot):
                x.start()
            comm_steps(b, ((1, stage1),))
            for i in range(n_blk):
                grads(b, 1, slot, i)
                softmax(0, i)

        drain(nb - 1)
        for i in range(n_rb):
            dq_rows(nb - 1, 1, (nb - 1) % 2, i)
        for i in range(n_blk):
            close_kv(nb - 1, i)
        for x in store_dq(nb - 1, (nb - 1) % 2):
            x.start()
        to_mate(nb - 1)

    slab = pltpu.VMEM((2, 2, rows // tok, tok, d), BF16)
    pl.run_scoped(attend, slab, slab, pltpu.VMEM((2, rows, seq), F32), pltpu.VMEM((rows, 128), F32), pltpu.VMEM((2, rows, 128), F32),
                  pltpu.VMEM((rows, seq), BF16), pltpu.VMEM((rows, seq), BF16), pltpu.VMEM((2, d, rows), BF16),
                  pltpu.VMEM((2, d, rows), BF16), pltpu.VMEM((d, seq), F32), pltpu.VMEM((d, seq), F32),
                  pltpu.VMEM((rows, 128), F32), pltpu.VMEM((rows, half), F32), pltpu.VMEM((rows, half), F32))
    n = nb

    def first_products(big, a_v, at, acc_v):
        pr = Products(big, a_v, at, ld_sem, b_sem)
        for x in pr.load_b(dy_hbm, dyp_hbm):
            x.start()
        for b in (n - 2, n - 1):
            stored(store_o(b, b % 2))
        for b in range(n):
            handed(op_hbm, o_v, 0, b, b % 2).wait_recv()

        def fetch(r):
            return pr.load_a(r, o_hbm.at[:, k, rel[r]], op_hbm.at[:, rel[r]])

        def save(r):
            return pltpu.make_async_copy(acc_v.at[r], acc_hbm.at[r], acc_sem.at[r])
        for r in range(2):
            for x in fetch(r):
                x.start()

        todo = [((stage2, n - 3), (stage3, n - 4)), ((stage1, n - 1), (stage2, n - 2), (stage3, n - 3)),
                ((stage2, n - 1), (stage3, n - 2)), ((stage3, n - 1),)]

        def steps(i):
            for stage, b in todo[i]:
                if b >= 0:
                    stage(b)
        steps(0)
        steps(1)
        for r in range(4):
            for x in fetch(r):
                x.wait()
            pr.turn(0, a_v.at[r % 2, 0])
            pr.turn(1, a_v.at[r % 2, 1])
            if r + 2 < 4:
                for x in fetch(r + 2):
                    x.start()
            if r == 0:
                for x in pr.load_b(dy_hbm, dyp_hbm):
                    x.wait()
            pr.columns(acc_v.at[r], 0, 4)
            save(r).start()
            if r % 2 == 1:
                steps(2 + r // 2)
        for r in range(4):
            save(r).wait()

    pl.run_scoped(first_products, pltpu.VMEM((2,) + dy_hbm.shape, BF16), pltpu.VMEM((2, 2, nb, tok, d), BF16),
                  pltpu.VMEM((2, d, nb * tok), BF16), pltpu.VMEM((4, 2, d, dy_hbm.shape[1] // 2), F32))
    for b in (n - 2, n - 1):
        stored(store_dq(b, b % 2))
    for b in range(n):
        handed(dqp_hbm, dq_v, 1, b, b % 2).wait_recv()
        fin_copy(b).wait()
        for cond, slot in ((c == 3, 0), (c >= 1, 1), (c >= 2, 2)):
            @pl.when(cond)
            def _():
                r_copy(b, 0, slot, cw).wait_send()


def attention(q, do, kv, kv0, dy, dy_p, cos_t, sin_t):
    nb, _, hp, tok, d = q.shape
    seq = tok * 8
    rows = hp * tok
    any_spec = pl.BlockSpec(memory_space=pl.ANY)
    vmem = pl.BlockSpec(memory_space=pltpu.VMEM)
    dma = pltpu.SemaphoreType.DMA
    slab = pltpu.VMEM((2, 2, hp, tok, d), BF16)
    out = jax.ShapeDtypeStruct(q.shape, BF16)
    outp = jax.ShapeDtypeStruct((nb, hp, tok, d), BF16)
    return pl.pallas_call(
        functools.partial(attn_body, nb, tok, seq, d),
        in_specs=[any_spec] * 6 + [vmem, vmem],
        out_specs=[any_spec] * 6,
        out_shape=[out, out, jax.ShapeDtypeStruct(kv.shape, BF16), outp, outp,
                   jax.ShapeDtypeStruct((4, 2, d, dy.shape[1] // 2), F32)],
        scratch_shapes=[pltpu.VMEM((nb + 1, seq, 2 * d), BF16), slab, slab,
                        pltpu.VMEM((nb, 4, tok, 2 * d), BF16), pltpu.VMEM((nb, 3, tok, 2 * d), BF16),
                        dma((nb - 1, 7)), dma((nb - 1, 7)), dma((nb, 4)), dma((nb, 4)), dma((nb, 3)), dma((nb, 3)),
                        dma((nb,)), dma((2, 2)), dma((2, 2)), dma((nb,)), dma((2, nb)), dma((2, nb)), dma((11,)),
                        dma((2, 2)), dma((2,)), dma((4,))],
        compiler_params=pltpu.CompilerParams(collective_id=1, has_side_effects=True, vmem_limit_bytes=63 * 2**20),
        cost_estimate=pl.CostEstimate(flops=24 * nb * rows * seq * d, bytes_accessed=40 * 2**20,
                                      transcendentals=2 * nb * rows * seq),
        name="attention",
    )(q, do, kv, kv0, dy, dy_p, cos_t, sin_t)


def proj_body(nb, tok, x_hbm, g_ref, wq_hbm, wk_ref, wv_ref, wo_hbm, dy_hbm, cos_ref, sin_ref,
              kv0_hbm, hn_hbm, q_hbm, do_hbm, kv_hbm, wqf_hbm, wof_hbm, hnp_hbm, dyp_hbm,
              x_v, hn_v, dy_v, wq_v, wo_v, kv_v, out_v,
              send, recv, x_sem, dy_sem, own_sem, out_sem, misc_sem, w_sem, p_send, p_recv, kv_send, kv_recv):
    n_tok, e = x_hbm.shape
    d = kv_v.shape[1] // 2
    half = d // 2
    mc = 2 * tok
    me, k, mate, cw, ccw = ring_ids()
    base = 2 * (me // 2)

    def head(off, par):
        return lax.rem(base + 2 * off + 8, 8) + par
    enter((mate, cw, ccw))

    fulls = (wq_v, wo_v)
    locs = (wq_hbm, wo_hbm)

    def half_of(w, ref, j):
        n = ref.shape[0] // 2
        return ref.at[pl.ds(j * n, n)]

    sends = []

    def send_full(w, h, j, to, own=False):
        src = locs[w] if own else fulls[w].at[h]
        c = rdma(src, fulls[w].at[h], send.at[w, j], recv.at[w, j], to)
        c.start()
        sends.append(c)

    def send_half(w, h, part, j, to):
        c = rdma(half_of(w, fulls[w].at[h], part), half_of(w, fulls[w].at[h], part), send.at[w, j], recv.at[w, j], to)
        c.start()
        sends.append(c)

    def wait_full(w, h, j):
        rdma(fulls[w].at[h], fulls[w].at[h], send.at[w, j], recv.at[w, j], mate).wait_recv()

    def wait_half(w, h, part, j):
        ref = half_of(w, fulls[w].at[h], part)
        rdma(ref, ref, send.at[w, j], recv.at[w, j], mate).wait_recv()

    for w in range(2):
        send_full(w, me, 0, cw, True)
        send_full(w, me, 1, ccw, True)
        send_full(w, me, 4, mate, True)
    own = [pltpu.make_async_copy(locs[w], fulls[w].at[me], own_sem.at[w]) for w in range(2)]
    xs = [pltpu.make_async_copy(x_hbm.at[pl.ds(b * tok, tok)], x_v.at[pl.ds(b * tok, tok)], x_sem.at[b]) for b in range(nb)]
    for c in xs:
        c.start()
    for c in own:
        c.start()
    dyc = pltpu.make_async_copy(dy_hbm, dy_v, dy_sem)
    dyc.start()

    gain = g_ref[...].astype(F32)
    for b in range(nb):
        xs[b].wait()

        @pl.loop(0, tok // 16, unroll=2)
        def _(r):
            rs = pl.ds(pl.multiple_of(b * tok + r * 16, 16), 16)
            x = x_v[rs, :].astype(F32)
            c = x - jnp.mean(x, axis=1, keepdims=True)
            inv = lax.rsqrt(jnp.mean(c * c, axis=1, keepdims=True) + LN_EPS)
            hn_v[rs, :] = (c * inv * gain).astype(BF16)
    hn_out = pltpu.make_async_copy(hn_v, hn_hbm, misc_sem.at[0])
    hn_out.start()
    to_mate = [rdma(hn_v, hnp_hbm, p_send.at[0], p_recv.at[0], mate), rdma(dy_hbm, dyp_hbm, p_send.at[1], p_recv.at[1], mate)]
    for c in to_mate:
        c.start()

    def rope_rows(raw):
        lo, hi = raw[:, :half], raw[:, half:d]
        cs, sn = jnp.concatenate([cos_ref[...]] * 2, axis=0), jnp.concatenate([sin_ref[...]] * 2, axis=0)
        return lo * cs - hi * sn, hi * cs + lo * sn

    @pl.loop(0, n_tok // mc)
    def _(i):
        rs = pl.ds(pl.multiple_of(i * mc, mc), mc)
        lo, hi = rope_rows(dot_nn(hn_v[rs, :], wk_ref[...]))
        kv_v[rs, :half] = lo.astype(BF16)
        kv_v[rs, half:d] = hi.astype(BF16)
        kv_v[rs, d:] = dot_nn(hn_v[rs, :], wv_ref[...]).astype(BF16)
    kv_out = pltpu.make_async_copy(kv_v, kv_hbm, misc_sem.at[1])
    kv_out.start()

    outs = []
    saves = []

    def save(w, h):
        c = pltpu.make_async_copy(fulls[w].at[h], (wqf_hbm, wof_hbm)[w].at[h], w_sem.at[len(saves)])
        c.start()
        saves.append(c)

    def project(w, h):
        slot = len(outs) % 4
        if len(outs) >= 4:
            outs[-4].wait()

        @pl.loop(0, n_tok // mc)
        def _(i):
            rs = pl.ds(pl.multiple_of(i * mc, mc), mc)
            if w == 0:
                lo, hi = rope_rows(dot_nn(hn_v[rs, :], wq_v[h]))
                o0 = lo.reshape(2, tok, half).astype(BF16)
                o1 = hi.reshape(2, tok, half).astype(BF16)
                out_v[slot, pl.ds(2 * i, 2), :, :half] = o0
                out_v[slot, pl.ds(2 * i, 2), :, half:] = o1
            else:
                out_v[slot, pl.ds(2 * i, 2)] = dot_nt(dy_v[rs, :], wo_v[h]).reshape(2, tok, d).astype(BF16)
        c = pltpu.make_async_copy(out_v.at[slot], (q_hbm, do_hbm)[w].at[:, lax.rem(h, 2), h // 2], out_sem.at[slot])
        c.start()
        outs.append(c)
        save(w, h)

    other = 1 - k
    for w in range(2):
        own[w].wait()
        if w == 1:
            dyc.wait()
        project(w, me)
        wait_full(w, mate, 4)
        project(w, mate)
    for w in range(2):
        wait_full(w, head(-1, k), 0)
        send_half(w, head(-1, k), 0, 2, cw)
        wait_full(w, head(1, k), 1)
        send_half(w, head(1, k), 1, 3, ccw)
        send_full(w, head(-1, k), 5, mate)
        send_full(w, head(1, k), 6, mate)
        project(w, head(-1, k))
        project(w, head(1, k))
        wait_full(w, head(-1, other), 5)
        project(w, head(-1, other))
        wait_full(w, head(1, other), 6)
        project(w, head(1, other))

    def early(n):
        def blk(j):
            return kv0_hbm.at[n, pl.ds(pl.multiple_of(j * tok, 16), tok)]
        return Gather((me, k, mate, cw, ccw), me // 2, blk, lambda t: kv_send.at[n, t], lambda t: kv_recv.at[n, t])
    first, second = early(0), early(1)
    first.own(kv_v.at[pl.ds(0, tok)])
    own0 = pltpu.make_async_copy(kv_v.at[pl.ds(0, tok)], first.block(me), misc_sem.at[2])
    own0.start()
    for w in range(2):
        wait_half(w, head(2, k), 0, 2)
        send_half(w, head(2, k), 0, 7, mate)
        wait_half(w, head(2, k), 1, 3)
        send_half(w, head(2, k), 1, 8, mate)
        project(w, head(2, k))
        if w == 1:
            first.forward()
            second.own(kv_v.at[pl.ds(tok, tok)])
        wait_half(w, head(2, other), 0, 7)
        wait_half(w, head(2, other), 1, 8)
        project(w, head(2, other))
    first.last()
    for c in outs[-4:] + saves + [hn_out, kv_out, own0]:
        c.wait()
    first.ready()
    first.drain()
    second.arrived()
    second.ready((3,))
    second.drain((0, 2, 3))
    for c in sends:
        c.wait_send()
    for c in to_mate:
        c.wait()


def project(x, gain, wq, w_k, w_v, wo, dy, cos_t, sin_t):
    nb, tok, e = x.shape
    d = wq.shape[1]
    n_heads = 8
    n_tok = nb * tok
    any_spec = pl.BlockSpec(memory_space=pl.ANY)
    vmem = pl.BlockSpec(memory_space=pltpu.VMEM)
    act = jax.ShapeDtypeStruct((nb, 2, n_heads // 2, tok, d), BF16)
    dma = pltpu.SemaphoreType.DMA
    flops = 2 * n_tok * e * (2 * n_heads + 2) * d
    kv0, hn, q, do, kv, wqf, wof, hn_p, dy_p = pl.pallas_call(
        functools.partial(proj_body, nb, tok),
        in_specs=[any_spec, vmem, any_spec, vmem, vmem, any_spec, any_spec, vmem, vmem],
        out_specs=[any_spec] * 9,
        out_shape=[jax.ShapeDtypeStruct((2, tok * n_heads, 2 * d), BF16), jax.ShapeDtypeStruct((n_tok, e), BF16), act, act, jax.ShapeDtypeStruct((n_tok, 2 * d), BF16),
                   jax.ShapeDtypeStruct((n_heads, e, d), BF16), jax.ShapeDtypeStruct((n_heads, d, e), BF16),
                   jax.ShapeDtypeStruct((n_tok, e), BF16), jax.ShapeDtypeStruct((n_tok, e), BF16)],
        scratch_shapes=[pltpu.VMEM((n_tok, e), BF16), pltpu.VMEM((n_tok, e), BF16), pltpu.VMEM((n_tok, e), BF16),
                        pltpu.VMEM((n_heads, e, d), BF16), pltpu.VMEM((n_heads, d, e), BF16),
                        pltpu.VMEM((n_tok, 2 * d), BF16), pltpu.VMEM((4, nb, tok, d), BF16),
                        dma((2, 9)), dma((2, 9)), dma((nb,)), dma(()), dma((2,)), dma((4,)), dma((3,)), dma((16,)), dma((2,)), dma((2,)), dma((2, 7)), dma((2, 7))],
        compiler_params=pltpu.CompilerParams(collective_id=0, has_side_effects=True, vmem_limit_bytes=60 * 2**20),
        cost_estimate=pl.CostEstimate(flops=flops, bytes_accessed=60 * 2**20, transcendentals=0),
        name="project",
    )(x.reshape(n_tok, e), gain, wq, w_k, w_v, wo, dy.reshape(n_tok, e), cos_t, sin_t)
    return kv0, hn, q, do, kv.reshape(nb, tok, 2 * d), wqf, wof, hn_p, dy_p


def grads_body(nb, tok, o_hbm, acc_hbm, dq_hbm, dqp_hbm, hn_hbm, hnp_hbm, dy_hbm, dkv_hbm,
               wq_hbm, wo_hbm, wk_hbm, wv_hbm, x_hbm, g_ref, cos_ref, sin_ref,
               y_hbm, gx_hbm, gln_ref, gwo_ref, gwq_ref, gkv_hbm,
               acc, acc_kv, rbuf, rbuf_kv, kind, kp, dkv_v, fin_kv, gln_acc, gl_recv,
               rs_send, rs_recv, kv_send, kv_recv, ag_send, ag_recv, gl_send, gl_rsem, kp_sem, ld_sem, b_sem, t_sem, a_sem):
    n_tok, e = x_hbm.shape
    d = wk_hbm.shape[1]
    half = d // 2
    eh, eq = e // 2, e // 4
    me, k, mate, cw, ccw = ring_ids()
    c = me // 2
    rel = [lax.rem(c + o, 4) for o in (3, 1, 2, 0)]
    enter([lax.rem(me + o, 8) for o in range(1, 8)])

    order = ((2, 1), (2, 0))

    def hop(s, dr, j):
        first = acc_hbm.at[dr, dr] if s == 0 else acc.at[s, dr, dr]
        src = first if j == 0 else rbuf.at[s, dr, j - 1]
        return rdma(src, rbuf.at[s, dr, j], rs_send.at[s, dr, j], rs_recv.at[s, dr, j], (cw, ccw)[dr])

    def hop_kv(dr, j):
        src = acc_kv.at[dr, dr] if j == 0 else rbuf_kv.at[dr, j - 1]
        return rdma(src, rbuf_kv.at[dr, j], kv_send.at[dr, j], kv_recv.at[dr, j], (cw, ccw)[dr])

    def add(dst, term):
        @pl.loop(0, dst.shape[0] // 32)
        def _(i):
            rs = pl.ds(pl.multiple_of(i * 32, 32), 32)
            dst[rs, :] = dst[rs, :] + term[rs, :]

    def pass_on(s, j):
        for dr in range(2):
            hop(s, dr, j - 1).wait_recv()
            add(rbuf.at[s, dr, j - 1], acc.at[s, order[dr][j - 1], dr])
            hop(s, dr, j).start()

    def pass_on_kv(j):
        for dr in range(2):
            hop_kv(dr, j - 1).wait_recv()
            add(rbuf_kv.at[dr, j - 1], acc_kv.at[order[dr][j - 1], dr])
            hop_kv(dr, j).start()

    def finish(s, out):
        for dr in range(2):
            hop(s, dr, 2).wait_recv()

            @pl.loop(0, d // 32)
            def _(i):
                rs = pl.ds(pl.multiple_of(i * 32, 32), 32)
                out[rs, dr * eh:(dr + 1) * eh] = (rbuf[s, dr, 2, rs, :] + acc[s, 3, dr, rs, :]).astype(BF16)

    def piece(kk, j, lo=0, n=None):
        return gkv_hbm.at[kk, pl.ds(lo, d if n is None else n), pl.ds(pl.multiple_of(j * eq, 128), eq)]

    def ag(tag, ref, to, src=None):
        return rdma(ref if src is None else src, ref, ag_send.at[tag], ag_recv.at[tag], to)

    def ag_far(tag, to):
        return ag(tag, piece(k, rel[(0, 1)[tag - 3]], (tag - 3) * half, half), to)

    own_piece = pltpu.make_async_copy(fin_kv, piece(k, c), t_sem.at[5])

    def finish_kv():
        for dr in range(2):
            hop_kv(dr, 2).wait_recv()
            fin_kv[:, dr * (eq // 2):(dr + 1) * (eq // 2)] = rbuf_kv[dr, 2] + acc_kv[3, dr]
        ag(0, piece(k, c), cw, fin_kv).start()
        ag(1, piece(k, c), ccw, fin_kv).start()
        ag(2, piece(k, c), mate, fin_kv).start()
        own_piece.start()

    def ag_forward():
        ag(0, piece(k, rel[0]), cw).wait_recv()
        ag_far(3, cw).start()
        ag(1, piece(k, rel[1]), cw).wait_recv()
        ag_far(4, ccw).start()
        ag(5, piece(k, rel[0]), mate).start()
        ag(6, piece(k, rel[1]), mate).start()

    def ag_last():
        far = [piece(k, rel[2], i * half, half) for i in range(2)]
        for i in range(2):
            ag(3 + i, far[i], cw).wait_recv()
            ag(7 + i, far[i], mate).start()
        ag(2, piece(1 - k, c), mate).wait_recv()
        ag(5, piece(1 - k, rel[0]), mate).wait_recv()
        ag(6, piece(1 - k, rel[1]), mate).wait_recv()
        for i in range(2):
            ag(7 + i, piece(1 - k, rel[2], i * half, half), mate).wait_recv()
        for tag in range(3):
            ag(tag, piece(k, c), cw, fin_kv).wait_send()
        for tag in (3, 4, 7, 8):
            ag(tag, far[0], cw).wait_send()
        for tag in (5, 6):
            ag(tag, piece(k, c), cw).wait_send()
        own_piece.wait()

    dkv_in = pltpu.make_async_copy(dkv_hbm, dkv_v, t_sem.at[4])
    dkv_in.start()
    kp_copy = rdma(kind.at[1 - k], kp, kp_sem.at[0], kp_sem.at[1], mate)

    for dr in range(2):
        hop(0, dr, 0).start()
    acc_in = [pltpu.make_async_copy(acc_hbm.at[r], acc.at[0, r], a_sem.at[r]) for r in range(4)]
    for r in (2, 1, 0, 3):
        acc_in[r].start()

    def products(big, a_v, at):
        pr = Products(big, a_v, at, ld_sem, b_sem)
        hn_in = pr.load_b(hn_hbm, hnp_hbm)

        def fetch(r):
            return pr.load_a(r, dq_hbm.at[:, k, rel[r]], dqp_hbm.at[:, rel[r]])
        dkv_in.wait()
        for b in range(nb):
            lo, hi = dkv_v[b, :, :half].astype(F32), dkv_v[b, :, half:d].astype(F32)
            cs, sn = cos_ref[...], sin_ref[...]
            kind[0, b, :, :half] = (lo * cs + hi * sn).astype(BF16)
            kind[0, b, :, half:] = (hi * cs - lo * sn).astype(BF16)
            kind[1, b] = dkv_v[b, :, d:]
        kp_copy.start()
        for x in hn_in:
            x.start()
        for r in range(2):
            for x in fetch(r):
                x.start()
        pr.turn(0, kind.at[k])
        for x in hn_in:
            x.wait()
        kp_copy.wait_recv()
        pr.turn(1, kp)
        for r in range(4):
            for dr in range(2):
                acc_kv[r, dr] = pr.both(pl.ds(pl.multiple_of(rel[r] * eq + dr * (eq // 2), 128), eq // 2))
        for dr in range(2):
            hop_kv(dr, 0).start()
        for r in range(4):
            for x in fetch(r):
                x.wait()
            pr.turn(0, a_v.at[r % 2, 0])
            pr.turn(1, a_v.at[r % 2, 1])
            if r + 2 < 4:
                for x in fetch(r + 2):
                    x.start()
            if r < 2:
                pr.columns(acc.at[1, r], 0, 2, 2 * r)
                hop(1, r, 0).start()
                pr.columns(acc.at[1, r], 2, 4, 2 * r)
            else:
                pr.columns(acc.at[1, r], 0, 4)

    pl.run_scoped(products, pltpu.VMEM((2, n_tok, e), BF16), pltpu.VMEM((2, 2, nb, tok, d), BF16), pltpu.VMEM((2, d, n_tok), BF16))
    for r in range(4):
        acc_in[r].wait()
    pass_on(0, 1)
    pass_on_kv(1)

    mc = 2 * tok
    units = nb // 2

    def attn_out(wo_v, o_v, x_v, y_v):
        w_in = pltpu.make_async_copy(wo_hbm, wo_v, b_sem.at[0])
        w_in.start()

        def load(u):
            return (pltpu.make_async_copy(o_hbm.at[pl.ds(2 * u, 2)], o_v.at[u % 2], ld_sem.at[u % 2, 0]),
                    pltpu.make_async_copy(x_hbm.at[pl.ds(u * mc, mc)], x_v.at[u % 2], ld_sem.at[u % 2, 1]))

        def put(u):
            return pltpu.make_async_copy(y_v.at[u % 2], y_hbm.at[pl.ds(u * mc, mc)], t_sem.at[u % 2])
        for x in load(0):
            x.start()
        w_in.wait()
        for u in range(units):
            if u + 1 < units:
                for x in load(u + 1):
                    x.start()
            for x in load(u):
                x.wait()
            if u >= 2:
                put(u - 2).wait()
            sl = u % 2

            @pl.loop(0, 4)
            def _(n):
                cols = pl.ds(pl.multiple_of(n * eq, 128), eq)
                o_rows = jnp.concatenate([jnp.concatenate([o_v[sl, i, h % 2, h // 2] for h in range(8)], axis=1) for i in range(2)], axis=0)
                r = dot_nn(o_rows, wo_v[:, cols])
                y_v[sl, :, cols] = (x_v[sl, :, cols].astype(F32) + r).astype(BF16)
            put(u).start()
        for u in range(max(0, units - 2), units):
            put(u).wait()

    pl.run_scoped(attn_out, pltpu.VMEM((8 * d, e), BF16), pltpu.VMEM((2, 2, 2, 4, tok, d), BF16),
                  pltpu.VMEM((2, mc, e), BF16), pltpu.VMEM((2, mc, e), BF16))
    pass_on(1, 1)

    def hidden_grad(wq_v, wk_v, wv_v, dq_v, x_v, dy_v, dh, gx_v):
        w_in = pltpu.make_async_copy(wq_hbm, wq_v, b_sem.at[0])
        w_in.start()
        w2_in = (pltpu.make_async_copy(wk_hbm, wk_v, b_sem.at[1]), pltpu.make_async_copy(wv_hbm, wv_v, ld_sem.at[1, 1]))
        for x in w2_in:
            x.start()

        def load(u):
            return (pltpu.make_async_copy(dq_hbm.at[pl.ds(2 * u, 2)], dq_v, ld_sem.at[0, 0]),
                    pltpu.make_async_copy(x_hbm.at[pl.ds(u * mc, mc)], x_v, ld_sem.at[0, 1]),
                    pltpu.make_async_copy(dy_hbm.at[pl.ds(u * mc, mc)], dy_v, ld_sem.at[1, 0]))

        def put(u):
            return pltpu.make_async_copy(gx_v, gx_hbm.at[pl.ds(u * mc, mc)], t_sem.at[0])
        gain = g_ref[...].astype(F32)
        gln_acc[...] = jnp.zeros_like(gln_acc)
        for x in load(0):
            x.start()
        w_in.wait()
        for x in w2_in:
            x.wait()
        for u in range(units):
            for x in load(u):
                x.wait()

            @pl.loop(0, 4)
            def _(n):
                rows = pl.ds(pl.multiple_of(n * eq, 128), eq)
                t = None
                for h in range(8):
                    a = jnp.concatenate([dq_v[i, h % 2, h // 2] for i in range(2)], axis=0)
                    p = dot_nt(a, wq_v[h, rows, :])
                    t = p if t is None else t + p
                for j in range(2):
                    a = jnp.concatenate([kind[j, 2 * u + i] for i in range(2)], axis=0)
                    t = t + dot_nt(a, (wk_v, wv_v)[j][rows, :])
                dh[:, rows] = t
            if u >= 1:
                put(u - 1).wait()

            @pl.loop(0, mc // 16)
            def _(r):
                rs = pl.ds(pl.multiple_of(r * 16, 16), 16)
                x = x_v[rs, :].astype(F32)
                cx = x - jnp.mean(x, axis=1, keepdims=True)
                inv = lax.rsqrt(jnp.mean(cx * cx, axis=1, keepdims=True) + LN_EPS)
                xh = cx * inv
                g = dh[rs, :]
                pr = g * xh
                gln_acc[...] += pr[:8] + pr[8:]
                gh = g * gain
                m1 = jnp.mean(gh, axis=1, keepdims=True)
                m2 = jnp.mean(gh * xh, axis=1, keepdims=True)
                gx_v[rs, :] = (inv * (gh - m1 - xh * m2) + dy_v[rs, :].astype(F32)).astype(BF16)
            put(u).start()
            if u + 1 < units:
                for x in load(u + 1):
                    x.start()
            if u == units // 2 - 1:
                pass_on(0, 2)
                pass_on_kv(2)
        put(units - 1).wait()

    pl.run_scoped(hidden_grad, pltpu.VMEM((8, e, d), BF16), pltpu.VMEM((e, d), BF16), pltpu.VMEM((e, d), BF16), pltpu.VMEM((2, 2, 4, tok, d), BF16),
                  pltpu.VMEM((mc, e), BF16), pltpu.VMEM((mc, e), BF16), pltpu.VMEM((mc, e), F32), pltpu.VMEM((mc, e), BF16))
    gl_recv[me] = jnp.sum(gln_acc[...], axis=0, keepdims=True)
    pass_on(1, 2)
    finish(0, gwo_ref)
    finish_kv()
    gl = [rdma(gl_recv.at[me], gl_recv.at[me], gl_send.at[o - 1], gl_rsem.at[o - 1], lax.rem(me + o, 8)) for o in range(1, 8)]
    for x in gl:
        x.start()
    finish(1, gwq_ref)
    ag_forward()
    for o in range(1, 8):
        src = lax.rem(me + 8 - o, 8)
        rdma(gl_recv.at[src], gl_recv.at[src], gl_send.at[o - 1], gl_rsem.at[o - 1], mate).wait_recv()
    total = gl_recv[0]
    for i in range(1, 8):
        total = total + gl_recv[i]
    gln_ref[...] = total
    ag_last()
    for x in gl:
        x.wait_send()
    kp_copy.wait_send()
    for dr in range(2):
        for j in range(3):
            hop_kv(dr, j).wait_send()
            for s in range(2):
                hop(s, dr, j).wait_send()


def gradients(o, acc, dq, dq_p, hn, hn_p, dy, dkv, wqf, wof, w_k, w_v, x, gain, cos_t, sin_t):
    nb, tok, e = x.shape
    n_tok = nb * tok
    d = dq.shape[-1]
    any_spec = pl.BlockSpec(memory_space=pl.ANY)
    vmem = pl.BlockSpec(memory_space=pltpu.VMEM)
    dma = pltpu.SemaphoreType.DMA
    tokens = jax.ShapeDtypeStruct((n_tok, e), BF16)
    y, gx, gln, gwo, gwq_t, gkv_t = pl.pallas_call(
        functools.partial(grads_body, nb, tok),
        in_specs=[any_spec] * 13 + [vmem, vmem, vmem],
        out_specs=[any_spec, any_spec, vmem, vmem, vmem, any_spec],
        out_shape=[tokens, tokens, jax.ShapeDtypeStruct((1, e), F32), jax.ShapeDtypeStruct((d, e), BF16),
                   jax.ShapeDtypeStruct((d, e), BF16), jax.ShapeDtypeStruct((2, d, e), F32)],
        scratch_shapes=[pltpu.VMEM((2, 4, 2, d, e // 2), F32), pltpu.VMEM((4, 2, d, e // 8), F32),
                        pltpu.VMEM((2, 2, 3, d, e // 2), F32), pltpu.VMEM((2, 3, d, e // 8), F32),
                        pltpu.VMEM((2, nb, tok, d), BF16), pltpu.VMEM((nb, tok, d), BF16), pltpu.VMEM((nb, tok, 2 * d), BF16),
                        pltpu.VMEM((d, e // 4), F32), pltpu.VMEM((8, e), F32), pltpu.VMEM((8, 1, e), F32),
                        dma((2, 2, 3)), dma((2, 2, 3)), dma((2, 3)), dma((2, 3)), dma((9,)), dma((9,)), dma((7,)), dma((7,)),
                        dma((2,)), dma((2, 2)), dma((2,)), dma((6,)), dma((4,))],
        compiler_params=pltpu.CompilerParams(collective_id=2, has_side_effects=True, vmem_limit_bytes=63 * 2**20),
        cost_estimate=pl.CostEstimate(flops=10 * n_tok * e * e, bytes_accessed=120 * 2**20, transcendentals=0),
        name="gradients",
    )(o, acc, dq, dq_p, hn, hn_p, dy.reshape(n_tok, e), dkv, wqf, wof.reshape(8 * d, e), w_k, w_v, x.reshape(n_tok, e),
      gain, cos_t, sin_t)
    y, gx, gwq, gwk, gwv, gwo, gln = place(nb, y, gx, gwq_t, gkv_t, gwo, gln)
    return y.reshape(nb, tok, e), gx.reshape(nb, tok, e), gln.reshape(e), gwq, gwk, gwv, gwo


def place_body(y_in, gx_in, gq_in, gkv_in, go_in, gl_in, y, gx, gq, gk, gv, go, gl):
    y[...] = y_in[...]
    gx[...] = gx_in[...]
    gq[...] = gq_in[...].astype(F32).T.astype(BF16)
    gk[...] = gkv_in[0].T
    gv[...] = gkv_in[1].T
    go[...] = go_in[...]
    gl[...] = gl_in[...]


def place(steps, y, gx, gwq_t, gkv_t, gwo, gln):
    n_tok, e = y.shape
    d = gwo.shape[0]
    act = pl.BlockSpec((n_tok // steps, e), lambda i: (i, 0))
    cols = pl.BlockSpec((d, e // steps), lambda i: (0, i))
    turned = pl.BlockSpec((e // steps, d), lambda i: (i, 0))
    small = pl.BlockSpec((d // steps, e), lambda i: (i, 0))
    line = pl.BlockSpec((1, e), lambda i: (0, 0))
    return pl.pallas_call(
        place_body,
        grid=(steps,),
        in_specs=[act, act, cols, pl.BlockSpec((2, d, e // steps), lambda i: (0, 0, i)), small, line],
        out_specs=[act, act, turned, turned, turned, small, line],
        out_shape=[jax.ShapeDtypeStruct(y.shape, BF16), jax.ShapeDtypeStruct(y.shape, BF16), jax.ShapeDtypeStruct((e, d), BF16),
                   jax.ShapeDtypeStruct((e, d), F32), jax.ShapeDtypeStruct((e, d), F32), jax.ShapeDtypeStruct((d, e), BF16),
                   jax.ShapeDtypeStruct((1, e), F32)],
        compiler_params=pltpu.CompilerParams(dimension_semantics=("arbitrary",)),
        cost_estimate=pl.CostEstimate(flops=0, bytes_accessed=8 * y.size + 24 * gwo.size, transcendentals=0),
        name="place",
    )(y, gx, gwq_t, gkv_t, gwo, gln)


def solution(mesh):
    act_spec = P('dp', 'tp', None)

    def device_step(x_loc, ln_scale, wq_loc, w_k, w_v, wo_loc, dy_loc):
        n_batch, tok, model_dim = x_loc.shape
        d = w_k.shape[1]
        t0 = lax.axis_index('tp') * tok
        cos_t, sin_t = rope_tables(t0 + jnp.arange(tok), d)

        gain = ln_scale.reshape(1, model_dim)
        kv0, hn, q, do, kv_loc, wq_h, wo_h, hn_p, dy_p = project(x_loc, gain, wq_loc, w_k, w_v, wo_loc, dy_loc, cos_t, sin_t)
        o, dq, dkv_loc, o_p, dq_p, acc = attention(q, do, kv_loc, kv0, dy_loc.reshape(-1, model_dim), dy_p, cos_t, sin_t)
        return gradients(o, acc, dq, dq_p, hn, hn_p, dy_loc, dkv_loc, wq_h, wo_h, w_k, w_v, x_loc, gain, cos_t, sin_t)

    return jax.shard_map(device_step, mesh=mesh, in_specs=(act_spec, P(None), P(None, 'tp'), P(None, None), P(None, None), P('tp', None), act_spec), out_specs=(act_spec, act_spec, P('dp'), P('dp', 'tp'), P('dp', None), P('dp', None), P(('dp', 'tp'), None)), check_vma=False)
```

```python
import functools
import jax
import jax.numpy as jnp
from jax import lax
from jax.experimental import pallas as pl
from jax.experimental.pallas import tpu as pltpu
from jax.sharding import PartitionSpec as P

LN_EPS = 1e-6
ROPE_BASE = 10000.0
LOG2E = 1.4426950408889634
F32 = jnp.float32
BF16 = jnp.bfloat16


def rope_tables(positions, head_dim):
    half_dim = head_dim // 2
    inv_freq = ROPE_BASE ** (-2.0 * jnp.arange(half_dim, dtype=F32) / head_dim)
    angles = positions.astype(F32)[:, None] * inv_freq[None, :]
    return jnp.cos(angles), jnp.sin(angles)


def rotate(vectors, cos_t, sin_t):
    half_dim = vectors.shape[-1] // 2
    lo_half = vectors[..., :half_dim]
    hi_half = vectors[..., half_dim:]
    return jnp.concatenate([lo_half * cos_t - hi_half * sin_t, hi_half * cos_t + lo_half * sin_t], axis=-1)


def dot_nn(a, b):
    return lax.dot_general(a, b, (((1,), (0,)), ((), ())), preferred_element_type=F32)


def dot_nt(a, b):
    return lax.dot_general(a, b, (((1,), (1,)), ((), ())), preferred_element_type=F32)


def rdma(src, dst, send, recv, to):
    return pltpu.make_async_remote_copy(src_ref=src, dst_ref=dst, send_sem=send, recv_sem=recv,
                                        device_id={'tp': to}, device_id_type=pl.DeviceIdType.MESH)


def ring_ids():
    me = lax.axis_index('tp')
    k = lax.rem(me, 2)
    return me, k, me + 1 - 2 * k, lax.rem(me + 2, 8), lax.rem(me + 6, 8)


def enter(peers):
    barrier = pltpu.get_barrier_semaphore()
    for p in peers:
        pl.semaphore_signal(barrier, inc=1, device_id={'tp': p}, device_id_type=pl.DeviceIdType.MESH)
    pl.semaphore_wait(barrier, len(peers))


class Products:
    def __init__(self, big, a_v, at, ld_sem, b_sem):
        self.big, self.a_v, self.at, self.ld_sem, self.b_sem = big, a_v, at, ld_sem, b_sem
        self.nb, self.tok = a_v.shape[2], a_v.shape[3]
        self.eq = big.shape[2] // 4

    def load_b(self, own, other):
        return (pltpu.make_async_copy(own, self.big.at[0], self.b_sem.at[0]),
                pltpu.make_async_copy(other, self.big.at[1], self.b_sem.at[1]))

    def load_a(self, i, own, other):
        return (pltpu.make_async_copy(own, self.a_v.at[i % 2, 0], self.ld_sem.at[i % 2, 0]),
                pltpu.make_async_copy(other, self.a_v.at[i % 2, 1], self.ld_sem.at[i % 2, 1]))

    def turn(self, j, src):
        tok = self.tok
        for i in range(self.nb // 2):
            self.at[j, :, 2 * i * tok:(2 * i + 2) * tok] = jnp.concatenate([src[2 * i], src[2 * i + 1]], axis=0).T

    def both(self, cols):
        return dot_nn(self.at[0], self.big[0, :, cols]) + dot_nn(self.at[1], self.big[1, :, cols])

    def columns(self, dst, first, last, turned=0):
        eq = self.eq

        @pl.loop(first, last)
        def _(n):
            m = lax.rem(n + turned, 4)
            cols = pl.ds(pl.multiple_of(m * eq, 128), eq)
            dst[m // 2, :, pl.ds(pl.multiple_of(lax.rem(m, 2) * eq, 128), eq)] = self.both(cols)


class Gather:
    def __init__(self, ids, c, block, send, recv):
        self.me, _, self.mate, self.cw, self.ccw = ids
        self.c, self.block, self.send, self.recv = c, block, send, recv

    def copy(self, j, tag, to, src=None):
        ref = self.block(j)
        return rdma(ref if src is None else src, ref, self.send(tag), self.recv(tag), to)

    def own(self, src):
        @pl.when(self.c <= 2)
        def _():
            self.copy(self.me, 0, self.cw, src).start()

        @pl.when(self.c == 0)
        def _():
            self.copy(self.me, 2, self.ccw, src).start()
        self.copy(self.me, 3, self.mate, src).start()

    def arrived(self):
        @pl.when(self.c >= 1)
        def _():
            self.copy(self.me - 2, 0, self.cw).wait_recv()

        @pl.when(self.c == 3)
        def _():
            self.copy(self.me - 6, 2, self.ccw).wait_recv()

    def pass_on(self, src=lambda j: None):
        @pl.when(self.c >= 1)
        def _():
            @pl.when(self.c <= 2)
            def _():
                self.copy(self.me - 2, 1, self.cw, src(self.me - 2)).start()
            self.copy(self.me - 2, 4, self.mate, src(self.me - 2)).start()

        @pl.when(self.c == 3)
        def _():
            self.copy(self.me - 6, 6, self.mate, src(self.me - 6)).start()

    def forward(self):
        self.arrived()
        self.pass_on()

    def last(self):
        @pl.when(self.c >= 2)
        def _():
            self.copy(self.me - 4, 1, self.cw).wait_recv()
            self.copy(self.me - 4, 5, self.mate).start()

    def ready(self, tags=(3, 4, 5, 6)):
        if 3 in tags:
            self.copy(self.mate, 3, self.mate).wait_recv()
        for n, tag in ((1, 4), (2, 5), (3, 6)):
            if tag not in tags:
                continue

            @pl.when(self.c >= n)
            def _():
                self.copy(self.mate - 2 * n, tag, self.mate).wait_recv()

    def drain(self, tags=range(7)):
        c = self.c
        conds = (c <= 2, (c >= 1) & (c <= 2), c == 0, c >= 0, c >= 1, c >= 2, c == 3)
        for tag in tags:
            @pl.when(conds[tag])
            def _():
                self.copy(self.me, tag, self.mate).wait_send()


def attn_body(nb, tok, seq, d, q_hbm, do_hbm, kvl_hbm, kv0_hbm, dy_hbm, dyp_hbm, cos_ref, sin_ref,
              o_hbm, dq_hbm, dkv_hbm, op_hbm, dqp_hbm, acc_hbm,
              kv_all, o_v, dq_v, mrecv, rrecv,
              kv_send, kv_recv, m_send, m_recv, r_send, r_recv, own_sem, in_sem, out_sem, fin_sem, p_send, p_recv, first_sem,
              ld_sem, b_sem, acc_sem):
    scale = d ** -0.5
    rows = o_v.shape[2] * tok
    n_blk = seq // 256
    rb = 2 * rows // n_blk
    n_rb = rows // rb
    half = d // 2
    me, k, mate, cw, ccw = ring_ids()
    c = me // 2
    rel = [lax.rem(c + o, 4) for o in (3, 1, 2, 0)]

    def blk(j):
        return pl.ds(pl.multiple_of(j * tok, 16), tok)

    def kvb(b, j):
        return kv_all.at[b, blk(j)]

    def gather(b):
        return Gather((me, k, mate, cw, ccw), c, lambda j: kvb(b, j), lambda t: kv_send.at[b - 1, t], lambda t: kv_recv.at[b - 1, t])

    def own(b):
        gather(b).own(kvl_hbm.at[b])

    def own_copy(b):
        return pltpu.make_async_copy(kvl_hbm.at[b], kvb(b, me), own_sem.at[b])

    def ready(b):
        own_copy(b).wait()

        @pl.when(b == 1)
        def _():
            gather(1).ready((4, 5, 6))

        @pl.when(b > 1)
        def _():
            gather(b).ready()

    def drain(b):
        @pl.when(b == 1)
        def _():
            gather(1).drain((1, 4, 5, 6))

        @pl.when(b > 1)
        def _():
            gather(b).drain()

    def m_copy(b, n):
        return rdma(kvb(b, 2 * n + 1 - k), mrecv.at[b, n], m_send.at[b, n], m_recv.at[b, n], mate)

    def r_copy(b, n, slot, to):
        return rdma(kvb(b, 2 * n + k), rrecv.at[b, slot], r_send.at[b, slot], r_recv.at[b, slot], to)

    def add_into(b, n, other):
        v = kv_all[b, blk(2 * n + k), :].astype(F32) + other[...].astype(F32)
        kv_all[b, blk(2 * n + k), :] = v.astype(BF16)

    def fin_copy(b):
        return pltpu.make_async_copy(kvb(b, me), dkv_hbm.at[b], fin_sem.at[b])

    def to_mate(b):
        for n in range(4):
            @pl.when(c >= n)
            def _():
                m_copy(b, n).start()

    def stage1(b):
        for n in range(4):
            @pl.when(c >= n)
            def _():
                m_copy(b, n).wait()
                add_into(b, n, mrecv.at[b, n])

        @pl.when(c == 3)
        def _():
            r_copy(b, 1, 2, ccw).start()
            r_copy(b, 2, 1, ccw).start()
            r_copy(b, 0, 0, cw).start()
            fin_copy(b).start()

        @pl.when(c == 2)
        def _():
            r_copy(b, 0, 1, ccw).start()

    def stage2(b):
        @pl.when(c == 2)
        def _():
            r_copy(b, 1, 2, ccw).wait_recv()
            add_into(b, 1, rrecv.at[b, 2])
            r_copy(b, 1, 2, ccw).start()
            r_copy(b, 2, 1, ccw).wait_recv()
            add_into(b, 2, rrecv.at[b, 1])
            fin_copy(b).start()

        @pl.when(c == 1)
        def _():
            r_copy(b, 0, 1, ccw).wait_recv()
            add_into(b, 0, rrecv.at[b, 1])
            r_copy(b, 0, 1, ccw).start()

    def stage3(b):
        @pl.when(c == 0)
        def _():
            r_copy(b, 0, 0, cw).wait_recv()
            add_into(b, 0, rrecv.at[b, 0])
            r_copy(b, 0, 1, ccw).wait_recv()
            add_into(b, 0, rrecv.at[b, 1])
            fin_copy(b).start()

        @pl.when(c == 1)
        def _():
            r_copy(b, 1, 2, ccw).wait_recv()
            add_into(b, 1, rrecv.at[b, 2])
            fin_copy(b).start()

    def handed(dst, src, n, b, slot):
        return rdma(src.at[slot, 1 - k], dst.at[b], p_send.at[n, b], p_recv.at[n, b], mate)

    def store_o(b, slot):
        return (pltpu.make_async_copy(o_v.at[slot], o_hbm.at[b], out_sem.at[0, slot]), handed(op_hbm, o_v, 0, b, slot))

    def store_dq(b, slot):
        return (pltpu.make_async_copy(dq_v.at[slot], dq_hbm.at[b], out_sem.at[1, slot]), handed(dqp_hbm, dq_v, 1, b, slot))

    def stored(x):
        x[0].wait()
        x[1].wait_send()

    def attend(q_v, do_v, s_buf, m_buf, l_buf, p_buf, ds_buf, q_t, do_t, dk_t, dv_t, d_buf, cos4, sin4):
        def load(b, slot):
            return (pltpu.make_async_copy(q_hbm.at[b], q_v.at[slot], in_sem.at[0, slot]),
                    pltpu.make_async_copy(do_hbm.at[b], do_v.at[slot], in_sem.at[1, slot]))

        def scores(b, g, slot, i):
            w = min(512, seq)
            if (i * 256) % w:
                return
            cols = slice(i * 256, i * 256 + w)
            s = dot_nt(q_v[slot, g].reshape(rows, d), kv_all[b, cols, :d]) * (scale * LOG2E)
            col = lax.broadcasted_iota(jnp.int32, (tok, w), 1) + i * 256
            row = lax.broadcasted_iota(jnp.int32, (tok, w), 0) + me * tok
            s = jnp.concatenate([jnp.where(col <= row, s[j * tok:(j + 1) * tok], -1e30) for j in range(rows // tok)], axis=0)
            s_buf[g, :, cols] = s
            m = s[:, :128]
            for j in range(128, w, 128):
                m = jnp.maximum(m, s[:, j:j + 128])
            m_buf[...] = m if i == 0 else jnp.maximum(m_buf[...], m)

        parts = max(1, min(5, n_blk))
        part = [j * (rows // 16) // parts * 16 for j in range(parts + 1)] + [rows] * n_blk

        def softmax(g, i):
            for r in range(part[i], part[i + 1], 16):
                rs = slice(r, r + 16)
                m = jnp.max(m_buf[rs, :], axis=1, keepdims=True)
                l = None
                for j in range(0, seq, 128):
                    e = jnp.exp2(s_buf[g, rs, j:j + 128] - m)
                    s_buf[g, rs, j:j + 128] = e
                    l = e if l is None else l + e
                l_buf[g, rs, :] = jnp.broadcast_to(1.0 / jnp.sum(l, axis=1, keepdims=True), (16, 128))

        def turn(g, slot, i):
            rs = slice(i * rb, (i + 1) * rb)
            q_t[g, :, rs] = q_v[slot, g].reshape(rows, d)[rs].T
            do_t[g, :, rs] = do_v[slot, g].reshape(rows, d)[rs].T

        def out_rows(b, g, slot, i):
            rs = slice(i * rb, (i + 1) * rb)
            p = (s_buf[g, rs, :] * jnp.concatenate([l_buf[g, rs, :]] * (seq // 128), axis=1)).astype(BF16)
            p_buf[rs, :] = p
            o = dot_nn(p, kv_all[b, :, d:])
            dvec = jnp.sum(o * do_v[slot, g].reshape(rows, d)[rs].astype(F32), axis=1, keepdims=True)
            d_buf[rs, :] = jnp.broadcast_to(dvec, (rb, 128))
            put_rows(o_v, slot, g, i, o.astype(BF16))

        def put_rows(ref, slot, g, i, v):
            r = i * rb
            while r < (i + 1) * rb:
                n = min((i + 1) * rb - r, tok - r % tok)
                ref[slot, g, r // tok, r % tok:r % tok + n, :] = v[r - i * rb:r - i * rb + n]
                r += n

        def dq_rows(b, g, slot, i):
            rs = slice(i * rb, (i + 1) * rb)
            dq = dot_nn(ds_buf[rs, :], kv_all[b, :, :d]) * scale
            lo, hi = dq[:, :half], dq[:, half:]
            cs, sn = cos4[rs, :], sin4[rs, :]
            put_rows(dq_v, slot, g, i, jnp.concatenate([(lo * cs + hi * sn).astype(BF16), (hi * cs - lo * sn).astype(BF16)], axis=1))

        def grads(b, g, slot, i):
            cols = slice(i * 256, (i + 1) * 256)
            do = do_v[slot, g].reshape(rows, d)
            p = p_buf[:, cols]
            dp = dot_nt(do, kv_all[b, cols, d:])
            dvec = d_buf[...]
            if i > 0 and part[i] > part[i - 1]:
                z = None
                for r in range(part[i - 1], part[i], 8):
                    v = l_buf[1 - g, r:r + 8, :]
                    z = v if z is None else jnp.minimum(z, v)
                dvec = dvec + jnp.concatenate([jnp.minimum(z, 0.0)] * (rows // 8), axis=0)
            dd = jnp.concatenate([dvec, dvec], axis=1)
            ds = (p.astype(F32) * (dp - dd)).astype(BF16)
            ds_buf[:, cols] = ds
            dk = dot_nn(q_t[g], ds)
            dv = dot_nn(do_t[g], p)
            if g == 0:
                dk_t[:, cols] = dk
                dv_t[:, cols] = dv
            else:
                dk_t[:, cols] += dk
                dv_t[:, cols] += dv

        def close_kv(b, i):
            cols = slice(i * 256, (i + 1) * 256)
            kv_all[b, cols, :d] = (dk_t[:, cols] * scale).T.astype(BF16)
            kv_all[b, cols, d:] = dv_t[:, cols].T.astype(BF16)

        enter((mate, cw, ccw))
        gather(1).pass_on(lambda j: kv0_hbm.at[1, blk(j)])
        for b in range(2, min(4, nb)):
            own(b)
        for x in load(0, 0):
            x.start()

        def first(j):
            return pltpu.make_async_copy(kv0_hbm.at[0, blk(j)], kvb(0, j), first_sem.at[j])

        def second(j, n):
            return pltpu.make_async_copy(kv0_hbm.at[1, blk(j)], kvb(1, j), first_sem.at[8 + n])
        arrived = ((c >= 0, mate, 0), (c >= 1, me - 2, 1), (c == 3, me - 6, 2))
        for j in range(8):
            @pl.when(j <= 2 * c + 1)
            def _():
                first(j).start()
        for b in range(1, nb):
            own_copy(b).start()
        for cond, j, i in arrived:
            @pl.when(cond)
            def _():
                second(j, i).start()

        @pl.loop(2 * c + 2, 8)
        def _(j):
            for b in range(nb):
                kv_all[b, blk(j), :] = jnp.zeros((tok, 2 * d), BF16)
        for j in range(rows // tok):
            cos4[j * tok:(j + 1) * tok, :] = cos_ref[...]
            sin4[j * tok:(j + 1) * tok, :] = sin_ref[...]
        ds_buf[...] = jnp.zeros_like(ds_buf)
        for x in load(0, 0):
            x.wait()
        for i in range(n_rb):
            turn(0, 0, i)
        for j in range(8):
            @pl.when(j <= 2 * c + 1)
            def _():
                first(j).wait()
        for cond, j, i in arrived:
            @pl.when(cond)
            def _():
                second(j, i).wait()
        for i in range(n_blk):
            scores(0, 0, 0, i)
        for i in range(n_blk):
            softmax(0, i)

        def comm_steps(b, steps):
            for lag, stage in steps:
                @pl.when(b >= lag)
                def _():
                    stage(b - lag)

        @pl.loop(0, nb)
        def _(b):
            slot = lax.rem(b, 2)
            nxt = jnp.minimum(b + 1, nb - 1)
            prev = jnp.maximum(b - 1, 0)

            @pl.when(b + 1 < nb)
            def _():
                for x in load(b + 1, 1 - slot):
                    x.start()

            @pl.when((b >= 1) & (b + 2 < nb))
            def _():
                gather(b + 2).forward()

            @pl.when(b + 4 < nb)
            def _():
                own(b + 4)

            @pl.when((b >= 1) & (b + 1 < nb))
            def _():
                gather(b + 1).last()
            comm_steps(b, ((3, stage2), (4, stage3)))

            @pl.when(b >= 2)
            def _():
                drain(b - 1)

            @pl.when(b >= 2)
            def _():
                stored(store_o(b - 2, slot))
            spare = jnp.where(b >= 1, b - 1, nb)
            for i in range(n_blk):
                scores(b, 1, slot, i)
                if i % 2 == 1:
                    out_rows(b, 0, slot, i // 2)
                    dq_rows(prev, 1, 1 - slot, i // 2)
                    turn(1, slot, i // 2)
            for i in range(n_blk):
                close_kv(spare, i)

            @pl.when(b >= 1)
            def _():
                for x in store_dq(b - 1, 1 - slot):
                    x.start()
                to_mate(b - 1)

            @pl.when(b == 0)
            def _():
                gather(1).last()
            for i in range(n_blk):
                grads(b, 0, slot, i)
                softmax(1, i)

            @pl.when(b + 1 < nb)
            def _():
                for x in load(b + 1, 1 - slot):
                    x.wait()
                ready(b + 1)
            if nb > 2:
                @pl.when(b == 0)
                def _():
                    gather(2).forward()

            @pl.when(b >= 2)
            def _():
                stored(store_dq(b - 2, slot))
            nslot = lax.rem(nxt, 2)
            for i in range(n_blk):
                scores(nxt, 0, nslot, i)
                if i % 2 == 1:
                    out_rows(b, 1, slot, i // 2)
                    dq_rows(b, 0, slot, i // 2)
                    turn(0, nslot, i // 2)
            for x in store_o(b, slot):
                x.start()
            comm_steps(b, ((1, stage1),))
            for i in range(n_blk):
                grads(b, 1, slot, i)
                softmax(0, i)

        drain(nb - 1)
        for i in range(n_rb):
            dq_rows(nb - 1, 1, (nb - 1) % 2, i)
        for i in range(n_blk):
            close_kv(nb - 1, i)
        for x in store_dq(nb - 1, (nb - 1) % 2):
            x.start()
        to_mate(nb - 1)

    slab = pltpu.VMEM((2, 2, rows // tok, tok, d), BF16)
    pl.run_scoped(attend, slab, slab, pltpu.VMEM((2, rows, seq), F32), pltpu.VMEM((rows, 128), F32), pltpu.VMEM((2, rows, 128), F32),
                  pltpu.VMEM((rows, seq), BF16), pltpu.VMEM((rows, seq), BF16), pltpu.VMEM((2, d, rows), BF16),
                  pltpu.VMEM((2, d, rows), BF16), pltpu.VMEM((d, seq), F32), pltpu.VMEM((d, seq), F32),
                  pltpu.VMEM((rows, 128), F32), pltpu.VMEM((rows, half), F32), pltpu.VMEM((rows, half), F32))
    n = nb

    def first_products(big, a_v, at, acc_v):
        pr = Products(big, a_v, at, ld_sem, b_sem)
        for x in pr.load_b(dy_hbm, dyp_hbm):
            x.start()
        for b in (n - 2, n - 1):
            stored(store_o(b, b % 2))
        for b in range(n):
            handed(op_hbm, o_v, 0, b, b % 2).wait_recv()

        def fetch(r):
            return pr.load_a(r, o_hbm.at[:, k, rel[r]], op_hbm.at[:, rel[r]])

        def save(r):
            return pltpu.make_async_copy(acc_v.at[r], acc_hbm.at[r], acc_sem.at[r])
        for r in range(2):
            for x in fetch(r):
                x.start()

        todo = [((stage2, n - 3), (stage3, n - 4)), ((stage1, n - 1), (stage2, n - 2), (stage3, n - 3)),
                ((stage2, n - 1), (stage3, n - 2)), ((stage3, n - 1),)]

        def steps(i):
            for stage, b in todo[i]:
                if b >= 0:
                    stage(b)
        steps(0)
        steps(1)
        for r in range(4):
            for x in fetch(r):
                x.wait()
            pr.turn(0, a_v.at[r % 2, 0])
            pr.turn(1, a_v.at[r % 2, 1])
            if r + 2 < 4:
                for x in fetch(r + 2):
                    x.start()
            if r == 0:
                for x in pr.load_b(dy_hbm, dyp_hbm):
                    x.wait()
            pr.columns(acc_v.at[r], 0, 4)
            save(r).start()
            if r % 2 == 1:
                steps(2 + r // 2)
        for r in range(4):
            save(r).wait()

    pl.run_scoped(first_products, pltpu.VMEM((2,) + dy_hbm.shape, BF16), pltpu.VMEM((2, 2, nb, tok, d), BF16),
                  pltpu.VMEM((2, d, nb * tok), BF16), pltpu.VMEM((4, 2, d, dy_hbm.shape[1] // 2), F32))
    for b in (n - 2, n - 1):
        stored(store_dq(b, b % 2))
    for b in range(n):
        handed(dqp_hbm, dq_v, 1, b, b % 2).wait_recv()
        fin_copy(b).wait()
        for cond, slot in ((c == 3, 0), (c >= 1, 1), (c >= 2, 2)):
            @pl.when(cond)
            def _():
                r_copy(b, 0, slot, cw).wait_send()


def attention(q, do, kv, kv0, dy, dy_p, cos_t, sin_t):
    nb, _, hp, tok, d = q.shape
    seq = tok * 8
    rows = hp * tok
    any_spec = pl.BlockSpec(memory_space=pl.ANY)
    vmem = pl.BlockSpec(memory_space=pltpu.VMEM)
    dma = pltpu.SemaphoreType.DMA
    slab = pltpu.VMEM((2, 2, hp, tok, d), BF16)
    out = jax.ShapeDtypeStruct(q.shape, BF16)
    outp = jax.ShapeDtypeStruct((nb, hp, tok, d), BF16)
    return pl.pallas_call(
        functools.partial(attn_body, nb, tok, seq, d),
        in_specs=[any_spec] * 6 + [vmem, vmem],
        out_specs=[any_spec] * 6,
        out_shape=[out, out, jax.ShapeDtypeStruct(kv.shape, BF16), outp, outp,
                   jax.ShapeDtypeStruct((4, 2, d, dy.shape[1] // 2), F32)],
        scratch_shapes=[pltpu.VMEM((nb + 1, seq, 2 * d), BF16), slab, slab,
                        pltpu.VMEM((nb, 4, tok, 2 * d), BF16), pltpu.VMEM((nb, 3, tok, 2 * d), BF16),
                        dma((nb - 1, 7)), dma((nb - 1, 7)), dma((nb, 4)), dma((nb, 4)), dma((nb, 3)), dma((nb, 3)),
                        dma((nb,)), dma((2, 2)), dma((2, 2)), dma((nb,)), dma((2, nb)), dma((2, nb)), dma((11,)),
                        dma((2, 2)), dma((2,)), dma((4,))],
        compiler_params=pltpu.CompilerParams(collective_id=1, has_side_effects=True, vmem_limit_bytes=63 * 2**20),
        cost_estimate=pl.CostEstimate(flops=24 * nb * rows * seq * d, bytes_accessed=40 * 2**20,
                                      transcendentals=2 * nb * rows * seq),
        name="attention",
    )(q, do, kv, kv0, dy, dy_p, cos_t, sin_t)


def proj_body(nb, tok, x_hbm, g_ref, wq_hbm, wk_ref, wv_ref, wo_hbm, dy_hbm, cos_ref, sin_ref,
              kv0_hbm, hn_hbm, q_hbm, do_hbm, kv_hbm, wqf_hbm, wof_hbm, hnp_hbm, dyp_hbm,
              x_v, hn_v, dy_v, wq_v, wo_v, kv_v, out_v,
              send, recv, x_sem, dy_sem, own_sem, out_sem, misc_sem, w_sem, p_send, p_recv, kv_send, kv_recv):
    n_tok, e = x_hbm.shape
    d = kv_v.shape[1] // 2
    half = d // 2
    mc = 2 * tok
    me, k, mate, cw, ccw = ring_ids()
    base = 2 * (me // 2)

    def head(off, par):
        return lax.rem(base + 2 * off + 8, 8) + par
    enter((mate, cw, ccw))

    fulls = (wq_v, wo_v)
    locs = (wq_hbm, wo_hbm)

    def half_of(w, ref, j):
        n = ref.shape[0] // 2
        return ref.at[pl.ds(j * n, n)]

    sends = []

    def send_full(w, h, j, to, own=False):
        src = locs[w] if own else fulls[w].at[h]
        c = rdma(src, fulls[w].at[h], send.at[w, j], recv.at[w, j], to)
        c.start()
        sends.append(c)

    def send_half(w, h, part, j, to):
        c = rdma(half_of(w, fulls[w].at[h], part), half_of(w, fulls[w].at[h], part), send.at[w, j], recv.at[w, j], to)
        c.start()
        sends.append(c)

    def wait_full(w, h, j):
        rdma(fulls[w].at[h], fulls[w].at[h], send.at[w, j], recv.at[w, j], mate).wait_recv()

    def wait_half(w, h, part, j):
        ref = half_of(w, fulls[w].at[h], part)
        rdma(ref, ref, send.at[w, j], recv.at[w, j], mate).wait_recv()

    for w in range(2):
        send_full(w, me, 0, cw, True)
        send_full(w, me, 1, ccw, True)
        send_full(w, me, 4, mate, True)
    own = [pltpu.make_async_copy(locs[w], fulls[w].at[me], own_sem.at[w]) for w in range(2)]
    xs = [pltpu.make_async_copy(x_hbm.at[pl.ds(b * tok, tok)], x_v.at[pl.ds(b * tok, tok)], x_sem.at[b]) for b in range(nb)]
    for c in xs:
        c.start()
    for c in own:
        c.start()
    dyc = pltpu.make_async_copy(dy_hbm, dy_v, dy_sem)
    dyc.start()

    gain = g_ref[...].astype(F32)
    for b in range(nb):
        xs[b].wait()

        @pl.loop(0, tok // 16, unroll=2)
        def _(r):
            rs = pl.ds(pl.multiple_of(b * tok + r * 16, 16), 16)
            x = x_v[rs, :].astype(F32)
            c = x - jnp.mean(x, axis=1, keepdims=True)
            inv = lax.rsqrt(jnp.mean(c * c, axis=1, keepdims=True) + LN_EPS)
            hn_v[rs, :] = (c * inv * gain).astype(BF16)
    hn_out = pltpu.make_async_copy(hn_v, hn_hbm, misc_sem.at[0])
    hn_out.start()
    to_mate = [rdma(hn_v, hnp_hbm, p_send.at[0], p_recv.at[0], mate), rdma(dy_hbm, dyp_hbm, p_send.at[1], p_recv.at[1], mate)]
    for c in to_mate:
        c.start()

    def rope_rows(raw):
        lo, hi = raw[:, :half], raw[:, half:d]
        cs, sn = jnp.concatenate([cos_ref[...]] * 2, axis=0), jnp.concatenate([sin_ref[...]] * 2, axis=0)
        return lo * cs - hi * sn, hi * cs + lo * sn

    @pl.loop(0, n_tok // mc)
    def _(i):
        rs = pl.ds(pl.multiple_of(i * mc, mc), mc)
        lo, hi = rope_rows(dot_nn(hn_v[rs, :], wk_ref[...]))
        kv_v[rs, :half] = lo.astype(BF16)
        kv_v[rs, half:d] = hi.astype(BF16)
        kv_v[rs, d:] = dot_nn(hn_v[rs, :], wv_ref[...]).astype(BF16)
    kv_out = pltpu.make_async_copy(kv_v, kv_hbm, misc_sem.at[1])
    kv_out.start()

    outs = []
    saves = []

    def save(w, h):
        c = pltpu.make_async_copy(fulls[w].at[h], (wqf_hbm, wof_hbm)[w].at[h], w_sem.at[len(saves)])
        c.start()
        saves.append(c)

    def project(w, h):
        slot = len(outs) % 4
        if len(outs) >= 4:
            outs[-4].wait()

        @pl.loop(0, n_tok // mc)
        def _(i):
            rs = pl.ds(pl.multiple_of(i * mc, mc), mc)
            if w == 0:
                lo, hi = rope_rows(dot_nn(hn_v[rs, :], wq_v[h]))
                o0 = lo.reshape(2, tok, half).astype(BF16)
                o1 = hi.reshape(2, tok, half).astype(BF16)
                out_v[slot, pl.ds(2 * i, 2), :, :half] = o0
                out_v[slot, pl.ds(2 * i, 2), :, half:] = o1
            else:
                out_v[slot, pl.ds(2 * i, 2)] = dot_nt(dy_v[rs, :], wo_v[h]).reshape(2, tok, d).astype(BF16)
        c = pltpu.make_async_copy(out_v.at[slot], (q_hbm, do_hbm)[w].at[:, lax.rem(h, 2), h // 2], out_sem.at[slot])
        c.start()
        outs.append(c)
        save(w, h)

    other = 1 - k
    for w in range(2):
        own[w].wait()
        if w == 1:
            dyc.wait()
        project(w, me)
        wait_full(w, mate, 4)
        project(w, mate)
    for w in range(2):
        wait_full(w, head(-1, k), 0)
        send_half(w, head(-1, k), 0, 2, cw)
        wait_full(w, head(1, k), 1)
        send_half(w, head(1, k), 1, 3, ccw)
        send_full(w, head(-1, k), 5, mate)
        send_full(w, head(1, k), 6, mate)
        project(w, head(-1, k))
        project(w, head(1, k))
        wait_full(w, head(-1, other), 5)
        project(w, head(-1, other))
        wait_full(w, head(1, other), 6)
        project(w, head(1, other))

    def early(n):
        def blk(j):
            return kv0_hbm.at[n, pl.ds(pl.multiple_of(j * tok, 16), tok)]
        return Gather((me, k, mate, cw, ccw), me // 2, blk, lambda t: kv_send.at[n, t], lambda t: kv_recv.at[n, t])
    first, second = early(0), early(1)
    first.own(kv_v.at[pl.ds(0, tok)])
    own0 = pltpu.make_async_copy(kv_v.at[pl.ds(0, tok)], first.block(me), misc_sem.at[2])
    own0.start()
    for w in range(2):
        wait_half(w, head(2, k), 0, 2)
        send_half(w, head(2, k), 0, 7, mate)
        wait_half(w, head(2, k), 1, 3)
        send_half(w, head(2, k), 1, 8, mate)
        project(w, head(2, k))
        if w == 1:
            first.forward()
            second.own(kv_v.at[pl.ds(tok, tok)])
        wait_half(w, head(2, other), 0, 7)
        wait_half(w, head(2, other), 1, 8)
        project(w, head(2, other))
    first.last()
    for c in outs[-4:] + saves + [hn_out, kv_out, own0]:
        c.wait()
    first.ready()
    first.drain()
    second.arrived()
    second.ready((3,))
    second.drain((0, 2, 3))
    for c in sends:
        c.wait_send()
    for c in to_mate:
        c.wait()


def project(x, gain, wq, w_k, w_v, wo, dy, cos_t, sin_t):
    nb, tok, e = x.shape
    d = wq.shape[1]
    n_heads = 8
    n_tok = nb * tok
    any_spec = pl.BlockSpec(memory_space=pl.ANY)
    vmem = pl.BlockSpec(memory_space=pltpu.VMEM)
    act = jax.ShapeDtypeStruct((nb, 2, n_heads // 2, tok, d), BF16)
    dma = pltpu.SemaphoreType.DMA
    flops = 2 * n_tok * e * (2 * n_heads + 2) * d
    kv0, hn, q, do, kv, wqf, wof, hn_p, dy_p = pl.pallas_call(
        functools.partial(proj_body, nb, tok),
        in_specs=[any_spec, vmem, any_spec, vmem, vmem, any_spec, any_spec, vmem, vmem],
        out_specs=[any_spec] * 9,
        out_shape=[jax.ShapeDtypeStruct((2, tok * n_heads, 2 * d), BF16), jax.ShapeDtypeStruct((n_tok, e), BF16), act, act, jax.ShapeDtypeStruct((n_tok, 2 * d), BF16),
                   jax.ShapeDtypeStruct((n_heads, e, d), BF16), jax.ShapeDtypeStruct((n_heads, d, e), BF16),
                   jax.ShapeDtypeStruct((n_tok, e), BF16), jax.ShapeDtypeStruct((n_tok, e), BF16)],
        scratch_shapes=[pltpu.VMEM((n_tok, e), BF16), pltpu.VMEM((n_tok, e), BF16), pltpu.VMEM((n_tok, e), BF16),
                        pltpu.VMEM((n_heads, e, d), BF16), pltpu.VMEM((n_heads, d, e), BF16),
                        pltpu.VMEM((n_tok, 2 * d), BF16), pltpu.VMEM((4, nb, tok, d), BF16),
                        dma((2, 9)), dma((2, 9)), dma((nb,)), dma(()), dma((2,)), dma((4,)), dma((3,)), dma((16,)), dma((2,)), dma((2,)), dma((2, 7)), dma((2, 7))],
        compiler_params=pltpu.CompilerParams(collective_id=0, has_side_effects=True, vmem_limit_bytes=60 * 2**20),
        cost_estimate=pl.CostEstimate(flops=flops, bytes_accessed=60 * 2**20, transcendentals=0),
        name="project",
    )(x.reshape(n_tok, e), gain, wq, w_k, w_v, wo, dy.reshape(n_tok, e), cos_t, sin_t)
    return kv0, hn, q, do, kv.reshape(nb, tok, 2 * d), wqf, wof, hn_p, dy_p


def grads_body(nb, tok, o_hbm, acc_hbm, dq_hbm, dqp_hbm, hn_hbm, hnp_hbm, dy_hbm, dkv_hbm,
               wq_hbm, wo_hbm, wk_hbm, wv_hbm, x_hbm, g_ref, cos_ref, sin_ref,
               y_hbm, gx_hbm, gln_ref, gwo_ref, gwq_ref, gkv_hbm,
               acc, acc_kv, rbuf, rbuf_kv, kind, kp, dkv_v, fin_kv, gln_acc, gl_recv,
               rs_send, rs_recv, kv_send, kv_recv, ag_send, ag_recv, gl_send, gl_rsem, kp_sem, ld_sem, b_sem, t_sem, a_sem):
    n_tok, e = x_hbm.shape
    d = wk_hbm.shape[1]
    half = d // 2
    eh, eq = e // 2, e // 4
    me, k, mate, cw, ccw = ring_ids()
    c = me // 2
    rel = [lax.rem(c + o, 4) for o in (3, 1, 2, 0)]
    enter([lax.rem(me + o, 8) for o in range(1, 8)])

    order = ((2, 1), (2, 0))

    def hop(s, dr, j):
        first = acc_hbm.at[dr, dr] if s == 0 else acc.at[s, dr, dr]
        src = first if j == 0 else rbuf.at[s, dr, j - 1]
        return rdma(src, rbuf.at[s, dr, j], rs_send.at[s, dr, j], rs_recv.at[s, dr, j], (cw, ccw)[dr])

    def hop_kv(dr, j):
        src = acc_kv.at[dr, dr] if j == 0 else rbuf_kv.at[dr, j - 1]
        return rdma(src, rbuf_kv.at[dr, j], kv_send.at[dr, j], kv_recv.at[dr, j], (cw, ccw)[dr])

    def add(dst, term):
        @pl.loop(0, dst.shape[0] // 32)
        def _(i):
            rs = pl.ds(pl.multiple_of(i * 32, 32), 32)
            dst[rs, :] = dst[rs, :] + term[rs, :]

    def pass_on(s, j):
        for dr in range(2):
            hop(s, dr, j - 1).wait_recv()
            add(rbuf.at[s, dr, j - 1], acc.at[s, order[dr][j - 1], dr])
            hop(s, dr, j).start()

    def pass_on_kv(j):
        for dr in range(2):
            hop_kv(dr, j - 1).wait_recv()
            add(rbuf_kv.at[dr, j - 1], acc_kv.at[order[dr][j - 1], dr])
            hop_kv(dr, j).start()

    def finish(s, out):
        for dr in range(2):
            hop(s, dr, 2).wait_recv()

            @pl.loop(0, d // 32)
            def _(i):
                rs = pl.ds(pl.multiple_of(i * 32, 32), 32)
                out[rs, dr * eh:(dr + 1) * eh] = (rbuf[s, dr, 2, rs, :] + acc[s, 3, dr, rs, :]).astype(BF16)

    def piece(kk, j, lo=0, n=None):
        return gkv_hbm.at[kk, pl.ds(lo, d if n is None else n), pl.ds(pl.multiple_of(j * eq, 128), eq)]

    def ag(tag, ref, to, src=None):
        return rdma(ref if src is None else src, ref, ag_send.at[tag], ag_recv.at[tag], to)

    def ag_far(tag, to):
        return ag(tag, piece(k, rel[(0, 1)[tag - 3]], (tag - 3) * half, half), to)

    own_piece = pltpu.make_async_copy(fin_kv, piece(k, c), t_sem.at[5])

    def finish_kv():
        for dr in range(2):
            hop_kv(dr, 2).wait_recv()
            fin_kv[:, dr * (eq // 2):(dr + 1) * (eq // 2)] = rbuf_kv[dr, 2] + acc_kv[3, dr]
        ag(0, piece(k, c), cw, fin_kv).start()
        ag(1, piece(k, c), ccw, fin_kv).start()
        ag(2, piece(k, c), mate, fin_kv).start()
        own_piece.start()

    def ag_forward():
        ag(0, piece(k, rel[0]), cw).wait_recv()
        ag_far(3, cw).start()
        ag(1, piece(k, rel[1]), cw).wait_recv()
        ag_far(4, ccw).start()
        ag(5, piece(k, rel[0]), mate).start()
        ag(6, piece(k, rel[1]), mate).start()

    def ag_last():
        far = [piece(k, rel[2], i * half, half) for i in range(2)]
        for i in range(2):
            ag(3 + i, far[i], cw).wait_recv()
            ag(7 + i, far[i], mate).start()
        ag(2, piece(1 - k, c), mate).wait_recv()
        ag(5, piece(1 - k, rel[0]), mate).wait_recv()
        ag(6, piece(1 - k, rel[1]), mate).wait_recv()
        for i in range(2):
            ag(7 + i, piece(1 - k, rel[2], i * half, half), mate).wait_recv()
        for tag in range(3):
            ag(tag, piece(k, c), cw, fin_kv).wait_send()
        for tag in (3, 4, 7, 8):
            ag(tag, far[0], cw).wait_send()
        for tag in (5, 6):
            ag(tag, piece(k, c), cw).wait_send()
        own_piece.wait()

    dkv_in = pltpu.make_async_copy(dkv_hbm, dkv_v, t_sem.at[4])
    dkv_in.start()
    kp_copy = rdma(kind.at[1 - k], kp, kp_sem.at[0], kp_sem.at[1], mate)

    for dr in range(2):
        hop(0, dr, 0).start()
    acc_in = [pltpu.make_async_copy(acc_hbm.at[r], acc.at[0, r], a_sem.at[r]) for r in range(4)]
    for r in (2, 1, 0, 3):
        acc_in[r].start()

    def products(big, a_v, at):
        pr = Products(big, a_v, at, ld_sem, b_sem)
        hn_in = pr.load_b(hn_hbm, hnp_hbm)

        def fetch(r):
            return pr.load_a(r, dq_hbm.at[:, k, rel[r]], dqp_hbm.at[:, rel[r]])
        dkv_in.wait()
        for b in range(nb):
            lo, hi = dkv_v[b, :, :half].astype(F32), dkv_v[b, :, half:d].astype(F32)
            cs, sn = cos_ref[...], sin_ref[...]
            kind[0, b, :, :half] = (lo * cs + hi * sn).astype(BF16)
            kind[0, b, :, half:] = (hi * cs - lo * sn).astype(BF16)
            kind[1, b] = dkv_v[b, :, d:]
        kp_copy.start()
        for x in hn_in:
            x.start()
        for r in range(2):
            for x in fetch(r):
                x.start()
        pr.turn(0, kind.at[k])
        for x in hn_in:
            x.wait()
        kp_copy.wait_recv()
        pr.turn(1, kp)
        for r in range(4):
            for dr in range(2):
                acc_kv[r, dr] = pr.both(pl.ds(pl.multiple_of(rel[r] * eq + dr * (eq // 2), 128), eq // 2))
        for dr in range(2):
            hop_kv(dr, 0).start()
        for r in range(4):
            for x in fetch(r):
                x.wait()
            pr.turn(0, a_v.at[r % 2, 0])
            pr.turn(1, a_v.at[r % 2, 1])
            if r + 2 < 4:
                for x in fetch(r + 2):
                    x.start()
            if r < 2:
                pr.columns(acc.at[1, r], 0, 2, 2 * r)
                hop(1, r, 0).start()
                pr.columns(acc.at[1, r], 2, 4, 2 * r)
            else:
                pr.columns(acc.at[1, r], 0, 4)

    pl.run_scoped(products, pltpu.VMEM((2, n_tok, e), BF16), pltpu.VMEM((2, 2, nb, tok, d), BF16), pltpu.VMEM((2, d, n_tok), BF16))
    for r in range(4):
        acc_in[r].wait()
    pass_on(0, 1)
    pass_on_kv(1)

    mc = 2 * tok
    units = nb // 2

    def attn_out(wo_v, o_v, x_v, y_v):
        w_in = pltpu.make_async_copy(wo_hbm, wo_v, b_sem.at[0])
        w_in.start()

        def load(u):
            return (pltpu.make_async_copy(o_hbm.at[pl.ds(2 * u, 2)], o_v.at[u % 2], ld_sem.at[u % 2, 0]),
                    pltpu.make_async_copy(x_hbm.at[pl.ds(u * mc, mc)], x_v.at[u % 2], ld_sem.at[u % 2, 1]))

        def put(u):
            return pltpu.make_async_copy(y_v.at[u % 2], y_hbm.at[pl.ds(u * mc, mc)], t_sem.at[u % 2])
        for x in load(0):
            x.start()
        w_in.wait()
        for u in range(units):
            if u + 1 < units:
                for x in load(u + 1):
                    x.start()
            for x in load(u):
                x.wait()
            if u >= 2:
                put(u - 2).wait()
            sl = u % 2

            @pl.loop(0, 4)
            def _(n):
                cols = pl.ds(pl.multiple_of(n * eq, 128), eq)
                o_rows = jnp.concatenate([jnp.concatenate([o_v[sl, i, h % 2, h // 2] for h in range(8)], axis=1) for i in range(2)], axis=0)
                r = dot_nn(o_rows, wo_v[:, cols])
                y_v[sl, :, cols] = (x_v[sl, :, cols].astype(F32) + r).astype(BF16)
            put(u).start()
        for u in range(max(0, units - 2), units):
            put(u).wait()

    pl.run_scoped(attn_out, pltpu.VMEM((8 * d, e), BF16), pltpu.VMEM((2, 2, 2, 4, tok, d), BF16),
                  pltpu.VMEM((2, mc, e), BF16), pltpu.VMEM((2, mc, e), BF16))
    pass_on(1, 1)

    def hidden_grad(wq_v, wk_v, wv_v, dq_v, x_v, dy_v, dh, gx_v):
        w_in = pltpu.make_async_copy(wq_hbm, wq_v, b_sem.at[0])
        w_in.start()
        w2_in = (pltpu.make_async_copy(wk_hbm, wk_v, b_sem.at[1]), pltpu.make_async_copy(wv_hbm, wv_v, ld_sem.at[1, 1]))
        for x in w2_in:
            x.start()

        def load(u):
            return (pltpu.make_async_copy(dq_hbm.at[pl.ds(2 * u, 2)], dq_v, ld_sem.at[0, 0]),
                    pltpu.make_async_copy(x_hbm.at[pl.ds(u * mc, mc)], x_v, ld_sem.at[0, 1]),
                    pltpu.make_async_copy(dy_hbm.at[pl.ds(u * mc, mc)], dy_v, ld_sem.at[1, 0]))

        def put(u):
            return pltpu.make_async_copy(gx_v, gx_hbm.at[pl.ds(u * mc, mc)], t_sem.at[0])
        gain = g_ref[...].astype(F32)
        gln_acc[...] = jnp.zeros_like(gln_acc)
        for x in load(0):
            x.start()
        w_in.wait()
        for x in w2_in:
            x.wait()
        for u in range(units):
            for x in load(u):
                x.wait()

            @pl.loop(0, 4)
            def _(n):
                rows = pl.ds(pl.multiple_of(n * eq, 128), eq)
                t = None
                for h in range(8):
                    a = jnp.concatenate([dq_v[i, h % 2, h // 2] for i in range(2)], axis=0)
                    p = dot_nt(a, wq_v[h, rows, :])
                    t = p if t is None else t + p
                for j in range(2):
                    a = jnp.concatenate([kind[j, 2 * u + i] for i in range(2)], axis=0)
                    t = t + dot_nt(a, (wk_v, wv_v)[j][rows, :])
                dh[:, rows] = t
            if u >= 1:
                put(u - 1).wait()

            @pl.loop(0, mc // 16)
            def _(r):
                rs = pl.ds(pl.multiple_of(r * 16, 16), 16)
                x = x_v[rs, :].astype(F32)
                cx = x - jnp.mean(x, axis=1, keepdims=True)
                inv = lax.rsqrt(jnp.mean(cx * cx, axis=1, keepdims=True) + LN_EPS)
                xh = cx * inv
                g = dh[rs, :]
                pr = g * xh
                gln_acc[...] += pr[:8] + pr[8:]
                gh = g * gain
                m1 = jnp.mean(gh, axis=1, keepdims=True)
                m2 = jnp.mean(gh * xh, axis=1, keepdims=True)
                gx_v[rs, :] = (inv * (gh - m1 - xh * m2) + dy_v[rs, :].astype(F32)).astype(BF16)
            put(u).start()
            if u + 1 < units:
                for x in load(u + 1):
                    x.start()
            if u == units // 2 - 1:
                pass_on(0, 2)
                pass_on_kv(2)
        put(units - 1).wait()

    pl.run_scoped(hidden_grad, pltpu.VMEM((8, e, d), BF16), pltpu.VMEM((e, d), BF16), pltpu.VMEM((e, d), BF16), pltpu.VMEM((2, 2, 4, tok, d), BF16),
                  pltpu.VMEM((mc, e), BF16), pltpu.VMEM((mc, e), BF16), pltpu.VMEM((mc, e), F32), pltpu.VMEM((mc, e), BF16))
    gl_recv[me] = jnp.sum(gln_acc[...], axis=0, keepdims=True)
    pass_on(1, 2)
    finish(0, gwo_ref)
    finish_kv()
    gl = [rdma(gl_recv.at[me], gl_recv.at[me], gl_send.at[o - 1], gl_rsem.at[o - 1], lax.rem(me + o, 8)) for o in range(1, 8)]
    for x in gl:
        x.start()
    finish(1, gwq_ref)
    ag_forward()
    for o in range(1, 8):
        src = lax.rem(me + 8 - o, 8)
        rdma(gl_recv.at[src], gl_recv.at[src], gl_send.at[o - 1], gl_rsem.at[o - 1], mate).wait_recv()
    total = gl_recv[0]
    for i in range(1, 8):
        total = total + gl_recv[i]
    gln_ref[...] = total
    ag_last()
    for x in gl:
        x.wait_send()
    kp_copy.wait_send()
    for dr in range(2):
        for j in range(3):
            hop_kv(dr, j).wait_send()
            for s in range(2):
                hop(s, dr, j).wait_send()


def gradients(o, acc, dq, dq_p, hn, hn_p, dy, dkv, wqf, wof, w_k, w_v, x, gain, cos_t, sin_t):
    nb, tok, e = x.shape
    n_tok = nb * tok
    d = dq.shape[-1]
    any_spec = pl.BlockSpec(memory_space=pl.ANY)
    vmem = pl.BlockSpec(memory_space=pltpu.VMEM)
    dma = pltpu.SemaphoreType.DMA
    tokens = jax.ShapeDtypeStruct((n_tok, e), BF16)
    y, gx, gln, gwo, gwq_t, gkv_t = pl.pallas_call(
        functools.partial(grads_body, nb, tok),
        in_specs=[any_spec] * 13 + [vmem, vmem, vmem],
        out_specs=[any_spec, any_spec, vmem, vmem, vmem, any_spec],
        out_shape=[tokens, tokens, jax.ShapeDtypeStruct((1, e), F32), jax.ShapeDtypeStruct((d, e), BF16),
                   jax.ShapeDtypeStruct((d, e), BF16), jax.ShapeDtypeStruct((2, d, e), F32)],
        scratch_shapes=[pltpu.VMEM((2, 4, 2, d, e // 2), F32), pltpu.VMEM((4, 2, d, e // 8), F32),
                        pltpu.VMEM((2, 2, 3, d, e // 2), F32), pltpu.VMEM((2, 3, d, e // 8), F32),
                        pltpu.VMEM((2, nb, tok, d), BF16), pltpu.VMEM((nb, tok, d), BF16), pltpu.VMEM((nb, tok, 2 * d), BF16),
                        pltpu.VMEM((d, e // 4), F32), pltpu.VMEM((8, e), F32), pltpu.VMEM((8, 1, e), F32),
                        dma((2, 2, 3)), dma((2, 2, 3)), dma((2, 3)), dma((2, 3)), dma((9,)), dma((9,)), dma((7,)), dma((7,)),
                        dma((2,)), dma((2, 2)), dma((2,)), dma((6,)), dma((4,))],
        compiler_params=pltpu.CompilerParams(collective_id=2, has_side_effects=True, vmem_limit_bytes=63 * 2**20),
        cost_estimate=pl.CostEstimate(flops=10 * n_tok * e * e, bytes_accessed=120 * 2**20, transcendentals=0),
        name="gradients",
    )(o, acc, dq, dq_p, hn, hn_p, dy.reshape(n_tok, e), dkv, wqf, wof.reshape(8 * d, e), w_k, w_v, x.reshape(n_tok, e),
      gain, cos_t, sin_t)
    y, gx, gwq, gwk, gwv, gwo, gln = place(nb, y, gx, gwq_t, gkv_t, gwo, gln)
    return y.reshape(nb, tok, e), gx.reshape(nb, tok, e), gln.reshape(e), gwq, gwk, gwv, gwo


def place_body(y_in, gx_in, gq_in, gkv_in, go_in, gl_in, y, gx, gq, gk, gv, go, gl):
    y[...] = y_in[...]
    gx[...] = gx_in[...]
    gq[...] = gq_in[...].astype(F32).T.astype(BF16)
    gk[...] = gkv_in[0].T
    gv[...] = gkv_in[1].T
    go[...] = go_in[...]
    gl[...] = gl_in[...]


def place(steps, y, gx, gwq_t, gkv_t, gwo, gln):
    n_tok, e = y.shape
    d = gwo.shape[0]
    act = pl.BlockSpec((n_tok // steps, e), lambda i: (i, 0))
    cols = pl.BlockSpec((d, e // steps), lambda i: (0, i))
    turned = pl.BlockSpec((e // steps, d), lambda i: (i, 0))
    small = pl.BlockSpec((d // steps, e), lambda i: (i, 0))
    line = pl.BlockSpec((1, e), lambda i: (0, 0))
    return pl.pallas_call(
        place_body,
        grid=(steps,),
        in_specs=[act, act, cols, pl.BlockSpec((2, d, e // steps), lambda i: (0, 0, i)), small, line],
        out_specs=[act, act, turned, turned, turned, small, line],
        out_shape=[jax.ShapeDtypeStruct(y.shape, BF16), jax.ShapeDtypeStruct(y.shape, BF16), jax.ShapeDtypeStruct((e, d), BF16),
                   jax.ShapeDtypeStruct((e, d), F32), jax.ShapeDtypeStruct((e, d), F32), jax.ShapeDtypeStruct((d, e), BF16),
                   jax.ShapeDtypeStruct((1, e), F32)],
        compiler_params=pltpu.CompilerParams(dimension_semantics=("arbitrary",)),
        cost_estimate=pl.CostEstimate(flops=0, bytes_accessed=8 * y.size + 24 * gwo.size, transcendentals=0),
        name="place",
    )(y, gx, gwq_t, gkv_t, gwo, gln)


def solution(mesh):
    act_spec = P('dp', 'tp', None)

    def device_step(x_loc, ln_scale, wq_loc, w_k, w_v, wo_loc, dy_loc):
        n_batch, tok, model_dim = x_loc.shape
        d = w_k.shape[1]
        t0 = lax.axis_index('tp') * tok
        cos_t, sin_t = rope_tables(t0 + jnp.arange(tok), d)

        gain = ln_scale.reshape(1, model_dim)
        kv0, hn, q, do, kv_loc, wq_h, wo_h, hn_p, dy_p = project(x_loc, gain, wq_loc, w_k, w_v, wo_loc, dy_loc, cos_t, sin_t)
        o, dq, dkv_loc, o_p, dq_p, acc = attention(q, do, kv_loc, kv0, dy_loc.reshape(-1, model_dim), dy_p, cos_t, sin_t)
        return gradients(o, acc, dq, dq_p, hn, hn_p, dy_loc, dkv_loc, wq_h, wo_h, w_k, w_v, x_loc, gain, cos_t, sin_t)

    return jax.shard_map(device_step, mesh=mesh, in_specs=(act_spec, P(None), P(None, 'tp'), P(None, None), P(None, None), P('tp', None), act_spec), out_specs=(act_spec, act_spec, P('dp'), P('dp', 'tp'), P('dp', None), P('dp', None), P(('dp', 'tp'), None)), check_vma=False)
```

```python
import functools
import jax
import jax.numpy as jnp
from jax import lax
from jax.experimental import pallas as pl
from jax.experimental.pallas import tpu as pltpu
from jax.sharding import PartitionSpec as P

LN_EPS = 1e-6
ROPE_BASE = 10000.0
LOG2E = 1.4426950408889634
F32 = jnp.float32
BF16 = jnp.bfloat16


def rope_tables(positions, head_dim):
    half_dim = head_dim // 2
    inv_freq = ROPE_BASE ** (-2.0 * jnp.arange(half_dim, dtype=F32) / head_dim)
    angles = positions.astype(F32)[:, None] * inv_freq[None, :]
    return jnp.cos(angles), jnp.sin(angles)


def rotate(vectors, cos_t, sin_t):
    half_dim = vectors.shape[-1] // 2
    lo_half = vectors[..., :half_dim]
    hi_half = vectors[..., half_dim:]
    return jnp.concatenate([lo_half * cos_t - hi_half * sin_t, hi_half * cos_t + lo_half * sin_t], axis=-1)


def dot_nn(a, b):
    return lax.dot_general(a, b, (((1,), (0,)), ((), ())), preferred_element_type=F32)


def dot_nt(a, b):
    return lax.dot_general(a, b, (((1,), (1,)), ((), ())), preferred_element_type=F32)


def rdma(src, dst, send, recv, to):
    return pltpu.make_async_remote_copy(src_ref=src, dst_ref=dst, send_sem=send, recv_sem=recv,
                                        device_id={'tp': to}, device_id_type=pl.DeviceIdType.MESH)


def ring_ids():
    me = lax.axis_index('tp')
    k = lax.rem(me, 2)
    return me, k, me + 1 - 2 * k, lax.rem(me + 2, 8), lax.rem(me + 6, 8)


def enter(peers):
    barrier = pltpu.get_barrier_semaphore()
    for p in peers:
        pl.semaphore_signal(barrier, inc=1, device_id={'tp': p}, device_id_type=pl.DeviceIdType.MESH)
    pl.semaphore_wait(barrier, len(peers))


class Products:
    def __init__(self, big, a_v, at, ld_sem, b_sem):
        self.big, self.a_v, self.at, self.ld_sem, self.b_sem = big, a_v, at, ld_sem, b_sem
        self.nb, self.tok = a_v.shape[2], a_v.shape[3]
        self.eq = big.shape[2] // 4

    def load_b(self, own, other):
        return (pltpu.make_async_copy(own, self.big.at[0], self.b_sem.at[0]),
                pltpu.make_async_copy(other, self.big.at[1], self.b_sem.at[1]))

    def load_a(self, i, own, other):
        return (pltpu.make_async_copy(own, self.a_v.at[i % 2, 0], self.ld_sem.at[i % 2, 0]),
                pltpu.make_async_copy(other, self.a_v.at[i % 2, 1], self.ld_sem.at[i % 2, 1]))

    def turn(self, j, src):
        tok = self.tok
        for i in range(self.nb // 2):
            self.at[j, :, 2 * i * tok:(2 * i + 2) * tok] = jnp.concatenate([src[2 * i], src[2 * i + 1]], axis=0).T

    def both(self, cols):
        return dot_nn(self.at[0], self.big[0, :, cols]) + dot_nn(self.at[1], self.big[1, :, cols])

    def columns(self, dst, first, last, turned=0):
        eq = self.eq

        @pl.loop(first, last)
        def _(n):
            m = lax.rem(n + turned, 4)
            cols = pl.ds(pl.multiple_of(m * eq, 128), eq)
            dst[m // 2, :, pl.ds(pl.multiple_of(lax.rem(m, 2) * eq, 128), eq)] = self.both(cols)


class Gather:
    def __init__(self, ids, c, block, send, recv):
        self.me, _, self.mate, self.cw, self.ccw = ids
        self.c, self.block, self.send, self.recv = c, block, send, recv

    def copy(self, j, tag, to, src=None):
        ref = self.block(j)
        return rdma(ref if src is None else src, ref, self.send(tag), self.recv(tag), to)

    def own(self, src):
        @pl.when(self.c <= 2)
        def _():
            self.copy(self.me, 0, self.cw, src).start()

        @pl.when(self.c == 0)
        def _():
            self.copy(self.me, 2, self.ccw, src).start()
        self.copy(self.me, 3, self.mate, src).start()

    def arrived(self):
        @pl.when(self.c >= 1)
        def _():
            self.copy(self.me - 2, 0, self.cw).wait_recv()

        @pl.when(self.c == 3)
        def _():
            self.copy(self.me - 6, 2, self.ccw).wait_recv()

    def pass_on(self, src=lambda j: None):
        @pl.when(self.c >= 1)
        def _():
            @pl.when(self.c <= 2)
            def _():
                self.copy(self.me - 2, 1, self.cw, src(self.me - 2)).start()
            self.copy(self.me - 2, 4, self.mate, src(self.me - 2)).start()

        @pl.when(self.c == 3)
        def _():
            self.copy(self.me - 6, 6, self.mate, src(self.me - 6)).start()

    def forward(self):
        self.arrived()
        self.pass_on()

    def last(self):
        @pl.when(self.c >= 2)
        def _():
            self.copy(self.me - 4, 1, self.cw).wait_recv()
            self.copy(self.me - 4, 5, self.mate).start()

    def ready(self, tags=(3, 4, 5, 6)):
        if 3 in tags:
            self.copy(self.mate, 3, self.mate).wait_recv()
        for n, tag in ((1, 4), (2, 5), (3, 6)):
            if tag not in tags:
                continue

            @pl.when(self.c >= n)
            def _():
                self.copy(self.mate - 2 * n, tag, self.mate).wait_recv()

    def drain(self, tags=range(7)):
        c = self.c
        conds = (c <= 2, (c >= 1) & (c <= 2), c == 0, c >= 0, c >= 1, c >= 2, c == 3)
        for tag in tags:
            @pl.when(conds[tag])
            def _():
                self.copy(self.me, tag, self.mate).wait_send()


def attn_body(nb, tok, seq, d, q_hbm, do_hbm, kvl_hbm, kv0_hbm, dy_hbm, dyp_hbm,
              o_hbm, ds_hbm, k_hbm, dkv_hbm, op_hbm, acc_hbm,
              kv_all, o_v, mrecv, rrecv,
              kv_send, kv_recv, m_send, m_recv, r_send, r_recv, own_sem, in_sem, out_sem, fin_sem, p_send, p_recv, first_sem,
              ld_sem, b_sem, acc_sem):
    scale = d ** -0.5
    rows = o_v.shape[2] * tok
    n_blk = seq // 256
    rb = 2 * rows // n_blk
    n_rb = rows // rb
    me, k, mate, cw, ccw = ring_ids()
    c = me // 2
    rel = [lax.rem(c + o, 4) for o in (3, 1, 2, 0)]

    def blk(j):
        return pl.ds(pl.multiple_of(j * tok, 16), tok)

    def kvb(b, j):
        return kv_all.at[b, blk(j)]

    def gather(b):
        return Gather((me, k, mate, cw, ccw), c, lambda j: kvb(b, j), lambda t: kv_send.at[b - 1, t], lambda t: kv_recv.at[b - 1, t])

    def own(b):
        gather(b).own(kvl_hbm.at[b])

    def own_copy(b):
        return pltpu.make_async_copy(kvl_hbm.at[b], kvb(b, me), own_sem.at[b])

    def ready(b):
        own_copy(b).wait()

        @pl.when(b == 1)
        def _():
            gather(1).ready((4, 5, 6))

        @pl.when(b > 1)
        def _():
            gather(b).ready()

    def drain(b):
        @pl.when(b == 1)
        def _():
            gather(1).drain((1, 4, 5, 6))

        @pl.when(b > 1)
        def _():
            gather(b).drain()

    def m_copy(b, n):
        return rdma(kvb(b, 2 * n + 1 - k), mrecv.at[b, n], m_send.at[b, n], m_recv.at[b, n], mate)

    def r_copy(b, n, slot, to):
        return rdma(kvb(b, 2 * n + k), rrecv.at[b, slot], r_send.at[b, slot], r_recv.at[b, slot], to)

    def add_into(b, n, other):
        v = kv_all[b, blk(2 * n + k), :].astype(F32) + other[...].astype(F32)
        kv_all[b, blk(2 * n + k), :] = v.astype(BF16)

    def fin_copy(b):
        return pltpu.make_async_copy(kvb(b, me), dkv_hbm.at[b], fin_sem.at[b])

    def to_mate(b):
        for n in range(4):
            @pl.when(c >= n)
            def _():
                m_copy(b, n).start()

    def stage1(b):
        for n in range(4):
            @pl.when(c >= n)
            def _():
                m_copy(b, n).wait()
                add_into(b, n, mrecv.at[b, n])

        @pl.when(c == 3)
        def _():
            r_copy(b, 1, 2, ccw).start()
            r_copy(b, 2, 1, ccw).start()
            r_copy(b, 0, 0, cw).start()
            fin_copy(b).start()

        @pl.when(c == 2)
        def _():
            r_copy(b, 0, 1, ccw).start()

    def stage2(b):
        @pl.when(c == 2)
        def _():
            r_copy(b, 1, 2, ccw).wait_recv()
            add_into(b, 1, rrecv.at[b, 2])
            r_copy(b, 1, 2, ccw).start()
            r_copy(b, 2, 1, ccw).wait_recv()
            add_into(b, 2, rrecv.at[b, 1])
            fin_copy(b).start()

        @pl.when(c == 1)
        def _():
            r_copy(b, 0, 1, ccw).wait_recv()
            add_into(b, 0, rrecv.at[b, 1])
            r_copy(b, 0, 1, ccw).start()

    def stage3(b):
        @pl.when(c == 0)
        def _():
            r_copy(b, 0, 0, cw).wait_recv()
            add_into(b, 0, rrecv.at[b, 0])
            r_copy(b, 0, 1, ccw).wait_recv()
            add_into(b, 0, rrecv.at[b, 1])
            fin_copy(b).start()

        @pl.when(c == 1)
        def _():
            r_copy(b, 1, 2, ccw).wait_recv()
            add_into(b, 1, rrecv.at[b, 2])
            fin_copy(b).start()

    def handed(b, slot):
        return rdma(o_v.at[slot, 1 - k], op_hbm.at[b], p_send.at[b], p_recv.at[b], mate)

    def store_o(b, slot):
        return (pltpu.make_async_copy(o_v.at[slot], o_hbm.at[b], out_sem.at[slot]), handed(b, slot))

    def stored(x):
        x[0].wait()
        x[1].wait_send()

    def attend(q_v, do_v, s_buf, m_buf, l_buf, p_buf, ds_buf, q_t, do_t, dk_t, dv_t, d_buf):
        def load(b, slot):
            return (pltpu.make_async_copy(q_hbm.at[b], q_v.at[slot], in_sem.at[0, slot]),
                    pltpu.make_async_copy(do_hbm.at[b], do_v.at[slot], in_sem.at[1, slot]))

        def scores(b, g, slot, i):
            w = min(512, seq)
            if (i * 256) % w:
                return
            cols = slice(i * 256, i * 256 + w)
            s = dot_nt(q_v[slot, g].reshape(rows, d), kv_all[b, cols, :d]) * (scale * LOG2E)
            col = lax.broadcasted_iota(jnp.int32, (tok, w), 1) + i * 256
            row = lax.broadcasted_iota(jnp.int32, (tok, w), 0) + me * tok
            s = jnp.concatenate([jnp.where(col <= row, s[j * tok:(j + 1) * tok], -1e30) for j in range(rows // tok)], axis=0)
            s_buf[g, :, cols] = s
            m = s[:, :128]
            for j in range(128, w, 128):
                m = jnp.maximum(m, s[:, j:j + 128])
            m_buf[...] = m if i == 0 else jnp.maximum(m_buf[...], m)

        parts = max(1, min(5, n_blk))
        part = [j * (rows // 16) // parts * 16 for j in range(parts + 1)] + [rows] * n_blk

        def softmax(g, i):
            for r in range(part[i], part[i + 1], 16):
                rs = slice(r, r + 16)
                m = jnp.max(m_buf[rs, :], axis=1, keepdims=True)
                l = None
                for j in range(0, seq, 128):
                    e = jnp.exp2(s_buf[g, rs, j:j + 128] - m)
                    s_buf[g, rs, j:j + 128] = e
                    l = e if l is None else l + e
                l_buf[g, rs, :] = jnp.broadcast_to(1.0 / jnp.sum(l, axis=1, keepdims=True), (16, 128))

        def turn(g, slot, i):
            rs = slice(i * rb, (i + 1) * rb)
            q_t[g, :, rs] = q_v[slot, g].reshape(rows, d)[rs].T
            do_t[g, :, rs] = do_v[slot, g].reshape(rows, d)[rs].T

        def out_rows(b, g, slot, i):
            rs = slice(i * rb, (i + 1) * rb)
            p = (s_buf[g, rs, :] * jnp.concatenate([l_buf[g, rs, :]] * (seq // 128), axis=1)).astype(BF16)
            p_buf[rs, :] = p
            o = dot_nn(p, kv_all[b, :, d:])
            dvec = jnp.sum(o * do_v[slot, g].reshape(rows, d)[rs].astype(F32), axis=1, keepdims=True)
            d_buf[rs, :] = jnp.broadcast_to(dvec, (rb, 128))
            put_rows(o_v, slot, g, i, o.astype(BF16))

        def put_rows(ref, slot, g, i, v):
            r = i * rb
            while r < (i + 1) * rb:
                n = min((i + 1) * rb - r, tok - r % tok)
                ref[slot, g, r // tok, r % tok:r % tok + n, :] = v[r - i * rb:r - i * rb + n]
                r += n

        def ds_copy(b, g):
            return pltpu.make_async_copy(ds_buf, ds_hbm.at[b, g], out_sem.at[2])

        def k_copy(b):
            return pltpu.make_async_copy(kv_all.at[b, :, pl.ds(0, d)], k_hbm.at[b], out_sem.at[3])

        def grads(b, g, slot, i):
            cols = slice(i * 256, (i + 1) * 256)
            do = do_v[slot, g].reshape(rows, d)
            p = p_buf[:, cols]
            dp = dot_nt(do, kv_all[b, cols, d:])
            dvec = d_buf[...]
            if i > 0 and part[i] > part[i - 1]:
                z = None
                for r in range(part[i - 1], part[i], 8):
                    v = l_buf[1 - g, r:r + 8, :]
                    z = v if z is None else jnp.minimum(z, v)
                dvec = dvec + jnp.concatenate([jnp.minimum(z, 0.0)] * (rows // 8), axis=0)
            dd = jnp.concatenate([dvec, dvec], axis=1)
            ds = (p.astype(F32) * (dp - dd)).astype(BF16)
            ds_buf[:, cols] = ds
            dk = dot_nn(q_t[g], ds)
            dv = dot_nn(do_t[g], p)
            if g == 0:
                dk_t[:, cols] = dk
                dv_t[:, cols] = dv
            else:
                dk_t[:, cols] += dk
                dv_t[:, cols] += dv

        def close_kv(b, i):
            cols = slice(i * 256, (i + 1) * 256)
            kv_all[b, cols, :d] = (dk_t[:, cols] * scale).T.astype(BF16)
            kv_all[b, cols, d:] = dv_t[:, cols].T.astype(BF16)

        enter((mate, cw, ccw))
        gather(1).pass_on(lambda j: kv0_hbm.at[1, blk(j)])
        if nb > 2:
            own(2)
        for x in load(0, 0):
            x.start()

        def first(j):
            return pltpu.make_async_copy(kv0_hbm.at[0, blk(j)], kvb(0, j), first_sem.at[j])

        def second(j, n):
            return pltpu.make_async_copy(kv0_hbm.at[1, blk(j)], kvb(1, j), first_sem.at[8 + n])
        arrived = ((c >= 0, mate, 0), (c >= 1, me - 2, 1), (c == 3, me - 6, 2))
        for j in range(8):
            @pl.when(j <= 2 * c + 1)
            def _():
                first(j).start()
        for b in range(1, nb):
            own_copy(b).start()
        for cond, j, i in arrived:
            @pl.when(cond)
            def _():
                second(j, i).start()

        @pl.loop(2 * c + 2, 8)
        def _(j):
            for b in range(nb):
                kv_all[b, blk(j), :] = jnp.zeros((tok, 2 * d), BF16)
        for x in load(0, 0):
            x.wait()
        for i in range(n_rb):
            turn(0, 0, i)
        for j in range(8):
            @pl.when(j <= 2 * c + 1)
            def _():
                first(j).wait()
        for cond, j, i in arrived:
            @pl.when(cond)
            def _():
                second(j, i).wait()
        for i in range(n_blk):
            scores(0, 0, 0, i)
        for i in range(n_blk):
            softmax(0, i)

        def comm_steps(b, steps):
            for lag, stage in steps:
                @pl.when(b >= lag)
                def _():
                    stage(b - lag)

        @pl.loop(0, nb)
        def _(b):
            slot = lax.rem(b, 2)
            nxt = jnp.minimum(b + 1, nb - 1)

            @pl.when(b + 1 < nb)
            def _():
                for x in load(b + 1, 1 - slot):
                    x.start()

            @pl.when(b + 3 < nb)
            def _():
                own(b + 3)

            @pl.when((b >= 1) & (b + 2 < nb))
            def _():
                gather(b + 2).forward()

            @pl.when((b >= 1) & (b + 1 < nb))
            def _():
                gather(b + 1).last()
            comm_steps(b, ((3, stage2), (4, stage3)))

            @pl.when(b >= 2)
            def _():
                drain(b - 1)

            @pl.when(b >= 2)
            def _():
                stored(store_o(b - 2, slot))

            @pl.when(b >= 1)
            def _():
                k_copy(b - 1).wait()
            k_copy(b).start()
            spare = jnp.where(b >= 1, b - 1, nb)
            for i in range(n_blk):
                scores(b, 1, slot, i)
                if i % 2 == 1:
                    out_rows(b, 0, slot, i // 2)
                    turn(1, slot, i // 2)
            for i in range(n_blk):
                close_kv(spare, i)

            @pl.when(b >= 1)
            def _():
                to_mate(b - 1)
                ds_copy(b - 1, 1).wait()

            @pl.when(b == 0)
            def _():
                gather(1).last()
            for i in range(n_blk):
                grads(b, 0, slot, i)
                softmax(1, i)
            ds_copy(b, 0).start()

            @pl.when(b + 1 < nb)
            def _():
                for x in load(b + 1, 1 - slot):
                    x.wait()
                ready(b + 1)
            if nb > 2:
                @pl.when(b == 0)
                def _():
                    gather(2).forward()

            nslot = lax.rem(nxt, 2)
            for i in range(n_blk):
                scores(nxt, 0, nslot, i)
                if i % 2 == 1:
                    out_rows(b, 1, slot, i // 2)
                    turn(0, nslot, i // 2)
            for x in store_o(b, slot):
                x.start()
            comm_steps(b, ((1, stage1),))
            ds_copy(b, 0).wait()
            for i in range(n_blk):
                grads(b, 1, slot, i)
                softmax(0, i)
            ds_copy(b, 1).start()

        drain(nb - 1)
        k_copy(nb - 1).wait()
        for i in range(n_blk):
            close_kv(nb - 1, i)
        to_mate(nb - 1)
        ds_copy(nb - 1, 1).wait()

    slab = pltpu.VMEM((2, 2, rows // tok, tok, d), BF16)
    pl.run_scoped(attend, slab, slab, pltpu.VMEM((2, rows, seq), F32), pltpu.VMEM((rows, 128), F32), pltpu.VMEM((2, rows, 128), F32),
                  pltpu.VMEM((rows, seq), BF16), pltpu.VMEM((rows, seq), BF16), pltpu.VMEM((2, d, rows), BF16),
                  pltpu.VMEM((2, d, rows), BF16), pltpu.VMEM((d, seq), F32), pltpu.VMEM((d, seq), F32),
                  pltpu.VMEM((rows, 128), F32))
    n = nb

    def first_products(big, a_v, at, acc_v):
        pr = Products(big, a_v, at, ld_sem, b_sem)
        for x in pr.load_b(dy_hbm, dyp_hbm):
            x.start()
        for b in (n - 2, n - 1):
            stored(store_o(b, b % 2))
        for b in range(n):
            handed(b, b % 2).wait_recv()

        def fetch(r):
            return pr.load_a(r, o_hbm.at[:, k, rel[r]], op_hbm.at[:, rel[r]])

        def save(r):
            return pltpu.make_async_copy(acc_v.at[r], acc_hbm.at[r], acc_sem.at[r])
        for r in range(2):
            for x in fetch(r):
                x.start()

        todo = [((stage2, n - 3), (stage3, n - 4)), ((stage1, n - 1), (stage2, n - 2), (stage3, n - 3)),
                ((stage2, n - 1), (stage3, n - 2)), ((stage3, n - 1),)]

        def steps(i):
            for stage, b in todo[i]:
                if b >= 0:
                    stage(b)
        steps(0)
        steps(1)
        for r in range(4):
            for x in fetch(r):
                x.wait()
            pr.turn(0, a_v.at[r % 2, 0])
            pr.turn(1, a_v.at[r % 2, 1])
            if r + 2 < 4:
                for x in fetch(r + 2):
                    x.start()
            if r == 0:
                for x in pr.load_b(dy_hbm, dyp_hbm):
                    x.wait()
            pr.columns(acc_v.at[r], 0, 4)
            save(r).start()
            if r % 2 == 1:
                steps(2 + r // 2)
        for r in range(4):
            save(r).wait()

    pl.run_scoped(first_products, pltpu.VMEM((2,) + dy_hbm.shape, BF16), pltpu.VMEM((2, 2, nb, tok, d), BF16),
                  pltpu.VMEM((2, d, nb * tok), BF16), pltpu.VMEM((4, 2, d, dy_hbm.shape[1] // 2), F32))
    for b in range(n):
        fin_copy(b).wait()
        for cond, slot in ((c == 3, 0), (c >= 1, 1), (c >= 2, 2)):
            @pl.when(cond)
            def _():
                r_copy(b, 0, slot, cw).wait_send()


def attention(q, do, kv, kv0, dy, dy_p):
    nb, _, hp, tok, d = q.shape
    seq = tok * 8
    rows = hp * tok
    any_spec = pl.BlockSpec(memory_space=pl.ANY)
    vmem = pl.BlockSpec(memory_space=pltpu.VMEM)
    dma = pltpu.SemaphoreType.DMA
    slab = pltpu.VMEM((2, 2, hp, tok, d), BF16)
    out = jax.ShapeDtypeStruct(q.shape, BF16)
    outp = jax.ShapeDtypeStruct((nb, hp, tok, d), BF16)
    return pl.pallas_call(
        functools.partial(attn_body, nb, tok, seq, d),
        in_specs=[any_spec] * 6,
        out_specs=[any_spec] * 6,
        out_shape=[out, jax.ShapeDtypeStruct((nb, 2, rows, seq), BF16), jax.ShapeDtypeStruct((nb, seq, d), BF16),
                   jax.ShapeDtypeStruct(kv.shape, BF16), outp,
                   jax.ShapeDtypeStruct((4, 2, d, dy.shape[1] // 2), F32)],
        scratch_shapes=[pltpu.VMEM((nb + 1, seq, 2 * d), BF16), slab,
                        pltpu.VMEM((nb, 4, tok, 2 * d), BF16), pltpu.VMEM((nb, 3, tok, 2 * d), BF16),
                        dma((nb - 1, 7)), dma((nb - 1, 7)), dma((nb, 4)), dma((nb, 4)), dma((nb, 3)), dma((nb, 3)),
                        dma((nb,)), dma((2, 2)), dma((4,)), dma((nb,)), dma((nb,)), dma((nb,)), dma((11,)),
                        dma((2, 2)), dma((2,)), dma((4,))],
        compiler_params=pltpu.CompilerParams(collective_id=1, has_side_effects=True, vmem_limit_bytes=63 * 2**20),
        cost_estimate=pl.CostEstimate(flops=24 * nb * rows * seq * d, bytes_accessed=40 * 2**20,
                                      transcendentals=2 * nb * rows * seq),
        name="attention",
    )(q, do, kv, kv0, dy, dy_p)


def proj_body(nb, tok, x_hbm, g_ref, wq_hbm, wk_ref, wv_ref, wo_hbm, dy_hbm, cos_ref, sin_ref,
              kv0_hbm, hn_hbm, q_hbm, do_hbm, kv_hbm, wqf_hbm, wof_hbm, hnp_hbm, dyp_hbm,
              x_v, hn_v, dy_v, wq_v, wo_v, kv_v, out_v,
              send, recv, x_sem, dy_sem, own_sem, out_sem, misc_sem, w_sem, p_send, p_recv, kv_send, kv_recv):
    n_tok, e = x_hbm.shape
    d = kv_v.shape[1] // 2
    half = d // 2
    mc = 2 * tok
    me, k, mate, cw, ccw = ring_ids()
    base = 2 * (me // 2)

    def head(off, par):
        return lax.rem(base + 2 * off + 8, 8) + par
    enter((mate, cw, ccw))

    fulls = (wq_v, wo_v)
    locs = (wq_hbm, wo_hbm)

    def half_of(w, ref, j):
        n = ref.shape[0] // 2
        return ref.at[pl.ds(j * n, n)]

    sends = []

    def send_full(w, h, j, to, own=False):
        src = locs[w] if own else fulls[w].at[h]
        c = rdma(src, fulls[w].at[h], send.at[w, j], recv.at[w, j], to)
        c.start()
        sends.append(c)

    def send_half(w, h, part, j, to):
        c = rdma(half_of(w, fulls[w].at[h], part), half_of(w, fulls[w].at[h], part), send.at[w, j], recv.at[w, j], to)
        c.start()
        sends.append(c)

    def wait_full(w, h, j):
        rdma(fulls[w].at[h], fulls[w].at[h], send.at[w, j], recv.at[w, j], mate).wait_recv()

    def wait_half(w, h, part, j):
        ref = half_of(w, fulls[w].at[h], part)
        rdma(ref, ref, send.at[w, j], recv.at[w, j], mate).wait_recv()

    for w in range(2):
        send_full(w, me, 0, cw, True)
        send_full(w, me, 1, ccw, True)
        send_full(w, me, 4, mate, True)
    own = [pltpu.make_async_copy(locs[w], fulls[w].at[me], own_sem.at[w]) for w in range(2)]
    xs = [pltpu.make_async_copy(x_hbm.at[pl.ds(b * tok, tok)], x_v.at[pl.ds(b * tok, tok)], x_sem.at[b]) for b in range(nb)]
    for c in xs:
        c.start()
    for c in own:
        c.start()
    dyc = pltpu.make_async_copy(dy_hbm, dy_v, dy_sem)
    dyc.start()

    gain = g_ref[...].astype(F32)
    for b in range(nb):
        xs[b].wait()

        @pl.loop(0, tok // 16, unroll=2)
        def _(r):
            rs = pl.ds(pl.multiple_of(b * tok + r * 16, 16), 16)
            x = x_v[rs, :].astype(F32)
            c = x - jnp.mean(x, axis=1, keepdims=True)
            inv = lax.rsqrt(jnp.mean(c * c, axis=1, keepdims=True) + LN_EPS)
            hn_v[rs, :] = (c * inv * gain).astype(BF16)
    hn_out = pltpu.make_async_copy(hn_v, hn_hbm, misc_sem.at[0])
    hn_out.start()
    to_mate = [rdma(hn_v, hnp_hbm, p_send.at[0], p_recv.at[0], mate), rdma(dy_hbm, dyp_hbm, p_send.at[1], p_recv.at[1], mate)]
    for c in to_mate:
        c.start()

    def rope_rows(raw):
        lo, hi = raw[:, :half], raw[:, half:d]
        cs, sn = jnp.concatenate([cos_ref[...]] * 2, axis=0), jnp.concatenate([sin_ref[...]] * 2, axis=0)
        return lo * cs - hi * sn, hi * cs + lo * sn

    @pl.loop(0, n_tok // mc)
    def _(i):
        rs = pl.ds(pl.multiple_of(i * mc, mc), mc)
        lo, hi = rope_rows(dot_nn(hn_v[rs, :], wk_ref[...]))
        kv_v[rs, :half] = lo.astype(BF16)
        kv_v[rs, half:d] = hi.astype(BF16)
        kv_v[rs, d:] = dot_nn(hn_v[rs, :], wv_ref[...]).astype(BF16)
    kv_out = pltpu.make_async_copy(kv_v, kv_hbm, misc_sem.at[1])
    kv_out.start()

    outs = []
    saves = []

    def save(w, h):
        c = pltpu.make_async_copy(fulls[w].at[h], (wqf_hbm, wof_hbm)[w].at[h], w_sem.at[len(saves)])
        c.start()
        saves.append(c)

    def project(w, h):
        slot = len(outs) % 4
        if len(outs) >= 4:
            outs[-4].wait()

        @pl.loop(0, n_tok // mc)
        def _(i):
            rs = pl.ds(pl.multiple_of(i * mc, mc), mc)
            if w == 0:
                lo, hi = rope_rows(dot_nn(hn_v[rs, :], wq_v[h]))
                o0 = lo.reshape(2, tok, half).astype(BF16)
                o1 = hi.reshape(2, tok, half).astype(BF16)
                out_v[slot, pl.ds(2 * i, 2), :, :half] = o0
                out_v[slot, pl.ds(2 * i, 2), :, half:] = o1
            else:
                out_v[slot, pl.ds(2 * i, 2)] = dot_nt(dy_v[rs, :], wo_v[h]).reshape(2, tok, d).astype(BF16)
        c = pltpu.make_async_copy(out_v.at[slot], (q_hbm, do_hbm)[w].at[:, lax.rem(h, 2), h // 2], out_sem.at[slot])
        c.start()
        outs.append(c)
        save(w, h)

    other = 1 - k
    for w in range(2):
        own[w].wait()
        if w == 1:
            dyc.wait()
        project(w, me)
        wait_full(w, mate, 4)
        project(w, mate)
    for w in range(2):
        wait_full(w, head(-1, k), 0)
        send_half(w, head(-1, k), 0, 2, cw)
        wait_full(w, head(1, k), 1)
        send_half(w, head(1, k), 1, 3, ccw)
        send_full(w, head(-1, k), 5, mate)
        send_full(w, head(1, k), 6, mate)
        project(w, head(-1, k))
        project(w, head(1, k))
        wait_full(w, head(-1, other), 5)
        project(w, head(-1, other))
        wait_full(w, head(1, other), 6)
        project(w, head(1, other))

    def early(n):
        def blk(j):
            return kv0_hbm.at[n, pl.ds(pl.multiple_of(j * tok, 16), tok)]
        return Gather((me, k, mate, cw, ccw), me // 2, blk, lambda t: kv_send.at[n, t], lambda t: kv_recv.at[n, t])
    first, second = early(0), early(1)
    first.own(kv_v.at[pl.ds(0, tok)])
    own0 = pltpu.make_async_copy(kv_v.at[pl.ds(0, tok)], first.block(me), misc_sem.at[2])
    own0.start()
    for w in range(2):
        wait_half(w, head(2, k), 0, 2)
        send_half(w, head(2, k), 0, 7, mate)
        wait_half(w, head(2, k), 1, 3)
        send_half(w, head(2, k), 1, 8, mate)
        project(w, head(2, k))
        if w == 1:
            first.forward()
            second.own(kv_v.at[pl.ds(tok, tok)])
        wait_half(w, head(2, other), 0, 7)
        wait_half(w, head(2, other), 1, 8)
        project(w, head(2, other))
    first.last()
    for c in outs[-4:] + saves + [hn_out, kv_out, own0]:
        c.wait()
    first.ready()
    first.drain()
    second.arrived()
    second.ready((3,))
    second.drain((0, 2, 3))
    for c in sends:
        c.wait_send()
    for c in to_mate:
        c.wait()


def project(x, gain, wq, w_k, w_v, wo, dy, cos_t, sin_t):
    nb, tok, e = x.shape
    d = wq.shape[1]
    n_heads = 8
    n_tok = nb * tok
    any_spec = pl.BlockSpec(memory_space=pl.ANY)
    vmem = pl.BlockSpec(memory_space=pltpu.VMEM)
    act = jax.ShapeDtypeStruct((nb, 2, n_heads // 2, tok, d), BF16)
    dma = pltpu.SemaphoreType.DMA
    flops = 2 * n_tok * e * (2 * n_heads + 2) * d
    kv0, hn, q, do, kv, wqf, wof, hn_p, dy_p = pl.pallas_call(
        functools.partial(proj_body, nb, tok),
        in_specs=[any_spec, vmem, any_spec, vmem, vmem, any_spec, any_spec, vmem, vmem],
        out_specs=[any_spec] * 9,
        out_shape=[jax.ShapeDtypeStruct((2, tok * n_heads, 2 * d), BF16), jax.ShapeDtypeStruct((n_tok, e), BF16), act, act, jax.ShapeDtypeStruct((n_tok, 2 * d), BF16),
                   jax.ShapeDtypeStruct((n_heads, e, d), BF16), jax.ShapeDtypeStruct((n_heads, d, e), BF16),
                   jax.ShapeDtypeStruct((n_tok, e), BF16), jax.ShapeDtypeStruct((n_tok, e), BF16)],
        scratch_shapes=[pltpu.VMEM((n_tok, e), BF16), pltpu.VMEM((n_tok, e), BF16), pltpu.VMEM((n_tok, e), BF16),
                        pltpu.VMEM((n_heads, e, d), BF16), pltpu.VMEM((n_heads, d, e), BF16),
                        pltpu.VMEM((n_tok, 2 * d), BF16), pltpu.VMEM((4, nb, tok, d), BF16),
                        dma((2, 9)), dma((2, 9)), dma((nb,)), dma(()), dma((2,)), dma((4,)), dma((3,)), dma((16,)), dma((2,)), dma((2,)), dma((2, 7)), dma((2, 7))],
        compiler_params=pltpu.CompilerParams(collective_id=0, has_side_effects=True, vmem_limit_bytes=60 * 2**20),
        cost_estimate=pl.CostEstimate(flops=flops, bytes_accessed=60 * 2**20, transcendentals=0),
        name="project",
    )(x.reshape(n_tok, e), gain, wq, w_k, w_v, wo, dy.reshape(n_tok, e), cos_t, sin_t)
    return kv0, hn, q, do, kv.reshape(nb, tok, 2 * d), wqf, wof, hn_p, dy_p


def grads_body(nb, tok, o_hbm, acc_hbm, ds_hbm, k_hbm, hn_hbm, hnp_hbm, dy_hbm, dkv_hbm,
               wq_hbm, wo_hbm, wk_hbm, wv_hbm, x_hbm, g_ref, cos_ref, sin_ref,
               y_hbm, gx_hbm, gln_ref, gwo_ref, gwq_ref, gkv_hbm, dq_hbm, dqp_hbm,
               acc, acc_kv, rbuf, rbuf_kv, kind, kp, dkv_v, fin_kv, gln_acc, gl_recv,
               rs_send, rs_recv, kv_send, kv_recv, ag_send, ag_recv, gl_send, gl_rsem, kp_sem, ld_sem, b_sem, t_sem, a_sem, q_send, q_recv, st_sem):
    n_tok, e = x_hbm.shape
    d = wk_hbm.shape[1]
    half = d // 2
    eh, eq = e // 2, e // 4
    me, k, mate, cw, ccw = ring_ids()
    c = me // 2
    rel = [lax.rem(c + o, 4) for o in (3, 1, 2, 0)]
    enter([lax.rem(me + o, 8) for o in range(1, 8)])

    order = ((2, 1), (2, 0))

    def hop(s, dr, j):
        first = acc_hbm.at[dr, dr] if s == 0 else acc.at[s, dr, dr]
        src = first if j == 0 else rbuf.at[s, dr, j - 1]
        return rdma(src, rbuf.at[s, dr, j], rs_send.at[s, dr, j], rs_recv.at[s, dr, j], (cw, ccw)[dr])

    def hop_kv(dr, j):
        src = acc_kv.at[dr, dr] if j == 0 else rbuf_kv.at[dr, j - 1]
        return rdma(src, rbuf_kv.at[dr, j], kv_send.at[dr, j], kv_recv.at[dr, j], (cw, ccw)[dr])

    def add(dst, term):
        @pl.loop(0, dst.shape[0] // 32)
        def _(i):
            rs = pl.ds(pl.multiple_of(i * 32, 32), 32)
            dst[rs, :] = dst[rs, :] + term[rs, :]

    def pass_on(s, j):
        for dr in range(2):
            hop(s, dr, j - 1).wait_recv()
            add(rbuf.at[s, dr, j - 1], acc.at[s, order[dr][j - 1], dr])
            hop(s, dr, j).start()

    def pass_on_kv(j):
        for dr in range(2):
            hop_kv(dr, j - 1).wait_recv()
            add(rbuf_kv.at[dr, j - 1], acc_kv.at[order[dr][j - 1], dr])
            hop_kv(dr, j).start()

    def finish(s, out):
        for dr in range(2):
            hop(s, dr, 2).wait_recv()

            @pl.loop(0, d // 32)
            def _(i):
                rs = pl.ds(pl.multiple_of(i * 32, 32), 32)
                out[rs, dr * eh:(dr + 1) * eh] = (rbuf[s, dr, 2, rs, :] + acc[s, 3, dr, rs, :]).astype(BF16)

    def piece(kk, j, lo=0, n=None):
        return gkv_hbm.at[kk, pl.ds(lo, d if n is None else n), pl.ds(pl.multiple_of(j * eq, 128), eq)]

    def ag(tag, ref, to, src=None):
        return rdma(ref if src is None else src, ref, ag_send.at[tag], ag_recv.at[tag], to)

    def ag_far(tag, to):
        return ag(tag, piece(k, rel[(0, 1)[tag - 3]], (tag - 3) * half, half), to)

    own_piece = pltpu.make_async_copy(fin_kv, piece(k, c), t_sem.at[5])

    def finish_kv():
        for dr in range(2):
            hop_kv(dr, 2).wait_recv()
            fin_kv[:, dr * (eq // 2):(dr + 1) * (eq // 2)] = rbuf_kv[dr, 2] + acc_kv[3, dr]
        ag(0, piece(k, c), cw, fin_kv).start()
        ag(1, piece(k, c), ccw, fin_kv).start()
        ag(2, piece(k, c), mate, fin_kv).start()
        own_piece.start()

    def ag_forward():
        ag(0, piece(k, rel[0]), cw).wait_recv()
        ag_far(3, cw).start()
        ag(1, piece(k, rel[1]), cw).wait_recv()
        ag_far(4, ccw).start()
        ag(5, piece(k, rel[0]), mate).start()
        ag(6, piece(k, rel[1]), mate).start()

    def ag_last():
        far = [piece(k, rel[2], i * half, half) for i in range(2)]
        for i in range(2):
            ag(3 + i, far[i], cw).wait_recv()
            ag(7 + i, far[i], mate).start()
        ag(2, piece(1 - k, c), mate).wait_recv()
        ag(5, piece(1 - k, rel[0]), mate).wait_recv()
        ag(6, piece(1 - k, rel[1]), mate).wait_recv()
        for i in range(2):
            ag(7 + i, piece(1 - k, rel[2], i * half, half), mate).wait_recv()
        for tag in range(3):
            ag(tag, piece(k, c), cw, fin_kv).wait_send()
        for tag in (3, 4, 7, 8):
            ag(tag, far[0], cw).wait_send()
        for tag in (5, 6):
            ag(tag, piece(k, c), cw).wait_send()
        own_piece.wait()

    dkv_in = pltpu.make_async_copy(dkv_hbm, dkv_v, t_sem.at[4])
    dkv_in.start()
    kp_copy = rdma(kind.at[1 - k], kp, kp_sem.at[0], kp_sem.at[1], mate)

    for dr in range(2):
        hop(0, dr, 0).start()
    acc_in = [pltpu.make_async_copy(acc_hbm.at[r], acc.at[0, r], a_sem.at[r]) for r in range(4)]
    for r in (2, 1, 0, 3):
        acc_in[r].start()

    rows, seq = ds_hbm.shape[2], ds_hbm.shape[3]

    def query_grads(ds_v, k_v, dq_st, cos4, sin4):
        for j in range(rows // tok):
            cos4[j * tok:(j + 1) * tok, :] = cos_ref[...]
            sin4[j * tok:(j + 1) * tok, :] = sin_ref[...]
        rb = 256 if rows % 256 == 0 else rows

        def load(b, g, slot):
            return (pltpu.make_async_copy(ds_hbm.at[b, g], ds_v.at[slot], ld_sem.at[slot, 0]),
                    pltpu.make_async_copy(k_hbm.at[b], k_v.at[slot], ld_sem.at[slot, 1]))

        def keep(b, g, slot):
            return pltpu.make_async_copy(dq_st.at[slot], dq_hbm.at[b, g], st_sem.at[slot])

        def hand(b, slot):
            return rdma(dq_st.at[slot], dqp_hbm.at[b], q_send.at[b], q_recv.at[b], mate)
        for mine in (False, True):
            g = k if mine else 1 - k
            for x in load(0, g, 0):
                x.start()

            @pl.loop(0, nb)
            def _(b):
                slot = lax.rem(b, 2)

                @pl.when(b + 1 < nb)
                def _():
                    for x in load(b + 1, g, 1 - slot):
                        x.start()

                @pl.when(b >= 2)
                def _():
                    keep(b - 2, g, slot).wait()
                    if not mine:
                        hand(b - 2, slot).wait_send()
                for x in load(b, g, slot):
                    x.wait()
                for i in range(rows // rb):
                    rs = slice(i * rb, (i + 1) * rb)
                    dq = dot_nn(ds_v[slot, rs, :], k_v[slot]) * (d ** -0.5)
                    lo, hi = dq[:, :half], dq[:, half:]
                    cs, sn = cos4[rs, :], sin4[rs, :]
                    v = jnp.concatenate([(lo * cs + hi * sn).astype(BF16), (hi * cs - lo * sn).astype(BF16)], axis=1)
                    r = i * rb
                    while r < (i + 1) * rb:
                        n = min((i + 1) * rb - r, tok - r % tok)
                        dq_st[slot, r // tok, r % tok:r % tok + n, :] = v[r - i * rb:r - i * rb + n]
                        r += n
                keep(b, g, slot).start()
                if not mine:
                    hand(b, slot).start()
            for b in (nb - 2, nb - 1):
                keep(b, g, b % 2).wait()
                if not mine:
                    hand(b, b % 2).wait_send()
        for b in range(nb):
            hand(b, b % 2).wait_recv()

    def products(big):
        hn_in = (pltpu.make_async_copy(hn_hbm, big.at[0], b_sem.at[0]), pltpu.make_async_copy(hnp_hbm, big.at[1], b_sem.at[1]))
        dkv_in.wait()
        for b in range(nb):
            lo, hi = dkv_v[b, :, :half].astype(F32), dkv_v[b, :, half:d].astype(F32)
            cs, sn = cos_ref[...], sin_ref[...]
            kind[0, b, :, :half] = (lo * cs + hi * sn).astype(BF16)
            kind[0, b, :, half:] = (hi * cs - lo * sn).astype(BF16)
            kind[1, b] = dkv_v[b, :, d:]
        kp_copy.start()
        for x in hn_in:
            x.start()
        pl.run_scoped(query_grads, pltpu.VMEM((2, rows, seq), BF16), pltpu.VMEM((2, seq, d), BF16),
                      pltpu.VMEM((2, rows // tok, tok, d), BF16), pltpu.VMEM((rows, half), F32), pltpu.VMEM((rows, half), F32))
        pl.run_scoped(functools.partial(small_products, big, hn_in), pltpu.VMEM((2, 2, nb, tok, d), BF16), pltpu.VMEM((2, d, n_tok), BF16))

    def small_products(big, hn_in, a_v, at):
        pr = Products(big, a_v, at, ld_sem, b_sem)

        def fetch(r):
            return pr.load_a(r, dq_hbm.at[:, k, rel[r]], dqp_hbm.at[:, rel[r]])
        for r in range(2):
            for x in fetch(r):
                x.start()
        pr.turn(0, kind.at[k])
        for x in hn_in:
            x.wait()
        kp_copy.wait_recv()
        pr.turn(1, kp)
        for r in range(4):
            for dr in range(2):
                acc_kv[r, dr] = pr.both(pl.ds(pl.multiple_of(rel[r] * eq + dr * (eq // 2), 128), eq // 2))
        for dr in range(2):
            hop_kv(dr, 0).start()
        for r in range(4):
            for x in fetch(r):
                x.wait()
            pr.turn(0, a_v.at[r % 2, 0])
            pr.turn(1, a_v.at[r % 2, 1])
            if r + 2 < 4:
                for x in fetch(r + 2):
                    x.start()
            if r < 2:
                pr.columns(acc.at[1, r], 0, 2, 2 * r)
                hop(1, r, 0).start()
                pr.columns(acc.at[1, r], 2, 4, 2 * r)
            else:
                pr.columns(acc.at[1, r], 0, 4)

    pl.run_scoped(products, pltpu.VMEM((2, n_tok, e), BF16))
    for r in range(4):
        acc_in[r].wait()
    pass_on(0, 1)
    pass_on_kv(1)

    mc = 2 * tok
    units = nb // 2

    def attn_out(wo_v, o_v, x_v, y_v):
        w_in = pltpu.make_async_copy(wo_hbm, wo_v, b_sem.at[0])
        w_in.start()

        def load(u):
            return (pltpu.make_async_copy(o_hbm.at[pl.ds(2 * u, 2)], o_v.at[u % 2], ld_sem.at[u % 2, 0]),
                    pltpu.make_async_copy(x_hbm.at[pl.ds(u * mc, mc)], x_v.at[u % 2], ld_sem.at[u % 2, 1]))

        def put(u):
            return pltpu.make_async_copy(y_v.at[u % 2], y_hbm.at[pl.ds(u * mc, mc)], t_sem.at[u % 2])
        for x in load(0):
            x.start()
        w_in.wait()
        for u in range(units):
            if u + 1 < units:
                for x in load(u + 1):
                    x.start()
            for x in load(u):
                x.wait()
            if u >= 2:
                put(u - 2).wait()
            sl = u % 2

            @pl.loop(0, 4)
            def _(n):
                cols = pl.ds(pl.multiple_of(n * eq, 128), eq)
                o_rows = jnp.concatenate([jnp.concatenate([o_v[sl, i, h % 2, h // 2] for h in range(8)], axis=1) for i in range(2)], axis=0)
                r = dot_nn(o_rows, wo_v[:, cols])
                y_v[sl, :, cols] = (x_v[sl, :, cols].astype(F32) + r).astype(BF16)
            put(u).start()
        for u in range(max(0, units - 2), units):
            put(u).wait()

    pl.run_scoped(attn_out, pltpu.VMEM((8 * d, e), BF16), pltpu.VMEM((2, 2, 2, 4, tok, d), BF16),
                  pltpu.VMEM((2, mc, e), BF16), pltpu.VMEM((2, mc, e), BF16))
    pass_on(1, 1)

    def hidden_grad(wq_v, wk_v, wv_v, dq_v, x_v, dy_v, dh, gx_v):
        w_in = pltpu.make_async_copy(wq_hbm, wq_v, b_sem.at[0])
        w_in.start()
        w2_in = (pltpu.make_async_copy(wk_hbm, wk_v, b_sem.at[1]), pltpu.make_async_copy(wv_hbm, wv_v, ld_sem.at[1, 1]))
        for x in w2_in:
            x.start()

        def load(u):
            return (pltpu.make_async_copy(dq_hbm.at[pl.ds(2 * u, 2)], dq_v, ld_sem.at[0, 0]),
                    pltpu.make_async_copy(x_hbm.at[pl.ds(u * mc, mc)], x_v, ld_sem.at[0, 1]),
                    pltpu.make_async_copy(dy_hbm.at[pl.ds(u * mc, mc)], dy_v, ld_sem.at[1, 0]))

        def put(u):
            return pltpu.make_async_copy(gx_v, gx_hbm.at[pl.ds(u * mc, mc)], t_sem.at[0])
        gain = g_ref[...].astype(F32)
        gln_acc[...] = jnp.zeros_like(gln_acc)
        for x in load(0):
            x.start()
        w_in.wait()
        for x in w2_in:
            x.wait()
        for u in range(units):
            for x in load(u):
                x.wait()

            @pl.loop(0, 4)
            def _(n):
                rows = pl.ds(pl.multiple_of(n * eq, 128), eq)
                t = None
                for h in range(8):
                    a = jnp.concatenate([dq_v[i, h % 2, h // 2] for i in range(2)], axis=0)
                    p = dot_nt(a, wq_v[h, rows, :])
                    t = p if t is None else t + p
                for j in range(2):
                    a = jnp.concatenate([kind[j, 2 * u + i] for i in range(2)], axis=0)
                    t = t + dot_nt(a, (wk_v, wv_v)[j][rows, :])
                dh[:, rows] = t
            if u >= 1:
                put(u - 1).wait()

            @pl.loop(0, mc // 16)
            def _(r):
                rs = pl.ds(pl.multiple_of(r * 16, 16), 16)
                x = x_v[rs, :].astype(F32)
                cx = x - jnp.mean(x, axis=1, keepdims=True)
                inv = lax.rsqrt(jnp.mean(cx * cx, axis=1, keepdims=True) + LN_EPS)
                xh = cx * inv
                g = dh[rs, :]
                pr = g * xh
                gln_acc[...] += pr[:8] + pr[8:]
                gh = g * gain
                m1 = jnp.mean(gh, axis=1, keepdims=True)
                m2 = jnp.mean(gh * xh, axis=1, keepdims=True)
                gx_v[rs, :] = (inv * (gh - m1 - xh * m2) + dy_v[rs, :].astype(F32)).astype(BF16)
            put(u).start()
            if u + 1 < units:
                for x in load(u + 1):
                    x.start()
            if u == units // 2 - 1:
                pass_on(0, 2)
                pass_on_kv(2)
        put(units - 1).wait()

    pl.run_scoped(hidden_grad, pltpu.VMEM((8, e, d), BF16), pltpu.VMEM((e, d), BF16), pltpu.VMEM((e, d), BF16), pltpu.VMEM((2, 2, 4, tok, d), BF16),
                  pltpu.VMEM((mc, e), BF16), pltpu.VMEM((mc, e), BF16), pltpu.VMEM((mc, e), F32), pltpu.VMEM((mc, e), BF16))
    gl_recv[me] = jnp.sum(gln_acc[...], axis=0, keepdims=True)
    pass_on(1, 2)
    finish(0, gwo_ref)
    finish_kv()
    gl = [rdma(gl_recv.at[me], gl_recv.at[me], gl_send.at[o - 1], gl_rsem.at[o - 1], lax.rem(me + o, 8)) for o in range(1, 8)]
    for x in gl:
        x.start()
    finish(1, gwq_ref)
    ag_forward()
    for o in range(1, 8):
        src = lax.rem(me + 8 - o, 8)
        rdma(gl_recv.at[src], gl_recv.at[src], gl_send.at[o - 1], gl_rsem.at[o - 1], mate).wait_recv()
    total = gl_recv[0]
    for i in range(1, 8):
        total = total + gl_recv[i]
    gln_ref[...] = total
    ag_last()
    for x in gl:
        x.wait_send()
    kp_copy.wait_send()
    for dr in range(2):
        for j in range(3):
            hop_kv(dr, j).wait_send()
            for s in range(2):
                hop(s, dr, j).wait_send()


def gradients(o, acc, ds, k_all, hn, hn_p, dy, dkv, wqf, wof, w_k, w_v, x, gain, cos_t, sin_t):
    nb, tok, e = x.shape
    n_tok = nb * tok
    d = o.shape[-1]
    any_spec = pl.BlockSpec(memory_space=pl.ANY)
    vmem = pl.BlockSpec(memory_space=pltpu.VMEM)
    dma = pltpu.SemaphoreType.DMA
    tokens = jax.ShapeDtypeStruct((n_tok, e), BF16)
    y, gx, gln, gwo, gwq_t, gkv_t, _, _ = pl.pallas_call(
        functools.partial(grads_body, nb, tok),
        in_specs=[any_spec] * 13 + [vmem, vmem, vmem],
        out_specs=[any_spec, any_spec, vmem, vmem, vmem, any_spec, any_spec, any_spec],
        out_shape=[tokens, tokens, jax.ShapeDtypeStruct((1, e), F32), jax.ShapeDtypeStruct((d, e), BF16),
                   jax.ShapeDtypeStruct((d, e), BF16), jax.ShapeDtypeStruct((2, d, e), F32),
                   jax.ShapeDtypeStruct(o.shape, BF16), jax.ShapeDtypeStruct((nb,) + o.shape[2:], BF16)],
        scratch_shapes=[pltpu.VMEM((2, 4, 2, d, e // 2), F32), pltpu.VMEM((4, 2, d, e // 8), F32),
                        pltpu.VMEM((2, 2, 3, d, e // 2), F32), pltpu.VMEM((2, 3, d, e // 8), F32),
                        pltpu.VMEM((2, nb, tok, d), BF16), pltpu.VMEM((nb, tok, d), BF16), pltpu.VMEM((nb, tok, 2 * d), BF16),
                        pltpu.VMEM((d, e // 4), F32), pltpu.VMEM((8, e), F32), pltpu.VMEM((8, 1, e), F32),
                        dma((2, 2, 3)), dma((2, 2, 3)), dma((2, 3)), dma((2, 3)), dma((9,)), dma((9,)), dma((7,)), dma((7,)),
                        dma((2,)), dma((2, 2)), dma((2,)), dma((6,)), dma((4,)), dma((nb,)), dma((nb,)), dma((2,))],
        compiler_params=pltpu.CompilerParams(collective_id=2, has_side_effects=True, vmem_limit_bytes=63 * 2**20),
        cost_estimate=pl.CostEstimate(flops=10 * n_tok * e * e, bytes_accessed=120 * 2**20, transcendentals=0),
        name="gradients",
    )(o, acc, ds, k_all, hn, hn_p, dy.reshape(n_tok, e), dkv, wqf, wof.reshape(8 * d, e), w_k, w_v, x.reshape(n_tok, e),
      gain, cos_t, sin_t)
    y, gx, gwq, gwk, gwv, gwo, gln = place(nb, y, gx, gwq_t, gkv_t, gwo, gln)
    return y.reshape(nb, tok, e), gx.reshape(nb, tok, e), gln.reshape(e), gwq, gwk, gwv, gwo


def place_body(y_in, gx_in, gq_in, gkv_in, go_in, gl_in, y, gx, gq, gk, gv, go, gl):
    y[...] = y_in[...]
    gx[...] = gx_in[...]
    gq[...] = gq_in[...].astype(F32).T.astype(BF16)
    gk[...] = gkv_in[0].T
    gv[...] = gkv_in[1].T
    go[...] = go_in[...]
    gl[...] = gl_in[...]


def place(steps, y, gx, gwq_t, gkv_t, gwo, gln):
    n_tok, e = y.shape
    d = gwo.shape[0]
    act = pl.BlockSpec((n_tok // steps, e), lambda i: (i, 0))
    cols = pl.BlockSpec((d, e // steps), lambda i: (0, i))
    turned = pl.BlockSpec((e // steps, d), lambda i: (i, 0))
    small = pl.BlockSpec((d // steps, e), lambda i: (i, 0))
    line = pl.BlockSpec((1, e), lambda i: (0, 0))
    return pl.pallas_call(
        place_body,
        grid=(steps,),
        in_specs=[act, act, cols, pl.BlockSpec((2, d, e // steps), lambda i: (0, 0, i)), small, line],
        out_specs=[act, act, turned, turned, turned, small, line],
        out_shape=[jax.ShapeDtypeStruct(y.shape, BF16), jax.ShapeDtypeStruct(y.shape, BF16), jax.ShapeDtypeStruct((e, d), BF16),
                   jax.ShapeDtypeStruct((e, d), F32), jax.ShapeDtypeStruct((e, d), F32), jax.ShapeDtypeStruct((d, e), BF16),
                   jax.ShapeDtypeStruct((1, e), F32)],
        compiler_params=pltpu.CompilerParams(dimension_semantics=("arbitrary",)),
        cost_estimate=pl.CostEstimate(flops=0, bytes_accessed=8 * y.size + 24 * gwo.size, transcendentals=0),
        name="place",
    )(y, gx, gwq_t, gkv_t, gwo, gln)


def solution(mesh):
    act_spec = P('dp', 'tp', None)

    def device_step(x_loc, ln_scale, wq_loc, w_k, w_v, wo_loc, dy_loc):
        n_batch, tok, model_dim = x_loc.shape
        d = w_k.shape[1]
        t0 = lax.axis_index('tp') * tok
        cos_t, sin_t = rope_tables(t0 + jnp.arange(tok), d)

        gain = ln_scale.reshape(1, model_dim)
        kv0, hn, q, do, kv_loc, wq_h, wo_h, hn_p, dy_p = project(x_loc, gain, wq_loc, w_k, w_v, wo_loc, dy_loc, cos_t, sin_t)
        o, ds, k_all, dkv_loc, _, acc = attention(q, do, kv_loc, kv0, dy_loc.reshape(-1, model_dim), dy_p)
        return gradients(o, acc, ds, k_all, hn, hn_p, dy_loc, dkv_loc, wq_h, wo_h, w_k, w_v, x_loc, gain, cos_t, sin_t)

    return jax.shard_map(device_step, mesh=mesh, in_specs=(act_spec, P(None), P(None, 'tp'), P(None, None), P(None, None), P('tp', None), act_spec), out_specs=(act_spec, act_spec, P('dp'), P('dp', 'tp'), P('dp', None), P('dp', None), P(('dp', 'tp'), None)), check_vma=False)
```

```python
import functools
import jax
import jax.numpy as jnp
from jax import lax
from jax.experimental import pallas as pl
from jax.experimental.pallas import tpu as pltpu
from jax.sharding import PartitionSpec as P

LN_EPS = 1e-6
ROPE_BASE = 10000.0
LOG2E = 1.4426950408889634
F32 = jnp.float32
BF16 = jnp.bfloat16


def rope_tables(positions, head_dim):
    half_dim = head_dim // 2
    inv_freq = ROPE_BASE ** (-2.0 * jnp.arange(half_dim, dtype=F32) / head_dim)
    angles = positions.astype(F32)[:, None] * inv_freq[None, :]
    return jnp.cos(angles), jnp.sin(angles)


def rotate(vectors, cos_t, sin_t):
    half_dim = vectors.shape[-1] // 2
    lo_half = vectors[..., :half_dim]
    hi_half = vectors[..., half_dim:]
    return jnp.concatenate([lo_half * cos_t - hi_half * sin_t, hi_half * cos_t + lo_half * sin_t], axis=-1)


def dot_nn(a, b):
    return lax.dot_general(a, b, (((1,), (0,)), ((), ())), preferred_element_type=F32)


def dot_nt(a, b):
    return lax.dot_general(a, b, (((1,), (1,)), ((), ())), preferred_element_type=F32)


def rdma(src, dst, send, recv, to):
    return pltpu.make_async_remote_copy(src_ref=src, dst_ref=dst, send_sem=send, recv_sem=recv,
                                        device_id={'tp': to}, device_id_type=pl.DeviceIdType.MESH)


def ring_ids():
    me = lax.axis_index('tp')
    k = lax.rem(me, 2)
    return me, k, me + 1 - 2 * k, lax.rem(me + 2, 8), lax.rem(me + 6, 8)


def enter(peers):
    barrier = pltpu.get_barrier_semaphore()
    for p in peers:
        pl.semaphore_signal(barrier, inc=1, device_id={'tp': p}, device_id_type=pl.DeviceIdType.MESH)
    pl.semaphore_wait(barrier, len(peers))


class Products:
    def __init__(self, big, a_v, at, ld_sem, b_sem):
        self.big, self.a_v, self.at, self.ld_sem, self.b_sem = big, a_v, at, ld_sem, b_sem
        self.nb, self.tok = a_v.shape[2], a_v.shape[3]
        self.eq = big.shape[2] // 4

    def load_b(self, own, other):
        return (pltpu.make_async_copy(own, self.big.at[0], self.b_sem.at[0]),
                pltpu.make_async_copy(other, self.big.at[1], self.b_sem.at[1]))

    def load_a(self, i, own, other):
        return (pltpu.make_async_copy(own, self.a_v.at[i % 2, 0], self.ld_sem.at[i % 2, 0]),
                pltpu.make_async_copy(other, self.a_v.at[i % 2, 1], self.ld_sem.at[i % 2, 1]))

    def turn(self, j, src):
        tok = self.tok
        for i in range(self.nb // 2):
            self.at[j, :, 2 * i * tok:(2 * i + 2) * tok] = jnp.concatenate([src[2 * i], src[2 * i + 1]], axis=0).T

    def both(self, cols):
        return dot_nn(self.at[0], self.big[0, :, cols]) + dot_nn(self.at[1], self.big[1, :, cols])

    def columns(self, dst, first, last, turned=0):
        eq = self.eq

        @pl.loop(first, last)
        def _(n):
            m = lax.rem(n + turned, 4)
            cols = pl.ds(pl.multiple_of(m * eq, 128), eq)
            dst[m // 2, :, pl.ds(pl.multiple_of(lax.rem(m, 2) * eq, 128), eq)] = self.both(cols)


class Gather:
    def __init__(self, ids, c, block, send, recv):
        self.me, _, self.mate, self.cw, self.ccw = ids
        self.c, self.block, self.send, self.recv = c, block, send, recv

    def copy(self, j, tag, to, src=None):
        ref = self.block(j)
        return rdma(ref if src is None else src, ref, self.send(tag), self.recv(tag), to)

    def own(self, src):
        @pl.when(self.c <= 2)
        def _():
            self.copy(self.me, 0, self.cw, src).start()

        @pl.when(self.c == 0)
        def _():
            self.copy(self.me, 2, self.ccw, src).start()
        self.copy(self.me, 3, self.mate, src).start()

    def arrived(self):
        @pl.when(self.c >= 1)
        def _():
            self.copy(self.me - 2, 0, self.cw).wait_recv()

        @pl.when(self.c == 3)
        def _():
            self.copy(self.me - 6, 2, self.ccw).wait_recv()

    def pass_on(self, src=lambda j: None):
        @pl.when(self.c >= 1)
        def _():
            @pl.when(self.c <= 2)
            def _():
                self.copy(self.me - 2, 1, self.cw, src(self.me - 2)).start()
            self.copy(self.me - 2, 4, self.mate, src(self.me - 2)).start()

        @pl.when(self.c == 3)
        def _():
            self.copy(self.me - 6, 6, self.mate, src(self.me - 6)).start()

    def forward(self):
        self.arrived()
        self.pass_on()

    def last(self):
        @pl.when(self.c >= 2)
        def _():
            self.copy(self.me - 4, 1, self.cw).wait_recv()
            self.copy(self.me - 4, 5, self.mate).start()

    def ready(self, tags=(3, 4, 5, 6)):
        if 3 in tags:
            self.copy(self.mate, 3, self.mate).wait_recv()
        for n, tag in ((1, 4), (2, 5), (3, 6)):
            if tag not in tags:
                continue

            @pl.when(self.c >= n)
            def _():
                self.copy(self.mate - 2 * n, tag, self.mate).wait_recv()

    def drain(self, tags=range(7)):
        c = self.c
        conds = (c <= 2, (c >= 1) & (c <= 2), c == 0, c >= 0, c >= 1, c >= 2, c == 3)
        for tag in tags:
            @pl.when(conds[tag])
            def _():
                self.copy(self.me, tag, self.mate).wait_send()


def attn_body(nb, tok, seq, d, q_hbm, do_hbm, kvl_hbm, kv0_hbm, dy_hbm, dyp_hbm, cos_ref, sin_ref,
              o_hbm, dq_hbm, dkv_hbm, op_hbm, dqp_hbm, acc_hbm,
              kv_all, o_v, dq_v, mrecv, rrecv,
              kv_send, kv_recv, m_send, m_recv, r_send, r_recv, own_sem, in_sem, out_sem, fin_sem, p_send, p_recv, first_sem,
              ld_sem, b_sem, acc_sem):
    scale = d ** -0.5
    rows = o_v.shape[2] * tok
    n_blk = seq // 256
    rb = 2 * rows // n_blk
    n_rb = rows // rb
    half = d // 2
    me, k, mate, cw, ccw = ring_ids()
    c = me // 2
    rel = [lax.rem(c + o, 4) for o in (3, 1, 2, 0)]

    def blk(j):
        return pl.ds(pl.multiple_of(j * tok, 16), tok)

    def kvb(b, j):
        return kv_all.at[b, blk(j)]

    def gather(b):
        return Gather((me, k, mate, cw, ccw), c, lambda j: kvb(b, j), lambda t: kv_send.at[b - 1, t], lambda t: kv_recv.at[b - 1, t])

    def own(b):
        gather(b).own(kvl_hbm.at[b])

    def own_copy(b):
        return pltpu.make_async_copy(kvl_hbm.at[b], kvb(b, me), own_sem.at[b])

    def ready(b):
        own_copy(b).wait()

        @pl.when(b == 1)
        def _():
            gather(1).ready((4, 5, 6))

        @pl.when(b > 1)
        def _():
            gather(b).ready()

    def drain(b):
        @pl.when(b == 1)
        def _():
            gather(1).drain((1, 4, 5, 6))

        @pl.when(b > 1)
        def _():
            gather(b).drain()

    def m_copy(b, n):
        return rdma(kvb(b, 2 * n + 1 - k), mrecv.at[b, n], m_send.at[b, n], m_recv.at[b, n], mate)

    def r_copy(b, n, slot, to):
        return rdma(kvb(b, 2 * n + k), rrecv.at[b, slot], r_send.at[b, slot], r_recv.at[b, slot], to)

    def add_into(b, n, other):
        v = kv_all[b, blk(2 * n + k), :].astype(F32) + other[...].astype(F32)
        kv_all[b, blk(2 * n + k), :] = v.astype(BF16)

    def fin_copy(b):
        return pltpu.make_async_copy(kvb(b, me), dkv_hbm.at[b], fin_sem.at[b])

    def to_mate(b):
        for n in range(4):
            @pl.when(c >= n)
            def _():
                m_copy(b, n).start()

    def stage1(b):
        for n in range(4):
            @pl.when(c >= n)
            def _():
                m_copy(b, n).wait()
                add_into(b, n, mrecv.at[b, n])

        @pl.when(c == 3)
        def _():
            r_copy(b, 1, 2, ccw).start()
            r_copy(b, 2, 1, ccw).start()
            r_copy(b, 0, 0, cw).start()
            fin_copy(b).start()

        @pl.when(c == 2)
        def _():
            r_copy(b, 0, 1, ccw).start()

    def stage2(b):
        @pl.when(c == 2)
        def _():
            r_copy(b, 1, 2, ccw).wait_recv()
            add_into(b, 1, rrecv.at[b, 2])
            r_copy(b, 1, 2, ccw).start()
            r_copy(b, 2, 1, ccw).wait_recv()
            add_into(b, 2, rrecv.at[b, 1])
            fin_copy(b).start()

        @pl.when(c == 1)
        def _():
            r_copy(b, 0, 1, ccw).wait_recv()
            add_into(b, 0, rrecv.at[b, 1])
            r_copy(b, 0, 1, ccw).start()

    def stage3(b):
        @pl.when(c == 0)
        def _():
            r_copy(b, 0, 0, cw).wait_recv()
            add_into(b, 0, rrecv.at[b, 0])
            r_copy(b, 0, 1, ccw).wait_recv()
            add_into(b, 0, rrecv.at[b, 1])
            fin_copy(b).start()

        @pl.when(c == 1)
        def _():
            r_copy(b, 1, 2, ccw).wait_recv()
            add_into(b, 1, rrecv.at[b, 2])
            fin_copy(b).start()

    def handed(dst, src, n, b, slot):
        return rdma(src.at[slot, 1 - k], dst.at[b], p_send.at[n, b], p_recv.at[n, b], mate)

    def store_o(b, slot):
        return (pltpu.make_async_copy(o_v.at[slot], o_hbm.at[b], out_sem.at[0, slot]), handed(op_hbm, o_v, 0, b, slot))

    def store_dq(b, slot):
        return (pltpu.make_async_copy(dq_v.at[slot], dq_hbm.at[b], out_sem.at[1, slot]), handed(dqp_hbm, dq_v, 1, b, slot))

    def stored(x):
        x[0].wait()
        x[1].wait_send()

    def attend(q_v, do_v, s_buf, m_buf, l_buf, p_buf, ds_buf, q_t, do_t, dk_t, dv_t, d_buf, cos4, sin4):
        def load(b, slot):
            return (pltpu.make_async_copy(q_hbm.at[b], q_v.at[slot], in_sem.at[0, slot]),
                    pltpu.make_async_copy(do_hbm.at[b], do_v.at[slot], in_sem.at[1, slot]))

        def scores(b, g, slot, i):
            w = min(512, seq)
            if (i * 256) % w:
                return
            cols = slice(i * 256, i * 256 + w)
            s = dot_nt(q_v[slot, g].reshape(rows, d), kv_all[b, cols, :d]) * (scale * LOG2E)
            col = lax.broadcasted_iota(jnp.int32, (tok, w), 1) + i * 256
            row = lax.broadcasted_iota(jnp.int32, (tok, w), 0) + me * tok
            s = jnp.concatenate([jnp.where(col <= row, s[j * tok:(j + 1) * tok], -1e30) for j in range(rows // tok)], axis=0)
            s_buf[g, :, cols] = s
            m = s[:, :128]
            for j in range(128, w, 128):
                m = jnp.maximum(m, s[:, j:j + 128])
            m_buf[...] = m if i == 0 else jnp.maximum(m_buf[...], m)

        parts = max(1, min(5, n_blk))
        part = [j * (rows // 16) // parts * 16 for j in range(parts + 1)] + [rows] * n_blk

        def softmax(g, i):
            for r in range(part[i], part[i + 1], 16):
                rs = slice(r, r + 16)
                m = jnp.max(m_buf[rs, :], axis=1, keepdims=True)
                l = None
                for j in range(0, seq, 128):
                    e = jnp.exp2(s_buf[g, rs, j:j + 128] - m)
                    s_buf[g, rs, j:j + 128] = e
                    l = e if l is None else l + e
                l_buf[g, rs, :] = jnp.broadcast_to(1.0 / jnp.sum(l, axis=1, keepdims=True), (16, 128))

        def turn(g, slot, i):
            rs = slice(i * rb, (i + 1) * rb)
            q_t[g, :, rs] = q_v[slot, g].reshape(rows, d)[rs].T
            do_t[g, :, rs] = do_v[slot, g].reshape(rows, d)[rs].T

        def out_rows(b, g, slot, i):
            rs = slice(i * rb, (i + 1) * rb)
            p = (s_buf[g, rs, :] * jnp.concatenate([l_buf[g, rs, :]] * (seq // 128), axis=1)).astype(BF16)
            p_buf[rs, :] = p
            o = dot_nn(p, kv_all[b, :, d:])
            dvec = jnp.sum(o * do_v[slot, g].reshape(rows, d)[rs].astype(F32), axis=1, keepdims=True)
            d_buf[rs, :] = jnp.broadcast_to(dvec, (rb, 128))
            put_rows(o_v, slot, g, i, o.astype(BF16))

        def put_rows(ref, slot, g, i, v):
            r = i * rb
            while r < (i + 1) * rb:
                n = min((i + 1) * rb - r, tok - r % tok)
                ref[slot, g, r // tok, r % tok:r % tok + n, :] = v[r - i * rb:r - i * rb + n]
                r += n

        def dq_rows(b, g, slot, i):
            rs = slice(i * rb, (i + 1) * rb)
            dq = dot_nn(ds_buf[rs, :], kv_all[b, :, :d]) * scale
            lo, hi = dq[:, :half], dq[:, half:]
            cs, sn = cos4[rs, :], sin4[rs, :]
            put_rows(dq_v, slot, g, i, jnp.concatenate([(lo * cs + hi * sn).astype(BF16), (hi * cs - lo * sn).astype(BF16)], axis=1))

        def grads(b, g, slot, i):
            cols = slice(i * 256, (i + 1) * 256)
            do = do_v[slot, g].reshape(rows, d)
            p = p_buf[:, cols]
            dp = dot_nt(do, kv_all[b, cols, d:])
            dvec = d_buf[...]
            if i > 0 and part[i] > part[i - 1]:
                z = None
                for r in range(part[i - 1], part[i], 8):
                    v = l_buf[1 - g, r:r + 8, :]
                    z = v if z is None else jnp.minimum(z, v)
                dvec = dvec + jnp.concatenate([jnp.minimum(z, 0.0)] * (rows // 8), axis=0)
            dd = jnp.concatenate([dvec, dvec], axis=1)
            ds = (p.astype(F32) * (dp - dd)).astype(BF16)
            ds_buf[:, cols] = ds
            dk = dot_nn(q_t[g], ds)
            dv = dot_nn(do_t[g], p)
            if g == 0:
                dk_t[:, cols] = dk
                dv_t[:, cols] = dv
            else:
                dk_t[:, cols] += dk
                dv_t[:, cols] += dv

        def close_kv(b, i):
            cols = slice(i * 256, (i + 1) * 256)
            kv_all[b, cols, :d] = (dk_t[:, cols] * scale).T.astype(BF16)
            kv_all[b, cols, d:] = dv_t[:, cols].T.astype(BF16)

        enter((mate, cw, ccw))
        gather(1).pass_on(lambda j: kv0_hbm.at[1, blk(j)])
        if nb > 2:
            own(2)
        for x in load(0, 0):
            x.start()

        def first(j):
            return pltpu.make_async_copy(kv0_hbm.at[0, blk(j)], kvb(0, j), first_sem.at[j])

        def second(j, n):
            return pltpu.make_async_copy(kv0_hbm.at[1, blk(j)], kvb(1, j), first_sem.at[8 + n])
        arrived = ((c >= 0, mate, 0), (c >= 1, me - 2, 1), (c == 3, me - 6, 2))
        for j in range(8):
            @pl.when(j <= 2 * c + 1)
            def _():
                first(j).start()
        for b in range(1, nb):
            own_copy(b).start()
        for cond, j, i in arrived:
            @pl.when(cond)
            def _():
                second(j, i).start()

        @pl.loop(2 * c + 2, 8)
        def _(j):
            for b in range(nb):
                kv_all[b, blk(j), :] = jnp.zeros((tok, 2 * d), BF16)
        for j in range(rows // tok):
            cos4[j * tok:(j + 1) * tok, :] = cos_ref[...]
            sin4[j * tok:(j + 1) * tok, :] = sin_ref[...]
        ds_buf[...] = jnp.zeros_like(ds_buf)
        for x in load(0, 0):
            x.wait()
        for i in range(n_rb):
            turn(0, 0, i)
        for j in range(8):
            @pl.when(j <= 2 * c + 1)
            def _():
                first(j).wait()
        for cond, j, i in arrived:
            @pl.when(cond)
            def _():
                second(j, i).wait()
        for i in range(n_blk):
            scores(0, 0, 0, i)
        for i in range(n_blk):
            softmax(0, i)

        def comm_steps(b, steps):
            for lag, stage in steps:
                @pl.when(b >= lag)
                def _():
                    stage(b - lag)

        @pl.loop(0, nb)
        def _(b):
            slot = lax.rem(b, 2)
            nxt = jnp.minimum(b + 1, nb - 1)
            prev = jnp.maximum(b - 1, 0)

            @pl.when(b + 1 < nb)
            def _():
                for x in load(b + 1, 1 - slot):
                    x.start()

            @pl.when(b + 3 < nb)
            def _():
                own(b + 3)

            @pl.when((b >= 1) & (b + 2 < nb))
            def _():
                gather(b + 2).forward()

            @pl.when((b >= 1) & (b + 1 < nb))
            def _():
                gather(b + 1).last()
            comm_steps(b, ((3, stage2), (4, stage3)))

            @pl.when(b >= 2)
            def _():
                drain(b - 1)

            @pl.when(b >= 2)
            def _():
                stored(store_o(b - 2, slot))
            spare = jnp.where(b >= 1, b - 1, nb)
            for i in range(n_blk):
                scores(b, 1, slot, i)
                if i % 2 == 1:
                    out_rows(b, 0, slot, i // 2)
                    dq_rows(prev, 1, 1 - slot, i // 2)
                    turn(1, slot, i // 2)
            for i in range(n_blk):
                close_kv(spare, i)

            @pl.when(b >= 1)
            def _():
                for x in store_dq(b - 1, 1 - slot):
                    x.start()
                to_mate(b - 1)

            @pl.when(b == 0)
            def _():
                gather(1).last()
            for i in range(n_blk):
                grads(b, 0, slot, i)
                softmax(1, i)

            @pl.when(b + 1 < nb)
            def _():
                for x in load(b + 1, 1 - slot):
                    x.wait()
                ready(b + 1)
            if nb > 2:
                @pl.when(b == 0)
                def _():
                    gather(2).forward()

            @pl.when(b >= 2)
            def _():
                stored(store_dq(b - 2, slot))
            nslot = lax.rem(nxt, 2)
            for i in range(n_blk):
                scores(nxt, 0, nslot, i)
                if i % 2 == 1:
                    out_rows(b, 1, slot, i // 2)
                    dq_rows(b, 0, slot, i // 2)
                    turn(0, nslot, i // 2)
            for x in store_o(b, slot):
                x.start()
            comm_steps(b, ((1, stage1),))
            for i in range(n_blk):
                grads(b, 1, slot, i)
                softmax(0, i)

        drain(nb - 1)
        for i in range(n_rb):
            dq_rows(nb - 1, 1, (nb - 1) % 2, i)
        for i in range(n_blk):
            close_kv(nb - 1, i)
        for x in store_dq(nb - 1, (nb - 1) % 2):
            x.start()
        to_mate(nb - 1)

    slab = pltpu.VMEM((2, 2, rows // tok, tok, d), BF16)
    pl.run_scoped(attend, slab, slab, pltpu.VMEM((2, rows, seq), F32), pltpu.VMEM((rows, 128), F32), pltpu.VMEM((2, rows, 128), F32),
                  pltpu.VMEM((rows, seq), BF16), pltpu.VMEM((rows, seq), BF16), pltpu.VMEM((2, d, rows), BF16),
                  pltpu.VMEM((2, d, rows), BF16), pltpu.VMEM((d, seq), F32), pltpu.VMEM((d, seq), F32),
                  pltpu.VMEM((rows, 128), F32), pltpu.VMEM((rows, half), F32), pltpu.VMEM((rows, half), F32))
    n = nb

    def first_products(big, a_v, at, acc_v):
        pr = Products(big, a_v, at, ld_sem, b_sem)
        for x in pr.load_b(dy_hbm, dyp_hbm):
            x.start()
        for b in (n - 2, n - 1):
            stored(store_o(b, b % 2))
        for b in range(n):
            handed(op_hbm, o_v, 0, b, b % 2).wait_recv()

        def fetch(r):
            return pr.load_a(r, o_hbm.at[:, k, rel[r]], op_hbm.at[:, rel[r]])

        def save(r):
            return pltpu.make_async_copy(acc_v.at[r], acc_hbm.at[r], acc_sem.at[r])
        for r in range(2):
            for x in fetch(r):
                x.start()

        todo = [((stage2, n - 3), (stage3, n - 4)), ((stage1, n - 1), (stage2, n - 2), (stage3, n - 3)),
                ((stage2, n - 1), (stage3, n - 2)), ((stage3, n - 1),)]

        def steps(i):
            for stage, b in todo[i]:
                if b >= 0:
                    stage(b)
        steps(0)
        steps(1)
        for r in range(2):
            for x in fetch(r):
                x.wait()
            pr.turn(0, a_v.at[r, 0])
            pr.turn(1, a_v.at[r, 1])
            if r == 0:
                for x in pr.load_b(dy_hbm, dyp_hbm):
                    x.wait()
            pr.columns(acc_v.at[r], 0, 4)
            save(r).start()
        steps(2)
        steps(3)
        for r in range(2):
            save(r).wait()

    pl.run_scoped(first_products, pltpu.VMEM((2,) + dy_hbm.shape, BF16), pltpu.VMEM((2, 2, nb, tok, d), BF16),
                  pltpu.VMEM((2, d, nb * tok), BF16), pltpu.VMEM((2, 2, d, dy_hbm.shape[1] // 2), F32))
    for b in (n - 2, n - 1):
        stored(store_dq(b, b % 2))
    for b in range(n):
        handed(dqp_hbm, dq_v, 1, b, b % 2).wait_recv()
        fin_copy(b).wait()
        for cond, slot in ((c == 3, 0), (c >= 1, 1), (c >= 2, 2)):
            @pl.when(cond)
            def _():
                r_copy(b, 0, slot, cw).wait_send()


def attention(q, do, kv, kv0, dy, dy_p, cos_t, sin_t):
    nb, _, hp, tok, d = q.shape
    seq = tok * 8
    rows = hp * tok
    any_spec = pl.BlockSpec(memory_space=pl.ANY)
    vmem = pl.BlockSpec(memory_space=pltpu.VMEM)
    dma = pltpu.SemaphoreType.DMA
    slab = pltpu.VMEM((2, 2, hp, tok, d), BF16)
    out = jax.ShapeDtypeStruct(q.shape, BF16)
    outp = jax.ShapeDtypeStruct((nb, hp, tok, d), BF16)
    return pl.pallas_call(
        functools.partial(attn_body, nb, tok, seq, d),
        in_specs=[any_spec] * 6 + [vmem, vmem],
        out_specs=[any_spec] * 6,
        out_shape=[out, out, jax.ShapeDtypeStruct(kv.shape, BF16), outp, outp,
                   jax.ShapeDtypeStruct((2, 2, d, dy.shape[1] // 2), F32)],
        scratch_shapes=[pltpu.VMEM((nb + 1, seq, 2 * d), BF16), slab, slab,
                        pltpu.VMEM((nb, 4, tok, 2 * d), BF16), pltpu.VMEM((nb, 3, tok, 2 * d), BF16),
                        dma((nb - 1, 7)), dma((nb - 1, 7)), dma((nb, 4)), dma((nb, 4)), dma((nb, 3)), dma((nb, 3)),
                        dma((nb,)), dma((2, 2)), dma((2, 2)), dma((nb,)), dma((2, nb)), dma((2, nb)), dma((11,)),
                        dma((2, 2)), dma((2,)), dma((4,))],
        compiler_params=pltpu.CompilerParams(collective_id=1, has_side_effects=True, vmem_limit_bytes=63 * 2**20),
        cost_estimate=pl.CostEstimate(flops=24 * nb * rows * seq * d, bytes_accessed=40 * 2**20,
                                      transcendentals=2 * nb * rows * seq),
        name="attention",
    )(q, do, kv, kv0, dy, dy_p, cos_t, sin_t)


def proj_body(nb, tok, x_hbm, g_ref, wq_hbm, wk_ref, wv_ref, wo_hbm, dy_hbm, cos_ref, sin_ref,
              kv0_hbm, hn_hbm, q_hbm, do_hbm, kv_hbm, wqf_hbm, wof_hbm, hnp_hbm, dyp_hbm,
              x_v, hn_v, dy_v, wq_v, wo_v, kv_v, out_v,
              send, recv, x_sem, dy_sem, own_sem, out_sem, misc_sem, w_sem, p_send, p_recv, kv_send, kv_recv):
    n_tok, e = x_hbm.shape
    d = kv_v.shape[1] // 2
    half = d // 2
    mc = 2 * tok
    me, k, mate, cw, ccw = ring_ids()
    base = 2 * (me // 2)

    def head(off, par):
        return lax.rem(base + 2 * off + 8, 8) + par
    enter((mate, cw, ccw))

    fulls = (wq_v, wo_v)
    locs = (wq_hbm, wo_hbm)

    def half_of(w, ref, j):
        n = ref.shape[0] // 2
        return ref.at[pl.ds(j * n, n)]

    sends = []

    def send_full(w, h, j, to, own=False):
        src = locs[w] if own else fulls[w].at[h]
        c = rdma(src, fulls[w].at[h], send.at[w, j], recv.at[w, j], to)
        c.start()
        sends.append(c)

    def send_half(w, h, part, j, to):
        c = rdma(half_of(w, fulls[w].at[h], part), half_of(w, fulls[w].at[h], part), send.at[w, j], recv.at[w, j], to)
        c.start()
        sends.append(c)

    def wait_full(w, h, j):
        rdma(fulls[w].at[h], fulls[w].at[h], send.at[w, j], recv.at[w, j], mate).wait_recv()

    def wait_half(w, h, part, j):
        ref = half_of(w, fulls[w].at[h], part)
        rdma(ref, ref, send.at[w, j], recv.at[w, j], mate).wait_recv()

    for w in range(2):
        send_full(w, me, 0, cw, True)
        send_full(w, me, 1, ccw, True)
        send_full(w, me, 4, mate, True)
    own = [pltpu.make_async_copy(locs[w], fulls[w].at[me], own_sem.at[w]) for w in range(2)]
    xs = [pltpu.make_async_copy(x_hbm.at[pl.ds(b * tok, tok)], x_v.at[pl.ds(b * tok, tok)], x_sem.at[b]) for b in range(nb)]
    for c in xs:
        c.start()
    for c in own:
        c.start()
    dyc = pltpu.make_async_copy(dy_hbm, dy_v, dy_sem)
    dyc.start()

    gain = g_ref[...].astype(F32)
    for b in range(nb):
        xs[b].wait()

        @pl.loop(0, tok // 16, unroll=2)
        def _(r):
            rs = pl.ds(pl.multiple_of(b * tok + r * 16, 16), 16)
            x = x_v[rs, :].astype(F32)
            c = x - jnp.mean(x, axis=1, keepdims=True)
            inv = lax.rsqrt(jnp.mean(c * c, axis=1, keepdims=True) + LN_EPS)
            hn_v[rs, :] = (c * inv * gain).astype(BF16)
    hn_out = pltpu.make_async_copy(hn_v, hn_hbm, misc_sem.at[0])
    hn_out.start()
    to_mate = [rdma(hn_v, hnp_hbm, p_send.at[0], p_recv.at[0], mate), rdma(dy_hbm, dyp_hbm, p_send.at[1], p_recv.at[1], mate)]
    for c in to_mate:
        c.start()

    def rope_rows(raw):
        lo, hi = raw[:, :half], raw[:, half:d]
        cs, sn = jnp.concatenate([cos_ref[...]] * 2, axis=0), jnp.concatenate([sin_ref[...]] * 2, axis=0)
        return lo * cs - hi * sn, hi * cs + lo * sn

    @pl.loop(0, n_tok // mc)
    def _(i):
        rs = pl.ds(pl.multiple_of(i * mc, mc), mc)
        lo, hi = rope_rows(dot_nn(hn_v[rs, :], wk_ref[...]))
        kv_v[rs, :half] = lo.astype(BF16)
        kv_v[rs, half:d] = hi.astype(BF16)
        kv_v[rs, d:] = dot_nn(hn_v[rs, :], wv_ref[...]).astype(BF16)
    kv_out = pltpu.make_async_copy(kv_v, kv_hbm, misc_sem.at[1])
    kv_out.start()

    outs = []
    saves = []

    def save(w, h):
        c = pltpu.make_async_copy(fulls[w].at[h], (wqf_hbm, wof_hbm)[w].at[h], w_sem.at[len(saves)])
        c.start()
        saves.append(c)

    def project(w, h):
        slot = len(outs) % 4
        if len(outs) >= 4:
            outs[-4].wait()

        @pl.loop(0, n_tok // mc)
        def _(i):
            rs = pl.ds(pl.multiple_of(i * mc, mc), mc)
            if w == 0:
                lo, hi = rope_rows(dot_nn(hn_v[rs, :], wq_v[h]))
                o0 = lo.reshape(2, tok, half).astype(BF16)
                o1 = hi.reshape(2, tok, half).astype(BF16)
                out_v[slot, pl.ds(2 * i, 2), :, :half] = o0
                out_v[slot, pl.ds(2 * i, 2), :, half:] = o1
            else:
                out_v[slot, pl.ds(2 * i, 2)] = dot_nt(dy_v[rs, :], wo_v[h]).reshape(2, tok, d).astype(BF16)
        c = pltpu.make_async_copy(out_v.at[slot], (q_hbm, do_hbm)[w].at[:, lax.rem(h, 2), h // 2], out_sem.at[slot])
        c.start()
        outs.append(c)
        save(w, h)

    other = 1 - k
    for w in range(2):
        own[w].wait()
        if w == 1:
            dyc.wait()
        project(w, me)
        wait_full(w, mate, 4)
        project(w, mate)
    for w in range(2):
        wait_full(w, head(-1, k), 0)
        send_half(w, head(-1, k), 0, 2, cw)
        wait_full(w, head(1, k), 1)
        send_half(w, head(1, k), 1, 3, ccw)
        send_full(w, head(-1, k), 5, mate)
        send_full(w, head(1, k), 6, mate)
        project(w, head(-1, k))
        project(w, head(1, k))
        wait_full(w, head(-1, other), 5)
        project(w, head(-1, other))
        wait_full(w, head(1, other), 6)
        project(w, head(1, other))

    def early(n):
        def blk(j):
            return kv0_hbm.at[n, pl.ds(pl.multiple_of(j * tok, 16), tok)]
        return Gather((me, k, mate, cw, ccw), me // 2, blk, lambda t: kv_send.at[n, t], lambda t: kv_recv.at[n, t])
    first, second = early(0), early(1)
    first.own(kv_v.at[pl.ds(0, tok)])
    own0 = pltpu.make_async_copy(kv_v.at[pl.ds(0, tok)], first.block(me), misc_sem.at[2])
    own0.start()
    for w in range(2):
        wait_half(w, head(2, k), 0, 2)
        send_half(w, head(2, k), 0, 7, mate)
        wait_half(w, head(2, k), 1, 3)
        send_half(w, head(2, k), 1, 8, mate)
        project(w, head(2, k))
        if w == 1:
            first.forward()
            second.own(kv_v.at[pl.ds(tok, tok)])
        wait_half(w, head(2, other), 0, 7)
        wait_half(w, head(2, other), 1, 8)
        project(w, head(2, other))
    first.last()
    for c in outs[-4:] + saves + [hn_out, kv_out, own0]:
        c.wait()
    first.ready()
    first.drain()
    second.arrived()
    second.ready((3,))
    second.drain((0, 2, 3))
    for c in sends:
        c.wait_send()
    for c in to_mate:
        c.wait()


def project(x, gain, wq, w_k, w_v, wo, dy, cos_t, sin_t):
    nb, tok, e = x.shape
    d = wq.shape[1]
    n_heads = 8
    n_tok = nb * tok
    any_spec = pl.BlockSpec(memory_space=pl.ANY)
    vmem = pl.BlockSpec(memory_space=pltpu.VMEM)
    act = jax.ShapeDtypeStruct((nb, 2, n_heads // 2, tok, d), BF16)
    dma = pltpu.SemaphoreType.DMA
    flops = 2 * n_tok * e * (2 * n_heads + 2) * d
    kv0, hn, q, do, kv, wqf, wof, hn_p, dy_p = pl.pallas_call(
        functools.partial(proj_body, nb, tok),
        in_specs=[any_spec, vmem, any_spec, vmem, vmem, any_spec, any_spec, vmem, vmem],
        out_specs=[any_spec] * 9,
        out_shape=[jax.ShapeDtypeStruct((2, tok * n_heads, 2 * d), BF16), jax.ShapeDtypeStruct((n_tok, e), BF16), act, act, jax.ShapeDtypeStruct((n_tok, 2 * d), BF16),
                   jax.ShapeDtypeStruct((n_heads, e, d), BF16), jax.ShapeDtypeStruct((n_heads, d, e), BF16),
                   jax.ShapeDtypeStruct((n_tok, e), BF16), jax.ShapeDtypeStruct((n_tok, e), BF16)],
        scratch_shapes=[pltpu.VMEM((n_tok, e), BF16), pltpu.VMEM((n_tok, e), BF16), pltpu.VMEM((n_tok, e), BF16),
                        pltpu.VMEM((n_heads, e, d), BF16), pltpu.VMEM((n_heads, d, e), BF16),
                        pltpu.VMEM((n_tok, 2 * d), BF16), pltpu.VMEM((4, nb, tok, d), BF16),
                        dma((2, 9)), dma((2, 9)), dma((nb,)), dma(()), dma((2,)), dma((4,)), dma((3,)), dma((16,)), dma((2,)), dma((2,)), dma((2, 7)), dma((2, 7))],
        compiler_params=pltpu.CompilerParams(collective_id=0, has_side_effects=True, vmem_limit_bytes=60 * 2**20),
        cost_estimate=pl.CostEstimate(flops=flops, bytes_accessed=60 * 2**20, transcendentals=0),
        name="project",
    )(x.reshape(n_tok, e), gain, wq, w_k, w_v, wo, dy.reshape(n_tok, e), cos_t, sin_t)
    return kv0, hn, q, do, kv.reshape(nb, tok, 2 * d), wqf, wof, hn_p, dy_p


def grads_body(nb, tok, o_hbm, op_hbm, acc_hbm, dq_hbm, dqp_hbm, hn_hbm, hnp_hbm, dy_hbm, dyp_hbm, dkv_hbm,
               wq_hbm, wo_hbm, wk_hbm, wv_hbm, x_hbm, g_ref, cos_ref, sin_ref,
               y_hbm, gx_hbm, gln_ref, gwo_ref, gwq_ref, gkv_hbm,
               acc, acc_kv, rbuf, rbuf_kv, kind, kp, dkv_v, fin_kv, gln_acc, gl_recv,
               rs_send, rs_recv, kv_send, kv_recv, ag_send, ag_recv, gl_send, gl_rsem, kp_sem, ld_sem, b_sem, t_sem, a_sem):
    n_tok, e = x_hbm.shape
    d = wk_hbm.shape[1]
    half = d // 2
    eh, eq = e // 2, e // 4
    me, k, mate, cw, ccw = ring_ids()
    c = me // 2
    rel = [lax.rem(c + o, 4) for o in (3, 1, 2, 0)]
    enter([lax.rem(me + o, 8) for o in range(1, 8)])

    order = ((2, 1), (2, 0))

    def hop(s, dr, j):
        first = acc_hbm.at[dr, dr] if s == 0 else acc.at[s, dr, dr]
        src = first if j == 0 else rbuf.at[s, dr, j - 1]
        return rdma(src, rbuf.at[s, dr, j], rs_send.at[s, dr, j], rs_recv.at[s, dr, j], (cw, ccw)[dr])

    def hop_kv(dr, j):
        src = acc_kv.at[dr, dr] if j == 0 else rbuf_kv.at[dr, j - 1]
        return rdma(src, rbuf_kv.at[dr, j], kv_send.at[dr, j], kv_recv.at[dr, j], (cw, ccw)[dr])

    def add(dst, term):
        @pl.loop(0, dst.shape[0] // 32)
        def _(i):
            rs = pl.ds(pl.multiple_of(i * 32, 32), 32)
            dst[rs, :] = dst[rs, :] + term[rs, :]

    def pass_on(s, j):
        for dr in range(2):
            hop(s, dr, j - 1).wait_recv()
            add(rbuf.at[s, dr, j - 1], acc.at[s, order[dr][j - 1], dr])
            hop(s, dr, j).start()

    def pass_on_kv(j):
        for dr in range(2):
            hop_kv(dr, j - 1).wait_recv()
            add(rbuf_kv.at[dr, j - 1], acc_kv.at[order[dr][j - 1], dr])
            hop_kv(dr, j).start()

    def finish(s, out):
        for dr in range(2):
            hop(s, dr, 2).wait_recv()

            @pl.loop(0, d // 32)
            def _(i):
                rs = pl.ds(pl.multiple_of(i * 32, 32), 32)
                out[rs, dr * eh:(dr + 1) * eh] = (rbuf[s, dr, 2, rs, :] + acc[s, 3, dr, rs, :]).astype(BF16)

    def piece(kk, j, lo=0, n=None):
        return gkv_hbm.at[kk, pl.ds(lo, d if n is None else n), pl.ds(pl.multiple_of(j * eq, 128), eq)]

    def ag(tag, ref, to, src=None):
        return rdma(ref if src is None else src, ref, ag_send.at[tag], ag_recv.at[tag], to)

    def ag_far(tag, to):
        return ag(tag, piece(k, rel[(0, 1)[tag - 3]], (tag - 3) * half, half), to)

    own_piece = pltpu.make_async_copy(fin_kv, piece(k, c), t_sem.at[5])

    def finish_kv():
        for dr in range(2):
            hop_kv(dr, 2).wait_recv()
            fin_kv[:, dr * (eq // 2):(dr + 1) * (eq // 2)] = rbuf_kv[dr, 2] + acc_kv[3, dr]
        ag(0, piece(k, c), cw, fin_kv).start()
        ag(1, piece(k, c), ccw, fin_kv).start()
        ag(2, piece(k, c), mate, fin_kv).start()
        own_piece.start()

    def ag_forward():
        ag(0, piece(k, rel[0]), cw).wait_recv()
        ag_far(3, cw).start()
        ag(1, piece(k, rel[1]), cw).wait_recv()
        ag_far(4, ccw).start()
        ag(5, piece(k, rel[0]), mate).start()
        ag(6, piece(k, rel[1]), mate).start()

    def ag_last():
        far = [piece(k, rel[2], i * half, half) for i in range(2)]
        for i in range(2):
            ag(3 + i, far[i], cw).wait_recv()
            ag(7 + i, far[i], mate).start()
        ag(2, piece(1 - k, c), mate).wait_recv()
        ag(5, piece(1 - k, rel[0]), mate).wait_recv()
        ag(6, piece(1 - k, rel[1]), mate).wait_recv()
        for i in range(2):
            ag(7 + i, piece(1 - k, rel[2], i * half, half), mate).wait_recv()
        for tag in range(3):
            ag(tag, piece(k, c), cw, fin_kv).wait_send()
        for tag in (3, 4, 7, 8):
            ag(tag, far[0], cw).wait_send()
        for tag in (5, 6):
            ag(tag, piece(k, c), cw).wait_send()
        own_piece.wait()

    dkv_in = pltpu.make_async_copy(dkv_hbm, dkv_v, t_sem.at[4])
    dkv_in.start()
    kp_copy = rdma(kind.at[1 - k], kp, kp_sem.at[0], kp_sem.at[1], mate)

    for dr in range(2):
        hop(0, dr, 0).start()
    acc_in = [pltpu.make_async_copy(acc_hbm.at[r], acc.at[0, r], a_sem.at[r]) for r in range(2)]
    for x in acc_in:
        x.start()

    def products(big, a_v, at):
        pr = Products(big, a_v, at, ld_sem, b_sem)
        dy_in = pr.load_b(dy_hbm, dyp_hbm)
        hn_in = pr.load_b(hn_hbm, hnp_hbm)
        jobs = [(0, 2), (0, 3)] + [(1, r) for r in range(4)]

        def fetch(i):
            s, r = jobs[i]
            return pr.load_a(i, (o_hbm, dq_hbm)[s].at[:, k, rel[r]], (op_hbm, dqp_hbm)[s].at[:, rel[r]])
        for x in dy_in:
            x.start()
        for i in range(2):
            for x in fetch(i):
                x.start()
        dkv_in.wait()
        for b in range(nb):
            lo, hi = dkv_v[b, :, :half].astype(F32), dkv_v[b, :, half:d].astype(F32)
            cs, sn = cos_ref[...], sin_ref[...]
            kind[0, b, :, :half] = (lo * cs + hi * sn).astype(BF16)
            kind[0, b, :, half:] = (hi * cs - lo * sn).astype(BF16)
            kind[1, b] = dkv_v[b, :, d:]
        kp_copy.start()
        for i, (s, r) in enumerate(jobs):
            if i == 2:
                pr.turn(0, kind.at[k])
                kp_copy.wait_recv()
                pr.turn(1, kp)
                for x in hn_in:
                    x.wait()
                for q in range(4):
                    for dr in range(2):
                        acc_kv[q, dr] = pr.both(pl.ds(pl.multiple_of(rel[q] * eq + dr * (eq // 2), 128), eq // 2))
                for dr in range(2):
                    hop_kv(dr, 0).start()
            for x in fetch(i):
                x.wait()
            pr.turn(0, a_v.at[i % 2, 0])
            pr.turn(1, a_v.at[i % 2, 1])
            if i + 2 < len(jobs):
                for x in fetch(i + 2):
                    x.start()
            if i == 0:
                for x in dy_in:
                    x.wait()
            if s == 1 and r < 2:
                pr.columns(acc.at[s, r], 0, 2, 2 * r)
                hop(s, r, 0).start()
                pr.columns(acc.at[s, r], 2, 4, 2 * r)
            else:
                pr.columns(acc.at[s, r], 0, 4)
            if i == 1:
                for x in hn_in:
                    x.start()

    pl.run_scoped(products, pltpu.VMEM((2, n_tok, e), BF16), pltpu.VMEM((2, 2, nb, tok, d), BF16), pltpu.VMEM((2, d, n_tok), BF16))
    for x in acc_in:
        x.wait()
    pass_on(0, 1)
    pass_on_kv(1)

    mc = 2 * tok
    units = nb // 2

    def attn_out(wo_v, o_v, x_v, y_v):
        w_in = pltpu.make_async_copy(wo_hbm, wo_v, b_sem.at[0])
        w_in.start()

        def load(u):
            return (pltpu.make_async_copy(o_hbm.at[pl.ds(2 * u, 2)], o_v.at[u % 2], ld_sem.at[u % 2, 0]),
                    pltpu.make_async_copy(x_hbm.at[pl.ds(u * mc, mc)], x_v.at[u % 2], ld_sem.at[u % 2, 1]))

        def put(u):
            return pltpu.make_async_copy(y_v.at[u % 2], y_hbm.at[pl.ds(u * mc, mc)], t_sem.at[u % 2])
        for x in load(0):
            x.start()
        w_in.wait()
        for u in range(units):
            if u + 1 < units:
                for x in load(u + 1):
                    x.start()
            for x in load(u):
                x.wait()
            if u >= 2:
                put(u - 2).wait()
            sl = u % 2

            @pl.loop(0, 4)
            def _(n):
                cols = pl.ds(pl.multiple_of(n * eq, 128), eq)
                o_rows = jnp.concatenate([jnp.concatenate([o_v[sl, i, h % 2, h // 2] for h in range(8)], axis=1) for i in range(2)], axis=0)
                r = dot_nn(o_rows, wo_v[:, cols])
                y_v[sl, :, cols] = (x_v[sl, :, cols].astype(F32) + r).astype(BF16)
            put(u).start()
        for u in range(max(0, units - 2), units):
            put(u).wait()

    pl.run_scoped(attn_out, pltpu.VMEM((8 * d, e), BF16), pltpu.VMEM((2, 2, 2, 4, tok, d), BF16),
                  pltpu.VMEM((2, mc, e), BF16), pltpu.VMEM((2, mc, e), BF16))
    pass_on(1, 1)

    def hidden_grad(wq_v, wk_v, wv_v, dq_v, x_v, dy_v, dh, gx_v):
        w_in = pltpu.make_async_copy(wq_hbm, wq_v, b_sem.at[0])
        w_in.start()
        w2_in = (pltpu.make_async_copy(wk_hbm, wk_v, b_sem.at[1]), pltpu.make_async_copy(wv_hbm, wv_v, ld_sem.at[1, 1]))
        for x in w2_in:
            x.start()

        def load(u):
            return (pltpu.make_async_copy(dq_hbm.at[pl.ds(2 * u, 2)], dq_v, ld_sem.at[0, 0]),
                    pltpu.make_async_copy(x_hbm.at[pl.ds(u * mc, mc)], x_v, ld_sem.at[0, 1]),
                    pltpu.make_async_copy(dy_hbm.at[pl.ds(u * mc, mc)], dy_v, ld_sem.at[1, 0]))

        def put(u):
            return pltpu.make_async_copy(gx_v, gx_hbm.at[pl.ds(u * mc, mc)], t_sem.at[0])
        gain = g_ref[...].astype(F32)
        gln_acc[...] = jnp.zeros_like(gln_acc)
        for x in load(0):
            x.start()
        w_in.wait()
        for x in w2_in:
            x.wait()
        for u in range(units):
            for x in load(u):
                x.wait()

            @pl.loop(0, 4)
            def _(n):
                rows = pl.ds(pl.multiple_of(n * eq, 128), eq)
                t = None
                for h in range(8):
                    a = jnp.concatenate([dq_v[i, h % 2, h // 2] for i in range(2)], axis=0)
                    p = dot_nt(a, wq_v[h, rows, :])
                    t = p if t is None else t + p
                for j in range(2):
                    a = jnp.concatenate([kind[j, 2 * u + i] for i in range(2)], axis=0)
                    t = t + dot_nt(a, (wk_v, wv_v)[j][rows, :])
                dh[:, rows] = t
            if u >= 1:
                put(u - 1).wait()

            @pl.loop(0, mc // 16)
            def _(r):
                rs = pl.ds(pl.multiple_of(r * 16, 16), 16)
                x = x_v[rs, :].astype(F32)
                cx = x - jnp.mean(x, axis=1, keepdims=True)
                inv = lax.rsqrt(jnp.mean(cx * cx, axis=1, keepdims=True) + LN_EPS)
                xh = cx * inv
                g = dh[rs, :]
                pr = g * xh
                gln_acc[...] += pr[:8] + pr[8:]
                gh = g * gain
                m1 = jnp.mean(gh, axis=1, keepdims=True)
                m2 = jnp.mean(gh * xh, axis=1, keepdims=True)
                gx_v[rs, :] = (inv * (gh - m1 - xh * m2) + dy_v[rs, :].astype(F32)).astype(BF16)
            put(u).start()
            if u + 1 < units:
                for x in load(u + 1):
                    x.start()
            if u == units // 2 - 1:
                pass_on(0, 2)
                pass_on_kv(2)
        put(units - 1).wait()

    pl.run_scoped(hidden_grad, pltpu.VMEM((8, e, d), BF16), pltpu.VMEM((e, d), BF16), pltpu.VMEM((e, d), BF16), pltpu.VMEM((2, 2, 4, tok, d), BF16),
                  pltpu.VMEM((mc, e), BF16), pltpu.VMEM((mc, e), BF16), pltpu.VMEM((mc, e), F32), pltpu.VMEM((mc, e), BF16))
    gl_recv[me] = jnp.sum(gln_acc[...], axis=0, keepdims=True)
    pass_on(1, 2)
    finish(0, gwo_ref)
    finish_kv()
    gl = [rdma(gl_recv.at[me], gl_recv.at[me], gl_send.at[o - 1], gl_rsem.at[o - 1], lax.rem(me + o, 8)) for o in range(1, 8)]
    for x in gl:
        x.start()
    finish(1, gwq_ref)
    ag_forward()
    for o in range(1, 8):
        src = lax.rem(me + 8 - o, 8)
        rdma(gl_recv.at[src], gl_recv.at[src], gl_send.at[o - 1], gl_rsem.at[o - 1], mate).wait_recv()
    total = gl_recv[0]
    for i in range(1, 8):
        total = total + gl_recv[i]
    gln_ref[...] = total
    ag_last()
    for x in gl:
        x.wait_send()
    kp_copy.wait_send()
    for dr in range(2):
        for j in range(3):
            hop_kv(dr, j).wait_send()
            for s in range(2):
                hop(s, dr, j).wait_send()


def gradients(o, o_p, acc, dq, dq_p, hn, hn_p, dy, dy_p, dkv, wqf, wof, w_k, w_v, x, gain, cos_t, sin_t):
    nb, tok, e = x.shape
    n_tok = nb * tok
    d = dq.shape[-1]
    any_spec = pl.BlockSpec(memory_space=pl.ANY)
    vmem = pl.BlockSpec(memory_space=pltpu.VMEM)
    dma = pltpu.SemaphoreType.DMA
    tokens = jax.ShapeDtypeStruct((n_tok, e), BF16)
    y, gx, gln, gwo, gwq_t, gkv_t = pl.pallas_call(
        functools.partial(grads_body, nb, tok),
        in_specs=[any_spec] * 15 + [vmem, vmem, vmem],
        out_specs=[any_spec, any_spec, vmem, vmem, vmem, any_spec],
        out_shape=[tokens, tokens, jax.ShapeDtypeStruct((1, e), F32), jax.ShapeDtypeStruct((d, e), BF16),
                   jax.ShapeDtypeStruct((d, e), BF16), jax.ShapeDtypeStruct((2, d, e), F32)],
        scratch_shapes=[pltpu.VMEM((2, 4, 2, d, e // 2), F32), pltpu.VMEM((4, 2, d, e // 8), F32),
                        pltpu.VMEM((2, 2, 3, d, e // 2), F32), pltpu.VMEM((2, 3, d, e // 8), F32),
                        pltpu.VMEM((2, nb, tok, d), BF16), pltpu.VMEM((nb, tok, d), BF16), pltpu.VMEM((nb, tok, 2 * d), BF16),
                        pltpu.VMEM((d, e // 4), F32), pltpu.VMEM((8, e), F32), pltpu.VMEM((8, 1, e), F32),
                        dma((2, 2, 3)), dma((2, 2, 3)), dma((2, 3)), dma((2, 3)), dma((9,)), dma((9,)), dma((7,)), dma((7,)),
                        dma((2,)), dma((2, 2)), dma((2,)), dma((6,)), dma((4,))],
        compiler_params=pltpu.CompilerParams(collective_id=2, has_side_effects=True, vmem_limit_bytes=63 * 2**20),
        cost_estimate=pl.CostEstimate(flops=10 * n_tok * e * e, bytes_accessed=120 * 2**20, transcendentals=0),
        name="gradients",
    )(o, o_p, acc, dq, dq_p, hn, hn_p, dy.reshape(n_tok, e), dy_p, dkv, wqf, wof.reshape(8 * d, e), w_k, w_v, x.reshape(n_tok, e),
      gain, cos_t, sin_t)
    y, gx, gwq, gwk, gwv, gwo, gln = place(nb, y, gx, gwq_t, gkv_t, gwo, gln)
    return y.reshape(nb, tok, e), gx.reshape(nb, tok, e), gln.reshape(e), gwq, gwk, gwv, gwo


def place_body(steps, y_in, gx_in, gq_in, gkv_in, go_in, gl_in, y, gx, gq, gk, gv, go, gl,
               y_v, gx_v, gq_v, gkv_v, go_v, gl_v, gq_t, gk_t, gv_t, in_sem, y_sem, out_sem, t_sem):
    n, w = y_in.shape[0] // steps, gq_in.shape[1] // steps
    small_in = [pltpu.make_async_copy(s, v, in_sem.at[i]) for i, (s, v) in enumerate(((gkv_in, gkv_v), (gq_in, gq_v), (go_in, go_v), (gl_in, gl_v)))]
    small_out = [pltpu.make_async_copy(v, o, out_sem.at[i]) for i, (v, o) in enumerate(((go_v, go), (gl_v, gl)))]

    def rows(i, size):
        return pl.ds(i * size, size)
    moves = [(pltpu.make_async_copy(s.at[rows(i, n)], v.at[rows(i, n)], y_sem.at[0, j, i]),
              pltpu.make_async_copy(v.at[rows(i, n)], o.at[rows(i, n)], y_sem.at[1, j, i]))
             for i in range(steps) for j, (s, v, o) in enumerate(((y_in, y_v, y), (gx_in, gx_v, gx)))]
    for x in small_in:
        x.start()
    for x, _ in moves:
        x.start()
    small_in[0].wait()
    small_in[1].wait()
    turned = []
    for i in range(steps):
        for j, (v, o) in enumerate(((gk_t, gk), (gv_t, gv), (gq_t, gq))):
            t = (gkv_v[j, :, i * w:(i + 1) * w] if j < 2 else gq_v[:, i * w:(i + 1) * w].astype(F32)).T
            v[i * w:(i + 1) * w, :] = t.astype(v.dtype)
            c = pltpu.make_async_copy(v.at[rows(i, w)], o.at[rows(i, w)], t_sem.at[j, i])
            c.start()
            turned.append(c)
        for x, z in moves[2 * i:2 * i + 2]:
            x.wait()
            z.start()
    for x, z in zip(small_in[2:], small_out):
        x.wait()
        z.start()
    for c in turned + small_out + [z for _, z in moves]:
        c.wait()


def place(steps, y, gx, gwq_t, gkv_t, gwo, gln):
    e = y.shape[1]
    d = gwo.shape[0]
    any_spec = pl.BlockSpec(memory_space=pl.ANY)
    dma = pltpu.SemaphoreType.DMA
    vm = pltpu.VMEM
    return pl.pallas_call(
        functools.partial(place_body, steps),
        in_specs=[any_spec] * 6,
        out_specs=[any_spec] * 7,
        out_shape=[jax.ShapeDtypeStruct(y.shape, BF16), jax.ShapeDtypeStruct(y.shape, BF16), jax.ShapeDtypeStruct((e, d), BF16),
                   jax.ShapeDtypeStruct((e, d), F32), jax.ShapeDtypeStruct((e, d), F32), jax.ShapeDtypeStruct((d, e), BF16),
                   jax.ShapeDtypeStruct((1, e), F32)],
        scratch_shapes=[vm(y.shape, BF16), vm(y.shape, BF16), vm((d, e), BF16), vm((2, d, e), F32), vm((d, e), BF16), vm((1, e), F32),
                        vm((e, d), BF16), vm((e, d), F32), vm((e, d), F32),
                        dma((4,)), dma((2, 2, steps)), dma((2,)), dma((3, steps))],
        compiler_params=pltpu.CompilerParams(vmem_limit_bytes=63 * 2**20),
        cost_estimate=pl.CostEstimate(flops=0, bytes_accessed=8 * y.size + 24 * gwo.size, transcendentals=0),
        name="place",
    )(y, gx, gwq_t, gkv_t, gwo, gln)


def solution(mesh):
    act_spec = P('dp', 'tp', None)

    def device_step(x_loc, ln_scale, wq_loc, w_k, w_v, wo_loc, dy_loc):
        n_batch, tok, model_dim = x_loc.shape
        d = w_k.shape[1]
        t0 = lax.axis_index('tp') * tok
        cos_t, sin_t = rope_tables(t0 + jnp.arange(tok), d)

        gain = ln_scale.reshape(1, model_dim)
        kv0, hn, q, do, kv_loc, wq_h, wo_h, hn_p, dy_p = project(x_loc, gain, wq_loc, w_k, w_v, wo_loc, dy_loc, cos_t, sin_t)
        o, dq, dkv_loc, o_p, dq_p, acc = attention(q, do, kv_loc, kv0, dy_loc.reshape(-1, model_dim), dy_p, cos_t, sin_t)
        return gradients(o, o_p, acc, dq, dq_p, hn, hn_p, dy_loc, dy_p, dkv_loc, wq_h, wo_h, w_k, w_v, x_loc, gain, cos_t, sin_t)

    return jax.shard_map(device_step, mesh=mesh, in_specs=(act_spec, P(None), P(None, 'tp'), P(None, None), P(None, None), P('tp', None), act_spec), out_specs=(act_spec, act_spec, P('dp'), P('dp', 'tp'), P('dp', None), P('dp', None), P(('dp', 'tp'), None)), check_vma=False)
```

```python
import functools
import jax
import jax.numpy as jnp
from jax import lax
from jax.experimental import pallas as pl
from jax.experimental.pallas import tpu as pltpu
from jax.sharding import PartitionSpec as P

LN_EPS = 1e-6
ROPE_BASE = 10000.0
LOG2E = 1.4426950408889634
F32 = jnp.float32
BF16 = jnp.bfloat16


def rope_tables(positions, head_dim):
    half_dim = head_dim // 2
    inv_freq = ROPE_BASE ** (-2.0 * jnp.arange(half_dim, dtype=F32) / head_dim)
    angles = positions.astype(F32)[:, None] * inv_freq[None, :]
    return jnp.cos(angles), jnp.sin(angles)


def rotate(vectors, cos_t, sin_t):
    half_dim = vectors.shape[-1] // 2
    lo_half = vectors[..., :half_dim]
    hi_half = vectors[..., half_dim:]
    return jnp.concatenate([lo_half * cos_t - hi_half * sin_t, hi_half * cos_t + lo_half * sin_t], axis=-1)


def dot_nn(a, b):
    return lax.dot_general(a, b, (((1,), (0,)), ((), ())), preferred_element_type=F32)


def dot_nt(a, b):
    return lax.dot_general(a, b, (((1,), (1,)), ((), ())), preferred_element_type=F32)


def rdma(src, dst, send, recv, to):
    return pltpu.make_async_remote_copy(src_ref=src, dst_ref=dst, send_sem=send, recv_sem=recv,
                                        device_id={'tp': to}, device_id_type=pl.DeviceIdType.MESH)


def ring_ids():
    me = lax.axis_index('tp')
    k = lax.rem(me, 2)
    return me, k, me + 1 - 2 * k, lax.rem(me + 2, 8), lax.rem(me + 6, 8)


def enter(peers):
    barrier = pltpu.get_barrier_semaphore()
    for p in peers:
        pl.semaphore_signal(barrier, inc=1, device_id={'tp': p}, device_id_type=pl.DeviceIdType.MESH)
    pl.semaphore_wait(barrier, len(peers))


class Products:
    def __init__(self, big, a_v, at, ld_sem, b_sem):
        self.big, self.a_v, self.at, self.ld_sem, self.b_sem = big, a_v, at, ld_sem, b_sem
        self.nb, self.tok = a_v.shape[2], a_v.shape[3]
        self.eq = big.shape[2] // 4

    def load_b(self, own, other):
        return (pltpu.make_async_copy(own, self.big.at[0], self.b_sem.at[0]),
                pltpu.make_async_copy(other, self.big.at[1], self.b_sem.at[1]))

    def load_a(self, i, own, other):
        return (pltpu.make_async_copy(own, self.a_v.at[i % 2, 0], self.ld_sem.at[i % 2, 0]),
                pltpu.make_async_copy(other, self.a_v.at[i % 2, 1], self.ld_sem.at[i % 2, 1]))

    def turn(self, j, src):
        tok = self.tok
        for i in range(self.nb // 2):
            self.at[j, :, 2 * i * tok:(2 * i + 2) * tok] = jnp.concatenate([src[2 * i], src[2 * i + 1]], axis=0).T

    def both(self, cols):
        return dot_nn(self.at[0], self.big[0, :, cols]) + dot_nn(self.at[1], self.big[1, :, cols])

    def columns(self, dst, first, last, turned=0):
        eq = self.eq

        @pl.loop(first, last)
        def _(n):
            m = lax.rem(n + turned, 4)
            cols = pl.ds(pl.multiple_of(m * eq, 128), eq)
            dst[m // 2, :, pl.ds(pl.multiple_of(lax.rem(m, 2) * eq, 128), eq)] = self.both(cols)


class Gather:
    def __init__(self, ids, c, block, send, recv):
        self.me, _, self.mate, self.cw, self.ccw = ids
        self.c, self.block, self.send, self.recv = c, block, send, recv

    def copy(self, j, tag, to, src=None):
        ref = self.block(j)
        return rdma(ref if src is None else src, ref, self.send(tag), self.recv(tag), to)

    def own(self, src):
        @pl.when(self.c <= 2)
        def _():
            self.copy(self.me, 0, self.cw, src).start()

        @pl.when(self.c == 0)
        def _():
            self.copy(self.me, 2, self.ccw, src).start()
        self.copy(self.me, 3, self.mate, src).start()

    def arrived(self):
        @pl.when(self.c >= 1)
        def _():
            self.copy(self.me - 2, 0, self.cw).wait_recv()

        @pl.when(self.c == 3)
        def _():
            self.copy(self.me - 6, 2, self.ccw).wait_recv()

    def pass_on(self, src=lambda j: None):
        @pl.when(self.c >= 1)
        def _():
            @pl.when(self.c <= 2)
            def _():
                self.copy(self.me - 2, 1, self.cw, src(self.me - 2)).start()
            self.copy(self.me - 2, 4, self.mate, src(self.me - 2)).start()

        @pl.when(self.c == 3)
        def _():
            self.copy(self.me - 6, 6, self.mate, src(self.me - 6)).start()

    def forward(self):
        self.arrived()
        self.pass_on()

    def last(self):
        @pl.when(self.c >= 2)
        def _():
            self.copy(self.me - 4, 1, self.cw).wait_recv()
            self.copy(self.me - 4, 5, self.mate).start()

    def ready(self, tags=(3, 4, 5, 6)):
        if 3 in tags:
            self.copy(self.mate, 3, self.mate).wait_recv()
        for n, tag in ((1, 4), (2, 5), (3, 6)):
            if tag not in tags:
                continue

            @pl.when(self.c >= n)
            def _():
                self.copy(self.mate - 2 * n, tag, self.mate).wait_recv()

    def drain(self, tags=range(7)):
        c = self.c
        conds = (c <= 2, (c >= 1) & (c <= 2), c == 0, c >= 0, c >= 1, c >= 2, c == 3)
        for tag in tags:
            @pl.when(conds[tag])
            def _():
                self.copy(self.me, tag, self.mate).wait_send()


def attn_body(nb, tok, seq, d, q_hbm, do_hbm, kvl_hbm, kv0_hbm, dy_hbm, dyp_hbm, cos_ref, sin_ref,
              o_hbm, dq_hbm, dkv_hbm, op_hbm, dqp_hbm, acc_hbm,
              kv_all, o_v, dq_v, mrecv, rrecv, big,
              kv_send, kv_recv, m_send, m_recv, r_send, r_recv, own_sem, in_sem, out_sem, fin_sem, p_send, p_recv, first_sem,
              ld_sem, b_sem, acc_sem):
    scale = d ** -0.5
    rows = o_v.shape[2] * tok
    n_blk = seq // 256
    rb = 2 * rows // n_blk
    n_rb = rows // rb
    half = d // 2
    me, k, mate, cw, ccw = ring_ids()
    c = me // 2
    rel = [lax.rem(c + o, 4) for o in (3, 1, 2, 0)]

    def blk(j):
        return pl.ds(pl.multiple_of(j * tok, 16), tok)

    def kvb(b, j):
        return kv_all.at[b, blk(j)]

    def gather(b):
        return Gather((me, k, mate, cw, ccw), c, lambda j: kvb(b, j), lambda t: kv_send.at[b - 1, t], lambda t: kv_recv.at[b - 1, t])

    def own(b):
        gather(b).own(kvl_hbm.at[b])

    def own_copy(b):
        return pltpu.make_async_copy(kvl_hbm.at[b], kvb(b, me), own_sem.at[b])

    def ready(b):
        own_copy(b).wait()

        @pl.when(b == 1)
        def _():
            gather(1).ready((4, 5, 6))

        @pl.when(b > 1)
        def _():
            gather(b).ready()

    def drain(b):
        @pl.when(b == 1)
        def _():
            gather(1).drain((1, 4, 5, 6))

        @pl.when(b > 1)
        def _():
            gather(b).drain()

    def m_copy(b, n):
        return rdma(kvb(b, 2 * n + 1 - k), mrecv.at[lax.rem(b, 2), n], m_send.at[b, n], m_recv.at[b, n], mate)

    def r_copy(b, n, slot, to):
        return rdma(kvb(b, 2 * n + k), rrecv.at[b, slot], r_send.at[b, slot], r_recv.at[b, slot], to)

    def add_into(b, n, other):
        v = kv_all[b, blk(2 * n + k), :].astype(F32) + other[...].astype(F32)
        kv_all[b, blk(2 * n + k), :] = v.astype(BF16)

    def fin_copy(b):
        return pltpu.make_async_copy(kvb(b, me), dkv_hbm.at[b], fin_sem.at[b])

    def to_mate(b):
        for n in range(4):
            @pl.when(c >= n)
            def _():
                m_copy(b, n).start()

    def stage1(b):
        for n in range(4):
            @pl.when(c >= n)
            def _():
                m_copy(b, n).wait()
                add_into(b, n, mrecv.at[lax.rem(b, 2), n])

        @pl.when(c == 3)
        def _():
            r_copy(b, 1, 2, ccw).start()
            r_copy(b, 2, 1, ccw).start()
            r_copy(b, 0, 0, cw).start()
            fin_copy(b).start()

        @pl.when(c == 2)
        def _():
            r_copy(b, 0, 1, ccw).start()

    def stage2(b):
        @pl.when(c == 2)
        def _():
            r_copy(b, 1, 2, ccw).wait_recv()
            add_into(b, 1, rrecv.at[b, 2])
            r_copy(b, 1, 2, ccw).start()
            r_copy(b, 2, 1, ccw).wait_recv()
            add_into(b, 2, rrecv.at[b, 1])
            fin_copy(b).start()

        @pl.when(c == 1)
        def _():
            r_copy(b, 0, 1, ccw).wait_recv()
            add_into(b, 0, rrecv.at[b, 1])
            r_copy(b, 0, 1, ccw).start()

    def stage3(b):
        @pl.when(c == 0)
        def _():
            r_copy(b, 0, 0, cw).wait_recv()
            add_into(b, 0, rrecv.at[b, 0])
            r_copy(b, 0, 1, ccw).wait_recv()
            add_into(b, 0, rrecv.at[b, 1])
            fin_copy(b).start()

        @pl.when(c == 1)
        def _():
            r_copy(b, 1, 2, ccw).wait_recv()
            add_into(b, 1, rrecv.at[b, 2])
            fin_copy(b).start()

    def handed(dst, src, n, b, slot):
        return rdma(src.at[slot, 1 - k], dst.at[b], p_send.at[n, b], p_recv.at[n, b], mate)

    def store_o(b, slot):
        return (pltpu.make_async_copy(o_v.at[slot], o_hbm.at[b], out_sem.at[0, slot]), handed(op_hbm, o_v, 0, b, slot))

    def store_dq(b, slot):
        return (pltpu.make_async_copy(dq_v.at[slot], dq_hbm.at[b], out_sem.at[1, slot]), handed(dqp_hbm, dq_v, 1, b, slot))

    def stored(x):
        x[0].wait()
        x[1].wait_send()

    load_dy = (pltpu.make_async_copy(dy_hbm, big.at[0], b_sem.at[0]), pltpu.make_async_copy(dyp_hbm, big.at[1], b_sem.at[1]))

    def attend(q_v, do_v, s_buf, m_buf, l_buf, p_buf, ds_buf, q_t, do_t, dk_t, dv_t, d_buf, cos4, sin4):
        def load(b, slot):
            return (pltpu.make_async_copy(q_hbm.at[b], q_v.at[slot], in_sem.at[0, slot]),
                    pltpu.make_async_copy(do_hbm.at[b], do_v.at[slot], in_sem.at[1, slot]))

        def scores(b, g, slot, i):
            w = min(512, seq)
            if (i * 256) % w:
                return
            cols = slice(i * 256, i * 256 + w)
            s = dot_nt(q_v[slot, g].reshape(rows, d), kv_all[b, cols, :d]) * (scale * LOG2E)
            col = lax.broadcasted_iota(jnp.int32, (tok, w), 1) + i * 256
            row = lax.broadcasted_iota(jnp.int32, (tok, w), 0) + me * tok
            s = jnp.concatenate([jnp.where(col <= row, s[j * tok:(j + 1) * tok], -1e30) for j in range(rows // tok)], axis=0)
            s_buf[g, :, cols] = s
            m = s[:, :128]
            for j in range(128, w, 128):
                m = jnp.maximum(m, s[:, j:j + 128])
            m_buf[...] = m if i == 0 else jnp.maximum(m_buf[...], m)

        parts = max(1, min(5, n_blk))
        part = [j * (rows // 16) // parts * 16 for j in range(parts + 1)] + [rows] * n_blk

        def softmax(g, i):
            for r in range(part[i], part[i + 1], 16):
                rs = slice(r, r + 16)
                m = jnp.max(m_buf[rs, :], axis=1, keepdims=True)
                l = None
                for j in range(0, seq, 128):
                    e = jnp.exp2(s_buf[g, rs, j:j + 128] - m)
                    s_buf[g, rs, j:j + 128] = e
                    l = e if l is None else l + e
                l_buf[g, rs, :] = jnp.broadcast_to(1.0 / jnp.sum(l, axis=1, keepdims=True), (16, 128))

        def turn(g, slot, i):
            rs = slice(i * rb, (i + 1) * rb)
            q_t[g, :, rs] = q_v[slot, g].reshape(rows, d)[rs].T
            do_t[g, :, rs] = do_v[slot, g].reshape(rows, d)[rs].T

        def out_rows(b, g, slot, i):
            rs = slice(i * rb, (i + 1) * rb)
            p = (s_buf[g, rs, :] * jnp.concatenate([l_buf[g, rs, :]] * (seq // 128), axis=1)).astype(BF16)
            p_buf[rs, :] = p
            o = dot_nn(p, kv_all[b, :, d:])
            dvec = jnp.sum(o * do_v[slot, g].reshape(rows, d)[rs].astype(F32), axis=1, keepdims=True)
            d_buf[rs, :] = jnp.broadcast_to(dvec, (rb, 128))
            put_rows(o_v, slot, g, i, o.astype(BF16))

        def put_rows(ref, slot, g, i, v):
            r = i * rb
            while r < (i + 1) * rb:
                n = min((i + 1) * rb - r, tok - r % tok)
                ref[slot, g, r // tok, r % tok:r % tok + n, :] = v[r - i * rb:r - i * rb + n]
                r += n

        def dq_rows(b, g, slot, i):
            rs = slice(i * rb, (i + 1) * rb)
            dq = dot_nn(ds_buf[rs, :], kv_all[b, :, :d]) * scale
            lo, hi = dq[:, :half], dq[:, half:]
            cs, sn = cos4[rs, :], sin4[rs, :]
            put_rows(dq_v, slot, g, i, jnp.concatenate([(lo * cs + hi * sn).astype(BF16), (hi * cs - lo * sn).astype(BF16)], axis=1))

        def grads(b, g, slot, i):
            cols = slice(i * 256, (i + 1) * 256)
            do = do_v[slot, g].reshape(rows, d)
            p = p_buf[:, cols]
            dp = dot_nt(do, kv_all[b, cols, d:])
            dvec = d_buf[...]
            if i > 0 and part[i] > part[i - 1]:
                z = None
                for r in range(part[i - 1], part[i], 8):
                    v = l_buf[1 - g, r:r + 8, :]
                    z = v if z is None else jnp.minimum(z, v)
                dvec = dvec + jnp.concatenate([jnp.minimum(z, 0.0)] * (rows // 8), axis=0)
            dd = jnp.concatenate([dvec, dvec], axis=1)
            ds = (p.astype(F32) * (dp - dd)).astype(BF16)
            ds_buf[:, cols] = ds
            dk = dot_nn(q_t[g], ds)
            dv = dot_nn(do_t[g], p)
            if g == 0:
                dk_t[:, cols] = dk
                dv_t[:, cols] = dv
            else:
                dk_t[:, cols] += dk
                dv_t[:, cols] += dv

        def close_kv(b, i):
            cols = slice(i * 256, (i + 1) * 256)
            kv_all[b, cols, :d] = (dk_t[:, cols] * scale).T.astype(BF16)
            kv_all[b, cols, d:] = dv_t[:, cols].T.astype(BF16)

        enter((mate, cw, ccw))
        gather(1).pass_on(lambda j: kv0_hbm.at[1, blk(j)])
        if nb > 2:
            own(2)
        for x in load(0, 0):
            x.start()

        def first(j):
            return pltpu.make_async_copy(kv0_hbm.at[0, blk(j)], kvb(0, j), first_sem.at[j])

        def second(j, n):
            return pltpu.make_async_copy(kv0_hbm.at[1, blk(j)], kvb(1, j), first_sem.at[8 + n])
        arrived = ((c >= 0, mate, 0), (c >= 1, me - 2, 1), (c == 3, me - 6, 2))
        for j in range(8):
            @pl.when(j <= 2 * c + 1)
            def _():
                first(j).start()
        for b in range(1, nb):
            own_copy(b).start()
        for cond, j, i in arrived:
            @pl.when(cond)
            def _():
                second(j, i).start()

        @pl.loop(2 * c + 2, 8)
        def _(j):
            for b in range(nb):
                kv_all[b, blk(j), :] = jnp.zeros((tok, 2 * d), BF16)
        for j in range(rows // tok):
            cos4[j * tok:(j + 1) * tok, :] = cos_ref[...]
            sin4[j * tok:(j + 1) * tok, :] = sin_ref[...]
        ds_buf[...] = jnp.zeros_like(ds_buf)
        for x in load(0, 0):
            x.wait()
        for i in range(n_rb):
            turn(0, 0, i)
        for j in range(8):
            @pl.when(j <= 2 * c + 1)
            def _():
                first(j).wait()
        for cond, j, i in arrived:
            @pl.when(cond)
            def _():
                second(j, i).wait()
        for i in range(n_blk):
            scores(0, 0, 0, i)
        for i in range(n_blk):
            softmax(0, i)

        def comm_steps(b, steps):
            for lag, stage in steps:
                @pl.when(b >= lag)
                def _():
                    stage(b - lag)

        @pl.loop(0, nb)
        def _(b):
            slot = lax.rem(b, 2)
            nxt = jnp.minimum(b + 1, nb - 1)
            prev = jnp.maximum(b - 1, 0)

            @pl.when(b + 1 < nb)
            def _():
                for x in load(b + 1, 1 - slot):
                    x.start()

            @pl.when(b + 3 < nb)
            def _():
                own(b + 3)

            @pl.when((b >= 1) & (b + 2 < nb))
            def _():
                gather(b + 2).forward()

            @pl.when(b == 1)
            def _():
                for x in load_dy:
                    x.start()
            comm_steps(b, ((3, stage2), (4, stage3)))

            @pl.when(b >= 2)
            def _():
                drain(b - 1)

            @pl.when(b >= 2)
            def _():
                stored(store_o(b - 2, slot))
            spare = jnp.where(b >= 1, b - 1, nb)
            for i in range(n_blk):
                scores(b, 1, slot, i)
                if i % 2 == 1:
                    out_rows(b, 0, slot, i // 2)
                    dq_rows(prev, 1, 1 - slot, i // 2)
                    turn(1, slot, i // 2)
            for i in range(n_blk):
                close_kv(spare, i)

            @pl.when(b + 1 < nb)
            def _():
                gather(b + 1).last()

            @pl.when(b >= 1)
            def _():
                for x in store_dq(b - 1, 1 - slot):
                    x.start()
                to_mate(b - 1)

            for i in range(n_blk):
                grads(b, 0, slot, i)
                softmax(1, i)

            @pl.when(b + 1 < nb)
            def _():
                for x in load(b + 1, 1 - slot):
                    x.wait()
                ready(b + 1)
            if nb > 2:
                @pl.when(b == 0)
                def _():
                    gather(2).forward()

            @pl.when(b >= 2)
            def _():
                stored(store_dq(b - 2, slot))
            nslot = lax.rem(nxt, 2)
            for i in range(n_blk):
                scores(nxt, 0, nslot, i)
                if i % 2 == 1:
                    out_rows(b, 1, slot, i // 2)
                    dq_rows(b, 0, slot, i // 2)
                    turn(0, nslot, i // 2)
            for x in store_o(b, slot):
                x.start()
            comm_steps(b, ((1, stage1),))
            for i in range(n_blk):
                grads(b, 1, slot, i)
                softmax(0, i)

        drain(nb - 1)
        for i in range(n_rb):
            dq_rows(nb - 1, 1, (nb - 1) % 2, i)
        for i in range(n_blk):
            close_kv(nb - 1, i)
        for x in store_dq(nb - 1, (nb - 1) % 2):
            x.start()
        to_mate(nb - 1)

    slab = pltpu.VMEM((2, 2, rows // tok, tok, d), BF16)
    pl.run_scoped(attend, slab, slab, pltpu.VMEM((2, rows, seq), F32), pltpu.VMEM((rows, 128), F32), pltpu.VMEM((2, rows, 128), F32),
                  pltpu.VMEM((rows, seq), BF16), pltpu.VMEM((rows, seq), BF16), pltpu.VMEM((2, d, rows), BF16),
                  pltpu.VMEM((2, d, rows), BF16), pltpu.VMEM((d, seq), F32), pltpu.VMEM((d, seq), F32),
                  pltpu.VMEM((rows, 128), F32), pltpu.VMEM((rows, half), F32), pltpu.VMEM((rows, half), F32))
    n = nb

    def first_products(a_v, at, acc_v):
        pr = Products(big, a_v, at, ld_sem, b_sem)
        for b in (n - 2, n - 1):
            stored(store_o(b, b % 2))
        for b in range(n):
            handed(op_hbm, o_v, 0, b, b % 2).wait_recv()

        def fetch(r):
            return pr.load_a(r, o_hbm.at[:, k, rel[r]], op_hbm.at[:, rel[r]])

        def save(r):
            return pltpu.make_async_copy(acc_v.at[r], acc_hbm.at[r], acc_sem.at[r])
        for r in range(2):
            for x in fetch(r):
                x.start()

        todo = [((stage2, n - 3), (stage3, n - 4)), ((stage1, n - 1), (stage2, n - 2), (stage3, n - 3)),
                ((stage2, n - 1), (stage3, n - 2)), ((stage3, n - 1),)]

        def steps(i):
            for stage, b in todo[i]:
                if b >= 0:
                    stage(b)
        steps(0)
        steps(1)
        for r in range(2):
            for x in fetch(r):
                x.wait()
            pr.turn(0, a_v.at[r, 0])
            pr.turn(1, a_v.at[r, 1])
            if r == 0:
                for x in load_dy:
                    x.wait()
            pr.columns(acc_v.at[r], 0, 4)
            save(r).start()
        steps(2)
        steps(3)
        for r in range(2):
            save(r).wait()

    pl.run_scoped(first_products, pltpu.VMEM((2, 2, nb, tok, d), BF16),
                  pltpu.VMEM((2, d, nb * tok), BF16), pltpu.VMEM((2, 2, d, dy_hbm.shape[1] // 2), F32))
    for b in (n - 2, n - 1):
        stored(store_dq(b, b % 2))
    for b in range(n):
        handed(dqp_hbm, dq_v, 1, b, b % 2).wait_recv()
        fin_copy(b).wait()
        for cond, slot in ((c == 3, 0), (c >= 1, 1), (c >= 2, 2)):
            @pl.when(cond)
            def _():
                r_copy(b, 0, slot, cw).wait_send()


def attention(q, do, kv, kv0, dy, dy_p, cos_t, sin_t):
    nb, _, hp, tok, d = q.shape
    seq = tok * 8
    rows = hp * tok
    any_spec = pl.BlockSpec(memory_space=pl.ANY)
    vmem = pl.BlockSpec(memory_space=pltpu.VMEM)
    dma = pltpu.SemaphoreType.DMA
    slab = pltpu.VMEM((2, 2, hp, tok, d), BF16)
    out = jax.ShapeDtypeStruct(q.shape, BF16)
    outp = jax.ShapeDtypeStruct((nb, hp, tok, d), BF16)
    return pl.pallas_call(
        functools.partial(attn_body, nb, tok, seq, d),
        in_specs=[any_spec] * 6 + [vmem, vmem],
        out_specs=[any_spec] * 6,
        out_shape=[out, out, jax.ShapeDtypeStruct(kv.shape, BF16), outp, outp,
                   jax.ShapeDtypeStruct((2, 2, d, dy.shape[1] // 2), F32)],
        scratch_shapes=[pltpu.VMEM((nb + 1, seq, 2 * d), BF16), slab, slab,
                        pltpu.VMEM((2, 4, tok, 2 * d), BF16), pltpu.VMEM((nb, 3, tok, 2 * d), BF16),
                        pltpu.VMEM((2,) + dy.shape, BF16),
                        dma((nb - 1, 7)), dma((nb - 1, 7)), dma((nb, 4)), dma((nb, 4)), dma((nb, 3)), dma((nb, 3)),
                        dma((nb,)), dma((2, 2)), dma((2, 2)), dma((nb,)), dma((2, nb)), dma((2, nb)), dma((11,)),
                        dma((2, 2)), dma((2,)), dma((4,))],
        compiler_params=pltpu.CompilerParams(collective_id=1, has_side_effects=True, vmem_limit_bytes=63 * 2**20),
        cost_estimate=pl.CostEstimate(flops=24 * nb * rows * seq * d, bytes_accessed=40 * 2**20,
                                      transcendentals=2 * nb * rows * seq),
        name="attention",
    )(q, do, kv, kv0, dy, dy_p, cos_t, sin_t)


def proj_body(nb, tok, x_hbm, g_ref, wq_hbm, wk_ref, wv_ref, wo_hbm, dy_hbm, cos_ref, sin_ref,
              kv0_hbm, hn_hbm, q_hbm, do_hbm, kv_hbm, wqf_hbm, wof_hbm, hnp_hbm, dyp_hbm,
              x_v, hn_v, dy_v, wq_v, wo_v, kv_v, out_v,
              send, recv, x_sem, dy_sem, own_sem, out_sem, misc_sem, w_sem, p_send, p_recv, kv_send, kv_recv):
    n_tok, e = x_hbm.shape
    d = kv_v.shape[1] // 2
    half = d // 2
    mc = 2 * tok
    me, k, mate, cw, ccw = ring_ids()
    base = 2 * (me // 2)

    def head(off, par):
        return lax.rem(base + 2 * off + 8, 8) + par
    enter((mate, cw, ccw))

    fulls = (wq_v, wo_v)
    locs = (wq_hbm, wo_hbm)

    def half_of(w, ref, j):
        n = ref.shape[0] // 2
        return ref.at[pl.ds(j * n, n)]

    sends = []

    def send_full(w, h, j, to, own=False):
        src = locs[w] if own else fulls[w].at[h]
        c = rdma(src, fulls[w].at[h], send.at[w, j], recv.at[w, j], to)
        c.start()
        sends.append(c)

    def send_half(w, h, part, j, to):
        c = rdma(half_of(w, fulls[w].at[h], part), half_of(w, fulls[w].at[h], part), send.at[w, j], recv.at[w, j], to)
        c.start()
        sends.append(c)

    def wait_full(w, h, j):
        rdma(fulls[w].at[h], fulls[w].at[h], send.at[w, j], recv.at[w, j], mate).wait_recv()

    def wait_half(w, h, part, j):
        ref = half_of(w, fulls[w].at[h], part)
        rdma(ref, ref, send.at[w, j], recv.at[w, j], mate).wait_recv()

    for w in range(2):
        send_full(w, me, 0, cw, True)
        send_full(w, me, 1, ccw, True)
        send_full(w, me, 4, mate, True)
    own = [pltpu.make_async_copy(locs[w], fulls[w].at[me], own_sem.at[w]) for w in range(2)]
    xs = [pltpu.make_async_copy(x_hbm.at[pl.ds(b * tok, tok)], x_v.at[pl.ds(b * tok, tok)], x_sem.at[b]) for b in range(nb)]
    for c in xs:
        c.start()
    for c in own:
        c.start()
    dyc = pltpu.make_async_copy(dy_hbm, dy_v, dy_sem)
    dyc.start()

    gain = g_ref[...].astype(F32)
    for b in range(nb):
        xs[b].wait()

        @pl.loop(0, tok // 16, unroll=2)
        def _(r):
            rs = pl.ds(pl.multiple_of(b * tok + r * 16, 16), 16)
            x = x_v[rs, :].astype(F32)
            c = x - jnp.mean(x, axis=1, keepdims=True)
            inv = lax.rsqrt(jnp.mean(c * c, axis=1, keepdims=True) + LN_EPS)
            hn_v[rs, :] = (c * inv * gain).astype(BF16)
    hn_out = pltpu.make_async_copy(hn_v, hn_hbm, misc_sem.at[0])
    hn_out.start()
    to_mate = [rdma(hn_v, hnp_hbm, p_send.at[0], p_recv.at[0], mate), rdma(dy_hbm, dyp_hbm, p_send.at[1], p_recv.at[1], mate)]
    for c in to_mate:
        c.start()

    def rope_rows(raw):
        lo, hi = raw[:, :half], raw[:, half:d]
        cs, sn = jnp.concatenate([cos_ref[...]] * 2, axis=0), jnp.concatenate([sin_ref[...]] * 2, axis=0)
        return lo * cs - hi * sn, hi * cs + lo * sn

    @pl.loop(0, n_tok // mc)
    def _(i):
        rs = pl.ds(pl.multiple_of(i * mc, mc), mc)
        lo, hi = rope_rows(dot_nn(hn_v[rs, :], wk_ref[...]))
        kv_v[rs, :half] = lo.astype(BF16)
        kv_v[rs, half:d] = hi.astype(BF16)
        kv_v[rs, d:] = dot_nn(hn_v[rs, :], wv_ref[...]).astype(BF16)
    kv_out = pltpu.make_async_copy(kv_v, kv_hbm, misc_sem.at[1])
    kv_out.start()

    outs = []
    saves = []

    def save(w, h):
        c = pltpu.make_async_copy(fulls[w].at[h], (wqf_hbm, wof_hbm)[w].at[h], w_sem.at[len(saves)])
        c.start()
        saves.append(c)

    def project(w, h):
        slot = len(outs) % 4
        if len(outs) >= 4:
            outs[-4].wait()

        @pl.loop(0, n_tok // mc)
        def _(i):
            rs = pl.ds(pl.multiple_of(i * mc, mc), mc)
            if w == 0:
                lo, hi = rope_rows(dot_nn(hn_v[rs, :], wq_v[h]))
                o0 = lo.reshape(2, tok, half).astype(BF16)
                o1 = hi.reshape(2, tok, half).astype(BF16)
                out_v[slot, pl.ds(2 * i, 2), :, :half] = o0
                out_v[slot, pl.ds(2 * i, 2), :, half:] = o1
            else:
                out_v[slot, pl.ds(2 * i, 2)] = dot_nt(dy_v[rs, :], wo_v[h]).reshape(2, tok, d).astype(BF16)
        c = pltpu.make_async_copy(out_v.at[slot], (q_hbm, do_hbm)[w].at[:, lax.rem(h, 2), h // 2], out_sem.at[slot])
        c.start()
        outs.append(c)
        save(w, h)

    other = 1 - k
    for w in range(2):
        own[w].wait()
        if w == 1:
            dyc.wait()
        project(w, me)
        wait_full(w, mate, 4)
        project(w, mate)
    for w in range(2):
        wait_full(w, head(-1, k), 0)
        send_half(w, head(-1, k), 0, 2, cw)
        wait_full(w, head(1, k), 1)
        send_half(w, head(1, k), 1, 3, ccw)
        send_full(w, head(-1, k), 5, mate)
        send_full(w, head(1, k), 6, mate)
        project(w, head(-1, k))
        project(w, head(1, k))
        wait_full(w, head(-1, other), 5)
        project(w, head(-1, other))
        wait_full(w, head(1, other), 6)
        project(w, head(1, other))

    def early(n):
        def blk(j):
            return kv0_hbm.at[n, pl.ds(pl.multiple_of(j * tok, 16), tok)]
        return Gather((me, k, mate, cw, ccw), me // 2, blk, lambda t: kv_send.at[n, t], lambda t: kv_recv.at[n, t])
    first, second = early(0), early(1)
    first.own(kv_v.at[pl.ds(0, tok)])
    own0 = pltpu.make_async_copy(kv_v.at[pl.ds(0, tok)], first.block(me), misc_sem.at[2])
    own0.start()
    for w in range(2):
        wait_half(w, head(2, k), 0, 2)
        send_half(w, head(2, k), 0, 7, mate)
        wait_half(w, head(2, k), 1, 3)
        send_half(w, head(2, k), 1, 8, mate)
        project(w, head(2, k))
        if w == 1:
            first.forward()
            second.own(kv_v.at[pl.ds(tok, tok)])
        wait_half(w, head(2, other), 0, 7)
        wait_half(w, head(2, other), 1, 8)
        project(w, head(2, other))
    first.last()
    for c in outs[-4:] + saves + [hn_out, kv_out, own0]:
        c.wait()
    first.ready()
    first.drain()
    second.arrived()
    second.ready((3,))
    second.drain((0, 2, 3))
    for c in sends:
        c.wait_send()
    for c in to_mate:
        c.wait()


def project(x, gain, wq, w_k, w_v, wo, dy, cos_t, sin_t):
    nb, tok, e = x.shape
    d = wq.shape[1]
    n_heads = 8
    n_tok = nb * tok
    any_spec = pl.BlockSpec(memory_space=pl.ANY)
    vmem = pl.BlockSpec(memory_space=pltpu.VMEM)
    act = jax.ShapeDtypeStruct((nb, 2, n_heads // 2, tok, d), BF16)
    dma = pltpu.SemaphoreType.DMA
    flops = 2 * n_tok * e * (2 * n_heads + 2) * d
    kv0, hn, q, do, kv, wqf, wof, hn_p, dy_p = pl.pallas_call(
        functools.partial(proj_body, nb, tok),
        in_specs=[any_spec, vmem, any_spec, vmem, vmem, any_spec, any_spec, vmem, vmem],
        out_specs=[any_spec] * 9,
        out_shape=[jax.ShapeDtypeStruct((2, tok * n_heads, 2 * d), BF16), jax.ShapeDtypeStruct((n_tok, e), BF16), act, act, jax.ShapeDtypeStruct((n_tok, 2 * d), BF16),
                   jax.ShapeDtypeStruct((n_heads, e, d), BF16), jax.ShapeDtypeStruct((n_heads, d, e), BF16),
                   jax.ShapeDtypeStruct((n_tok, e), BF16), jax.ShapeDtypeStruct((n_tok, e), BF16)],
        scratch_shapes=[pltpu.VMEM((n_tok, e), BF16), pltpu.VMEM((n_tok, e), BF16), pltpu.VMEM((n_tok, e), BF16),
                        pltpu.VMEM((n_heads, e, d), BF16), pltpu.VMEM((n_heads, d, e), BF16),
                        pltpu.VMEM((n_tok, 2 * d), BF16), pltpu.VMEM((4, nb, tok, d), BF16),
                        dma((2, 9)), dma((2, 9)), dma((nb,)), dma(()), dma((2,)), dma((4,)), dma((3,)), dma((16,)), dma((2,)), dma((2,)), dma((2, 7)), dma((2, 7))],
        compiler_params=pltpu.CompilerParams(collective_id=0, has_side_effects=True, vmem_limit_bytes=60 * 2**20),
        cost_estimate=pl.CostEstimate(flops=flops, bytes_accessed=60 * 2**20, transcendentals=0),
        name="project",
    )(x.reshape(n_tok, e), gain, wq, w_k, w_v, wo, dy.reshape(n_tok, e), cos_t, sin_t)
    return kv0, hn, q, do, kv.reshape(nb, tok, 2 * d), wqf, wof, hn_p, dy_p


def grads_body(nb, tok, o_hbm, op_hbm, acc_hbm, dq_hbm, dqp_hbm, hn_hbm, hnp_hbm, dy_hbm, dyp_hbm, dkv_hbm,
               wq_hbm, wo_hbm, wk_hbm, wv_hbm, x_hbm, g_ref, cos_ref, sin_ref,
               y_hbm, gx_hbm, gln_ref, gwo_ref, gwq_ref, gkv_hbm,
               acc, acc_kv, rbuf, rbuf_kv, kind, kp, dkv_v, fin_kv, gln_acc, gl_recv,
               rs_send, rs_recv, kv_send, kv_recv, ag_send, ag_recv, gl_send, gl_rsem, kp_sem, ld_sem, b_sem, t_sem, a_sem):
    n_tok, e = x_hbm.shape
    d = wk_hbm.shape[1]
    half = d // 2
    eh, eq = e // 2, e // 4
    me, k, mate, cw, ccw = ring_ids()
    c = me // 2
    rel = [lax.rem(c + o, 4) for o in (3, 1, 2, 0)]
    enter([lax.rem(me + o, 8) for o in range(1, 8)])

    order = ((2, 1), (2, 0))

    def hop(s, dr, j):
        first = acc_hbm.at[dr, dr] if s == 0 else acc.at[s, dr, dr]
        src = first if j == 0 else rbuf.at[s, dr, j - 1]
        return rdma(src, rbuf.at[s, dr, j], rs_send.at[s, dr, j], rs_recv.at[s, dr, j], (cw, ccw)[dr])

    def hop_kv(dr, j):
        src = acc_kv.at[dr, dr] if j == 0 else rbuf_kv.at[dr, j - 1]
        return rdma(src, rbuf_kv.at[dr, j], kv_send.at[dr, j], kv_recv.at[dr, j], (cw, ccw)[dr])

    def add(dst, term):
        @pl.loop(0, dst.shape[0] // 32)
        def _(i):
            rs = pl.ds(pl.multiple_of(i * 32, 32), 32)
            dst[rs, :] = dst[rs, :] + term[rs, :]

    def pass_on(s, j):
        for dr in range(2):
            hop(s, dr, j - 1).wait_recv()
            add(rbuf.at[s, dr, j - 1], acc.at[s, order[dr][j - 1], dr])
            hop(s, dr, j).start()

    def pass_on_kv(j):
        for dr in range(2):
            hop_kv(dr, j - 1).wait_recv()
            add(rbuf_kv.at[dr, j - 1], acc_kv.at[order[dr][j - 1], dr])
            hop_kv(dr, j).start()

    def finish(s, out):
        for dr in range(2):
            hop(s, dr, 2).wait_recv()

            @pl.loop(0, d // 32)
            def _(i):
                rs = pl.ds(pl.multiple_of(i * 32, 32), 32)
                out[rs, dr * eh:(dr + 1) * eh] = (rbuf[s, dr, 2, rs, :] + acc[s, 3, dr, rs, :]).astype(BF16)

    def piece(kk, j, lo=0, n=None):
        return gkv_hbm.at[kk, pl.ds(lo, d if n is None else n), pl.ds(pl.multiple_of(j * eq, 128), eq)]

    def ag(tag, ref, to, src=None):
        return rdma(ref if src is None else src, ref, ag_send.at[tag], ag_recv.at[tag], to)

    def ag_far(tag, to):
        return ag(tag, piece(k, rel[(0, 1)[tag - 3]], (tag - 3) * half, half), to)

    own_piece = pltpu.make_async_copy(fin_kv, piece(k, c), t_sem.at[5])

    def finish_kv():
        for dr in range(2):
            hop_kv(dr, 2).wait_recv()
            fin_kv[:, dr * (eq // 2):(dr + 1) * (eq // 2)] = rbuf_kv[dr, 2] + acc_kv[3, dr]
        ag(0, piece(k, c), cw, fin_kv).start()
        ag(1, piece(k, c), ccw, fin_kv).start()
        ag(2, piece(k, c), mate, fin_kv).start()
        own_piece.start()

    def ag_forward():
        ag(0, piece(k, rel[0]), cw).wait_recv()
        ag_far(3, cw).start()
        ag(1, piece(k, rel[1]), cw).wait_recv()
        ag_far(4, ccw).start()
        ag(5, piece(k, rel[0]), mate).start()
        ag(6, piece(k, rel[1]), mate).start()

    def ag_last():
        far = [piece(k, rel[2], i * half, half) for i in range(2)]
        for i in range(2):
            ag(3 + i, far[i], cw).wait_recv()
            ag(7 + i, far[i], mate).start()
        ag(2, piece(1 - k, c), mate).wait_recv()
        ag(5, piece(1 - k, rel[0]), mate).wait_recv()
        ag(6, piece(1 - k, rel[1]), mate).wait_recv()
        for i in range(2):
            ag(7 + i, piece(1 - k, rel[2], i * half, half), mate).wait_recv()
        for tag in range(3):
            ag(tag, piece(k, c), cw, fin_kv).wait_send()
        for tag in (3, 4, 7, 8):
            ag(tag, far[0], cw).wait_send()
        for tag in (5, 6):
            ag(tag, piece(k, c), cw).wait_send()
        own_piece.wait()

    dkv_in = pltpu.make_async_copy(dkv_hbm, dkv_v, t_sem.at[4])
    dkv_in.start()
    kp_copy = rdma(kind.at[1 - k], kp, kp_sem.at[0], kp_sem.at[1], mate)

    for dr in range(2):
        hop(0, dr, 0).start()
    acc_in = [pltpu.make_async_copy(acc_hbm.at[r], acc.at[0, r], a_sem.at[r]) for r in range(2)]
    for x in acc_in:
        x.start()

    def products(big, a_v, at):
        pr = Products(big, a_v, at, ld_sem, b_sem)
        dy_in = pr.load_b(dy_hbm, dyp_hbm)
        hn_in = pr.load_b(hn_hbm, hnp_hbm)
        jobs = [(0, 2), (0, 3)] + [(1, r) for r in range(4)]

        def fetch(i):
            s, r = jobs[i]
            return pr.load_a(i, (o_hbm, dq_hbm)[s].at[:, k, rel[r]], (op_hbm, dqp_hbm)[s].at[:, rel[r]])
        for x in dy_in:
            x.start()
        for i in range(2):
            for x in fetch(i):
                x.start()
        dkv_in.wait()
        for b in range(nb):
            lo, hi = dkv_v[b, :, :half].astype(F32), dkv_v[b, :, half:d].astype(F32)
            cs, sn = cos_ref[...], sin_ref[...]
            kind[0, b, :, :half] = (lo * cs + hi * sn).astype(BF16)
            kind[0, b, :, half:] = (hi * cs - lo * sn).astype(BF16)
            kind[1, b] = dkv_v[b, :, d:]
        kp_copy.start()
        for i, (s, r) in enumerate(jobs):
            if i == 2:
                pr.turn(0, kind.at[k])
                kp_copy.wait_recv()
                pr.turn(1, kp)
                for x in hn_in:
                    x.wait()
                for q in range(4):
                    for dr in range(2):
                        acc_kv[q, dr] = pr.both(pl.ds(pl.multiple_of(rel[q] * eq + dr * (eq // 2), 128), eq // 2))
                for dr in range(2):
                    hop_kv(dr, 0).start()
            for x in fetch(i):
                x.wait()
            pr.turn(0, a_v.at[i % 2, 0])
            pr.turn(1, a_v.at[i % 2, 1])
            if i + 2 < len(jobs):
                for x in fetch(i + 2):
                    x.start()
            if i == 0:
                for x in dy_in:
                    x.wait()
            if s == 1 and r < 2:
                pr.columns(acc.at[s, r], 0, 2, 2 * r)
                hop(s, r, 0).start()
                pr.columns(acc.at[s, r], 2, 4, 2 * r)
            else:
                pr.columns(acc.at[s, r], 0, 4)
            if i == 1:
                for x in hn_in:
                    x.start()

    pl.run_scoped(products, pltpu.VMEM((2, n_tok, e), BF16), pltpu.VMEM((2, 2, nb, tok, d), BF16), pltpu.VMEM((2, d, n_tok), BF16))
    for x in acc_in:
        x.wait()
    pass_on(0, 1)
    pass_on_kv(1)

    mc = 2 * tok
    units = nb // 2

    def attn_out(wo_v, o_v, x_v, y_v):
        w_in = pltpu.make_async_copy(wo_hbm, wo_v, b_sem.at[0])
        w_in.start()

        def load(u):
            return (pltpu.make_async_copy(o_hbm.at[pl.ds(2 * u, 2)], o_v.at[u % 2], ld_sem.at[u % 2, 0]),
                    pltpu.make_async_copy(x_hbm.at[pl.ds(u * mc, mc)], x_v.at[u % 2], ld_sem.at[u % 2, 1]))

        def put(u):
            return pltpu.make_async_copy(y_v.at[u % 2], y_hbm.at[pl.ds(u * mc, mc)], t_sem.at[u % 2])
        for x in load(0):
            x.start()
        w_in.wait()
        for u in range(units):
            if u + 1 < units:
                for x in load(u + 1):
                    x.start()
            for x in load(u):
                x.wait()
            if u >= 2:
                put(u - 2).wait()
            sl = u % 2

            @pl.loop(0, 4)
            def _(n):
                cols = pl.ds(pl.multiple_of(n * eq, 128), eq)
                o_rows = jnp.concatenate([jnp.concatenate([o_v[sl, i, h % 2, h // 2] for h in range(8)], axis=1) for i in range(2)], axis=0)
                r = dot_nn(o_rows, wo_v[:, cols])
                y_v[sl, :, cols] = (x_v[sl, :, cols].astype(F32) + r).astype(BF16)
            put(u).start()
        for u in range(max(0, units - 2), units):
            put(u).wait()

    pl.run_scoped(attn_out, pltpu.VMEM((8 * d, e), BF16), pltpu.VMEM((2, 2, 2, 4, tok, d), BF16),
                  pltpu.VMEM((2, mc, e), BF16), pltpu.VMEM((2, mc, e), BF16))
    pass_on(1, 1)

    def hidden_grad(wq_v, wk_v, wv_v, dq_v, x_v, dy_v, dh, gx_v):
        w_in = pltpu.make_async_copy(wq_hbm, wq_v, b_sem.at[0])
        w_in.start()
        w2_in = (pltpu.make_async_copy(wk_hbm, wk_v, b_sem.at[1]), pltpu.make_async_copy(wv_hbm, wv_v, ld_sem.at[1, 1]))
        for x in w2_in:
            x.start()

        def load(u):
            return (pltpu.make_async_copy(dq_hbm.at[pl.ds(2 * u, 2)], dq_v, ld_sem.at[0, 0]),
                    pltpu.make_async_copy(x_hbm.at[pl.ds(u * mc, mc)], x_v, ld_sem.at[0, 1]),
                    pltpu.make_async_copy(dy_hbm.at[pl.ds(u * mc, mc)], dy_v, ld_sem.at[1, 0]))

        def put(u):
            return pltpu.make_async_copy(gx_v, gx_hbm.at[pl.ds(u * mc, mc)], t_sem.at[0])
        gain = g_ref[...].astype(F32)
        gln_acc[...] = jnp.zeros_like(gln_acc)
        for x in load(0):
            x.start()
        w_in.wait()
        for x in w2_in:
            x.wait()
        for u in range(units):
            for x in load(u):
                x.wait()

            @pl.loop(0, 4)
            def _(n):
                rows = pl.ds(pl.multiple_of(n * eq, 128), eq)
                t = None
                for h in range(8):
                    a = jnp.concatenate([dq_v[i, h % 2, h // 2] for i in range(2)], axis=0)
                    p = dot_nt(a, wq_v[h, rows, :])
                    t = p if t is None else t + p
                for j in range(2):
                    a = jnp.concatenate([kind[j, 2 * u + i] for i in range(2)], axis=0)
                    t = t + dot_nt(a, (wk_v, wv_v)[j][rows, :])
                dh[:, rows] = t
            if u >= 1:
                put(u - 1).wait()

            @pl.loop(0, mc // 16)
            def _(r):
                rs = pl.ds(pl.multiple_of(r * 16, 16), 16)
                x = x_v[rs, :].astype(F32)
                cx = x - jnp.mean(x, axis=1, keepdims=True)
                inv = lax.rsqrt(jnp.mean(cx * cx, axis=1, keepdims=True) + LN_EPS)
                xh = cx * inv
                g = dh[rs, :]
                pr = g * xh
                gln_acc[...] += pr[:8] + pr[8:]
                gh = g * gain
                m1 = jnp.mean(gh, axis=1, keepdims=True)
                m2 = jnp.mean(gh * xh, axis=1, keepdims=True)
                gx_v[rs, :] = (inv * (gh - m1 - xh * m2) + dy_v[rs, :].astype(F32)).astype(BF16)
            put(u).start()
            if u + 1 < units:
                for x in load(u + 1):
                    x.start()
            if u == units // 2 - 1:
                pass_on(0, 2)
                pass_on_kv(2)
        put(units - 1).wait()

    pl.run_scoped(hidden_grad, pltpu.VMEM((8, e, d), BF16), pltpu.VMEM((e, d), BF16), pltpu.VMEM((e, d), BF16), pltpu.VMEM((2, 2, 4, tok, d), BF16),
                  pltpu.VMEM((mc, e), BF16), pltpu.VMEM((mc, e), BF16), pltpu.VMEM((mc, e), F32), pltpu.VMEM((mc, e), BF16))
    gl_recv[me] = jnp.sum(gln_acc[...], axis=0, keepdims=True)
    pass_on(1, 2)
    finish(0, gwo_ref)
    finish_kv()
    gl = [rdma(gl_recv.at[me], gl_recv.at[me], gl_send.at[o - 1], gl_rsem.at[o - 1], lax.rem(me + o, 8)) for o in range(1, 8)]
    for x in gl:
        x.start()
    finish(1, gwq_ref)
    ag_forward()
    for o in range(1, 8):
        src = lax.rem(me + 8 - o, 8)
        rdma(gl_recv.at[src], gl_recv.at[src], gl_send.at[o - 1], gl_rsem.at[o - 1], mate).wait_recv()
    total = gl_recv[0]
    for i in range(1, 8):
        total = total + gl_recv[i]
    gln_ref[...] = total
    ag_last()
    for x in gl:
        x.wait_send()
    kp_copy.wait_send()
    for dr in range(2):
        for j in range(3):
            hop_kv(dr, j).wait_send()
            for s in range(2):
                hop(s, dr, j).wait_send()


def gradients(o, o_p, acc, dq, dq_p, hn, hn_p, dy, dy_p, dkv, wqf, wof, w_k, w_v, x, gain, cos_t, sin_t):
    nb, tok, e = x.shape
    n_tok = nb * tok
    d = dq.shape[-1]
    any_spec = pl.BlockSpec(memory_space=pl.ANY)
    vmem = pl.BlockSpec(memory_space=pltpu.VMEM)
    dma = pltpu.SemaphoreType.DMA
    tokens = jax.ShapeDtypeStruct((n_tok, e), BF16)
    y, gx, gln, gwo, gwq_t, gkv_t = pl.pallas_call(
        functools.partial(grads_body, nb, tok),
        in_specs=[any_spec] * 15 + [vmem, vmem, vmem],
        out_specs=[any_spec, any_spec, vmem, vmem, vmem, any_spec],
        out_shape=[tokens, tokens, jax.ShapeDtypeStruct((1, e), F32), jax.ShapeDtypeStruct((d, e), BF16),
                   jax.ShapeDtypeStruct((d, e), BF16), jax.ShapeDtypeStruct((2, d, e), F32)],
        scratch_shapes=[pltpu.VMEM((2, 4, 2, d, e // 2), F32), pltpu.VMEM((4, 2, d, e // 8), F32),
                        pltpu.VMEM((2, 2, 3, d, e // 2), F32), pltpu.VMEM((2, 3, d, e // 8), F32),
                        pltpu.VMEM((2, nb, tok, d), BF16), pltpu.VMEM((nb, tok, d), BF16), pltpu.VMEM((nb, tok, 2 * d), BF16),
                        pltpu.VMEM((d, e // 4), F32), pltpu.VMEM((8, e), F32), pltpu.VMEM((8, 1, e), F32),
                        dma((2, 2, 3)), dma((2, 2, 3)), dma((2, 3)), dma((2, 3)), dma((9,)), dma((9,)), dma((7,)), dma((7,)),
                        dma((2,)), dma((2, 2)), dma((2,)), dma((6,)), dma((4,))],
        compiler_params=pltpu.CompilerParams(collective_id=2, has_side_effects=True, vmem_limit_bytes=63 * 2**20),
        cost_estimate=pl.CostEstimate(flops=10 * n_tok * e * e, bytes_accessed=120 * 2**20, transcendentals=0),
        name="gradients",
    )(o, o_p, acc, dq, dq_p, hn, hn_p, dy.reshape(n_tok, e), dy_p, dkv, wqf, wof.reshape(8 * d, e), w_k, w_v, x.reshape(n_tok, e),
      gain, cos_t, sin_t)
    y, gx, gwq, gwk, gwv, gwo, gln = place(nb, y, gx, gwq_t, gkv_t, gwo, gln)
    return y.reshape(nb, tok, e), gx.reshape(nb, tok, e), gln.reshape(e), gwq, gwk, gwv, gwo


def place_body(steps, y_in, gx_in, gq_in, gkv_in, go_in, gl_in, y, gx, gq, gk, gv, go, gl,
               y_v, gx_v, gq_v, gkv_v, go_v, gl_v, gq_t, gk_t, gv_t, in_sem, y_sem, out_sem, t_sem):
    n, w = y_in.shape[0] // steps, gq_in.shape[1] // steps
    small_in = [pltpu.make_async_copy(s, v, in_sem.at[i]) for i, (s, v) in enumerate(((gkv_in, gkv_v), (gq_in, gq_v), (go_in, go_v), (gl_in, gl_v)))]
    small_out = [pltpu.make_async_copy(v, o, out_sem.at[i]) for i, (v, o) in enumerate(((go_v, go), (gl_v, gl)))]

    def rows(i, size):
        return pl.ds(i * size, size)
    moves = [(pltpu.make_async_copy(s.at[rows(i, n)], v.at[rows(i, n)], y_sem.at[0, j, i]),
              pltpu.make_async_copy(v.at[rows(i, n)], o.at[rows(i, n)], y_sem.at[1, j, i]))
             for i in range(steps) for j, (s, v, o) in enumerate(((y_in, y_v, y), (gx_in, gx_v, gx)))]
    for x in small_in:
        x.start()
    for x, _ in moves:
        x.start()
    small_in[0].wait()
    small_in[1].wait()
    turned = []
    for i in range(steps):
        for j, (v, o) in enumerate(((gk_t, gk), (gv_t, gv), (gq_t, gq))):
            t = (gkv_v[j, :, i * w:(i + 1) * w] if j < 2 else gq_v[:, i * w:(i + 1) * w].astype(F32)).T
            v[i * w:(i + 1) * w, :] = t.astype(v.dtype)
            c = pltpu.make_async_copy(v.at[rows(i, w)], o.at[rows(i, w)], t_sem.at[j, i])
            c.start()
            turned.append(c)
        for x, z in moves[2 * i:2 * i + 2]:
            x.wait()
            z.start()
    for x, z in zip(small_in[2:], small_out):
        x.wait()
        z.start()
    for c in turned + small_out + [z for _, z in moves]:
        c.wait()


def place(steps, y, gx, gwq_t, gkv_t, gwo, gln):
    e = y.shape[1]
    d = gwo.shape[0]
    any_spec = pl.BlockSpec(memory_space=pl.ANY)
    dma = pltpu.SemaphoreType.DMA
    vm = pltpu.VMEM
    return pl.pallas_call(
        functools.partial(place_body, steps),
        in_specs=[any_spec] * 6,
        out_specs=[any_spec] * 7,
        out_shape=[jax.ShapeDtypeStruct(y.shape, BF16), jax.ShapeDtypeStruct(y.shape, BF16), jax.ShapeDtypeStruct((e, d), BF16),
                   jax.ShapeDtypeStruct((e, d), F32), jax.ShapeDtypeStruct((e, d), F32), jax.ShapeDtypeStruct((d, e), BF16),
                   jax.ShapeDtypeStruct((1, e), F32)],
        scratch_shapes=[vm(y.shape, BF16), vm(y.shape, BF16), vm((d, e), BF16), vm((2, d, e), F32), vm((d, e), BF16), vm((1, e), F32),
                        vm((e, d), BF16), vm((e, d), F32), vm((e, d), F32),
                        dma((4,)), dma((2, 2, steps)), dma((2,)), dma((3, steps))],
        compiler_params=pltpu.CompilerParams(vmem_limit_bytes=63 * 2**20),
        cost_estimate=pl.CostEstimate(flops=0, bytes_accessed=8 * y.size + 24 * gwo.size, transcendentals=0),
        name="place",
    )(y, gx, gwq_t, gkv_t, gwo, gln)


def solution(mesh):
    act_spec = P('dp', 'tp', None)

    def device_step(x_loc, ln_scale, wq_loc, w_k, w_v, wo_loc, dy_loc):
        n_batch, tok, model_dim = x_loc.shape
        d = w_k.shape[1]
        t0 = lax.axis_index('tp') * tok
        cos_t, sin_t = rope_tables(t0 + jnp.arange(tok), d)

        gain = ln_scale.reshape(1, model_dim)
        kv0, hn, q, do, kv_loc, wq_h, wo_h, hn_p, dy_p = project(x_loc, gain, wq_loc, w_k, w_v, wo_loc, dy_loc, cos_t, sin_t)
        o, dq, dkv_loc, o_p, dq_p, acc = attention(q, do, kv_loc, kv0, dy_loc.reshape(-1, model_dim), dy_p, cos_t, sin_t)
        return gradients(o, o_p, acc, dq, dq_p, hn, hn_p, dy_loc, dy_p, dkv_loc, wq_h, wo_h, w_k, w_v, x_loc, gain, cos_t, sin_t)

    return jax.shard_map(device_step, mesh=mesh, in_specs=(act_spec, P(None), P(None, 'tp'), P(None, None), P(None, None), P('tp', None), act_spec), out_specs=(act_spec, act_spec, P('dp'), P('dp', 'tp'), P('dp', None), P('dp', None), P(('dp', 'tp'), None)), check_vma=False)
```

```python
import functools
import jax
import jax.numpy as jnp
from jax import lax
from jax.experimental import pallas as pl
from jax.experimental.pallas import tpu as pltpu
from jax.sharding import PartitionSpec as P

LN_EPS = 1e-6
ROPE_BASE = 10000.0
LOG2E = 1.4426950408889634
F32 = jnp.float32
BF16 = jnp.bfloat16


def rope_tables(positions, head_dim):
    half_dim = head_dim // 2
    inv_freq = ROPE_BASE ** (-2.0 * jnp.arange(half_dim, dtype=F32) / head_dim)
    angles = positions.astype(F32)[:, None] * inv_freq[None, :]
    return jnp.cos(angles), jnp.sin(angles)


def rotate(vectors, cos_t, sin_t):
    half_dim = vectors.shape[-1] // 2
    lo_half = vectors[..., :half_dim]
    hi_half = vectors[..., half_dim:]
    return jnp.concatenate([lo_half * cos_t - hi_half * sin_t, hi_half * cos_t + lo_half * sin_t], axis=-1)


def dot_nn(a, b):
    return lax.dot_general(a, b, (((1,), (0,)), ((), ())), preferred_element_type=F32)


def dot_nt(a, b):
    return lax.dot_general(a, b, (((1,), (1,)), ((), ())), preferred_element_type=F32)


def rdma(src, dst, send, recv, to):
    return pltpu.make_async_remote_copy(src_ref=src, dst_ref=dst, send_sem=send, recv_sem=recv,
                                        device_id={'tp': to}, device_id_type=pl.DeviceIdType.MESH)


def ring_ids():
    me = lax.axis_index('tp')
    k = lax.rem(me, 2)
    return me, k, me + 1 - 2 * k, lax.rem(me + 2, 8), lax.rem(me + 6, 8)


def enter(peers):
    barrier = pltpu.get_barrier_semaphore()
    for p in peers:
        pl.semaphore_signal(barrier, inc=1, device_id={'tp': p}, device_id_type=pl.DeviceIdType.MESH)
    pl.semaphore_wait(barrier, len(peers))


class Products:
    def __init__(self, big, a_v, at, ld_sem, b_sem):
        self.big, self.a_v, self.at, self.ld_sem, self.b_sem = big, a_v, at, ld_sem, b_sem
        self.nb, self.tok = a_v.shape[2], a_v.shape[3]
        self.eq = big.shape[2] // 4

    def load_b(self, own, other):
        return (pltpu.make_async_copy(own, self.big.at[0], self.b_sem.at[0]),
                pltpu.make_async_copy(other, self.big.at[1], self.b_sem.at[1]))

    def load_a(self, i, own, other):
        return (pltpu.make_async_copy(own, self.a_v.at[i % 2, 0], self.ld_sem.at[i % 2, 0]),
                pltpu.make_async_copy(other, self.a_v.at[i % 2, 1], self.ld_sem.at[i % 2, 1]))

    def turn(self, j, src):
        tok = self.tok
        for i in range(self.nb // 2):
            self.at[j, :, 2 * i * tok:(2 * i + 2) * tok] = jnp.concatenate([src[2 * i], src[2 * i + 1]], axis=0).T

    def both(self, cols):
        return dot_nn(self.at[0], self.big[0, :, cols]) + dot_nn(self.at[1], self.big[1, :, cols])

    def columns(self, dst, first, last, turned=0):
        eq = self.eq

        @pl.loop(first, last)
        def _(n):
            m = lax.rem(n + turned, 4)
            cols = pl.ds(pl.multiple_of(m * eq, 128), eq)
            dst[m // 2, :, pl.ds(pl.multiple_of(lax.rem(m, 2) * eq, 128), eq)] = self.both(cols)


class Gather:
    def __init__(self, ids, c, block, send, recv):
        self.me, _, self.mate, self.cw, self.ccw = ids
        self.c, self.block, self.send, self.recv = c, block, send, recv

    def copy(self, j, tag, to, src=None):
        ref = self.block(j)
        return rdma(ref if src is None else src, ref, self.send(tag), self.recv(tag), to)

    def own(self, src):
        @pl.when(self.c <= 2)
        def _():
            self.copy(self.me, 0, self.cw, src).start()

        @pl.when(self.c == 0)
        def _():
            self.copy(self.me, 2, self.ccw, src).start()
        self.copy(self.me, 3, self.mate, src).start()

    def arrived(self):
        @pl.when(self.c >= 1)
        def _():
            self.copy(self.me - 2, 0, self.cw).wait_recv()

        @pl.when(self.c == 3)
        def _():
            self.copy(self.me - 6, 2, self.ccw).wait_recv()

    def pass_on(self, src=lambda j: None):
        @pl.when(self.c >= 1)
        def _():
            @pl.when(self.c <= 2)
            def _():
                self.copy(self.me - 2, 1, self.cw, src(self.me - 2)).start()
            self.copy(self.me - 2, 4, self.mate, src(self.me - 2)).start()

        @pl.when(self.c == 3)
        def _():
            self.copy(self.me - 6, 6, self.mate, src(self.me - 6)).start()

    def forward(self):
        self.arrived()
        self.pass_on()

    def last(self):
        @pl.when(self.c >= 2)
        def _():
            self.copy(self.me - 4, 1, self.cw).wait_recv()
            self.copy(self.me - 4, 5, self.mate).start()

    def ready(self, tags=(3, 4, 5, 6)):
        if 3 in tags:
            self.copy(self.mate, 3, self.mate).wait_recv()
        for n, tag in ((1, 4), (2, 5), (3, 6)):
            if tag not in tags:
                continue

            @pl.when(self.c >= n)
            def _():
                self.copy(self.mate - 2 * n, tag, self.mate).wait_recv()

    def drain(self, tags=range(7)):
        c = self.c
        conds = (c <= 2, (c >= 1) & (c <= 2), c == 0, c >= 0, c >= 1, c >= 2, c == 3)
        for tag in tags:
            @pl.when(conds[tag])
            def _():
                self.copy(self.me, tag, self.mate).wait_send()


def attn_body(nb, tok, seq, d, q_hbm, do_hbm, kvl_hbm, kv0_hbm, dy_hbm, dyp_hbm, cos_ref, sin_ref,
              o_hbm, dq_hbm, dkv_hbm, op_hbm, dqp_hbm, acc_hbm,
              kv_all, o_v, dq_v, mrecv, rrecv, big,
              kv_send, kv_recv, m_send, m_recv, r_send, r_recv, own_sem, in_sem, out_sem, fin_sem, p_send, p_recv, first_sem,
              ld_sem, b_sem, acc_sem):
    scale = d ** -0.5
    rows = o_v.shape[2] * tok
    n_blk = seq // 256
    rb = 2 * rows // n_blk
    n_rb = rows // rb
    half = d // 2
    me, k, mate, cw, ccw = ring_ids()
    c = me // 2
    rel = [lax.rem(c + o, 4) for o in (3, 1, 2, 0)]

    def blk(j):
        return pl.ds(pl.multiple_of(j * tok, 16), tok)

    def kvb(b, j):
        return kv_all.at[b, blk(j)]

    def gather(b):
        return Gather((me, k, mate, cw, ccw), c, lambda j: kvb(b, j), lambda t: kv_send.at[b - 1, t], lambda t: kv_recv.at[b - 1, t])

    def own(b):
        gather(b).own(kvl_hbm.at[b])

    def own_copy(b):
        return pltpu.make_async_copy(kvl_hbm.at[b], kvb(b, me), own_sem.at[b])

    def ready(b):
        own_copy(b).wait()

        @pl.when(b == 1)
        def _():
            gather(1).ready((4, 5, 6))

        @pl.when(b > 1)
        def _():
            gather(b).ready()

    def drain(b):
        @pl.when(b == 1)
        def _():
            gather(1).drain((1, 4, 5, 6))

        @pl.when(b > 1)
        def _():
            gather(b).drain()

    def m_copy(b, n):
        return rdma(kvb(b, 2 * n + 1 - k), mrecv.at[lax.rem(b, 2), n], m_send.at[b, n], m_recv.at[b, n], mate)

    def r_copy(b, n, slot, to):
        return rdma(kvb(b, 2 * n + k), rrecv.at[b, slot], r_send.at[b, slot], r_recv.at[b, slot], to)

    def add_into(b, n, other):
        v = kv_all[b, blk(2 * n + k), :].astype(F32) + other[...].astype(F32)
        kv_all[b, blk(2 * n + k), :] = v.astype(BF16)

    def fin_copy(b):
        return pltpu.make_async_copy(kvb(b, me), dkv_hbm.at[b], fin_sem.at[b])

    def to_mate(b):
        for n in range(4):
            @pl.when(c >= n)
            def _():
                m_copy(b, n).start()

    def stage1(b):
        for n in range(4):
            @pl.when(c >= n)
            def _():
                m_copy(b, n).wait()
                add_into(b, n, mrecv.at[lax.rem(b, 2), n])

        @pl.when(c == 3)
        def _():
            r_copy(b, 1, 2, ccw).start()
            r_copy(b, 2, 1, ccw).start()
            r_copy(b, 0, 0, cw).start()
            fin_copy(b).start()

        @pl.when(c == 2)
        def _():
            r_copy(b, 0, 1, ccw).start()

    def stage2(b):
        @pl.when(c == 2)
        def _():
            r_copy(b, 1, 2, ccw).wait_recv()
            add_into(b, 1, rrecv.at[b, 2])
            r_copy(b, 1, 2, ccw).start()
            r_copy(b, 2, 1, ccw).wait_recv()
            add_into(b, 2, rrecv.at[b, 1])
            fin_copy(b).start()

        @pl.when(c == 1)
        def _():
            r_copy(b, 0, 1, ccw).wait_recv()
            add_into(b, 0, rrecv.at[b, 1])
            r_copy(b, 0, 1, ccw).start()

    def stage3(b):
        @pl.when(c == 0)
        def _():
            r_copy(b, 0, 0, cw).wait_recv()
            add_into(b, 0, rrecv.at[b, 0])
            r_copy(b, 0, 1, ccw).wait_recv()
            add_into(b, 0, rrecv.at[b, 1])
            fin_copy(b).start()

        @pl.when(c == 1)
        def _():
            r_copy(b, 1, 2, ccw).wait_recv()
            add_into(b, 1, rrecv.at[b, 2])
            fin_copy(b).start()

    def handed(dst, src, n, b, slot):
        return rdma(src.at[slot, 1 - k], dst.at[b], p_send.at[n, b], p_recv.at[n, b], mate)

    def store_o(b, slot):
        return (pltpu.make_async_copy(o_v.at[slot], o_hbm.at[b], out_sem.at[0, slot]), handed(op_hbm, o_v, 0, b, slot))

    def store_dq(b, slot):
        return (pltpu.make_async_copy(dq_v.at[slot], dq_hbm.at[b], out_sem.at[1, slot]), handed(dqp_hbm, dq_v, 1, b, slot))

    def stored(x):
        x[0].wait()
        x[1].wait_send()

    load_dy = (pltpu.make_async_copy(dy_hbm, big.at[0], b_sem.at[0]), pltpu.make_async_copy(dyp_hbm, big.at[1], b_sem.at[1]))

    def attend(q_v, do_v, s_buf, m_buf, l_buf, p_buf, ds_buf, q_t, do_t, dk_t, dv_t, d_buf, cos4, sin4):
        def load(b, slot):
            return (pltpu.make_async_copy(q_hbm.at[b], q_v.at[slot], in_sem.at[0, slot]),
                    pltpu.make_async_copy(do_hbm.at[b], do_v.at[slot], in_sem.at[1, slot]))

        def scores(b, g, slot, i):
            w = min(512, seq)
            if (i * 256) % w:
                return
            cols = slice(i * 256, i * 256 + w)
            s = dot_nt(q_v[slot, g].reshape(rows, d), kv_all[b, cols, :d]) * (scale * LOG2E)
            col = lax.broadcasted_iota(jnp.int32, (tok, w), 1) + i * 256
            row = lax.broadcasted_iota(jnp.int32, (tok, w), 0) + me * tok
            s = jnp.concatenate([jnp.where(col <= row, s[j * tok:(j + 1) * tok], -1e30) for j in range(rows // tok)], axis=0)
            s_buf[g, :, cols] = s
            m = s[:, :128]
            for j in range(128, w, 128):
                m = jnp.maximum(m, s[:, j:j + 128])
            m_buf[...] = m if i == 0 else jnp.maximum(m_buf[...], m)

        parts = max(1, min(5, n_blk))
        part = [j * (rows // 16) // parts * 16 for j in range(parts + 1)] + [rows] * n_blk

        def softmax(g, i):
            for r in range(part[i], part[i + 1], 16):
                rs = slice(r, r + 16)
                m = jnp.max(m_buf[rs, :], axis=1, keepdims=True)
                l = None
                for j in range(0, seq, 128):
                    e = jnp.exp2(s_buf[g, rs, j:j + 128] - m)
                    s_buf[g, rs, j:j + 128] = e
                    l = e if l is None else l + e
                l_buf[g, rs, :] = jnp.broadcast_to(1.0 / jnp.sum(l, axis=1, keepdims=True), (16, 128))

        def turn(g, slot, i):
            rs = slice(i * rb, (i + 1) * rb)
            q_t[g, :, rs] = q_v[slot, g].reshape(rows, d)[rs].T
            do_t[g, :, rs] = do_v[slot, g].reshape(rows, d)[rs].T

        def out_rows(b, g, slot, i):
            rs = slice(i * rb, (i + 1) * rb)
            p = (s_buf[g, rs, :] * jnp.concatenate([l_buf[g, rs, :]] * (seq // 128), axis=1)).astype(BF16)
            p_buf[rs, :] = p
            o = dot_nn(p, kv_all[b, :, d:])
            dvec = jnp.sum(o * do_v[slot, g].reshape(rows, d)[rs].astype(F32), axis=1, keepdims=True)
            d_buf[rs, :] = jnp.broadcast_to(dvec, (rb, 128))
            put_rows(o_v, slot, g, i, o.astype(BF16))

        def put_rows(ref, slot, g, i, v):
            r = i * rb
            while r < (i + 1) * rb:
                n = min((i + 1) * rb - r, tok - r % tok)
                ref[slot, g, r // tok, r % tok:r % tok + n, :] = v[r - i * rb:r - i * rb + n]
                r += n

        def dq_rows(b, g, slot, i):
            rs = slice(i * rb, (i + 1) * rb)
            dq = dot_nn(ds_buf[rs, :], kv_all[b, :, :d]) * scale
            lo, hi = dq[:, :half], dq[:, half:]
            cs, sn = cos4[rs, :], sin4[rs, :]
            put_rows(dq_v, slot, g, i, jnp.concatenate([(lo * cs + hi * sn).astype(BF16), (hi * cs - lo * sn).astype(BF16)], axis=1))

        def grads(b, g, slot, i):
            cols = slice(i * 256, (i + 1) * 256)
            do = do_v[slot, g].reshape(rows, d)
            p = p_buf[:, cols]
            dp = dot_nt(do, kv_all[b, cols, d:])
            dvec = d_buf[...]
            if i > 0 and part[i] > part[i - 1]:
                z = None
                for r in range(part[i - 1], part[i], 8):
                    v = l_buf[1 - g, r:r + 8, :]
                    z = v if z is None else jnp.minimum(z, v)
                dvec = dvec + jnp.concatenate([jnp.minimum(z, 0.0)] * (rows // 8), axis=0)
            dd = jnp.concatenate([dvec, dvec], axis=1)
            ds = (p.astype(F32) * (dp - dd)).astype(BF16)
            ds_buf[:, cols] = ds
            dk = dot_nn(q_t[g], ds)
            dv = dot_nn(do_t[g], p)
            if g == 0:
                dk_t[:, cols] = dk
                dv_t[:, cols] = dv
            else:
                dk_t[:, cols] += dk
                dv_t[:, cols] += dv

        def close_kv(b, i):
            cols = slice(i * 256, (i + 1) * 256)
            kv_all[b, cols, :d] = (dk_t[:, cols] * scale).T.astype(BF16)
            kv_all[b, cols, d:] = dv_t[:, cols].T.astype(BF16)

        enter((mate, cw, ccw))
        gather(1).pass_on(lambda j: kv0_hbm.at[1, blk(j)])
        if nb > 2:
            own(2)
        for x in load(0, 0):
            x.start()

        def first(j):
            return pltpu.make_async_copy(kv0_hbm.at[0, blk(j)], kvb(0, j), first_sem.at[j])

        def second(j, n):
            return pltpu.make_async_copy(kv0_hbm.at[1, blk(j)], kvb(1, j), first_sem.at[8 + n])
        arrived = ((c >= 0, mate, 0), (c >= 1, me - 2, 1), (c == 3, me - 6, 2))
        for j in range(8):
            @pl.when(j <= 2 * c + 1)
            def _():
                first(j).start()
        for b in range(1, nb):
            own_copy(b).start()
        for cond, j, i in arrived:
            @pl.when(cond)
            def _():
                second(j, i).start()

        @pl.loop(2 * c + 2, 8)
        def _(j):
            for b in range(nb):
                kv_all[b, blk(j), :] = jnp.zeros((tok, 2 * d), BF16)
        for j in range(rows // tok):
            cos4[j * tok:(j + 1) * tok, :] = cos_ref[...]
            sin4[j * tok:(j + 1) * tok, :] = sin_ref[...]
        ds_buf[...] = jnp.zeros_like(ds_buf)
        for x in load(0, 0):
            x.wait()
        for i in range(n_rb):
            turn(0, 0, i)
        for j in range(8):
            @pl.when(j <= 2 * c + 1)
            def _():
                first(j).wait()
        for cond, j, i in arrived:
            @pl.when(cond)
            def _():
                second(j, i).wait()
        for i in range(n_blk):
            scores(0, 0, 0, i)
        for i in range(n_blk):
            softmax(0, i)

        def comm_steps(b, steps):
            for lag, stage in steps:
                @pl.when(b >= lag)
                def _():
                    stage(b - lag)

        @pl.loop(0, nb)
        def _(b):
            slot = lax.rem(b, 2)
            nxt = jnp.minimum(b + 1, nb - 1)
            prev = jnp.maximum(b - 1, 0)

            @pl.when(b + 1 < nb)
            def _():
                for x in load(b + 1, 1 - slot):
                    x.start()

            @pl.when(b + 3 < nb)
            def _():
                own(b + 3)

            @pl.when((b >= 1) & (b + 2 < nb))
            def _():
                gather(b + 2).forward()

            @pl.when(b == 1)
            def _():
                for x in load_dy:
                    x.start()
            comm_steps(b, ((3, stage2), (4, stage3)))

            @pl.when(b >= 2)
            def _():
                drain(b - 1)

            @pl.when(b >= 2)
            def _():
                stored(store_o(b - 2, slot))
            spare = jnp.where(b >= 1, b - 1, nb)
            for i in range(n_blk):
                scores(b, 1, slot, i)
                if i % 2 == 1:
                    out_rows(b, 0, slot, i // 2)
                    dq_rows(prev, 1, 1 - slot, i // 2)
                    turn(1, slot, i // 2)
            for i in range(n_blk):
                close_kv(spare, i)

            @pl.when(b + 1 < nb)
            def _():
                gather(b + 1).last()

            @pl.when(b >= 1)
            def _():
                for x in store_dq(b - 1, 1 - slot):
                    x.start()
                to_mate(b - 1)

            for i in range(n_blk):
                grads(b, 0, slot, i)
                softmax(1, i)

            @pl.when(b + 1 < nb)
            def _():
                for x in load(b + 1, 1 - slot):
                    x.wait()
                ready(b + 1)
            if nb > 2:
                @pl.when(b == 0)
                def _():
                    gather(2).forward()

            @pl.when(b >= 2)
            def _():
                stored(store_dq(b - 2, slot))
            nslot = lax.rem(nxt, 2)
            for i in range(n_blk):
                scores(nxt, 0, nslot, i)
                if i % 2 == 1:
                    out_rows(b, 1, slot, i // 2)
                    dq_rows(b, 0, slot, i // 2)
                    turn(0, nslot, i // 2)
            for x in store_o(b, slot):
                x.start()
            comm_steps(b, ((1, stage1),))
            for i in range(n_blk):
                grads(b, 1, slot, i)
                softmax(0, i)

        drain(nb - 1)
        for i in range(n_rb):
            dq_rows(nb - 1, 1, (nb - 1) % 2, i)
        for i in range(n_blk):
            close_kv(nb - 1, i)
        to_mate(nb - 1)
        for x in store_dq(nb - 1, (nb - 1) % 2):
            x.start()

    slab = pltpu.VMEM((2, 2, rows // tok, tok, d), BF16)
    pl.run_scoped(attend, slab, slab, pltpu.VMEM((2, rows, seq), F32), pltpu.VMEM((rows, 128), F32), pltpu.VMEM((2, rows, 128), F32),
                  pltpu.VMEM((rows, seq), BF16), pltpu.VMEM((rows, seq), BF16), pltpu.VMEM((2, d, rows), BF16),
                  pltpu.VMEM((2, d, rows), BF16), pltpu.VMEM((d, seq), F32), pltpu.VMEM((d, seq), F32),
                  pltpu.VMEM((rows, 128), F32), pltpu.VMEM((rows, half), F32), pltpu.VMEM((rows, half), F32))
    n = nb

    def first_products(a_v, at, acc_v):
        pr = Products(big, a_v, at, ld_sem, b_sem)
        for b in (n - 2, n - 1):
            stored(store_o(b, b % 2))
        for b in range(n):
            handed(op_hbm, o_v, 0, b, b % 2).wait_recv()

        def fetch(r):
            return pr.load_a(r, o_hbm.at[:, k, rel[r]], op_hbm.at[:, rel[r]])

        def save(r):
            return pltpu.make_async_copy(acc_v.at[r], acc_hbm.at[r], acc_sem.at[r])
        for r in range(2):
            for x in fetch(r):
                x.start()

        todo = [((stage2, n - 3), (stage3, n - 4)), ((stage1, n - 1), (stage2, n - 2), (stage3, n - 3)),
                ((stage2, n - 1), (stage3, n - 2)), ((stage3, n - 1),)]

        def steps(i):
            for stage, b in todo[i]:
                if b >= 0:
                    stage(b)
        steps(0)
        steps(1)
        for r in range(2):
            for x in fetch(r):
                x.wait()
            pr.turn(0, a_v.at[r, 0])
            pr.turn(1, a_v.at[r, 1])
            if r == 0:
                for x in load_dy:
                    x.wait()
            pr.columns(acc_v.at[r], 0, 4)
            save(r).start()
        steps(2)
        steps(3)
        for r in range(2):
            save(r).wait()

    pl.run_scoped(first_products, pltpu.VMEM((2, 2, nb, tok, d), BF16),
                  pltpu.VMEM((2, d, nb * tok), BF16), pltpu.VMEM((2, 2, d, dy_hbm.shape[1] // 2), F32))
    for b in (n - 2, n - 1):
        stored(store_dq(b, b % 2))
    for b in range(n):
        handed(dqp_hbm, dq_v, 1, b, b % 2).wait_recv()
        fin_copy(b).wait()
        for cond, slot in ((c == 3, 0), (c >= 1, 1), (c >= 2, 2)):
            @pl.when(cond)
            def _():
                r_copy(b, 0, slot, cw).wait_send()


def attention(q, do, kv, kv0, dy, dy_p, cos_t, sin_t):
    nb, _, hp, tok, d = q.shape
    seq = tok * 8
    rows = hp * tok
    any_spec = pl.BlockSpec(memory_space=pl.ANY)
    vmem = pl.BlockSpec(memory_space=pltpu.VMEM)
    dma = pltpu.SemaphoreType.DMA
    slab = pltpu.VMEM((2, 2, hp, tok, d), BF16)
    out = jax.ShapeDtypeStruct(q.shape, BF16)
    outp = jax.ShapeDtypeStruct((nb, hp, tok, d), BF16)
    return pl.pallas_call(
        functools.partial(attn_body, nb, tok, seq, d),
        in_specs=[any_spec] * 6 + [vmem, vmem],
        out_specs=[any_spec] * 6,
        out_shape=[out, out, jax.ShapeDtypeStruct(kv.shape, BF16), outp, outp,
                   jax.ShapeDtypeStruct((2, 2, d, dy.shape[1] // 2), F32)],
        scratch_shapes=[pltpu.VMEM((nb + 1, seq, 2 * d), BF16), slab, slab,
                        pltpu.VMEM((2, 4, tok, 2 * d), BF16), pltpu.VMEM((nb, 3, tok, 2 * d), BF16),
                        pltpu.VMEM((2,) + dy.shape, BF16),
                        dma((nb - 1, 7)), dma((nb - 1, 7)), dma((nb, 4)), dma((nb, 4)), dma((nb, 3)), dma((nb, 3)),
                        dma((nb,)), dma((2, 2)), dma((2, 2)), dma((nb,)), dma((2, nb)), dma((2, nb)), dma((11,)),
                        dma((2, 2)), dma((2,)), dma((4,))],
        compiler_params=pltpu.CompilerParams(collective_id=1, has_side_effects=True, vmem_limit_bytes=63 * 2**20),
        cost_estimate=pl.CostEstimate(flops=24 * nb * rows * seq * d, bytes_accessed=40 * 2**20,
                                      transcendentals=2 * nb * rows * seq),
        name="attention",
    )(q, do, kv, kv0, dy, dy_p, cos_t, sin_t)


def proj_body(nb, tok, x_hbm, g_ref, wq_hbm, wk_ref, wv_ref, wo_hbm, dy_hbm, cos_ref, sin_ref,
              kv0_hbm, hn_hbm, q_hbm, do_hbm, kv_hbm, wqf_hbm, wof_hbm, hnp_hbm, dyp_hbm,
              x_v, hn_v, dy_v, wq_v, wo_v, kv_v, out_v,
              send, recv, x_sem, dy_sem, own_sem, out_sem, misc_sem, w_sem, p_send, p_recv, kv_send, kv_recv):
    n_tok, e = x_hbm.shape
    d = kv_v.shape[1] // 2
    half = d // 2
    mc = 2 * tok
    me, k, mate, cw, ccw = ring_ids()
    base = 2 * (me // 2)

    def head(off, par):
        return lax.rem(base + 2 * off + 8, 8) + par
    enter((mate, cw, ccw))

    fulls = (wq_v, wo_v)
    locs = (wq_hbm, wo_hbm)

    def half_of(w, ref, j):
        n = ref.shape[0] // 2
        return ref.at[pl.ds(j * n, n)]

    sends = []

    def send_full(w, h, j, to, own=False):
        src = locs[w] if own else fulls[w].at[h]
        c = rdma(src, fulls[w].at[h], send.at[w, j], recv.at[w, j], to)
        c.start()
        sends.append(c)

    def send_half(w, h, part, j, to):
        c = rdma(half_of(w, fulls[w].at[h], part), half_of(w, fulls[w].at[h], part), send.at[w, j], recv.at[w, j], to)
        c.start()
        sends.append(c)

    def wait_full(w, h, j):
        rdma(fulls[w].at[h], fulls[w].at[h], send.at[w, j], recv.at[w, j], mate).wait_recv()

    def wait_half(w, h, part, j):
        ref = half_of(w, fulls[w].at[h], part)
        rdma(ref, ref, send.at[w, j], recv.at[w, j], mate).wait_recv()

    for w in range(2):
        send_full(w, me, 0, cw, True)
        send_full(w, me, 1, ccw, True)
        send_full(w, me, 4, mate, True)
    own = [pltpu.make_async_copy(locs[w], fulls[w].at[me], own_sem.at[w]) for w in range(2)]
    xs = [pltpu.make_async_copy(x_hbm.at[pl.ds(b * tok, tok)], x_v.at[pl.ds(b * tok, tok)], x_sem.at[b]) for b in range(nb)]
    for c in xs:
        c.start()
    for c in own:
        c.start()
    dyc = pltpu.make_async_copy(dy_hbm, dy_v, dy_sem)
    dyc.start()

    gain = g_ref[...].astype(F32).reshape(1, e)
    for b in range(nb):
        xs[b].wait()

        @pl.loop(0, tok // 16, unroll=2)
        def _(r):
            rs = pl.ds(pl.multiple_of(b * tok + r * 16, 16), 16)
            x = x_v[rs, :].astype(F32)
            c = x - jnp.mean(x, axis=1, keepdims=True)
            inv = lax.rsqrt(jnp.mean(c * c, axis=1, keepdims=True) + LN_EPS)
            hn_v[rs, :] = (c * inv * gain).astype(BF16)
    hn_out = pltpu.make_async_copy(hn_v, hn_hbm, misc_sem.at[0])
    hn_out.start()
    to_mate = [rdma(hn_v, hnp_hbm, p_send.at[0], p_recv.at[0], mate), rdma(dy_hbm, dyp_hbm, p_send.at[1], p_recv.at[1], mate)]
    for c in to_mate:
        c.start()

    def rope_rows(raw):
        lo, hi = raw[:, :half], raw[:, half:d]
        cs, sn = jnp.concatenate([cos_ref[...]] * 2, axis=0), jnp.concatenate([sin_ref[...]] * 2, axis=0)
        return lo * cs - hi * sn, hi * cs + lo * sn

    @pl.loop(0, n_tok // mc)
    def _(i):
        rs = pl.ds(pl.multiple_of(i * mc, mc), mc)
        lo, hi = rope_rows(dot_nn(hn_v[rs, :], wk_ref[...]))
        kv_v[rs, :half] = lo.astype(BF16)
        kv_v[rs, half:d] = hi.astype(BF16)
        kv_v[rs, d:] = dot_nn(hn_v[rs, :], wv_ref[...]).astype(BF16)
    kv_out = pltpu.make_async_copy(kv_v, kv_hbm, misc_sem.at[1])
    kv_out.start()

    outs = []
    saves = []

    def save(w, h):
        c = pltpu.make_async_copy(fulls[w].at[h], (wqf_hbm, wof_hbm)[w].at[h], w_sem.at[len(saves)])
        c.start()
        saves.append(c)

    def project(w, h):
        slot = len(outs) % 4
        if len(outs) >= 4:
            outs[-4].wait()

        @pl.loop(0, n_tok // mc)
        def _(i):
            rs = pl.ds(pl.multiple_of(i * mc, mc), mc)
            if w == 0:
                lo, hi = rope_rows(dot_nn(hn_v[rs, :], wq_v[h]))
                o0 = lo.reshape(2, tok, half).astype(BF16)
                o1 = hi.reshape(2, tok, half).astype(BF16)
                out_v[slot, pl.ds(2 * i, 2), :, :half] = o0
                out_v[slot, pl.ds(2 * i, 2), :, half:] = o1
            else:
                out_v[slot, pl.ds(2 * i, 2)] = dot_nt(dy_v[rs, :], wo_v[h]).reshape(2, tok, d).astype(BF16)
        c = pltpu.make_async_copy(out_v.at[slot], (q_hbm, do_hbm)[w].at[:, lax.rem(h, 2), h // 2], out_sem.at[slot])
        c.start()
        outs.append(c)
        save(w, h)

    other = 1 - k
    for w in range(2):
        own[w].wait()
        if w == 1:
            dyc.wait()
        project(w, me)
        wait_full(w, mate, 4)
        project(w, mate)
    for w in range(2):
        wait_full(w, head(-1, k), 0)
        send_half(w, head(-1, k), 0, 2, cw)
        wait_full(w, head(1, k), 1)
        send_half(w, head(1, k), 1, 3, ccw)
        send_full(w, head(-1, k), 5, mate)
        send_full(w, head(1, k), 6, mate)
        project(w, head(-1, k))
        project(w, head(1, k))
        wait_full(w, head(-1, other), 5)
        project(w, head(-1, other))
        wait_full(w, head(1, other), 6)
        project(w, head(1, other))

    def early(n):
        def blk(j):
            return kv0_hbm.at[n, pl.ds(pl.multiple_of(j * tok, 16), tok)]
        return Gather((me, k, mate, cw, ccw), me // 2, blk, lambda t: kv_send.at[n, t], lambda t: kv_recv.at[n, t])
    first, second = early(0), early(1)
    first.own(kv_v.at[pl.ds(0, tok)])
    own0 = pltpu.make_async_copy(kv_v.at[pl.ds(0, tok)], first.block(me), misc_sem.at[2])
    own0.start()
    for w in range(2):
        wait_half(w, head(2, k), 0, 2)
        send_half(w, head(2, k), 0, 7, mate)
        wait_half(w, head(2, k), 1, 3)
        send_half(w, head(2, k), 1, 8, mate)
        project(w, head(2, k))
        if w == 1:
            first.forward()
            second.own(kv_v.at[pl.ds(tok, tok)])
        wait_half(w, head(2, other), 0, 7)
        wait_half(w, head(2, other), 1, 8)
        project(w, head(2, other))
    first.last()
    for c in outs[-4:] + saves + [hn_out, kv_out, own0]:
        c.wait()
    first.ready()
    first.drain()
    second.arrived()
    second.ready((3,))
    second.drain((0, 2, 3))
    for c in sends:
        c.wait_send()
    for c in to_mate:
        c.wait()


def project(x, gain, wq, w_k, w_v, wo, dy, cos_t, sin_t):
    nb, tok, e = x.shape
    d = wq.shape[1]
    n_heads = 8
    n_tok = nb * tok
    any_spec = pl.BlockSpec(memory_space=pl.ANY)
    vmem = pl.BlockSpec(memory_space=pltpu.VMEM)
    act = jax.ShapeDtypeStruct((nb, 2, n_heads // 2, tok, d), BF16)
    dma = pltpu.SemaphoreType.DMA
    flops = 2 * n_tok * e * (2 * n_heads + 2) * d
    kv0, hn, q, do, kv, wqf, wof, hn_p, dy_p = pl.pallas_call(
        functools.partial(proj_body, nb, tok),
        in_specs=[any_spec, vmem, any_spec, vmem, vmem, any_spec, any_spec, vmem, vmem],
        out_specs=[any_spec] * 9,
        out_shape=[jax.ShapeDtypeStruct((2, tok * n_heads, 2 * d), BF16), jax.ShapeDtypeStruct((n_tok, e), BF16), act, act, jax.ShapeDtypeStruct((n_tok, 2 * d), BF16),
                   jax.ShapeDtypeStruct((n_heads, e, d), BF16), jax.ShapeDtypeStruct((n_heads, d, e), BF16),
                   jax.ShapeDtypeStruct((n_tok, e), BF16), jax.ShapeDtypeStruct((n_tok, e), BF16)],
        scratch_shapes=[pltpu.VMEM((n_tok, e), BF16), pltpu.VMEM((n_tok, e), BF16), pltpu.VMEM((n_tok, e), BF16),
                        pltpu.VMEM((n_heads, e, d), BF16), pltpu.VMEM((n_heads, d, e), BF16),
                        pltpu.VMEM((n_tok, 2 * d), BF16), pltpu.VMEM((4, nb, tok, d), BF16),
                        dma((2, 9)), dma((2, 9)), dma((nb,)), dma(()), dma((2,)), dma((4,)), dma((3,)), dma((16,)), dma((2,)), dma((2,)), dma((2, 7)), dma((2, 7))],
        compiler_params=pltpu.CompilerParams(collective_id=0, has_side_effects=True, vmem_limit_bytes=60 * 2**20),
        cost_estimate=pl.CostEstimate(flops=flops, bytes_accessed=60 * 2**20, transcendentals=0),
        name="project",
    )(x.reshape(n_tok, e), gain, wq, w_k, w_v, wo, dy.reshape(n_tok, e), cos_t, sin_t)
    return kv0, hn, q, do, kv.reshape(nb, tok, 2 * d), wqf, wof, hn_p, dy_p


def grads_body(nb, tok, o_hbm, op_hbm, acc_hbm, dq_hbm, dqp_hbm, hn_hbm, hnp_hbm, dy_hbm, dyp_hbm, dkv_hbm,
               wq_hbm, wo_hbm, wk_hbm, wv_hbm, x_hbm, g_ref, cos_ref, sin_ref,
               y_hbm, gx_hbm, gln_ref, gwo_ref, gwq_ref, gkv_hbm,
               acc, acc_kv, rbuf, rbuf_kv, kind, kp, dkv_v, fin_kv, gln_acc, gl_recv,
               rs_send, rs_recv, kv_send, kv_recv, ag_send, ag_recv, gl_send, gl_rsem, kp_sem, ld_sem, b_sem, t_sem, a_sem):
    n_tok, e = x_hbm.shape
    d = wk_hbm.shape[1]
    half = d // 2
    eh, eq = e // 2, e // 4
    me, k, mate, cw, ccw = ring_ids()
    c = me // 2
    rel = [lax.rem(c + o, 4) for o in (3, 1, 2, 0)]
    enter([lax.rem(me + o, 8) for o in range(1, 8)])

    order = ((2, 1), (2, 0))

    def hop(s, dr, j):
        first = acc_hbm.at[dr, dr] if s == 0 else acc.at[s, dr, dr]
        src = first if j == 0 else rbuf.at[s, dr, j - 1]
        return rdma(src, rbuf.at[s, dr, j], rs_send.at[s, dr, j], rs_recv.at[s, dr, j], (cw, ccw)[dr])

    def hop_kv(dr, j):
        src = acc_kv.at[dr, dr] if j == 0 else rbuf_kv.at[dr, j - 1]
        return rdma(src, rbuf_kv.at[dr, j], kv_send.at[dr, j], kv_recv.at[dr, j], (cw, ccw)[dr])

    def add(dst, term):
        @pl.loop(0, dst.shape[0] // 32)
        def _(i):
            rs = pl.ds(pl.multiple_of(i * 32, 32), 32)
            dst[rs, :] = dst[rs, :] + term[rs, :]

    def pass_on(s, j):
        for dr in range(2):
            hop(s, dr, j - 1).wait_recv()
            add(rbuf.at[s, dr, j - 1], acc.at[s, order[dr][j - 1], dr])
            hop(s, dr, j).start()

    def pass_on_kv(j):
        for dr in range(2):
            hop_kv(dr, j - 1).wait_recv()
            add(rbuf_kv.at[dr, j - 1], acc_kv.at[order[dr][j - 1], dr])
            hop_kv(dr, j).start()

    def finish(s, out):
        for dr in range(2):
            hop(s, dr, 2).wait_recv()

            @pl.loop(0, d // 32)
            def _(i):
                rs = pl.ds(pl.multiple_of(i * 32, 32), 32)
                out[rs, dr * eh:(dr + 1) * eh] = (rbuf[s, dr, 2, rs, :] + acc[s, 3, dr, rs, :]).astype(BF16)

    def piece(kk, j, lo=0, n=None):
        return gkv_hbm.at[kk, pl.ds(lo, d if n is None else n), pl.ds(pl.multiple_of(j * eq, 128), eq)]

    def ag(tag, ref, to, src=None):
        return rdma(ref if src is None else src, ref, ag_send.at[tag], ag_recv.at[tag], to)

    def ag_far(tag, to):
        return ag(tag, piece(k, rel[(0, 1)[tag - 3]], (tag - 3) * half, half), to)

    own_piece = pltpu.make_async_copy(fin_kv, piece(k, c), t_sem.at[5])

    def finish_kv():
        for dr in range(2):
            hop_kv(dr, 2).wait_recv()
            fin_kv[:, dr * (eq // 2):(dr + 1) * (eq // 2)] = rbuf_kv[dr, 2] + acc_kv[3, dr]
        ag(0, piece(k, c), cw, fin_kv).start()
        ag(1, piece(k, c), ccw, fin_kv).start()
        ag(2, piece(k, c), mate, fin_kv).start()
        own_piece.start()

    def ag_forward():
        ag(0, piece(k, rel[0]), cw).wait_recv()
        ag_far(3, cw).start()
        ag(1, piece(k, rel[1]), cw).wait_recv()
        ag_far(4, ccw).start()
        ag(5, piece(k, rel[0]), mate).start()
        ag(6, piece(k, rel[1]), mate).start()

    def ag_last():
        far = [piece(k, rel[2], i * half, half) for i in range(2)]
        for i in range(2):
            ag(3 + i, far[i], cw).wait_recv()
            ag(7 + i, far[i], mate).start()
        ag(2, piece(1 - k, c), mate).wait_recv()
        ag(5, piece(1 - k, rel[0]), mate).wait_recv()
        ag(6, piece(1 - k, rel[1]), mate).wait_recv()
        for i in range(2):
            ag(7 + i, piece(1 - k, rel[2], i * half, half), mate).wait_recv()
        for tag in range(3):
            ag(tag, piece(k, c), cw, fin_kv).wait_send()
        for tag in (3, 4, 7, 8):
            ag(tag, far[0], cw).wait_send()
        for tag in (5, 6):
            ag(tag, piece(k, c), cw).wait_send()
        own_piece.wait()

    dkv_in = pltpu.make_async_copy(dkv_hbm, dkv_v, t_sem.at[4])
    dkv_in.start()
    kp_copy = rdma(kind.at[1 - k], kp, kp_sem.at[0], kp_sem.at[1], mate)

    for dr in range(2):
        hop(0, dr, 0).start()
    acc_in = [pltpu.make_async_copy(acc_hbm.at[r], acc.at[0, r], a_sem.at[r]) for r in range(2)]
    for x in acc_in:
        x.start()

    def products(big, a_v, at):
        pr = Products(big, a_v, at, ld_sem, b_sem)
        dy_in = pr.load_b(dy_hbm, dyp_hbm)
        hn_in = pr.load_b(hn_hbm, hnp_hbm)
        jobs = [(0, 2), (0, 3)] + [(1, r) for r in range(4)]

        def fetch(i):
            s, r = jobs[i]
            return pr.load_a(i, (o_hbm, dq_hbm)[s].at[:, k, rel[r]], (op_hbm, dqp_hbm)[s].at[:, rel[r]])
        for x in dy_in:
            x.start()
        for i in range(2):
            for x in fetch(i):
                x.start()
        dkv_in.wait()
        for b in range(nb):
            lo, hi = dkv_v[b, :, :half].astype(F32), dkv_v[b, :, half:d].astype(F32)
            cs, sn = cos_ref[...], sin_ref[...]
            kind[0, b, :, :half] = (lo * cs + hi * sn).astype(BF16)
            kind[0, b, :, half:] = (hi * cs - lo * sn).astype(BF16)
            kind[1, b] = dkv_v[b, :, d:]
        kp_copy.start()
        for i, (s, r) in enumerate(jobs):
            if i == 2:
                pr.turn(0, kind.at[k])
                kp_copy.wait_recv()
                pr.turn(1, kp)
                for x in hn_in:
                    x.wait()
                for q in range(4):
                    for dr in range(2):
                        acc_kv[q, dr] = pr.both(pl.ds(pl.multiple_of(rel[q] * eq + dr * (eq // 2), 128), eq // 2))
                for dr in range(2):
                    hop_kv(dr, 0).start()
            for x in fetch(i):
                x.wait()
            pr.turn(0, a_v.at[i % 2, 0])
            pr.turn(1, a_v.at[i % 2, 1])
            if i + 2 < len(jobs):
                for x in fetch(i + 2):
                    x.start()
            if i == 0:
                for x in dy_in:
                    x.wait()
            if s == 1 and r < 2:
                pr.columns(acc.at[s, r], 0, 2, 2 * r)
                hop(s, r, 0).start()
                pr.columns(acc.at[s, r], 2, 4, 2 * r)
            else:
                pr.columns(acc.at[s, r], 0, 4)
            if i == 1:
                for x in hn_in:
                    x.start()

    pl.run_scoped(products, pltpu.VMEM((2, n_tok, e), BF16), pltpu.VMEM((2, 2, nb, tok, d), BF16), pltpu.VMEM((2, d, n_tok), BF16))
    for x in acc_in:
        x.wait()
    pass_on(0, 1)
    pass_on_kv(1)

    mc = 2 * tok
    units = nb // 2

    def attn_out(wo_v, o_v, x_v, y_v):
        w_in = pltpu.make_async_copy(wo_hbm, wo_v, b_sem.at[0])
        w_in.start()

        def load(u):
            return (pltpu.make_async_copy(o_hbm.at[pl.ds(2 * u, 2)], o_v.at[u % 2], ld_sem.at[u % 2, 0]),
                    pltpu.make_async_copy(x_hbm.at[pl.ds(u * mc, mc)], x_v.at[u % 2], ld_sem.at[u % 2, 1]))

        def put(u):
            return pltpu.make_async_copy(y_v.at[u % 2], y_hbm.at[pl.ds(u * mc, mc)], t_sem.at[u % 2])
        for x in load(0):
            x.start()
        w_in.wait()
        for u in range(units):
            if u + 1 < units:
                for x in load(u + 1):
                    x.start()
            for x in load(u):
                x.wait()
            if u >= 2:
                put(u - 2).wait()
            sl = u % 2

            @pl.loop(0, 4)
            def _(n):
                cols = pl.ds(pl.multiple_of(n * eq, 128), eq)
                o_rows = jnp.concatenate([jnp.concatenate([o_v[sl, i, h % 2, h // 2] for h in range(8)], axis=1) for i in range(2)], axis=0)
                r = dot_nn(o_rows, wo_v[:, cols])
                y_v[sl, :, cols] = (x_v[sl, :, cols].astype(F32) + r).astype(BF16)
            put(u).start()
        for u in range(max(0, units - 2), units):
            put(u).wait()

    pl.run_scoped(attn_out, pltpu.VMEM((8 * d, e), BF16), pltpu.VMEM((2, 2, 2, 4, tok, d), BF16),
                  pltpu.VMEM((2, mc, e), BF16), pltpu.VMEM((2, mc, e), BF16))
    pass_on(1, 1)

    def hidden_grad(wq_v, wk_v, wv_v, dq_v, x_v, dy_v, dh, gx_v):
        w_in = pltpu.make_async_copy(wq_hbm, wq_v, b_sem.at[0])
        w_in.start()
        w2_in = (pltpu.make_async_copy(wk_hbm, wk_v, b_sem.at[1]), pltpu.make_async_copy(wv_hbm, wv_v, ld_sem.at[1, 1]))
        for x in w2_in:
            x.start()

        def load(u):
            return (pltpu.make_async_copy(dq_hbm.at[pl.ds(2 * u, 2)], dq_v, ld_sem.at[0, 0]),
                    pltpu.make_async_copy(x_hbm.at[pl.ds(u * mc, mc)], x_v, ld_sem.at[0, 1]),
                    pltpu.make_async_copy(dy_hbm.at[pl.ds(u * mc, mc)], dy_v, ld_sem.at[1, 0]))

        def put(u):
            return pltpu.make_async_copy(gx_v, gx_hbm.at[pl.ds(u * mc, mc)], t_sem.at[0])
        gain = g_ref[...].astype(F32).reshape(1, e)
        gln_acc[...] = jnp.zeros_like(gln_acc)
        for x in load(0):
            x.start()
        w_in.wait()
        for x in w2_in:
            x.wait()
        for u in range(units):
            for x in load(u):
                x.wait()

            @pl.loop(0, 4)
            def _(n):
                rows = pl.ds(pl.multiple_of(n * eq, 128), eq)
                t = None
                for h in range(8):
                    a = jnp.concatenate([dq_v[i, h % 2, h // 2] for i in range(2)], axis=0)
                    p = dot_nt(a, wq_v[h, rows, :])
                    t = p if t is None else t + p
                for j in range(2):
                    a = jnp.concatenate([kind[j, 2 * u + i] for i in range(2)], axis=0)
                    t = t + dot_nt(a, (wk_v, wv_v)[j][rows, :])
                dh[:, rows] = t
            if u >= 1:
                put(u - 1).wait()

            @pl.loop(0, mc // 16)
            def _(r):
                rs = pl.ds(pl.multiple_of(r * 16, 16), 16)
                x = x_v[rs, :].astype(F32)
                cx = x - jnp.mean(x, axis=1, keepdims=True)
                inv = lax.rsqrt(jnp.mean(cx * cx, axis=1, keepdims=True) + LN_EPS)
                xh = cx * inv
                g = dh[rs, :]
                pr = g * xh
                gln_acc[...] += pr[:8] + pr[8:]
                gh = g * gain
                m1 = jnp.mean(gh, axis=1, keepdims=True)
                m2 = jnp.mean(gh * xh, axis=1, keepdims=True)
                gx_v[rs, :] = (inv * (gh - m1 - xh * m2) + dy_v[rs, :].astype(F32)).astype(BF16)
            put(u).start()
            if u + 1 < units:
                for x in load(u + 1):
                    x.start()
            if u == units // 2 - 1:
                pass_on(0, 2)
                pass_on_kv(2)
        put(units - 1).wait()

    pl.run_scoped(hidden_grad, pltpu.VMEM((8, e, d), BF16), pltpu.VMEM((e, d), BF16), pltpu.VMEM((e, d), BF16), pltpu.VMEM((2, 2, 4, tok, d), BF16),
                  pltpu.VMEM((mc, e), BF16), pltpu.VMEM((mc, e), BF16), pltpu.VMEM((mc, e), F32), pltpu.VMEM((mc, e), BF16))
    gl_recv[me] = jnp.sum(gln_acc[...], axis=0, keepdims=True)
    pass_on(1, 2)
    finish(0, gwo_ref)
    finish_kv()
    gl = [rdma(gl_recv.at[me], gl_recv.at[me], gl_send.at[o - 1], gl_rsem.at[o - 1], lax.rem(me + o, 8)) for o in range(1, 8)]
    for x in gl:
        x.start()
    finish(1, gwq_ref)
    ag_forward()
    for o in range(1, 8):
        src = lax.rem(me + 8 - o, 8)
        rdma(gl_recv.at[src], gl_recv.at[src], gl_send.at[o - 1], gl_rsem.at[o - 1], mate).wait_recv()
    total = gl_recv[0]
    for i in range(1, 8):
        total = total + gl_recv[i]
    gln_ref[...] = total
    ag_last()
    for x in gl:
        x.wait_send()
    kp_copy.wait_send()
    for dr in range(2):
        for j in range(3):
            hop_kv(dr, j).wait_send()
            for s in range(2):
                hop(s, dr, j).wait_send()


def gradients(o, o_p, acc, dq, dq_p, hn, hn_p, dy, dy_p, dkv, wqf, wof, w_k, w_v, x, gain, cos_t, sin_t):
    nb, tok, e = x.shape
    n_tok = nb * tok
    d = dq.shape[-1]
    any_spec = pl.BlockSpec(memory_space=pl.ANY)
    vmem = pl.BlockSpec(memory_space=pltpu.VMEM)
    dma = pltpu.SemaphoreType.DMA
    tokens = jax.ShapeDtypeStruct((n_tok, e), BF16)
    y, gx, gln, gwo, gwq_t, gkv_t = pl.pallas_call(
        functools.partial(grads_body, nb, tok),
        in_specs=[any_spec] * 15 + [vmem, vmem, vmem],
        out_specs=[any_spec, any_spec, vmem, vmem, vmem, any_spec],
        out_shape=[tokens, tokens, jax.ShapeDtypeStruct((1, e), F32), jax.ShapeDtypeStruct((d, e), BF16),
                   jax.ShapeDtypeStruct((d, e), BF16), jax.ShapeDtypeStruct((2, d, e), F32)],
        scratch_shapes=[pltpu.VMEM((2, 4, 2, d, e // 2), F32), pltpu.VMEM((4, 2, d, e // 8), F32),
                        pltpu.VMEM((2, 2, 3, d, e // 2), F32), pltpu.VMEM((2, 3, d, e // 8), F32),
                        pltpu.VMEM((2, nb, tok, d), BF16), pltpu.VMEM((nb, tok, d), BF16), pltpu.VMEM((nb, tok, 2 * d), BF16),
                        pltpu.VMEM((d, e // 4), F32), pltpu.VMEM((8, e), F32), pltpu.VMEM((8, 1, e), F32),
                        dma((2, 2, 3)), dma((2, 2, 3)), dma((2, 3)), dma((2, 3)), dma((9,)), dma((9,)), dma((7,)), dma((7,)),
                        dma((2,)), dma((2, 2)), dma((2,)), dma((6,)), dma((4,))],
        compiler_params=pltpu.CompilerParams(collective_id=2, has_side_effects=True, vmem_limit_bytes=63 * 2**20),
        cost_estimate=pl.CostEstimate(flops=10 * n_tok * e * e, bytes_accessed=120 * 2**20, transcendentals=0),
        name="gradients",
    )(o, o_p, acc, dq, dq_p, hn, hn_p, dy.reshape(n_tok, e), dy_p, dkv, wqf, wof.reshape(8 * d, e), w_k, w_v, x.reshape(n_tok, e),
      gain, cos_t, sin_t)
    y, gx, gwq, gwk, gwv, gwo, gln = place(nb, y, gx, gwq_t, gkv_t, gwo, gln)
    return y.reshape(nb, tok, e), gx.reshape(nb, tok, e), gln.reshape(e), gwq, gwk, gwv, gwo


def place_body(steps, y_in, gx_in, gq_in, gkv_in, go_in, gl_in, y, gx, gq, gk, gv, go, gl,
               y_v, gx_v, gq_v, gkv_v, go_v, gl_v, gq_t, gk_t, gv_t, in_sem, y_sem, out_sem, t_sem):
    n, w = y_in.shape[0] // steps, gq_in.shape[1] // steps
    small_in = [pltpu.make_async_copy(s, v, in_sem.at[i]) for i, (s, v) in enumerate(((gkv_in, gkv_v), (gq_in, gq_v), (go_in, go_v), (gl_in, gl_v)))]
    small_out = [pltpu.make_async_copy(v, o, out_sem.at[i]) for i, (v, o) in enumerate(((go_v, go), (gl_v, gl)))]

    def rows(i, size):
        return pl.ds(i * size, size)
    moves = [(pltpu.make_async_copy(s.at[rows(i, n)], v.at[rows(i, n)], y_sem.at[0, j, i]),
              pltpu.make_async_copy(v.at[rows(i, n)], o.at[rows(i, n)], y_sem.at[1, j, i]))
             for i in range(steps) for j, (s, v, o) in enumerate(((y_in, y_v, y), (gx_in, gx_v, gx)))]
    for x in small_in:
        x.start()
    for x, _ in moves:
        x.start()
    small_in[0].wait()
    small_in[1].wait()
    turned = []
    for i in range(steps):
        for j, (v, o) in enumerate(((gk_t, gk), (gv_t, gv), (gq_t, gq))):
            t = (gkv_v[j, :, i * w:(i + 1) * w] if j < 2 else gq_v[:, i * w:(i + 1) * w].astype(F32)).T
            v[i * w:(i + 1) * w, :] = t.astype(v.dtype)
            c = pltpu.make_async_copy(v.at[rows(i, w)], o.at[rows(i, w)], t_sem.at[j, i])
            c.start()
            turned.append(c)
        for x, z in moves[2 * i:2 * i + 2]:
            x.wait()
            z.start()
    for x, z in zip(small_in[2:], small_out):
        x.wait()
        z.start()
    for c in turned + small_out + [z for _, z in moves]:
        c.wait()


def place(steps, y, gx, gwq_t, gkv_t, gwo, gln):
    e = y.shape[1]
    d = gwo.shape[0]
    any_spec = pl.BlockSpec(memory_space=pl.ANY)
    dma = pltpu.SemaphoreType.DMA
    vm = pltpu.VMEM
    return pl.pallas_call(
        functools.partial(place_body, steps),
        in_specs=[any_spec] * 6,
        out_specs=[any_spec] * 7,
        out_shape=[jax.ShapeDtypeStruct(y.shape, BF16), jax.ShapeDtypeStruct(y.shape, BF16), jax.ShapeDtypeStruct((e, d), BF16),
                   jax.ShapeDtypeStruct((e, d), F32), jax.ShapeDtypeStruct((e, d), F32), jax.ShapeDtypeStruct((d, e), BF16),
                   jax.ShapeDtypeStruct((1, e), F32)],
        scratch_shapes=[vm(y.shape, BF16), vm(y.shape, BF16), vm((d, e), BF16), vm((2, d, e), F32), vm((d, e), BF16), vm((1, e), F32),
                        vm((e, d), BF16), vm((e, d), F32), vm((e, d), F32),
                        dma((4,)), dma((2, 2, steps)), dma((2,)), dma((3, steps))],
        compiler_params=pltpu.CompilerParams(vmem_limit_bytes=63 * 2**20),
        cost_estimate=pl.CostEstimate(flops=0, bytes_accessed=8 * y.size + 24 * gwo.size, transcendentals=0),
        name="place",
    )(y, gx, gwq_t, gkv_t, gwo, gln)


def solution(mesh):
    act_spec = P('dp', 'tp', None)

    def device_step(x_loc, ln_scale, wq_loc, w_k, w_v, wo_loc, dy_loc):
        n_batch, tok, model_dim = x_loc.shape
        d = w_k.shape[1]
        t0 = lax.axis_index('tp') * tok
        cos_t, sin_t = rope_tables(t0 + jnp.arange(tok), d)

        gain = ln_scale
        kv0, hn, q, do, kv_loc, wq_h, wo_h, hn_p, dy_p = project(x_loc, gain, wq_loc, w_k, w_v, wo_loc, dy_loc, cos_t, sin_t)
        o, dq, dkv_loc, o_p, dq_p, acc = attention(q, do, kv_loc, kv0, dy_loc.reshape(-1, model_dim), dy_p, cos_t, sin_t)
        return gradients(o, o_p, acc, dq, dq_p, hn, hn_p, dy_loc, dy_p, dkv_loc, wq_h, wo_h, w_k, w_v, x_loc, gain, cos_t, sin_t)

    return jax.shard_map(device_step, mesh=mesh, in_specs=(act_spec, P(None), P(None, 'tp'), P(None, None), P(None, None), P('tp', None), act_spec), out_specs=(act_spec, act_spec, P('dp'), P('dp', 'tp'), P('dp', None), P('dp', None), P(('dp', 'tp'), None)), check_vma=False)
```

```python
import functools
import jax
import jax.numpy as jnp
from jax import lax
from jax.experimental import pallas as pl
from jax.experimental.pallas import tpu as pltpu
from jax.sharding import PartitionSpec as P

LN_EPS = 1e-6
ROPE_BASE = 10000.0
LOG2E = 1.4426950408889634
F32 = jnp.float32
BF16 = jnp.bfloat16


def rope_tables(positions, head_dim):
    half_dim = head_dim // 2
    inv_freq = ROPE_BASE ** (-2.0 * jnp.arange(half_dim, dtype=F32) / head_dim)
    angles = positions.astype(F32)[:, None] * inv_freq[None, :]
    return jnp.cos(angles), jnp.sin(angles)


def rotate(vectors, cos_t, sin_t):
    half_dim = vectors.shape[-1] // 2
    lo_half = vectors[..., :half_dim]
    hi_half = vectors[..., half_dim:]
    return jnp.concatenate([lo_half * cos_t - hi_half * sin_t, hi_half * cos_t + lo_half * sin_t], axis=-1)


def dot_nn(a, b):
    return lax.dot_general(a, b, (((1,), (0,)), ((), ())), preferred_element_type=F32)


def dot_nt(a, b):
    return lax.dot_general(a, b, (((1,), (1,)), ((), ())), preferred_element_type=F32)


def rdma(src, dst, send, recv, to):
    return pltpu.make_async_remote_copy(src_ref=src, dst_ref=dst, send_sem=send, recv_sem=recv,
                                        device_id={'tp': to}, device_id_type=pl.DeviceIdType.MESH)


def ring_ids():
    me = lax.axis_index('tp')
    k = lax.rem(me, 2)
    return me, k, me + 1 - 2 * k, lax.rem(me + 2, 8), lax.rem(me + 6, 8)


def enter(peers):
    barrier = pltpu.get_barrier_semaphore()
    for p in peers:
        pl.semaphore_signal(barrier, inc=1, device_id={'tp': p}, device_id_type=pl.DeviceIdType.MESH)
    pl.semaphore_wait(barrier, len(peers))


class Products:
    def __init__(self, big, a_v, at, ld_sem, b_sem):
        self.big, self.a_v, self.at, self.ld_sem, self.b_sem = big, a_v, at, ld_sem, b_sem
        self.nb, self.tok = a_v.shape[2], a_v.shape[3]
        self.eq = big.shape[2] // 4

    def load_b(self, own, other):
        return (pltpu.make_async_copy(own, self.big.at[0], self.b_sem.at[0]),
                pltpu.make_async_copy(other, self.big.at[1], self.b_sem.at[1]))

    def load_a(self, i, own, other):
        return (pltpu.make_async_copy(own, self.a_v.at[i % 2, 0], self.ld_sem.at[i % 2, 0]),
                pltpu.make_async_copy(other, self.a_v.at[i % 2, 1], self.ld_sem.at[i % 2, 1]))

    def turn(self, j, src):
        tok = self.tok
        for i in range(self.nb // 2):
            self.at[j, :, 2 * i * tok:(2 * i + 2) * tok] = jnp.concatenate([src[2 * i], src[2 * i + 1]], axis=0).T

    def both(self, cols):
        return dot_nn(self.at[0], self.big[0, :, cols]) + dot_nn(self.at[1], self.big[1, :, cols])

    def columns(self, dst, first, last, turned=0):
        eq = self.eq

        @pl.loop(first, last)
        def _(n):
            m = lax.rem(n + turned, 4)
            cols = pl.ds(pl.multiple_of(m * eq, 128), eq)
            dst[m // 2, :, pl.ds(pl.multiple_of(lax.rem(m, 2) * eq, 128), eq)] = self.both(cols)


class Gather:
    def __init__(self, ids, c, block, send, recv):
        self.me, _, self.mate, self.cw, self.ccw = ids
        self.c, self.block, self.send, self.recv = c, block, send, recv

    def copy(self, j, tag, to, src=None):
        ref = self.block(j)
        return rdma(ref if src is None else src, ref, self.send(tag), self.recv(tag), to)

    def own(self, src):
        @pl.when(self.c <= 2)
        def _():
            self.copy(self.me, 0, self.cw, src).start()

        @pl.when(self.c == 0)
        def _():
            self.copy(self.me, 2, self.ccw, src).start()
        self.copy(self.me, 3, self.mate, src).start()

    def arrived(self):
        @pl.when(self.c >= 1)
        def _():
            self.copy(self.me - 2, 0, self.cw).wait_recv()

        @pl.when(self.c == 3)
        def _():
            self.copy(self.me - 6, 2, self.ccw).wait_recv()

    def pass_on(self, src=lambda j: None):
        @pl.when(self.c >= 1)
        def _():
            @pl.when(self.c <= 2)
            def _():
                self.copy(self.me - 2, 1, self.cw, src(self.me - 2)).start()
            self.copy(self.me - 2, 4, self.mate, src(self.me - 2)).start()

        @pl.when(self.c == 3)
        def _():
            self.copy(self.me - 6, 6, self.mate, src(self.me - 6)).start()

    def forward(self):
        self.arrived()
        self.pass_on()

    def last(self):
        @pl.when(self.c >= 2)
        def _():
            self.copy(self.me - 4, 1, self.cw).wait_recv()
            self.copy(self.me - 4, 5, self.mate).start()

    def ready(self, tags=(3, 4, 5, 6)):
        if 3 in tags:
            self.copy(self.mate, 3, self.mate).wait_recv()
        for n, tag in ((1, 4), (2, 5), (3, 6)):
            if tag not in tags:
                continue

            @pl.when(self.c >= n)
            def _():
                self.copy(self.mate - 2 * n, tag, self.mate).wait_recv()

    def drain(self, tags=range(7)):
        c = self.c
        conds = (c <= 2, (c >= 1) & (c <= 2), c == 0, c >= 0, c >= 1, c >= 2, c == 3)
        for tag in tags:
            @pl.when(conds[tag])
            def _():
                self.copy(self.me, tag, self.mate).wait_send()


def attn_body(nb, tok, seq, d, q_hbm, do_hbm, kvl_hbm, kv0_hbm, dy_hbm, dyp_hbm, cos_ref, sin_ref,
              o_hbm, dq_hbm, dkv_hbm, op_hbm, dqp_hbm, acc_hbm,
              kv_all, o_v, dq_v, mrecv, rrecv, big,
              kv_send, kv_recv, m_send, m_recv, r_send, r_recv, own_sem, in_sem, out_sem, fin_sem, p_send, p_recv, first_sem,
              ld_sem, b_sem, acc_sem):
    scale = d ** -0.5
    rows = o_v.shape[2] * tok
    n_blk = seq // 256
    rb = 2 * rows // n_blk
    n_rb = rows // rb
    half = d // 2
    me, k, mate, cw, ccw = ring_ids()
    c = me // 2
    rel = [lax.rem(c + o, 4) for o in (3, 1, 2, 0)]

    def blk(j):
        return pl.ds(pl.multiple_of(j * tok, 16), tok)

    def kvb(b, j):
        return kv_all.at[b, blk(j)]

    def gather(b):
        return Gather((me, k, mate, cw, ccw), c, lambda j: kvb(b, j), lambda t: kv_send.at[b - 1, t], lambda t: kv_recv.at[b - 1, t])

    def own(b):
        gather(b).own(kvl_hbm.at[b])

    def own_copy(b):
        return pltpu.make_async_copy(kvl_hbm.at[b], kvb(b, me), own_sem.at[b])

    def ready(b):
        own_copy(b).wait()

        @pl.when(b == 1)
        def _():
            gather(1).ready((4, 5, 6))

        @pl.when(b > 1)
        def _():
            gather(b).ready()

    def drain(b):
        @pl.when(b == 1)
        def _():
            gather(1).drain((1, 4, 5, 6))

        @pl.when(b > 1)
        def _():
            gather(b).drain()

    def m_copy(b, n):
        return rdma(kvb(b, 2 * n + 1 - k), mrecv.at[lax.rem(b, 2), n], m_send.at[b, n], m_recv.at[b, n], mate)

    def r_copy(b, n, slot, to):
        return rdma(kvb(b, 2 * n + k), rrecv.at[b, slot], r_send.at[b, slot], r_recv.at[b, slot], to)

    def add_into(b, n, other):
        v = kv_all[b, blk(2 * n + k), :].astype(F32) + other[...].astype(F32)
        kv_all[b, blk(2 * n + k), :] = v.astype(BF16)

    def fin_copy(b):
        return pltpu.make_async_copy(kvb(b, me), dkv_hbm.at[b], fin_sem.at[b])

    def to_mate(b):
        for n in range(4):
            @pl.when(c >= n)
            def _():
                m_copy(b, n).start()

    def stage1(b):
        for n in range(4):
            @pl.when(c >= n)
            def _():
                m_copy(b, n).wait()
                add_into(b, n, mrecv.at[lax.rem(b, 2), n])

        @pl.when(c == 3)
        def _():
            r_copy(b, 1, 2, ccw).start()
            r_copy(b, 2, 1, ccw).start()
            r_copy(b, 0, 0, cw).start()
            fin_copy(b).start()

        @pl.when(c == 2)
        def _():
            r_copy(b, 0, 1, ccw).start()

    def stage2(b):
        @pl.when(c == 2)
        def _():
            r_copy(b, 1, 2, ccw).wait_recv()
            add_into(b, 1, rrecv.at[b, 2])
            r_copy(b, 1, 2, ccw).start()
            r_copy(b, 2, 1, ccw).wait_recv()
            add_into(b, 2, rrecv.at[b, 1])
            fin_copy(b).start()

        @pl.when(c == 1)
        def _():
            r_copy(b, 0, 1, ccw).wait_recv()
            add_into(b, 0, rrecv.at[b, 1])
            r_copy(b, 0, 1, ccw).start()

    def stage3(b):
        @pl.when(c == 0)
        def _():
            r_copy(b, 0, 0, cw).wait_recv()
            add_into(b, 0, rrecv.at[b, 0])
            r_copy(b, 0, 1, ccw).wait_recv()
            add_into(b, 0, rrecv.at[b, 1])
            fin_copy(b).start()

        @pl.when(c == 1)
        def _():
            r_copy(b, 1, 2, ccw).wait_recv()
            add_into(b, 1, rrecv.at[b, 2])
            fin_copy(b).start()

    def handed(dst, src, n, b, slot):
        return rdma(src.at[slot, 1 - k], dst.at[b], p_send.at[n, b], p_recv.at[n, b], mate)

    def store_o(b, slot):
        return (pltpu.make_async_copy(o_v.at[slot], o_hbm.at[b], out_sem.at[0, slot]), handed(op_hbm, o_v, 0, b, slot))

    def store_dq(b, slot):
        return (pltpu.make_async_copy(dq_v.at[slot], dq_hbm.at[b], out_sem.at[1, slot]), handed(dqp_hbm, dq_v, 1, b, slot))

    def stored(x):
        x[0].wait()
        x[1].wait_send()

    load_dy = (pltpu.make_async_copy(dy_hbm, big.at[0], b_sem.at[0]), pltpu.make_async_copy(dyp_hbm, big.at[1], b_sem.at[1]))

    def attend(q_v, do_v, s_buf, m_buf, l_buf, p_buf, ds_buf, q_t, do_t, dk_t, dv_t, d_buf, cos4, sin4):
        def load(b, slot):
            return (pltpu.make_async_copy(q_hbm.at[b], q_v.at[slot], in_sem.at[0, slot]),
                    pltpu.make_async_copy(do_hbm.at[b], do_v.at[slot], in_sem.at[1, slot]))

        def scores(b, g, slot, i):
            w = min(512, seq)
            if (i * 256) % w:
                return
            cols = slice(i * 256, i * 256 + w)
            s = dot_nt(q_v[slot, g].reshape(rows, d), kv_all[b, cols, :d]) * (scale * LOG2E)
            col = lax.broadcasted_iota(jnp.int32, (tok, w), 1) + i * 256
            row = lax.broadcasted_iota(jnp.int32, (tok, w), 0) + me * tok
            s = jnp.concatenate([jnp.where(col <= row, s[j * tok:(j + 1) * tok], -1e30) for j in range(rows // tok)], axis=0)
            s_buf[g, :, cols] = s
            m = s[:, :128]
            for j in range(128, w, 128):
                m = jnp.maximum(m, s[:, j:j + 128])
            m_buf[...] = m if i == 0 else jnp.maximum(m_buf[...], m)

        parts = max(1, min(5, n_blk))
        part = [j * (rows // 16) // parts * 16 for j in range(parts + 1)] + [rows] * n_blk

        def softmax(g, i):
            for r in range(part[i], part[i + 1], 16):
                rs = slice(r, r + 16)
                m = jnp.max(m_buf[rs, :], axis=1, keepdims=True)
                l = None
                for j in range(0, seq, 128):
                    e = jnp.exp2(s_buf[g, rs, j:j + 128] - m)
                    s_buf[g, rs, j:j + 128] = e
                    l = e if l is None else l + e
                l_buf[g, rs, :] = jnp.broadcast_to(1.0 / jnp.sum(l, axis=1, keepdims=True), (16, 128))

        def turn(g, slot, i):
            rs = slice(i * rb, (i + 1) * rb)
            q_t[g, :, rs] = q_v[slot, g].reshape(rows, d)[rs].T
            do_t[g, :, rs] = do_v[slot, g].reshape(rows, d)[rs].T

        def out_rows(b, g, slot, i):
            rs = slice(i * rb, (i + 1) * rb)
            p = (s_buf[g, rs, :] * jnp.concatenate([l_buf[g, rs, :]] * (seq // 128), axis=1)).astype(BF16)
            p_buf[rs, :] = p
            o = dot_nn(p, kv_all[b, :, d:])
            dvec = jnp.sum(o * do_v[slot, g].reshape(rows, d)[rs].astype(F32), axis=1, keepdims=True)
            d_buf[rs, :] = jnp.broadcast_to(dvec, (rb, 128))
            put_rows(o_v, slot, g, i, o.astype(BF16))

        def put_rows(ref, slot, g, i, v):
            r = i * rb
            while r < (i + 1) * rb:
                n = min((i + 1) * rb - r, tok - r % tok)
                ref[slot, g, r // tok, r % tok:r % tok + n, :] = v[r - i * rb:r - i * rb + n]
                r += n

        def dq_rows(b, g, slot, i):
            rs = slice(i * rb, (i + 1) * rb)
            dq = dot_nn(ds_buf[rs, :], kv_all[b, :, :d]) * scale
            lo, hi = dq[:, :half], dq[:, half:]
            cs, sn = cos4[rs, :], sin4[rs, :]
            put_rows(dq_v, slot, g, i, jnp.concatenate([(lo * cs + hi * sn).astype(BF16), (hi * cs - lo * sn).astype(BF16)], axis=1))

        def grads(b, g, slot, i):
            cols = slice(i * 256, (i + 1) * 256)
            do = do_v[slot, g].reshape(rows, d)
            p = p_buf[:, cols]
            dp = dot_nt(do, kv_all[b, cols, d:])
            dvec = d_buf[...]
            if i > 0 and part[i] > part[i - 1]:
                z = None
                for r in range(part[i - 1], part[i], 8):
                    v = l_buf[1 - g, r:r + 8, :]
                    z = v if z is None else jnp.minimum(z, v)
                dvec = dvec + jnp.concatenate([jnp.minimum(z, 0.0)] * (rows // 8), axis=0)
            dd = jnp.concatenate([dvec, dvec], axis=1)
            ds = (p.astype(F32) * (dp - dd)).astype(BF16)
            ds_buf[:, cols] = ds
            dk = dot_nn(q_t[g], ds)
            dv = dot_nn(do_t[g], p)
            if g == 0:
                dk_t[:, cols] = dk
                dv_t[:, cols] = dv
            else:
                dk_t[:, cols] += dk
                dv_t[:, cols] += dv

        def close_kv(b, i):
            cols = slice(i * 256, (i + 1) * 256)
            kv_all[b, cols, :d] = (dk_t[:, cols] * scale).T.astype(BF16)
            kv_all[b, cols, d:] = dv_t[:, cols].T.astype(BF16)

        enter((mate, cw, ccw))
        gather(1).pass_on(lambda j: kv0_hbm.at[1, blk(j)])
        if nb > 2:
            own(2)
        for x in load(0, 0):
            x.start()

        def first(j):
            return pltpu.make_async_copy(kv0_hbm.at[0, blk(j)], kvb(0, j), first_sem.at[j])

        def second(j, n):
            return pltpu.make_async_copy(kv0_hbm.at[1, blk(j)], kvb(1, j), first_sem.at[8 + n])
        arrived = ((c >= 0, mate, 0), (c >= 1, me - 2, 1), (c == 3, me - 6, 2))
        for j in range(8):
            @pl.when(j <= 2 * c + 1)
            def _():
                first(j).start()
        for b in range(1, nb):
            own_copy(b).start()
        for cond, j, i in arrived:
            @pl.when(cond)
            def _():
                second(j, i).start()

        @pl.loop(2 * c + 2, 8)
        def _(j):
            for b in range(nb):
                kv_all[b, blk(j), :] = jnp.zeros((tok, 2 * d), BF16)
        for j in range(rows // tok):
            cos4[j * tok:(j + 1) * tok, :] = cos_ref[...]
            sin4[j * tok:(j + 1) * tok, :] = sin_ref[...]
        ds_buf[...] = jnp.zeros_like(ds_buf)
        for x in load(0, 0):
            x.wait()
        for i in range(n_rb):
            turn(0, 0, i)
        for j in range(8):
            @pl.when(j <= 2 * c + 1)
            def _():
                first(j).wait()
        for cond, j, i in arrived:
            @pl.when(cond)
            def _():
                second(j, i).wait()
        for i in range(n_blk):
            scores(0, 0, 0, i)
        for i in range(n_blk):
            softmax(0, i)

        def comm_steps(b, steps):
            for lag, stage in steps:
                @pl.when(b >= lag)
                def _():
                    stage(b - lag)

        @pl.loop(0, nb)
        def _(b):
            slot = lax.rem(b, 2)
            nxt = jnp.minimum(b + 1, nb - 1)
            prev = jnp.maximum(b - 1, 0)

            @pl.when(b + 1 < nb)
            def _():
                for x in load(b + 1, 1 - slot):
                    x.start()

            @pl.when(b + 3 < nb)
            def _():
                own(b + 3)

            @pl.when((b >= 1) & (b + 2 < nb))
            def _():
                gather(b + 2).forward()

            @pl.when(b == 1)
            def _():
                for x in load_dy:
                    x.start()
            comm_steps(b, ((3, stage2), (4, stage3)))

            @pl.when(b >= 2)
            def _():
                drain(b - 1)

            @pl.when(b >= 2)
            def _():
                stored(store_o(b - 2, slot))
            spare = jnp.where(b >= 1, b - 1, nb)
            for i in range(n_blk):
                scores(b, 1, slot, i)
                if i % 2 == 1:
                    out_rows(b, 0, slot, i // 2)
                    dq_rows(prev, 1, 1 - slot, i // 2)
                    turn(1, slot, i // 2)
            for i in range(n_blk):
                close_kv(spare, i)

            @pl.when(b + 1 < nb)
            def _():
                gather(b + 1).last()

            @pl.when(b >= 1)
            def _():
                for x in store_dq(b - 1, 1 - slot):
                    x.start()
                to_mate(b - 1)

            for i in range(n_blk):
                grads(b, 0, slot, i)
                softmax(1, i)

            @pl.when(b + 1 < nb)
            def _():
                for x in load(b + 1, 1 - slot):
                    x.wait()
                ready(b + 1)
            if nb > 2:
                @pl.when(b == 0)
                def _():
                    gather(2).forward()

            @pl.when(b >= 2)
            def _():
                stored(store_dq(b - 2, slot))
            nslot = lax.rem(nxt, 2)
            for i in range(n_blk):
                scores(nxt, 0, nslot, i)
                if i % 2 == 1:
                    out_rows(b, 1, slot, i // 2)
                    dq_rows(b, 0, slot, i // 2)
                    turn(0, nslot, i // 2)
            for x in store_o(b, slot):
                x.start()
            comm_steps(b, ((1, stage1),))
            for i in range(n_blk):
                grads(b, 1, slot, i)
                softmax(0, i)

        drain(nb - 1)
        for i in range(n_rb):
            dq_rows(nb - 1, 1, (nb - 1) % 2, i)
        for i in range(n_blk):
            close_kv(nb - 1, i)
        to_mate(nb - 1)
        for x in store_dq(nb - 1, (nb - 1) % 2):
            x.start()

    slab = pltpu.VMEM((2, 2, rows // tok, tok, d), BF16)
    pl.run_scoped(attend, slab, slab, pltpu.VMEM((2, rows, seq), F32), pltpu.VMEM((rows, 128), F32), pltpu.VMEM((2, rows, 128), F32),
                  pltpu.VMEM((rows, seq), BF16), pltpu.VMEM((rows, seq), BF16), pltpu.VMEM((2, d, rows), BF16),
                  pltpu.VMEM((2, d, rows), BF16), pltpu.VMEM((d, seq), F32), pltpu.VMEM((d, seq), F32),
                  pltpu.VMEM((rows, 128), F32), pltpu.VMEM((rows, half), F32), pltpu.VMEM((rows, half), F32))
    n = nb

    def first_products(a_v, at, acc_v):
        pr = Products(big, a_v, at, ld_sem, b_sem)
        for b in (n - 2, n - 1):
            stored(store_o(b, b % 2))
        for b in range(n):
            handed(op_hbm, o_v, 0, b, b % 2).wait_recv()

        def fetch(r):
            return pr.load_a(r, o_hbm.at[:, k, rel[r]], op_hbm.at[:, rel[r]])

        def save(r):
            return pltpu.make_async_copy(acc_v.at[r], acc_hbm.at[r], acc_sem.at[r])
        for r in range(2):
            for x in fetch(r):
                x.start()

        todo = [((stage2, n - 3), (stage3, n - 4)), ((stage1, n - 1), (stage2, n - 2), (stage3, n - 3)),
                ((stage2, n - 1), (stage3, n - 2)), ((stage3, n - 1),)]

        def steps(i):
            for stage, b in todo[i]:
                if b >= 0:
                    stage(b)
        steps(0)
        steps(1)
        for r in range(2):
            for x in fetch(r):
                x.wait()
            pr.turn(0, a_v.at[r, 0])
            pr.turn(1, a_v.at[r, 1])
            if r == 0:
                for x in load_dy:
                    x.wait()
            pr.columns(acc_v.at[r], 0, 4)
            save(r).start()
        steps(2)
        steps(3)
        for r in range(2):
            save(r).wait()

    pl.run_scoped(first_products, pltpu.VMEM((2, 2, nb, tok, d), BF16),
                  pltpu.VMEM((2, d, nb * tok), BF16), pltpu.VMEM((2, 2, d, dy_hbm.shape[1] // 2), F32))
    for b in (n - 2, n - 1):
        stored(store_dq(b, b % 2))
    for b in range(n):
        handed(dqp_hbm, dq_v, 1, b, b % 2).wait_recv()
        fin_copy(b).wait()
        for cond, slot in ((c == 3, 0), (c >= 1, 1), (c >= 2, 2)):
            @pl.when(cond)
            def _():
                r_copy(b, 0, slot, cw).wait_send()


def attention(q, do, kv, kv0, dy, dy_p, cos_t, sin_t):
    nb, _, hp, tok, d = q.shape
    seq = tok * 8
    rows = hp * tok
    any_spec = pl.BlockSpec(memory_space=pl.ANY)
    vmem = pl.BlockSpec(memory_space=pltpu.VMEM)
    dma = pltpu.SemaphoreType.DMA
    slab = pltpu.VMEM((2, 2, hp, tok, d), BF16)
    out = jax.ShapeDtypeStruct(q.shape, BF16)
    outp = jax.ShapeDtypeStruct((nb, hp, tok, d), BF16)
    return pl.pallas_call(
        functools.partial(attn_body, nb, tok, seq, d),
        in_specs=[any_spec] * 6 + [vmem, vmem],
        out_specs=[any_spec] * 6,
        out_shape=[out, out, jax.ShapeDtypeStruct(kv.shape, BF16), outp, outp,
                   jax.ShapeDtypeStruct((2, 2, d, dy.shape[1] // 2), F32)],
        scratch_shapes=[pltpu.VMEM((nb + 1, seq, 2 * d), BF16), slab, slab,
                        pltpu.VMEM((2, 4, tok, 2 * d), BF16), pltpu.VMEM((nb, 3, tok, 2 * d), BF16),
                        pltpu.VMEM((2,) + dy.shape, BF16),
                        dma((nb - 1, 7)), dma((nb - 1, 7)), dma((nb, 4)), dma((nb, 4)), dma((nb, 3)), dma((nb, 3)),
                        dma((nb,)), dma((2, 2)), dma((2, 2)), dma((nb,)), dma((2, nb)), dma((2, nb)), dma((11,)),
                        dma((2, 2)), dma((2,)), dma((4,))],
        compiler_params=pltpu.CompilerParams(collective_id=1, has_side_effects=True, vmem_limit_bytes=63 * 2**20),
        cost_estimate=pl.CostEstimate(flops=24 * nb * rows * seq * d, bytes_accessed=40 * 2**20,
                                      transcendentals=2 * nb * rows * seq),
        name="attention",
    )(q, do, kv, kv0, dy, dy_p, cos_t, sin_t)


def proj_body(nb, tok, x_hbm, g_ref, wq_hbm, wk_ref, wv_ref, wo_hbm, dy_hbm, cos_ref, sin_ref,
              kv0_hbm, hn_hbm, q_hbm, do_hbm, kv_hbm, wqf_hbm, wof_hbm, hnp_hbm, dyp_hbm,
              x_v, hn_v, dy_v, wq_v, wo_v, kv_v, out_v,
              send, recv, x_sem, dy_sem, own_sem, out_sem, misc_sem, w_sem, p_send, p_recv, kv_send, kv_recv):
    n_tok, e = x_hbm.shape
    d = kv_v.shape[1] // 2
    half = d // 2
    mc = 2 * tok
    me, k, mate, cw, ccw = ring_ids()
    base = 2 * (me // 2)

    def head(off, par):
        return lax.rem(base + 2 * off + 8, 8) + par
    enter((mate, cw, ccw))

    fulls = (wq_v, wo_v)
    locs = (wq_hbm, wo_hbm)

    def half_of(w, ref, j):
        n = ref.shape[0] // 2
        return ref.at[pl.ds(j * n, n)]

    sends = []

    def send_full(w, h, j, to, own=False):
        src = locs[w] if own else fulls[w].at[h]
        c = rdma(src, fulls[w].at[h], send.at[w, j], recv.at[w, j], to)
        c.start()
        sends.append(c)

    def send_half(w, h, part, j, to):
        c = rdma(half_of(w, fulls[w].at[h], part), half_of(w, fulls[w].at[h], part), send.at[w, j], recv.at[w, j], to)
        c.start()
        sends.append(c)

    def wait_full(w, h, j):
        rdma(fulls[w].at[h], fulls[w].at[h], send.at[w, j], recv.at[w, j], mate).wait_recv()

    def wait_half(w, h, part, j):
        ref = half_of(w, fulls[w].at[h], part)
        rdma(ref, ref, send.at[w, j], recv.at[w, j], mate).wait_recv()

    for w in range(2):
        send_full(w, me, 0, cw, True)
        send_full(w, me, 1, ccw, True)
        send_full(w, me, 4, mate, True)
    own = [pltpu.make_async_copy(locs[w], fulls[w].at[me], own_sem.at[w]) for w in range(2)]
    xs = [pltpu.make_async_copy(x_hbm.at[pl.ds(b * tok, tok)], x_v.at[pl.ds(b * tok, tok)], x_sem.at[b]) for b in range(nb)]
    for c in xs:
        c.start()
    for c in own:
        c.start()
    dyc = pltpu.make_async_copy(dy_hbm, dy_v, dy_sem)
    dyc.start()

    gain = g_ref[...].astype(F32).reshape(1, e)
    for b in range(nb):
        xs[b].wait()

        @pl.loop(0, tok // 16, unroll=2)
        def _(r):
            rs = pl.ds(pl.multiple_of(b * tok + r * 16, 16), 16)
            x = x_v[rs, :].astype(F32)
            c = x - jnp.mean(x, axis=1, keepdims=True)
            inv = lax.rsqrt(jnp.mean(c * c, axis=1, keepdims=True) + LN_EPS)
            hn_v[rs, :] = (c * inv * gain).astype(BF16)
    hn_out = pltpu.make_async_copy(hn_v, hn_hbm, misc_sem.at[0])
    hn_out.start()
    to_mate = [rdma(hn_v, hnp_hbm, p_send.at[0], p_recv.at[0], mate), rdma(dy_hbm, dyp_hbm, p_send.at[1], p_recv.at[1], mate)]
    for c in to_mate:
        c.start()

    def rope_rows(raw):
        lo, hi = raw[:, :half], raw[:, half:d]
        cs, sn = jnp.concatenate([cos_ref[...]] * 2, axis=0), jnp.concatenate([sin_ref[...]] * 2, axis=0)
        return lo * cs - hi * sn, hi * cs + lo * sn

    @pl.loop(0, n_tok // mc)
    def _(i):
        rs = pl.ds(pl.multiple_of(i * mc, mc), mc)
        lo, hi = rope_rows(dot_nn(hn_v[rs, :], wk_ref[...]))
        kv_v[rs, :half] = lo.astype(BF16)
        kv_v[rs, half:d] = hi.astype(BF16)
        kv_v[rs, d:] = dot_nn(hn_v[rs, :], wv_ref[...]).astype(BF16)
    kv_out = pltpu.make_async_copy(kv_v, kv_hbm, misc_sem.at[1])
    kv_out.start()

    outs = []
    saves = []

    def save(w, h):
        c = pltpu.make_async_copy(fulls[w].at[h], (wqf_hbm, wof_hbm)[w].at[h], w_sem.at[len(saves)])
        c.start()
        saves.append(c)

    def project(w, h):
        slot = len(outs) % 4
        if len(outs) >= 4:
            outs[-4].wait()

        @pl.loop(0, n_tok // mc)
        def _(i):
            rs = pl.ds(pl.multiple_of(i * mc, mc), mc)
            if w == 0:
                lo, hi = rope_rows(dot_nn(hn_v[rs, :], wq_v[h]))
                o0 = lo.reshape(2, tok, half).astype(BF16)
                o1 = hi.reshape(2, tok, half).astype(BF16)
                out_v[slot, pl.ds(2 * i, 2), :, :half] = o0
                out_v[slot, pl.ds(2 * i, 2), :, half:] = o1
            else:
                out_v[slot, pl.ds(2 * i, 2)] = dot_nt(dy_v[rs, :], wo_v[h]).reshape(2, tok, d).astype(BF16)
        c = pltpu.make_async_copy(out_v.at[slot], (q_hbm, do_hbm)[w].at[:, lax.rem(h, 2), h // 2], out_sem.at[slot])
        c.start()
        outs.append(c)
        save(w, h)

    other = 1 - k
    for w in range(2):
        own[w].wait()
        if w == 1:
            dyc.wait()
        project(w, me)
        wait_full(w, mate, 4)
        project(w, mate)
    for w in range(2):
        wait_full(w, head(-1, k), 0)
        send_half(w, head(-1, k), 0, 2, cw)
        wait_full(w, head(1, k), 1)
        send_half(w, head(1, k), 1, 3, ccw)
        send_full(w, head(-1, k), 5, mate)
        send_full(w, head(1, k), 6, mate)
        project(w, head(-1, k))
        project(w, head(1, k))
        wait_full(w, head(-1, other), 5)
        project(w, head(-1, other))
        wait_full(w, head(1, other), 6)
        project(w, head(1, other))

    def early(n):
        def blk(j):
            return kv0_hbm.at[n, pl.ds(pl.multiple_of(j * tok, 16), tok)]
        return Gather((me, k, mate, cw, ccw), me // 2, blk, lambda t: kv_send.at[n, t], lambda t: kv_recv.at[n, t])
    first, second = early(0), early(1)
    first.own(kv_v.at[pl.ds(0, tok)])
    own0 = pltpu.make_async_copy(kv_v.at[pl.ds(0, tok)], first.block(me), misc_sem.at[2])
    own0.start()
    for w in range(2):
        wait_half(w, head(2, k), 0, 2)
        send_half(w, head(2, k), 0, 7, mate)
        wait_half(w, head(2, k), 1, 3)
        send_half(w, head(2, k), 1, 8, mate)
        project(w, head(2, k))
        if w == 1:
            first.forward()
            second.own(kv_v.at[pl.ds(tok, tok)])
        wait_half(w, head(2, other), 0, 7)
        wait_half(w, head(2, other), 1, 8)
        project(w, head(2, other))
    first.last()
    for c in outs[-4:] + saves + [hn_out, kv_out, own0]:
        c.wait()
    first.ready()
    first.drain()
    second.arrived()
    second.ready((3,))
    second.drain((0, 2, 3))
    for c in sends:
        c.wait_send()
    for c in to_mate:
        c.wait()


def project(x, gain, wq, w_k, w_v, wo, dy, cos_t, sin_t):
    nb, tok, e = x.shape
    d = wq.shape[1]
    n_heads = 8
    n_tok = nb * tok
    any_spec = pl.BlockSpec(memory_space=pl.ANY)
    vmem = pl.BlockSpec(memory_space=pltpu.VMEM)
    act = jax.ShapeDtypeStruct((nb, 2, n_heads // 2, tok, d), BF16)
    dma = pltpu.SemaphoreType.DMA
    flops = 2 * n_tok * e * (2 * n_heads + 2) * d
    kv0, hn, q, do, kv, wqf, wof, hn_p, dy_p = pl.pallas_call(
        functools.partial(proj_body, nb, tok),
        in_specs=[any_spec, vmem, any_spec, vmem, vmem, any_spec, any_spec, vmem, vmem],
        out_specs=[any_spec] * 9,
        out_shape=[jax.ShapeDtypeStruct((2, tok * n_heads, 2 * d), BF16), jax.ShapeDtypeStruct((n_tok, e), BF16), act, act, jax.ShapeDtypeStruct((n_tok, 2 * d), BF16),
                   jax.ShapeDtypeStruct((n_heads, e, d), BF16), jax.ShapeDtypeStruct((n_heads, d, e), BF16),
                   jax.ShapeDtypeStruct((n_tok, e), BF16), jax.ShapeDtypeStruct((n_tok, e), BF16)],
        scratch_shapes=[pltpu.VMEM((n_tok, e), BF16), pltpu.VMEM((n_tok, e), BF16), pltpu.VMEM((n_tok, e), BF16),
                        pltpu.VMEM((n_heads, e, d), BF16), pltpu.VMEM((n_heads, d, e), BF16),
                        pltpu.VMEM((n_tok, 2 * d), BF16), pltpu.VMEM((4, nb, tok, d), BF16),
                        dma((2, 9)), dma((2, 9)), dma((nb,)), dma(()), dma((2,)), dma((4,)), dma((3,)), dma((16,)), dma((2,)), dma((2,)), dma((2, 7)), dma((2, 7))],
        compiler_params=pltpu.CompilerParams(collective_id=0, has_side_effects=True, vmem_limit_bytes=60 * 2**20),
        cost_estimate=pl.CostEstimate(flops=flops, bytes_accessed=60 * 2**20, transcendentals=0),
        name="project",
    )(x.reshape(n_tok, e), gain, wq, w_k, w_v, wo, dy.reshape(n_tok, e), cos_t, sin_t)
    return kv0, hn, q, do, kv.reshape(nb, tok, 2 * d), wqf, wof, hn_p, dy_p


def grads_body(nb, tok, o_hbm, op_hbm, acc_hbm, dq_hbm, dqp_hbm, hn_hbm, hnp_hbm, dy_hbm, dyp_hbm, dkv_hbm,
               wq_hbm, wo_hbm, wk_hbm, wv_hbm, x_hbm, g_ref, cos_ref, sin_ref,
               y_hbm, gx_hbm, gln_ref, gwo_ref, gwq_ref, gkv_hbm,
               acc, acc_kv, rbuf, rbuf_kv, kind, kp, dkv_v, fin_kv, gln_acc, gl_recv,
               rs_send, rs_recv, kv_send, kv_recv, ag_send, ag_recv, gl_send, gl_rsem, kp_sem, ld_sem, b_sem, t_sem, a_sem):
    n_tok, e = x_hbm.shape
    d = wk_hbm.shape[1]
    half = d // 2
    eh, eq = e // 2, e // 4
    me, k, mate, cw, ccw = ring_ids()
    c = me // 2
    rel = [lax.rem(c + o, 4) for o in (3, 1, 2, 0)]
    enter([lax.rem(me + o, 8) for o in range(1, 8)])

    order = ((2, 1), (2, 0))

    def hop(s, dr, j):
        first = acc_hbm.at[dr, dr] if s == 0 else acc.at[s, dr, dr]
        src = first if j == 0 else rbuf.at[s, dr, j - 1]
        return rdma(src, rbuf.at[s, dr, j], rs_send.at[s, dr, j], rs_recv.at[s, dr, j], (cw, ccw)[dr])

    def hop_kv(dr, j):
        src = acc_kv.at[dr, dr] if j == 0 else rbuf_kv.at[dr, j - 1]
        return rdma(src, rbuf_kv.at[dr, j], kv_send.at[dr, j], kv_recv.at[dr, j], (cw, ccw)[dr])

    def add(dst, term):
        @pl.loop(0, dst.shape[0] // 32)
        def _(i):
            rs = pl.ds(pl.multiple_of(i * 32, 32), 32)
            dst[rs, :] = dst[rs, :] + term[rs, :]

    def pass_on(s, j):
        for dr in range(2):
            hop(s, dr, j - 1).wait_recv()
            add(rbuf.at[s, dr, j - 1], acc.at[s, order[dr][j - 1], dr])
            hop(s, dr, j).start()

    def pass_on_kv(j):
        for dr in range(2):
            hop_kv(dr, j - 1).wait_recv()
            add(rbuf_kv.at[dr, j - 1], acc_kv.at[order[dr][j - 1], dr])
            hop_kv(dr, j).start()

    def finish(s, out):
        for dr in range(2):
            hop(s, dr, 2).wait_recv()

            @pl.loop(0, d // 32)
            def _(i):
                rs = pl.ds(pl.multiple_of(i * 32, 32), 32)
                out[rs, dr * eh:(dr + 1) * eh] = (rbuf[s, dr, 2, rs, :] + acc[s, 3, dr, rs, :]).astype(BF16)

    def piece(kk, j, lo=0, n=None):
        return gkv_hbm.at[kk, pl.ds(lo, d if n is None else n), pl.ds(pl.multiple_of(j * eq, 128), eq)]

    def ag(tag, ref, to, src=None):
        return rdma(ref if src is None else src, ref, ag_send.at[tag], ag_recv.at[tag], to)

    def ag_far(tag, to):
        return ag(tag, piece(k, rel[(0, 1)[tag - 3]], (tag - 3) * half, half), to)

    own_piece = pltpu.make_async_copy(fin_kv, piece(k, c), t_sem.at[5])

    def finish_kv():
        for dr in range(2):
            hop_kv(dr, 2).wait_recv()
            fin_kv[:, dr * (eq // 2):(dr + 1) * (eq // 2)] = rbuf_kv[dr, 2] + acc_kv[3, dr]
        ag(0, piece(k, c), cw, fin_kv).start()
        ag(1, piece(k, c), ccw, fin_kv).start()
        ag(2, piece(k, c), mate, fin_kv).start()
        own_piece.start()

    def ag_forward():
        ag(0, piece(k, rel[0]), cw).wait_recv()
        ag_far(3, cw).start()
        ag(1, piece(k, rel[1]), cw).wait_recv()
        ag_far(4, ccw).start()
        ag(5, piece(k, rel[0]), mate).start()
        ag(6, piece(k, rel[1]), mate).start()

    def ag_last():
        far = [piece(k, rel[2], i * half, half) for i in range(2)]
        for i in range(2):
            ag(3 + i, far[i], cw).wait_recv()
            ag(7 + i, far[i], mate).start()
        ag(2, piece(1 - k, c), mate).wait_recv()
        ag(5, piece(1 - k, rel[0]), mate).wait_recv()
        ag(6, piece(1 - k, rel[1]), mate).wait_recv()
        for i in range(2):
            ag(7 + i, piece(1 - k, rel[2], i * half, half), mate).wait_recv()
        for tag in range(3):
            ag(tag, piece(k, c), cw, fin_kv).wait_send()
        for tag in (3, 4, 7, 8):
            ag(tag, far[0], cw).wait_send()
        for tag in (5, 6):
            ag(tag, piece(k, c), cw).wait_send()
        own_piece.wait()

    dkv_in = pltpu.make_async_copy(dkv_hbm, dkv_v, t_sem.at[4])
    dkv_in.start()
    kp_copy = rdma(kind.at[1 - k], kp, kp_sem.at[0], kp_sem.at[1], mate)

    for dr in range(2):
        hop(0, dr, 0).start()
    acc_in = [pltpu.make_async_copy(acc_hbm.at[r], acc.at[0, r], a_sem.at[r]) for r in range(2)]
    for x in acc_in:
        x.start()

    def products(big, a_v, at):
        pr = Products(big, a_v, at, ld_sem, b_sem)
        dy_in = pr.load_b(dy_hbm, dyp_hbm)
        hn_in = pr.load_b(hn_hbm, hnp_hbm)
        jobs = [(0, 2), (0, 3)] + [(1, r) for r in range(4)]

        def fetch(i):
            s, r = jobs[i]
            return pr.load_a(i, (o_hbm, dq_hbm)[s].at[:, k, rel[r]], (op_hbm, dqp_hbm)[s].at[:, rel[r]])
        for x in dy_in:
            x.start()
        for i in range(2):
            for x in fetch(i):
                x.start()
        dkv_in.wait()
        for b in range(nb):
            lo, hi = dkv_v[b, :, :half].astype(F32), dkv_v[b, :, half:d].astype(F32)
            cs, sn = cos_ref[...], sin_ref[...]
            kind[0, b, :, :half] = (lo * cs + hi * sn).astype(BF16)
            kind[0, b, :, half:] = (hi * cs - lo * sn).astype(BF16)
            kind[1, b] = dkv_v[b, :, d:]
        kp_copy.start()
        for i, (s, r) in enumerate(jobs):
            if i == 2:
                pr.turn(0, kind.at[k])
                kp_copy.wait_recv()
                pr.turn(1, kp)
                for x in hn_in:
                    x.wait()
                for q in range(4):
                    for dr in range(2):
                        acc_kv[q, dr] = pr.both(pl.ds(pl.multiple_of(rel[q] * eq + dr * (eq // 2), 128), eq // 2))
                for dr in range(2):
                    hop_kv(dr, 0).start()
            for x in fetch(i):
                x.wait()
            pr.turn(0, a_v.at[i % 2, 0])
            pr.turn(1, a_v.at[i % 2, 1])
            if i + 2 < len(jobs):
                for x in fetch(i + 2):
                    x.start()
            if i == 0:
                for x in dy_in:
                    x.wait()
            if s == 1 and r < 2:
                pr.columns(acc.at[s, r], 0, 2, 2 * r)
                hop(s, r, 0).start()
                pr.columns(acc.at[s, r], 2, 4, 2 * r)
            else:
                pr.columns(acc.at[s, r], 0, 4)
            if i == 1:
                for x in hn_in:
                    x.start()

    pl.run_scoped(products, pltpu.VMEM((2, n_tok, e), BF16), pltpu.VMEM((2, 2, nb, tok, d), BF16), pltpu.VMEM((2, d, n_tok), BF16))
    for x in acc_in:
        x.wait()
    pass_on(0, 1)
    pass_on_kv(1)

    mc = 2 * tok
    units = nb // 2

    def attn_out(wo_v, o_v, x_v, y_v):
        w_in = pltpu.make_async_copy(wo_hbm, wo_v, b_sem.at[0])
        w_in.start()

        def load(u):
            return (pltpu.make_async_copy(o_hbm.at[pl.ds(2 * u, 2)], o_v.at[u % 2], ld_sem.at[u % 2, 0]),
                    pltpu.make_async_copy(x_hbm.at[pl.ds(u * mc, mc)], x_v.at[u % 2], ld_sem.at[u % 2, 1]))

        def put(u):
            return pltpu.make_async_copy(y_v.at[u % 2], y_hbm.at[pl.ds(u * mc, mc)], t_sem.at[u % 2])
        for x in load(0):
            x.start()
        w_in.wait()
        for u in range(units):
            if u + 1 < units:
                for x in load(u + 1):
                    x.start()
            for x in load(u):
                x.wait()
            if u >= 2:
                put(u - 2).wait()
            sl = u % 2

            @pl.loop(0, 4)
            def _(n):
                cols = pl.ds(pl.multiple_of(n * eq, 128), eq)
                o_rows = jnp.concatenate([jnp.concatenate([o_v[sl, i, h % 2, h // 2] for h in range(8)], axis=1) for i in range(2)], axis=0)
                r = dot_nn(o_rows, wo_v[:, cols])
                y_v[sl, :, cols] = (x_v[sl, :, cols].astype(F32) + r).astype(BF16)
            put(u).start()
        for u in range(max(0, units - 2), units):
            put(u).wait()

    pl.run_scoped(attn_out, pltpu.VMEM((8 * d, e), BF16), pltpu.VMEM((2, 2, 2, 4, tok, d), BF16),
                  pltpu.VMEM((2, mc, e), BF16), pltpu.VMEM((2, mc, e), BF16))
    pass_on(1, 1)

    def hidden_grad(wq_v, wk_v, wv_v, dq_v, x_v, dy_v, dh, gx_v):
        w_in = pltpu.make_async_copy(wq_hbm, wq_v, b_sem.at[0])
        w_in.start()
        w2_in = (pltpu.make_async_copy(wk_hbm, wk_v, b_sem.at[1]), pltpu.make_async_copy(wv_hbm, wv_v, ld_sem.at[1, 1]))
        for x in w2_in:
            x.start()

        def load(u):
            return (pltpu.make_async_copy(dq_hbm.at[pl.ds(2 * u, 2)], dq_v, ld_sem.at[0, 0]),
                    pltpu.make_async_copy(x_hbm.at[pl.ds(u * mc, mc)], x_v, ld_sem.at[0, 1]),
                    pltpu.make_async_copy(dy_hbm.at[pl.ds(u * mc, mc)], dy_v, ld_sem.at[1, 0]))

        def put(u):
            return pltpu.make_async_copy(gx_v, gx_hbm.at[pl.ds(u * mc, mc)], t_sem.at[0])
        gain = g_ref[...].astype(F32).reshape(1, e)
        gln_acc[...] = jnp.zeros_like(gln_acc)
        for x in load(0):
            x.start()
        w_in.wait()
        for x in w2_in:
            x.wait()
        for u in range(units):
            for x in load(u):
                x.wait()

            @pl.loop(0, 4)
            def _(n):
                rows = pl.ds(pl.multiple_of(n * eq, 128), eq)
                t = None
                for h in range(8):
                    a = jnp.concatenate([dq_v[i, h % 2, h // 2] for i in range(2)], axis=0)
                    p = dot_nt(a, wq_v[h, rows, :])
                    t = p if t is None else t + p
                for j in range(2):
                    a = jnp.concatenate([kind[j, 2 * u + i] for i in range(2)], axis=0)
                    t = t + dot_nt(a, (wk_v, wv_v)[j][rows, :])
                dh[:, rows] = t
            if u >= 1:
                put(u - 1).wait()

            @pl.loop(0, mc // 16)
            def _(r):
                rs = pl.ds(pl.multiple_of(r * 16, 16), 16)
                x = x_v[rs, :].astype(F32)
                cx = x - jnp.mean(x, axis=1, keepdims=True)
                inv = lax.rsqrt(jnp.mean(cx * cx, axis=1, keepdims=True) + LN_EPS)
                xh = cx * inv
                g = dh[rs, :]
                pr = g * xh
                gln_acc[...] += pr[:8] + pr[8:]
                gh = g * gain
                m1 = jnp.mean(gh, axis=1, keepdims=True)
                m2 = jnp.mean(gh * xh, axis=1, keepdims=True)
                gx_v[rs, :] = (inv * (gh - m1 - xh * m2) + dy_v[rs, :].astype(F32)).astype(BF16)
            put(u).start()
            if u + 1 < units:
                for x in load(u + 1):
                    x.start()
            if u == units // 2 - 1:
                pass_on_kv(2)
                pass_on(0, 2)
        put(units - 1).wait()

    pl.run_scoped(hidden_grad, pltpu.VMEM((8, e, d), BF16), pltpu.VMEM((e, d), BF16), pltpu.VMEM((e, d), BF16), pltpu.VMEM((2, 2, 4, tok, d), BF16),
                  pltpu.VMEM((mc, e), BF16), pltpu.VMEM((mc, e), BF16), pltpu.VMEM((mc, e), F32), pltpu.VMEM((mc, e), BF16))
    gl_recv[me] = jnp.sum(gln_acc[...], axis=0, keepdims=True)
    finish_kv()
    pass_on(1, 2)
    gl = [rdma(gl_recv.at[me], gl_recv.at[me], gl_send.at[o - 1], gl_rsem.at[o - 1], lax.rem(me + o, 8)) for o in range(1, 8)]
    for x in gl:
        x.start()
    for o in range(1, 8):
        src = lax.rem(me + 8 - o, 8)
        rdma(gl_recv.at[src], gl_recv.at[src], gl_send.at[o - 1], gl_rsem.at[o - 1], mate).wait_recv()
    total = gl_recv[0]
    for i in range(1, 8):
        total = total + gl_recv[i]
    gln_ref[...] = total
    finish(0, gwo_ref)
    ag_forward()
    finish(1, gwq_ref)
    ag_last()
    for x in gl:
        x.wait_send()
    kp_copy.wait_send()
    for dr in range(2):
        for j in range(3):
            hop_kv(dr, j).wait_send()
            for s in range(2):
                hop(s, dr, j).wait_send()


def gradients(o, o_p, acc, dq, dq_p, hn, hn_p, dy, dy_p, dkv, wqf, wof, w_k, w_v, x, gain, cos_t, sin_t):
    nb, tok, e = x.shape
    n_tok = nb * tok
    d = dq.shape[-1]
    any_spec = pl.BlockSpec(memory_space=pl.ANY)
    vmem = pl.BlockSpec(memory_space=pltpu.VMEM)
    dma = pltpu.SemaphoreType.DMA
    tokens = jax.ShapeDtypeStruct((n_tok, e), BF16)
    y, gx, gln, gwo, gwq_t, gkv_t = pl.pallas_call(
        functools.partial(grads_body, nb, tok),
        in_specs=[any_spec] * 15 + [vmem, vmem, vmem],
        out_specs=[any_spec, any_spec, vmem, vmem, vmem, any_spec],
        out_shape=[tokens, tokens, jax.ShapeDtypeStruct((1, e), F32), jax.ShapeDtypeStruct((d, e), BF16),
                   jax.ShapeDtypeStruct((d, e), BF16), jax.ShapeDtypeStruct((2, d, e), F32)],
        scratch_shapes=[pltpu.VMEM((2, 4, 2, d, e // 2), F32), pltpu.VMEM((4, 2, d, e // 8), F32),
                        pltpu.VMEM((2, 2, 3, d, e // 2), F32), pltpu.VMEM((2, 3, d, e // 8), F32),
                        pltpu.VMEM((2, nb, tok, d), BF16), pltpu.VMEM((nb, tok, d), BF16), pltpu.VMEM((nb, tok, 2 * d), BF16),
                        pltpu.VMEM((d, e // 4), F32), pltpu.VMEM((8, e), F32), pltpu.VMEM((8, 1, e), F32),
                        dma((2, 2, 3)), dma((2, 2, 3)), dma((2, 3)), dma((2, 3)), dma((9,)), dma((9,)), dma((7,)), dma((7,)),
                        dma((2,)), dma((2, 2)), dma((2,)), dma((6,)), dma((4,))],
        compiler_params=pltpu.CompilerParams(collective_id=2, has_side_effects=True, vmem_limit_bytes=63 * 2**20),
        cost_estimate=pl.CostEstimate(flops=10 * n_tok * e * e, bytes_accessed=120 * 2**20, transcendentals=0),
        name="gradients",
    )(o, o_p, acc, dq, dq_p, hn, hn_p, dy.reshape(n_tok, e), dy_p, dkv, wqf, wof.reshape(8 * d, e), w_k, w_v, x.reshape(n_tok, e),
      gain, cos_t, sin_t)
    y, gx, gwq, gwk, gwv, gwo, gln = place(nb, y, gx, gwq_t, gkv_t, gwo, gln)
    return y.reshape(nb, tok, e), gx.reshape(nb, tok, e), gln.reshape(e), gwq, gwk, gwv, gwo


def place_body(steps, y_in, gx_in, gq_in, gkv_in, go_in, gl_in, y, gx, gq, gk, gv, go, gl,
               y_v, gx_v, gq_v, gkv_v, go_v, gl_v, gq_t, gk_t, gv_t, in_sem, y_sem, out_sem, t_sem):
    n, w = y_in.shape[0] // steps, gq_in.shape[1] // steps
    small_in = [pltpu.make_async_copy(s, v, in_sem.at[i]) for i, (s, v) in enumerate(((gkv_in, gkv_v), (gq_in, gq_v), (go_in, go_v), (gl_in, gl_v)))]
    small_out = [pltpu.make_async_copy(v, o, out_sem.at[i]) for i, (v, o) in enumerate(((go_v, go), (gl_v, gl)))]

    def rows(i, size):
        return pl.ds(i * size, size)
    moves = [(pltpu.make_async_copy(s.at[rows(i, n)], v.at[rows(i, n)], y_sem.at[0, j, i]),
              pltpu.make_async_copy(v.at[rows(i, n)], o.at[rows(i, n)], y_sem.at[1, j, i]))
             for i in range(steps) for j, (s, v, o) in enumerate(((y_in, y_v, y), (gx_in, gx_v, gx)))]
    for x in small_in:
        x.start()
    for x, _ in moves:
        x.start()
    small_in[0].wait()
    small_in[1].wait()
    turned = []
    for i in range(steps):
        for j, (v, o) in enumerate(((gk_t, gk), (gv_t, gv), (gq_t, gq))):
            t = (gkv_v[j, :, i * w:(i + 1) * w] if j < 2 else gq_v[:, i * w:(i + 1) * w].astype(F32)).T
            v[i * w:(i + 1) * w, :] = t.astype(v.dtype)
            c = pltpu.make_async_copy(v.at[rows(i, w)], o.at[rows(i, w)], t_sem.at[j, i])
            c.start()
            turned.append(c)
        for x, z in moves[2 * i:2 * i + 2]:
            x.wait()
            z.start()
    for x, z in zip(small_in[2:], small_out):
        x.wait()
        z.start()
    for c in turned + small_out + [z for _, z in moves]:
        c.wait()


def place(steps, y, gx, gwq_t, gkv_t, gwo, gln):
    e = y.shape[1]
    d = gwo.shape[0]
    any_spec = pl.BlockSpec(memory_space=pl.ANY)
    dma = pltpu.SemaphoreType.DMA
    vm = pltpu.VMEM
    return pl.pallas_call(
        functools.partial(place_body, steps),
        in_specs=[any_spec] * 6,
        out_specs=[any_spec] * 7,
        out_shape=[jax.ShapeDtypeStruct(y.shape, BF16), jax.ShapeDtypeStruct(y.shape, BF16), jax.ShapeDtypeStruct((e, d), BF16),
                   jax.ShapeDtypeStruct((e, d), F32), jax.ShapeDtypeStruct((e, d), F32), jax.ShapeDtypeStruct((d, e), BF16),
                   jax.ShapeDtypeStruct((1, e), F32)],
        scratch_shapes=[vm(y.shape, BF16), vm(y.shape, BF16), vm((d, e), BF16), vm((2, d, e), F32), vm((d, e), BF16), vm((1, e), F32),
                        vm((e, d), BF16), vm((e, d), F32), vm((e, d), F32),
                        dma((4,)), dma((2, 2, steps)), dma((2,)), dma((3, steps))],
        compiler_params=pltpu.CompilerParams(vmem_limit_bytes=63 * 2**20),
        cost_estimate=pl.CostEstimate(flops=0, bytes_accessed=8 * y.size + 24 * gwo.size, transcendentals=0),
        name="place",
    )(y, gx, gwq_t, gkv_t, gwo, gln)


def solution(mesh):
    act_spec = P('dp', 'tp', None)

    def device_step(x_loc, ln_scale, wq_loc, w_k, w_v, wo_loc, dy_loc):
        n_batch, tok, model_dim = x_loc.shape
        d = w_k.shape[1]
        t0 = lax.axis_index('tp') * tok
        cos_t, sin_t = rope_tables(t0 + jnp.arange(tok), d)

        gain = ln_scale
        kv0, hn, q, do, kv_loc, wq_h, wo_h, hn_p, dy_p = project(x_loc, gain, wq_loc, w_k, w_v, wo_loc, dy_loc, cos_t, sin_t)
        o, dq, dkv_loc, o_p, dq_p, acc = attention(q, do, kv_loc, kv0, dy_loc.reshape(-1, model_dim), dy_p, cos_t, sin_t)
        return gradients(o, o_p, acc, dq, dq_p, hn, hn_p, dy_loc, dy_p, dkv_loc, wq_h, wo_h, w_k, w_v, x_loc, gain, cos_t, sin_t)

    return jax.shard_map(device_step, mesh=mesh, in_specs=(act_spec, P(None), P(None, 'tp'), P(None, None), P(None, None), P('tp', None), act_spec), out_specs=(act_spec, act_spec, P('dp'), P('dp', 'tp'), P('dp', None), P('dp', None), P(('dp', 'tp'), None)), check_vma=False)
```

```python
import functools
import jax
import jax.numpy as jnp
from jax import lax
from jax.experimental import pallas as pl
from jax.experimental.pallas import tpu as pltpu
from jax.sharding import PartitionSpec as P

LN_EPS = 1e-6
ROPE_BASE = 10000.0
LOG2E = 1.4426950408889634
F32 = jnp.float32
BF16 = jnp.bfloat16


def rope_tables(positions, head_dim):
    half_dim = head_dim // 2
    inv_freq = ROPE_BASE ** (-2.0 * jnp.arange(half_dim, dtype=F32) / head_dim)
    angles = positions.astype(F32)[:, None] * inv_freq[None, :]
    return jnp.cos(angles), jnp.sin(angles)


def rotate(vectors, cos_t, sin_t):
    half_dim = vectors.shape[-1] // 2
    lo_half = vectors[..., :half_dim]
    hi_half = vectors[..., half_dim:]
    return jnp.concatenate([lo_half * cos_t - hi_half * sin_t, hi_half * cos_t + lo_half * sin_t], axis=-1)


def dot_nn(a, b):
    return lax.dot_general(a, b, (((1,), (0,)), ((), ())), preferred_element_type=F32)


def dot_nt(a, b):
    return lax.dot_general(a, b, (((1,), (1,)), ((), ())), preferred_element_type=F32)


def rdma(src, dst, send, recv, to):
    return pltpu.make_async_remote_copy(src_ref=src, dst_ref=dst, send_sem=send, recv_sem=recv,
                                        device_id={'tp': to}, device_id_type=pl.DeviceIdType.MESH)


def ring_ids():
    me = lax.axis_index('tp')
    k = lax.rem(me, 2)
    return me, k, me + 1 - 2 * k, lax.rem(me + 2, 8), lax.rem(me + 6, 8)


def enter(peers):
    barrier = pltpu.get_barrier_semaphore()
    for p in peers:
        pl.semaphore_signal(barrier, inc=1, device_id={'tp': p}, device_id_type=pl.DeviceIdType.MESH)
    pl.semaphore_wait(barrier, len(peers))


class Products:
    def __init__(self, big, a_v, at, ld_sem, b_sem):
        self.big, self.a_v, self.at, self.ld_sem, self.b_sem = big, a_v, at, ld_sem, b_sem
        self.nb, self.tok = a_v.shape[2], a_v.shape[3]
        self.eq = big.shape[2] // 4

    def load_b(self, own, other):
        return (pltpu.make_async_copy(own, self.big.at[0], self.b_sem.at[0]),
                pltpu.make_async_copy(other, self.big.at[1], self.b_sem.at[1]))

    def load_a(self, i, own, other):
        return (pltpu.make_async_copy(own, self.a_v.at[i % 2, 0], self.ld_sem.at[i % 2, 0]),
                pltpu.make_async_copy(other, self.a_v.at[i % 2, 1], self.ld_sem.at[i % 2, 1]))

    def turn(self, j, src):
        tok = self.tok
        for i in range(self.nb // 2):
            self.at[j, :, 2 * i * tok:(2 * i + 2) * tok] = jnp.concatenate([src[2 * i], src[2 * i + 1]], axis=0).T

    def both(self, cols):
        return dot_nn(self.at[0], self.big[0, :, cols]) + dot_nn(self.at[1], self.big[1, :, cols])

    def columns(self, dst, first, last, turned=0):
        eq = self.eq

        @pl.loop(first, last)
        def _(n):
            m = lax.rem(n + turned, 4)
            cols = pl.ds(pl.multiple_of(m * eq, 128), eq)
            dst[m // 2, :, pl.ds(pl.multiple_of(lax.rem(m, 2) * eq, 128), eq)] = self.both(cols)


class Gather:
    def __init__(self, ids, c, block, send, recv):
        self.me, _, self.mate, self.cw, self.ccw = ids
        self.c, self.block, self.send, self.recv = c, block, send, recv

    def copy(self, j, tag, to, src=None):
        ref = self.block(j)
        return rdma(ref if src is None else src, ref, self.send(tag), self.recv(tag), to)

    def own(self, src):
        @pl.when(self.c <= 2)
        def _():
            self.copy(self.me, 0, self.cw, src).start()

        @pl.when(self.c == 0)
        def _():
            self.copy(self.me, 2, self.ccw, src).start()
        self.copy(self.me, 3, self.mate, src).start()

    def arrived(self):
        @pl.when(self.c >= 1)
        def _():
            self.copy(self.me - 2, 0, self.cw).wait_recv()

        @pl.when(self.c == 3)
        def _():
            self.copy(self.me - 6, 2, self.ccw).wait_recv()

    def pass_on(self, src=lambda j: None):
        @pl.when(self.c >= 1)
        def _():
            @pl.when(self.c <= 2)
            def _():
                self.copy(self.me - 2, 1, self.cw, src(self.me - 2)).start()
            self.copy(self.me - 2, 4, self.mate, src(self.me - 2)).start()

        @pl.when(self.c == 3)
        def _():
            self.copy(self.me - 6, 6, self.mate, src(self.me - 6)).start()

    def forward(self):
        self.arrived()
        self.pass_on()

    def last(self):
        @pl.when(self.c >= 2)
        def _():
            self.copy(self.me - 4, 1, self.cw).wait_recv()
            self.copy(self.me - 4, 5, self.mate).start()

    def ready(self, tags=(3, 4, 5, 6)):
        if 3 in tags:
            self.copy(self.mate, 3, self.mate).wait_recv()
        for n, tag in ((1, 4), (2, 5), (3, 6)):
            if tag not in tags:
                continue

            @pl.when(self.c >= n)
            def _():
                self.copy(self.mate - 2 * n, tag, self.mate).wait_recv()

    def drain(self, tags=range(7)):
        c = self.c
        conds = (c <= 2, (c >= 1) & (c <= 2), c == 0, c >= 0, c >= 1, c >= 2, c == 3)
        for tag in tags:
            @pl.when(conds[tag])
            def _():
                self.copy(self.me, tag, self.mate).wait_send()


def attn_body(nb, tok, seq, d, q_hbm, do_hbm, kvl_hbm, kv0_hbm, dy_hbm, dyp_hbm, cos_ref, sin_ref,
              o_hbm, dq_hbm, dkv_hbm, op_hbm, dqp_hbm, acc_hbm,
              kv_all, o_v, dq_v, mrecv, rrecv, big,
              kv_send, kv_recv, m_send, m_recv, r_send, r_recv, own_sem, in_sem, out_sem, fin_sem, p_send, p_recv, first_sem,
              ld_sem, b_sem, acc_sem):
    scale = d ** -0.5
    rows = o_v.shape[2] * tok
    n_blk = seq // 256
    rb = 2 * rows // n_blk
    n_rb = rows // rb
    half = d // 2
    me, k, mate, cw, ccw = ring_ids()
    c = me // 2
    rel = [lax.rem(c + o, 4) for o in (3, 1, 2, 0)]

    def blk(j):
        return pl.ds(pl.multiple_of(j * tok, 16), tok)

    def kvb(b, j):
        return kv_all.at[b, blk(j)]

    def gather(b):
        return Gather((me, k, mate, cw, ccw), c, lambda j: kvb(b, j), lambda t: kv_send.at[b - 1, t], lambda t: kv_recv.at[b - 1, t])

    def own(b):
        gather(b).own(kvl_hbm.at[b])

    def own_copy(b):
        return pltpu.make_async_copy(kvl_hbm.at[b], kvb(b, me), own_sem.at[b])

    def ready(b):
        own_copy(b).wait()

        @pl.when(b == 1)
        def _():
            gather(1).ready((4, 5, 6))

        @pl.when(b > 1)
        def _():
            gather(b).ready()

    def drain(b):
        @pl.when(b == 1)
        def _():
            gather(1).drain((1, 4, 5, 6))

        @pl.when(b > 1)
        def _():
            gather(b).drain()

    def m_copy(b, n):
        return rdma(kvb(b, 2 * n + 1 - k), mrecv.at[lax.rem(b, 2), n], m_send.at[b, n], m_recv.at[b, n], mate)

    def r_copy(b, n, slot, to):
        return rdma(kvb(b, 2 * n + k), rrecv.at[b, slot], r_send.at[b, slot], r_recv.at[b, slot], to)

    def add_into(b, n, other):
        v = kv_all[b, blk(2 * n + k), :].astype(F32) + other[...].astype(F32)
        kv_all[b, blk(2 * n + k), :] = v.astype(BF16)

    def fin_copy(b):
        return pltpu.make_async_copy(kvb(b, me), dkv_hbm.at[b], fin_sem.at[b])

    def to_mate(b):
        for n in range(4):
            @pl.when(c >= n)
            def _():
                m_copy(b, n).start()

    def stage1(b):
        for n in range(4):
            @pl.when(c >= n)
            def _():
                m_copy(b, n).wait()
                add_into(b, n, mrecv.at[lax.rem(b, 2), n])

        @pl.when(c == 3)
        def _():
            r_copy(b, 1, 2, ccw).start()
            r_copy(b, 2, 1, ccw).start()
            r_copy(b, 0, 0, cw).start()
            fin_copy(b).start()

        @pl.when(c == 2)
        def _():
            r_copy(b, 0, 1, ccw).start()

    def stage2(b):
        @pl.when(c == 2)
        def _():
            r_copy(b, 1, 2, ccw).wait_recv()
            add_into(b, 1, rrecv.at[b, 2])
            r_copy(b, 1, 2, ccw).start()
            r_copy(b, 2, 1, ccw).wait_recv()
            add_into(b, 2, rrecv.at[b, 1])
            fin_copy(b).start()

        @pl.when(c == 1)
        def _():
            r_copy(b, 0, 1, ccw).wait_recv()
            add_into(b, 0, rrecv.at[b, 1])
            r_copy(b, 0, 1, ccw).start()

    def stage3(b):
        @pl.when(c == 0)
        def _():
            r_copy(b, 0, 0, cw).wait_recv()
            add_into(b, 0, rrecv.at[b, 0])
            r_copy(b, 0, 1, ccw).wait_recv()
            add_into(b, 0, rrecv.at[b, 1])
            fin_copy(b).start()

        @pl.when(c == 1)
        def _():
            r_copy(b, 1, 2, ccw).wait_recv()
            add_into(b, 1, rrecv.at[b, 2])
            fin_copy(b).start()

    def handed(dst, src, n, b, slot):
        return rdma(src.at[slot, 1 - k], dst.at[b], p_send.at[n, b], p_recv.at[n, b], mate)

    def store_o(b, slot):
        return (pltpu.make_async_copy(o_v.at[slot], o_hbm.at[b], out_sem.at[0, slot]), handed(op_hbm, o_v, 0, b, slot))

    def store_dq(b, slot):
        return (pltpu.make_async_copy(dq_v.at[slot], dq_hbm.at[b], out_sem.at[1, slot]), handed(dqp_hbm, dq_v, 1, b, slot))

    def stored(x):
        x[0].wait()
        x[1].wait_send()

    load_dy = (pltpu.make_async_copy(dy_hbm, big.at[0], b_sem.at[0]), pltpu.make_async_copy(dyp_hbm, big.at[1], b_sem.at[1]))

    def attend(q_v, do_v, s_buf, m_buf, l_buf, p_buf, ds_buf, q_t, do_t, dk_t, dv_t, d_buf, cos4, sin4):
        def load(b, slot):
            return (pltpu.make_async_copy(q_hbm.at[b], q_v.at[slot], in_sem.at[0, slot]),
                    pltpu.make_async_copy(do_hbm.at[b], do_v.at[slot], in_sem.at[1, slot]))

        def scores(b, g, slot, i):
            w = min(512, seq)
            if (i * 256) % w:
                return
            cols = slice(i * 256, i * 256 + w)
            s = dot_nt(q_v[slot, g].reshape(rows, d), kv_all[b, cols, :d]) * (scale * LOG2E)
            col = lax.broadcasted_iota(jnp.int32, (tok, w), 1) + i * 256
            row = lax.broadcasted_iota(jnp.int32, (tok, w), 0) + me * tok
            s = jnp.concatenate([jnp.where(col <= row, s[j * tok:(j + 1) * tok], -1e30) for j in range(rows // tok)], axis=0)
            s_buf[g, :, cols] = s
            m = s[:, :128]
            for j in range(128, w, 128):
                m = jnp.maximum(m, s[:, j:j + 128])
            m_buf[...] = m if i == 0 else jnp.maximum(m_buf[...], m)

        parts = max(1, min(5, n_blk))
        part = [j * (rows // 16) // parts * 16 for j in range(parts + 1)] + [rows] * n_blk

        def softmax(g, i):
            for r in range(part[i], part[i + 1], 16):
                rs = slice(r, r + 16)
                m = jnp.max(m_buf[rs, :], axis=1, keepdims=True)
                l = None
                for j in range(0, seq, 128):
                    e = jnp.exp2(s_buf[g, rs, j:j + 128] - m)
                    s_buf[g, rs, j:j + 128] = e
                    l = e if l is None else l + e
                l_buf[g, rs, :] = jnp.broadcast_to(1.0 / jnp.sum(l, axis=1, keepdims=True), (16, 128))

        def turn(g, slot, i):
            rs = slice(i * rb, (i + 1) * rb)
            q_t[g, :, rs] = q_v[slot, g].reshape(rows, d)[rs].T
            do_t[g, :, rs] = do_v[slot, g].reshape(rows, d)[rs].T

        def out_rows(b, g, slot, i):
            rs = slice(i * rb, (i + 1) * rb)
            p = (s_buf[g, rs, :] * jnp.concatenate([l_buf[g, rs, :]] * (seq // 128), axis=1)).astype(BF16)
            p_buf[rs, :] = p
            o = dot_nn(p, kv_all[b, :, d:])
            dvec = jnp.sum(o * do_v[slot, g].reshape(rows, d)[rs].astype(F32), axis=1, keepdims=True)
            d_buf[rs, :] = jnp.broadcast_to(dvec, (rb, 128))
            put_rows(o_v, slot, g, i, o.astype(BF16))

        def put_rows(ref, slot, g, i, v):
            r = i * rb
            while r < (i + 1) * rb:
                n = min((i + 1) * rb - r, tok - r % tok)
                ref[slot, g, r // tok, r % tok:r % tok + n, :] = v[r - i * rb:r - i * rb + n]
                r += n

        def dq_rows(b, g, slot, i):
            rs = slice(i * rb, (i + 1) * rb)
            dq = dot_nn(ds_buf[rs, :], kv_all[b, :, :d]) * scale
            lo, hi = dq[:, :half], dq[:, half:]
            cs, sn = cos4[rs, :], sin4[rs, :]
            put_rows(dq_v, slot, g, i, jnp.concatenate([(lo * cs + hi * sn).astype(BF16), (hi * cs - lo * sn).astype(BF16)], axis=1))

        def grads(b, g, slot, i):
            cols = slice(i * 256, (i + 1) * 256)
            do = do_v[slot, g].reshape(rows, d)
            p = p_buf[:, cols]
            dp = dot_nt(do, kv_all[b, cols, d:])
            dvec = d_buf[...]
            if i > 0 and part[i] > part[i - 1]:
                z = None
                for r in range(part[i - 1], part[i], 8):
                    v = l_buf[1 - g, r:r + 8, :]
                    z = v if z is None else jnp.minimum(z, v)
                dvec = dvec + jnp.concatenate([jnp.minimum(z, 0.0)] * (rows // 8), axis=0)
            dd = jnp.concatenate([dvec, dvec], axis=1)
            ds = (p.astype(F32) * (dp - dd)).astype(BF16)
            ds_buf[:, cols] = ds
            dk = dot_nn(q_t[g], ds)
            dv = dot_nn(do_t[g], p)
            if g == 0:
                dk_t[:, cols] = dk
                dv_t[:, cols] = dv
            else:
                dk_t[:, cols] += dk
                dv_t[:, cols] += dv

        def close_kv(b, i):
            cols = slice(i * 256, (i + 1) * 256)
            kv_all[b, cols, :d] = (dk_t[:, cols] * scale).T.astype(BF16)
            kv_all[b, cols, d:] = dv_t[:, cols].T.astype(BF16)

        enter((mate, cw, ccw))
        gather(1).pass_on(lambda j: kv0_hbm.at[1, blk(j)])
        if nb > 2:
            own(2)
        for x in load(0, 0):
            x.start()

        def first(j):
            return pltpu.make_async_copy(kv0_hbm.at[0, blk(j)], kvb(0, j), first_sem.at[j])

        def second(j, n):
            return pltpu.make_async_copy(kv0_hbm.at[1, blk(j)], kvb(1, j), first_sem.at[8 + n])
        arrived = ((c >= 0, mate, 0), (c >= 1, me - 2, 1), (c == 3, me - 6, 2))
        for j in range(8):
            @pl.when(j <= 2 * c + 1)
            def _():
                first(j).start()
        for b in range(1, nb):
            own_copy(b).start()
        for cond, j, i in arrived:
            @pl.when(cond)
            def _():
                second(j, i).start()

        @pl.loop(2 * c + 2, 8)
        def _(j):
            for b in range(nb):
                kv_all[b, blk(j), :] = jnp.zeros((tok, 2 * d), BF16)
        for j in range(rows // tok):
            cos4[j * tok:(j + 1) * tok, :] = cos_ref[...]
            sin4[j * tok:(j + 1) * tok, :] = sin_ref[...]
        ds_buf[...] = jnp.zeros_like(ds_buf)
        for x in load(0, 0):
            x.wait()
        for i in range(n_rb):
            turn(0, 0, i)
        for j in range(8):
            @pl.when(j <= 2 * c + 1)
            def _():
                first(j).wait()
        for cond, j, i in arrived:
            @pl.when(cond)
            def _():
                second(j, i).wait()
        for i in range(n_blk):
            scores(0, 0, 0, i)
        for i in range(n_blk):
            softmax(0, i)

        def comm_steps(b, steps):
            for lag, stage in steps:
                @pl.when(b >= lag)
                def _():
                    stage(b - lag)

        @pl.loop(0, nb)
        def _(b):
            slot = lax.rem(b, 2)
            nxt = jnp.minimum(b + 1, nb - 1)
            prev = jnp.maximum(b - 1, 0)

            @pl.when(b + 1 < nb)
            def _():
                for x in load(b + 1, 1 - slot):
                    x.start()

            @pl.when(b + 3 < nb)
            def _():
                own(b + 3)

            @pl.when((b >= 1) & (b + 2 < nb))
            def _():
                gather(b + 2).forward()

            @pl.when(b == 1)
            def _():
                for x in load_dy:
                    x.start()
            comm_steps(b, ((3, stage2), (4, stage3)))

            @pl.when(b >= 2)
            def _():
                drain(b - 1)

            @pl.when(b >= 2)
            def _():
                stored(store_o(b - 2, slot))
            spare = jnp.where(b >= 1, b - 1, nb)
            for i in range(n_blk):
                scores(b, 1, slot, i)
                if i % 2 == 1:
                    out_rows(b, 0, slot, i // 2)
                    dq_rows(prev, 1, 1 - slot, i // 2)
                    turn(1, slot, i // 2)
            for i in range(n_blk):
                close_kv(spare, i)

            @pl.when(b + 1 < nb)
            def _():
                gather(b + 1).last()

            @pl.when(b >= 1)
            def _():
                for x in store_dq(b - 1, 1 - slot):
                    x.start()
                to_mate(b - 1)

            for i in range(n_blk):
                grads(b, 0, slot, i)
                softmax(1, i)

            @pl.when(b + 1 < nb)
            def _():
                for x in load(b + 1, 1 - slot):
                    x.wait()
                ready(b + 1)
            if nb > 2:
                @pl.when(b == 0)
                def _():
                    gather(2).forward()

            @pl.when(b >= 2)
            def _():
                stored(store_dq(b - 2, slot))
            nslot = lax.rem(nxt, 2)
            for i in range(n_blk):
                scores(nxt, 0, nslot, i)
                if i % 2 == 1:
                    out_rows(b, 1, slot, i // 2)
                    dq_rows(b, 0, slot, i // 2)
                    turn(0, nslot, i // 2)
            for x in store_o(b, slot):
                x.start()
            comm_steps(b, ((1, stage1),))
            for i in range(n_blk):
                grads(b, 1, slot, i)
                softmax(0, i)

        drain(nb - 1)
        for i in range(n_rb):
            dq_rows(nb - 1, 1, (nb - 1) % 2, i)
        for i in range(n_blk):
            close_kv(nb - 1, i)
        to_mate(nb - 1)
        for x in store_dq(nb - 1, (nb - 1) % 2):
            x.start()

    slab = pltpu.VMEM((2, 2, rows // tok, tok, d), BF16)
    pl.run_scoped(attend, slab, slab, pltpu.VMEM((2, rows, seq), F32), pltpu.VMEM((rows, 128), F32), pltpu.VMEM((2, rows, 128), F32),
                  pltpu.VMEM((rows, seq), BF16), pltpu.VMEM((rows, seq), BF16), pltpu.VMEM((2, d, rows), BF16),
                  pltpu.VMEM((2, d, rows), BF16), pltpu.VMEM((d, seq), F32), pltpu.VMEM((d, seq), F32),
                  pltpu.VMEM((rows, 128), F32), pltpu.VMEM((rows, half), F32), pltpu.VMEM((rows, half), F32))
    n = nb

    def first_products(a_v, at, acc_v):
        pr = Products(big, a_v, at, ld_sem, b_sem)
        for b in (n - 2, n - 1):
            stored(store_o(b, b % 2))
        for b in range(n):
            handed(op_hbm, o_v, 0, b, b % 2).wait_recv()

        def fetch(r):
            return pr.load_a(r, o_hbm.at[:, k, rel[r]], op_hbm.at[:, rel[r]])

        def save(r):
            return pltpu.make_async_copy(acc_v.at[r], acc_hbm.at[r], acc_sem.at[r])
        for r in range(2):
            for x in fetch(r):
                x.start()

        todo = [((stage2, n - 3), (stage3, n - 4)), ((stage1, n - 1), (stage2, n - 2), (stage3, n - 3)),
                ((stage2, n - 1), (stage3, n - 2)), ((stage3, n - 1),)]

        def steps(i):
            for stage, b in todo[i]:
                if b >= 0:
                    stage(b)
        steps(0)
        steps(1)
        for r in range(2):
            for x in fetch(r):
                x.wait()
            pr.turn(0, a_v.at[r, 0])
            pr.turn(1, a_v.at[r, 1])
            if r == 0:
                for x in load_dy:
                    x.wait()
            pr.columns(acc_v.at[r], 0, 4)
            save(r).start()
        steps(2)
        steps(3)
        for r in range(2):
            save(r).wait()

    pl.run_scoped(first_products, pltpu.VMEM((2, 2, nb, tok, d), BF16),
                  pltpu.VMEM((2, d, nb * tok), BF16), pltpu.VMEM((2, 2, d, dy_hbm.shape[1] // 2), F32))
    for b in (n - 2, n - 1):
        stored(store_dq(b, b % 2))
    for b in range(n):
        handed(dqp_hbm, dq_v, 1, b, b % 2).wait_recv()
        fin_copy(b).wait()
        for cond, slot in ((c == 3, 0), (c >= 1, 1), (c >= 2, 2)):
            @pl.when(cond)
            def _():
                r_copy(b, 0, slot, cw).wait_send()


def attention(q, do, kv, kv0, dy, dy_p, cos_t, sin_t):
    nb, _, hp, tok, d = q.shape
    seq = tok * 8
    rows = hp * tok
    any_spec = pl.BlockSpec(memory_space=pl.ANY)
    vmem = pl.BlockSpec(memory_space=pltpu.VMEM)
    dma = pltpu.SemaphoreType.DMA
    slab = pltpu.VMEM((2, 2, hp, tok, d), BF16)
    out = jax.ShapeDtypeStruct(q.shape, BF16)
    outp = jax.ShapeDtypeStruct((nb, hp, tok, d), BF16)
    return pl.pallas_call(
        functools.partial(attn_body, nb, tok, seq, d),
        in_specs=[any_spec] * 6 + [vmem, vmem],
        out_specs=[any_spec] * 6,
        out_shape=[out, out, jax.ShapeDtypeStruct(kv.shape, BF16), outp, outp,
                   jax.ShapeDtypeStruct((2, 2, d, dy.shape[1] // 2), F32)],
        scratch_shapes=[pltpu.VMEM((nb + 1, seq, 2 * d), BF16), slab, slab,
                        pltpu.VMEM((2, 4, tok, 2 * d), BF16), pltpu.VMEM((nb, 3, tok, 2 * d), BF16),
                        pltpu.VMEM((2,) + dy.shape, BF16),
                        dma((nb - 1, 7)), dma((nb - 1, 7)), dma((nb, 4)), dma((nb, 4)), dma((nb, 3)), dma((nb, 3)),
                        dma((nb,)), dma((2, 2)), dma((2, 2)), dma((nb,)), dma((2, nb)), dma((2, nb)), dma((11,)),
                        dma((2, 2)), dma((2,)), dma((4,))],
        compiler_params=pltpu.CompilerParams(collective_id=1, has_side_effects=True, vmem_limit_bytes=63 * 2**20),
        cost_estimate=pl.CostEstimate(flops=24 * nb * rows * seq * d, bytes_accessed=40 * 2**20,
                                      transcendentals=2 * nb * rows * seq),
        name="attention",
    )(q, do, kv, kv0, dy, dy_p, cos_t, sin_t)


def proj_body(nb, tok, x_hbm, g_ref, wq_hbm, wk_ref, wv_ref, wo_hbm, dy_hbm, cos_ref, sin_ref,
              kv0_hbm, hn_hbm, q_hbm, do_hbm, kv_hbm, wqf_hbm, wof_hbm, hnp_hbm, dyp_hbm,
              x_v, hn_v, dy_v, wq_v, wo_v, kv_v, out_v,
              send, recv, x_sem, dy_sem, own_sem, out_sem, misc_sem, w_sem, p_send, p_recv, kv_send, kv_recv):
    n_tok, e = x_hbm.shape
    d = kv_v.shape[1] // 2
    half = d // 2
    mc = 2 * tok
    me, k, mate, cw, ccw = ring_ids()
    base = 2 * (me // 2)

    def head(off, par):
        return lax.rem(base + 2 * off + 8, 8) + par
    enter((mate, cw, ccw))

    fulls = (wq_v, wo_v)
    locs = (wq_hbm, wo_hbm)

    def half_of(w, ref, j):
        n = ref.shape[0] // 2
        return ref.at[pl.ds(j * n, n)]

    sends = []

    def send_full(w, h, j, to, own=False):
        src = locs[w] if own else fulls[w].at[h]
        c = rdma(src, fulls[w].at[h], send.at[w, j], recv.at[w, j], to)
        c.start()
        sends.append(c)

    def send_half(w, h, part, j, to):
        c = rdma(half_of(w, fulls[w].at[h], part), half_of(w, fulls[w].at[h], part), send.at[w, j], recv.at[w, j], to)
        c.start()
        sends.append(c)

    def wait_full(w, h, j):
        rdma(fulls[w].at[h], fulls[w].at[h], send.at[w, j], recv.at[w, j], mate).wait_recv()

    def wait_half(w, h, part, j):
        ref = half_of(w, fulls[w].at[h], part)
        rdma(ref, ref, send.at[w, j], recv.at[w, j], mate).wait_recv()

    for w in range(2):
        send_full(w, me, 0, cw, True)
        send_full(w, me, 1, ccw, True)
        send_full(w, me, 4, mate, True)
    own = [pltpu.make_async_copy(locs[w], fulls[w].at[me], own_sem.at[w]) for w in range(2)]
    xs = [pltpu.make_async_copy(x_hbm.at[pl.ds(b * tok, tok)], x_v.at[pl.ds(b * tok, tok)], x_sem.at[b]) for b in range(nb)]
    for c in xs:
        c.start()
    for c in own:
        c.start()
    dyc = pltpu.make_async_copy(dy_hbm, dy_v, dy_sem)
    dyc.start()

    gain = g_ref[...].astype(F32).reshape(1, e)
    for b in range(nb):
        xs[b].wait()

        @pl.loop(0, tok // 16, unroll=2)
        def _(r):
            rs = pl.ds(pl.multiple_of(b * tok + r * 16, 16), 16)
            x = x_v[rs, :].astype(F32)
            c = x - jnp.mean(x, axis=1, keepdims=True)
            inv = lax.rsqrt(jnp.mean(c * c, axis=1, keepdims=True) + LN_EPS)
            hn_v[rs, :] = (c * inv * gain).astype(BF16)
    hn_out = pltpu.make_async_copy(hn_v, hn_hbm, misc_sem.at[0])
    hn_out.start()
    to_mate = [rdma(hn_v, hnp_hbm, p_send.at[0], p_recv.at[0], mate), rdma(dy_hbm, dyp_hbm, p_send.at[1], p_recv.at[1], mate)]
    for c in to_mate:
        c.start()

    def rope_rows(raw):
        lo, hi = raw[:, :half], raw[:, half:d]
        cs, sn = jnp.concatenate([cos_ref[...]] * 2, axis=0), jnp.concatenate([sin_ref[...]] * 2, axis=0)
        return lo * cs - hi * sn, hi * cs + lo * sn

    @pl.loop(0, n_tok // mc)
    def _(i):
        rs = pl.ds(pl.multiple_of(i * mc, mc), mc)
        lo, hi = rope_rows(dot_nn(hn_v[rs, :], wk_ref[...]))
        kv_v[rs, :half] = lo.astype(BF16)
        kv_v[rs, half:d] = hi.astype(BF16)
        kv_v[rs, d:] = dot_nn(hn_v[rs, :], wv_ref[...]).astype(BF16)
    kv_out = pltpu.make_async_copy(kv_v, kv_hbm, misc_sem.at[1])
    kv_out.start()

    outs = []
    saves = []

    def save(w, h):
        c = pltpu.make_async_copy(fulls[w].at[h], (wqf_hbm, wof_hbm)[w].at[h], w_sem.at[len(saves)])
        c.start()
        saves.append(c)

    def project(w, h):
        slot = len(outs) % 4
        if len(outs) >= 4:
            outs[-4].wait()

        @pl.loop(0, n_tok // mc)
        def _(i):
            rs = pl.ds(pl.multiple_of(i * mc, mc), mc)
            if w == 0:
                lo, hi = rope_rows(dot_nn(hn_v[rs, :], wq_v[h]))
                o0 = lo.reshape(2, tok, half).astype(BF16)
                o1 = hi.reshape(2, tok, half).astype(BF16)
                out_v[slot, pl.ds(2 * i, 2), :, :half] = o0
                out_v[slot, pl.ds(2 * i, 2), :, half:] = o1
            else:
                out_v[slot, pl.ds(2 * i, 2)] = dot_nt(dy_v[rs, :], wo_v[h]).reshape(2, tok, d).astype(BF16)
        c = pltpu.make_async_copy(out_v.at[slot], (q_hbm, do_hbm)[w].at[:, lax.rem(h, 2), h // 2], out_sem.at[slot])
        c.start()
        outs.append(c)
        save(w, h)

    other = 1 - k
    for w in range(2):
        own[w].wait()
        if w == 1:
            dyc.wait()
        project(w, me)
        wait_full(w, mate, 4)
        project(w, mate)
    for w in range(2):
        wait_full(w, head(-1, k), 0)
        send_half(w, head(-1, k), 0, 2, cw)
        wait_full(w, head(1, k), 1)
        send_half(w, head(1, k), 1, 3, ccw)
        send_full(w, head(-1, k), 5, mate)
        send_full(w, head(1, k), 6, mate)
        project(w, head(-1, k))
        project(w, head(1, k))
        wait_full(w, head(-1, other), 5)
        project(w, head(-1, other))
        wait_full(w, head(1, other), 6)
        project(w, head(1, other))

    def early(n):
        def blk(j):
            return kv0_hbm.at[n, pl.ds(pl.multiple_of(j * tok, 16), tok)]
        return Gather((me, k, mate, cw, ccw), me // 2, blk, lambda t: kv_send.at[n, t], lambda t: kv_recv.at[n, t])
    first, second = early(0), early(1)
    first.own(kv_v.at[pl.ds(0, tok)])
    own0 = pltpu.make_async_copy(kv_v.at[pl.ds(0, tok)], first.block(me), misc_sem.at[2])
    own0.start()
    for w in range(2):
        wait_half(w, head(2, k), 0, 2)
        send_half(w, head(2, k), 0, 7, mate)
        wait_half(w, head(2, k), 1, 3)
        send_half(w, head(2, k), 1, 8, mate)
        project(w, head(2, k))
        if w == 1:
            first.forward()
            second.own(kv_v.at[pl.ds(tok, tok)])
        wait_half(w, head(2, other), 0, 7)
        wait_half(w, head(2, other), 1, 8)
        project(w, head(2, other))
    first.last()
    for c in outs[-4:] + saves + [hn_out, kv_out, own0]:
        c.wait()
    first.ready()
    first.drain()
    second.arrived()
    second.ready((3,))
    second.drain((0, 2, 3))
    for c in sends:
        c.wait_send()
    for c in to_mate:
        c.wait()


def project(x, gain, wq, w_k, w_v, wo, dy, cos_t, sin_t):
    nb, tok, e = x.shape
    d = wq.shape[1]
    n_heads = 8
    n_tok = nb * tok
    any_spec = pl.BlockSpec(memory_space=pl.ANY)
    vmem = pl.BlockSpec(memory_space=pltpu.VMEM)
    act = jax.ShapeDtypeStruct((nb, 2, n_heads // 2, tok, d), BF16)
    dma = pltpu.SemaphoreType.DMA
    flops = 2 * n_tok * e * (2 * n_heads + 2) * d
    kv0, hn, q, do, kv, wqf, wof, hn_p, dy_p = pl.pallas_call(
        functools.partial(proj_body, nb, tok),
        in_specs=[any_spec, vmem, any_spec, vmem, vmem, any_spec, any_spec, vmem, vmem],
        out_specs=[any_spec] * 9,
        out_shape=[jax.ShapeDtypeStruct((2, tok * n_heads, 2 * d), BF16), jax.ShapeDtypeStruct((n_tok, e), BF16), act, act, jax.ShapeDtypeStruct((n_tok, 2 * d), BF16),
                   jax.ShapeDtypeStruct((n_heads, e, d), BF16), jax.ShapeDtypeStruct((n_heads, d, e), BF16),
                   jax.ShapeDtypeStruct((n_tok, e), BF16), jax.ShapeDtypeStruct((n_tok, e), BF16)],
        scratch_shapes=[pltpu.VMEM((n_tok, e), BF16), pltpu.VMEM((n_tok, e), BF16), pltpu.VMEM((n_tok, e), BF16),
                        pltpu.VMEM((n_heads, e, d), BF16), pltpu.VMEM((n_heads, d, e), BF16),
                        pltpu.VMEM((n_tok, 2 * d), BF16), pltpu.VMEM((4, nb, tok, d), BF16),
                        dma((2, 9)), dma((2, 9)), dma((nb,)), dma(()), dma((2,)), dma((4,)), dma((3,)), dma((16,)), dma((2,)), dma((2,)), dma((2, 7)), dma((2, 7))],
        compiler_params=pltpu.CompilerParams(collective_id=0, has_side_effects=True, vmem_limit_bytes=60 * 2**20),
        cost_estimate=pl.CostEstimate(flops=flops, bytes_accessed=60 * 2**20, transcendentals=0),
        name="project",
    )(x.reshape(n_tok, e), gain, wq, w_k, w_v, wo, dy.reshape(n_tok, e), cos_t, sin_t)
    return kv0, hn, q, do, kv.reshape(nb, tok, 2 * d), wqf, wof, hn_p, dy_p


def grads_body(nb, tok, o_hbm, op_hbm, acc_hbm, dq_hbm, dqp_hbm, hn_hbm, hnp_hbm, dy_hbm, dyp_hbm, dkv_hbm,
               wq_hbm, wo_hbm, wk_hbm, wv_hbm, x_hbm, g_ref, cos_ref, sin_ref,
               y_hbm, gx_hbm, gln_ref, gwo_ref, gwq_ref, gkv_hbm,
               acc, acc_kv, rbuf, rbuf_kv, kind, kp, dkv_v, fin_kv, gln_acc, gl_recv,
               rs_send, rs_recv, kv_send, kv_recv, ag_send, ag_recv, gl_send, gl_rsem, kp_sem, ld_sem, b_sem, t_sem, a_sem):
    n_tok, e = x_hbm.shape
    d = wk_hbm.shape[1]
    half = d // 2
    eh, eq = e // 2, e // 4
    me, k, mate, cw, ccw = ring_ids()
    c = me // 2
    rel = [lax.rem(c + o, 4) for o in (3, 1, 2, 0)]
    enter([lax.rem(me + o, 8) for o in range(1, 8)])

    order = ((2, 1), (2, 0))

    def hop(s, dr, j):
        first = acc_hbm.at[dr, dr] if s == 0 else acc.at[s, dr, dr]
        src = first if j == 0 else rbuf.at[s, dr, j - 1]
        return rdma(src, rbuf.at[s, dr, j], rs_send.at[s, dr, j], rs_recv.at[s, dr, j], (cw, ccw)[dr])

    def hop_kv(dr, j):
        src = acc_kv.at[dr, dr] if j == 0 else rbuf_kv.at[dr, j - 1]
        return rdma(src, rbuf_kv.at[dr, j], kv_send.at[dr, j], kv_recv.at[dr, j], (cw, ccw)[dr])

    def add(dst, term):
        @pl.loop(0, dst.shape[0] // 32)
        def _(i):
            rs = pl.ds(pl.multiple_of(i * 32, 32), 32)
            dst[rs, :] = dst[rs, :] + term[rs, :]

    def pass_on(s, j):
        for dr in range(2):
            hop(s, dr, j - 1).wait_recv()
            add(rbuf.at[s, dr, j - 1], acc.at[s, order[dr][j - 1], dr])
            hop(s, dr, j).start()

    def pass_on_kv(j):
        for dr in range(2):
            hop_kv(dr, j - 1).wait_recv()
            add(rbuf_kv.at[dr, j - 1], acc_kv.at[order[dr][j - 1], dr])
            hop_kv(dr, j).start()

    def finish(s, out):
        for dr in range(2):
            hop(s, dr, 2).wait_recv()

            @pl.loop(0, d // 32)
            def _(i):
                rs = pl.ds(pl.multiple_of(i * 32, 32), 32)
                out[rs, dr * eh:(dr + 1) * eh] = (rbuf[s, dr, 2, rs, :] + acc[s, 3, dr, rs, :]).astype(BF16)

    def piece(kk, j, lo=0, n=None):
        return gkv_hbm.at[kk, pl.ds(lo, d if n is None else n), pl.ds(pl.multiple_of(j * eq, 128), eq)]

    def ag(tag, ref, to, src=None):
        return rdma(ref if src is None else src, ref, ag_send.at[tag], ag_recv.at[tag], to)

    def ag_far(tag, to):
        return ag(tag, piece(k, rel[(0, 1)[tag - 3]], (tag - 3) * half, half), to)

    own_piece = pltpu.make_async_copy(fin_kv, piece(k, c), t_sem.at[5])

    def finish_kv():
        for dr in range(2):
            hop_kv(dr, 2).wait_recv()
            fin_kv[:, dr * (eq // 2):(dr + 1) * (eq // 2)] = rbuf_kv[dr, 2] + acc_kv[3, dr]
        ag(0, piece(k, c), cw, fin_kv).start()
        ag(1, piece(k, c), ccw, fin_kv).start()
        ag(2, piece(k, c), mate, fin_kv).start()
        own_piece.start()

    def ag_forward():
        ag(0, piece(k, rel[0]), cw).wait_recv()
        ag_far(3, cw).start()
        ag(1, piece(k, rel[1]), cw).wait_recv()
        ag_far(4, ccw).start()
        ag(5, piece(k, rel[0]), mate).start()
        ag(6, piece(k, rel[1]), mate).start()

    def ag_last():
        far = [piece(k, rel[2], i * half, half) for i in range(2)]
        for i in range(2):
            ag(3 + i, far[i], cw).wait_recv()
            ag(7 + i, far[i], mate).start()
        ag(2, piece(1 - k, c), mate).wait_recv()
        ag(5, piece(1 - k, rel[0]), mate).wait_recv()
        ag(6, piece(1 - k, rel[1]), mate).wait_recv()
        for i in range(2):
            ag(7 + i, piece(1 - k, rel[2], i * half, half), mate).wait_recv()
        for tag in range(3):
            ag(tag, piece(k, c), cw, fin_kv).wait_send()
        for tag in (3, 4, 7, 8):
            ag(tag, far[0], cw).wait_send()
        for tag in (5, 6):
            ag(tag, piece(k, c), cw).wait_send()
        own_piece.wait()

    dkv_in = pltpu.make_async_copy(dkv_hbm, dkv_v, t_sem.at[4])
    dkv_in.start()
    kp_copy = rdma(kind.at[1 - k], kp, kp_sem.at[0], kp_sem.at[1], mate)

    for dr in range(2):
        hop(0, dr, 0).start()
    acc_in = [pltpu.make_async_copy(acc_hbm.at[r], acc.at[0, r], a_sem.at[r]) for r in range(2)]
    for x in acc_in:
        x.start()

    def products(big, a_v, at):
        pr = Products(big, a_v, at, ld_sem, b_sem)
        dy_in = pr.load_b(dy_hbm, dyp_hbm)
        hn_in = pr.load_b(hn_hbm, hnp_hbm)
        jobs = [(0, 2), (0, 3)] + [(1, r) for r in range(4)]

        def fetch(i):
            s, r = jobs[i]
            return pr.load_a(i, (o_hbm, dq_hbm)[s].at[:, k, rel[r]], (op_hbm, dqp_hbm)[s].at[:, rel[r]])
        for x in dy_in:
            x.start()
        for i in range(2):
            for x in fetch(i):
                x.start()
        dkv_in.wait()
        for b in range(nb):
            lo, hi = dkv_v[b, :, :half].astype(F32), dkv_v[b, :, half:d].astype(F32)
            cs, sn = cos_ref[...], sin_ref[...]
            kind[0, b, :, :half] = (lo * cs + hi * sn).astype(BF16)
            kind[0, b, :, half:] = (hi * cs - lo * sn).astype(BF16)
            kind[1, b] = dkv_v[b, :, d:]
        kp_copy.start()
        for i, (s, r) in enumerate(jobs):
            if i == 2:
                pr.turn(0, kind.at[k])
                kp_copy.wait_recv()
                pr.turn(1, kp)
                for x in hn_in:
                    x.wait()
                for q in range(4):
                    for dr in range(2):
                        acc_kv[q, dr] = pr.both(pl.ds(pl.multiple_of(rel[q] * eq + dr * (eq // 2), 128), eq // 2))
                for dr in range(2):
                    hop_kv(dr, 0).start()
            for x in fetch(i):
                x.wait()
            pr.turn(0, a_v.at[i % 2, 0])
            pr.turn(1, a_v.at[i % 2, 1])
            if i + 2 < len(jobs):
                for x in fetch(i + 2):
                    x.start()
            if i == 0:
                for x in dy_in:
                    x.wait()
            if s == 1 and r < 2:
                pr.columns(acc.at[s, r], 0, 2, 2 * r)
                hop(s, r, 0).start()
                pr.columns(acc.at[s, r], 2, 4, 2 * r)
            else:
                pr.columns(acc.at[s, r], 0, 4)
            if i == 1:
                for x in hn_in:
                    x.start()

    pl.run_scoped(products, pltpu.VMEM((2, n_tok, e), BF16), pltpu.VMEM((2, 2, nb, tok, d), BF16), pltpu.VMEM((2, d, n_tok), BF16))
    for x in acc_in:
        x.wait()
    pass_on(0, 1)
    pass_on_kv(1)

    mc = 2 * tok
    units = nb // 2

    def attn_out(wo_v, o_v, x_v, y_v):
        w_in = pltpu.make_async_copy(wo_hbm, wo_v, b_sem.at[0])
        w_in.start()

        def load(u):
            return (pltpu.make_async_copy(o_hbm.at[pl.ds(2 * u, 2)], o_v.at[u % 2], ld_sem.at[u % 2, 0]),
                    pltpu.make_async_copy(x_hbm.at[pl.ds(u * mc, mc)], x_v.at[u % 2], ld_sem.at[u % 2, 1]))

        def put(u):
            return pltpu.make_async_copy(y_v.at[u % 2], y_hbm.at[pl.ds(u * mc, mc)], t_sem.at[u % 2])
        for x in load(0):
            x.start()
        w_in.wait()
        for u in range(units):
            if u + 1 < units:
                for x in load(u + 1):
                    x.start()
            for x in load(u):
                x.wait()
            if u >= 2:
                put(u - 2).wait()
            sl = u % 2

            @pl.loop(0, 4)
            def _(n):
                cols = pl.ds(pl.multiple_of(n * eq, 128), eq)
                o_rows = jnp.concatenate([jnp.concatenate([o_v[sl, i, h % 2, h // 2] for h in range(8)], axis=1) for i in range(2)], axis=0)
                r = dot_nn(o_rows, wo_v[:, cols])
                y_v[sl, :, cols] = (x_v[sl, :, cols].astype(F32) + r).astype(BF16)
            put(u).start()
        for u in range(max(0, units - 2), units):
            put(u).wait()

    pl.run_scoped(attn_out, pltpu.VMEM((8 * d, e), BF16), pltpu.VMEM((2, 2, 2, 4, tok, d), BF16),
                  pltpu.VMEM((2, mc, e), BF16), pltpu.VMEM((2, mc, e), BF16))
    pass_on(1, 1)

    def hidden_grad(wq_v, wk_v, wv_v, dq_v, x_v, dy_v, dh, gx_v):
        w_in = pltpu.make_async_copy(wq_hbm, wq_v, b_sem.at[0])
        w_in.start()
        w2_in = (pltpu.make_async_copy(wk_hbm, wk_v, b_sem.at[1]), pltpu.make_async_copy(wv_hbm, wv_v, ld_sem.at[1, 1]))
        for x in w2_in:
            x.start()

        def load(u):
            return (pltpu.make_async_copy(dq_hbm.at[pl.ds(2 * u, 2)], dq_v, ld_sem.at[0, 0]),
                    pltpu.make_async_copy(x_hbm.at[pl.ds(u * mc, mc)], x_v, ld_sem.at[0, 1]),
                    pltpu.make_async_copy(dy_hbm.at[pl.ds(u * mc, mc)], dy_v, ld_sem.at[1, 0]))

        def put(u):
            return pltpu.make_async_copy(gx_v, gx_hbm.at[pl.ds(u * mc, mc)], t_sem.at[0])
        gain = g_ref[...].astype(F32).reshape(1, e)
        gln_acc[...] = jnp.zeros_like(gln_acc)
        for x in load(0):
            x.start()
        w_in.wait()
        for x in w2_in:
            x.wait()
        for u in range(units):
            for x in load(u):
                x.wait()

            @pl.loop(0, 4)
            def _(n):
                rows = pl.ds(pl.multiple_of(n * eq, 128), eq)
                t = None
                for h in range(8):
                    a = jnp.concatenate([dq_v[i, h % 2, h // 2] for i in range(2)], axis=0)
                    p = dot_nt(a, wq_v[h, rows, :])
                    t = p if t is None else t + p
                for j in range(2):
                    a = jnp.concatenate([kind[j, 2 * u + i] for i in range(2)], axis=0)
                    t = t + dot_nt(a, (wk_v, wv_v)[j][rows, :])
                dh[:, rows] = t
            if u >= 1:
                put(u - 1).wait()

            @pl.loop(0, mc // 16)
            def _(r):
                rs = pl.ds(pl.multiple_of(r * 16, 16), 16)
                x = x_v[rs, :].astype(F32)
                cx = x - jnp.mean(x, axis=1, keepdims=True)
                inv = lax.rsqrt(jnp.mean(cx * cx, axis=1, keepdims=True) + LN_EPS)
                xh = cx * inv
                g = dh[rs, :]
                pr = g * xh
                gln_acc[...] += pr[:8] + pr[8:]
                gh = g * gain
                m1 = jnp.mean(gh, axis=1, keepdims=True)
                m2 = jnp.mean(gh * xh, axis=1, keepdims=True)
                gx_v[rs, :] = (inv * (gh - m1 - xh * m2) + dy_v[rs, :].astype(F32)).astype(BF16)
            put(u).start()
            if u + 1 < units:
                for x in load(u + 1):
                    x.start()
            if u == units // 2 - 1:
                pass_on_kv(2)
                pass_on(0, 2)
        put(units - 1).wait()

    pl.run_scoped(hidden_grad, pltpu.VMEM((8, e, d), BF16), pltpu.VMEM((e, d), BF16), pltpu.VMEM((e, d), BF16), pltpu.VMEM((2, 2, 4, tok, d), BF16),
                  pltpu.VMEM((mc, e), BF16), pltpu.VMEM((mc, e), BF16), pltpu.VMEM((mc, e), F32), pltpu.VMEM((mc, e), BF16))
    gl_recv[me] = jnp.sum(gln_acc[...], axis=0, keepdims=True)
    finish_kv()
    pass_on(1, 2)
    gl = [rdma(gl_recv.at[me], gl_recv.at[me], gl_send.at[o - 1], gl_rsem.at[o - 1], lax.rem(me + o, 8)) for o in range(1, 8)]
    for x in gl:
        x.start()
    finish(0, gwo_ref)
    ag_forward()
    finish(1, gwq_ref)
    for o in range(1, 8):
        src = lax.rem(me + 8 - o, 8)
        rdma(gl_recv.at[src], gl_recv.at[src], gl_send.at[o - 1], gl_rsem.at[o - 1], mate).wait_recv()
    total = gl_recv[0]
    for i in range(1, 8):
        total = total + gl_recv[i]
    gln_ref[...] = total
    ag_last()
    for x in gl:
        x.wait_send()
    kp_copy.wait_send()
    for dr in range(2):
        for j in range(3):
            hop_kv(dr, j).wait_send()
            for s in range(2):
                hop(s, dr, j).wait_send()


def gradients(o, o_p, acc, dq, dq_p, hn, hn_p, dy, dy_p, dkv, wqf, wof, w_k, w_v, x, gain, cos_t, sin_t):
    nb, tok, e = x.shape
    n_tok = nb * tok
    d = dq.shape[-1]
    any_spec = pl.BlockSpec(memory_space=pl.ANY)
    vmem = pl.BlockSpec(memory_space=pltpu.VMEM)
    dma = pltpu.SemaphoreType.DMA
    tokens = jax.ShapeDtypeStruct((n_tok, e), BF16)
    y, gx, gln, gwo, gwq_t, gkv_t = pl.pallas_call(
        functools.partial(grads_body, nb, tok),
        in_specs=[any_spec] * 15 + [vmem, vmem, vmem],
        out_specs=[any_spec, any_spec, vmem, vmem, vmem, any_spec],
        out_shape=[tokens, tokens, jax.ShapeDtypeStruct((1, e), F32), jax.ShapeDtypeStruct((d, e), BF16),
                   jax.ShapeDtypeStruct((d, e), BF16), jax.ShapeDtypeStruct((2, d, e), F32)],
        scratch_shapes=[pltpu.VMEM((2, 4, 2, d, e // 2), F32), pltpu.VMEM((4, 2, d, e // 8), F32),
                        pltpu.VMEM((2, 2, 3, d, e // 2), F32), pltpu.VMEM((2, 3, d, e // 8), F32),
                        pltpu.VMEM((2, nb, tok, d), BF16), pltpu.VMEM((nb, tok, d), BF16), pltpu.VMEM((nb, tok, 2 * d), BF16),
                        pltpu.VMEM((d, e // 4), F32), pltpu.VMEM((8, e), F32), pltpu.VMEM((8, 1, e), F32),
                        dma((2, 2, 3)), dma((2, 2, 3)), dma((2, 3)), dma((2, 3)), dma((9,)), dma((9,)), dma((7,)), dma((7,)),
                        dma((2,)), dma((2, 2)), dma((2,)), dma((6,)), dma((4,))],
        compiler_params=pltpu.CompilerParams(collective_id=2, has_side_effects=True, vmem_limit_bytes=63 * 2**20),
        cost_estimate=pl.CostEstimate(flops=10 * n_tok * e * e, bytes_accessed=120 * 2**20, transcendentals=0),
        name="gradients",
    )(o, o_p, acc, dq, dq_p, hn, hn_p, dy.reshape(n_tok, e), dy_p, dkv, wqf, wof.reshape(8 * d, e), w_k, w_v, x.reshape(n_tok, e),
      gain, cos_t, sin_t)
    y, gx, gwq, gwk, gwv, gwo, gln = place(nb, y, gx, gwq_t, gkv_t, gwo, gln)
    return y.reshape(nb, tok, e), gx.reshape(nb, tok, e), gln.reshape(e), gwq, gwk, gwv, gwo


def place_body(steps, y_in, gx_in, gq_in, gkv_in, go_in, gl_in, y, gx, gq, gk, gv, go, gl,
               y_v, gx_v, gq_v, gkv_v, go_v, gl_v, gq_t, gk_t, gv_t, in_sem, y_sem, out_sem, t_sem):
    n, w = y_in.shape[0] // steps, gq_in.shape[1] // steps
    small_in = [pltpu.make_async_copy(s, v, in_sem.at[i]) for i, (s, v) in enumerate(((gkv_in, gkv_v), (gq_in, gq_v), (go_in, go_v), (gl_in, gl_v)))]
    small_out = [pltpu.make_async_copy(v, o, out_sem.at[i]) for i, (v, o) in enumerate(((go_v, go), (gl_v, gl)))]

    def rows(i, size):
        return pl.ds(i * size, size)
    moves = [(pltpu.make_async_copy(s.at[rows(i, n)], v.at[rows(i, n)], y_sem.at[0, j, i]),
              pltpu.make_async_copy(v.at[rows(i, n)], o.at[rows(i, n)], y_sem.at[1, j, i]))
             for i in range(steps) for j, (s, v, o) in enumerate(((y_in, y_v, y), (gx_in, gx_v, gx)))]
    for x in small_in:
        x.start()
    for x, _ in moves:
        x.start()
    small_in[0].wait()
    small_in[1].wait()
    turned = []
    for i in range(steps):
        for j, (v, o) in enumerate(((gk_t, gk), (gv_t, gv), (gq_t, gq))):
            t = (gkv_v[j, :, i * w:(i + 1) * w] if j < 2 else gq_v[:, i * w:(i + 1) * w].astype(F32)).T
            v[i * w:(i + 1) * w, :] = t.astype(v.dtype)
            c = pltpu.make_async_copy(v.at[rows(i, w)], o.at[rows(i, w)], t_sem.at[j, i])
            c.start()
            turned.append(c)
        for x, z in moves[2 * i:2 * i + 2]:
            x.wait()
            z.start()
    for x, z in zip(small_in[2:], small_out):
        x.wait()
        z.start()
    for c in turned + small_out + [z for _, z in moves]:
        c.wait()


def place(steps, y, gx, gwq_t, gkv_t, gwo, gln):
    e = y.shape[1]
    d = gwo.shape[0]
    any_spec = pl.BlockSpec(memory_space=pl.ANY)
    dma = pltpu.SemaphoreType.DMA
    vm = pltpu.VMEM
    return pl.pallas_call(
        functools.partial(place_body, steps),
        in_specs=[any_spec] * 6,
        out_specs=[any_spec] * 7,
        out_shape=[jax.ShapeDtypeStruct(y.shape, BF16), jax.ShapeDtypeStruct(y.shape, BF16), jax.ShapeDtypeStruct((e, d), BF16),
                   jax.ShapeDtypeStruct((e, d), F32), jax.ShapeDtypeStruct((e, d), F32), jax.ShapeDtypeStruct((d, e), BF16),
                   jax.ShapeDtypeStruct((1, e), F32)],
        scratch_shapes=[vm(y.shape, BF16), vm(y.shape, BF16), vm((d, e), BF16), vm((2, d, e), F32), vm((d, e), BF16), vm((1, e), F32),
                        vm((e, d), BF16), vm((e, d), F32), vm((e, d), F32),
                        dma((4,)), dma((2, 2, steps)), dma((2,)), dma((3, steps))],
        compiler_params=pltpu.CompilerParams(vmem_limit_bytes=63 * 2**20),
        cost_estimate=pl.CostEstimate(flops=0, bytes_accessed=8 * y.size + 24 * gwo.size, transcendentals=0),
        name="place",
    )(y, gx, gwq_t, gkv_t, gwo, gln)


def solution(mesh):
    act_spec = P('dp', 'tp', None)

    def device_step(x_loc, ln_scale, wq_loc, w_k, w_v, wo_loc, dy_loc):
        n_batch, tok, model_dim = x_loc.shape
        d = w_k.shape[1]
        t0 = lax.axis_index('tp') * tok
        cos_t, sin_t = rope_tables(t0 + jnp.arange(tok), d)

        gain = ln_scale
        kv0, hn, q, do, kv_loc, wq_h, wo_h, hn_p, dy_p = project(x_loc, gain, wq_loc, w_k, w_v, wo_loc, dy_loc, cos_t, sin_t)
        o, dq, dkv_loc, o_p, dq_p, acc = attention(q, do, kv_loc, kv0, dy_loc.reshape(-1, model_dim), dy_p, cos_t, sin_t)
        return gradients(o, o_p, acc, dq, dq_p, hn, hn_p, dy_loc, dy_p, dkv_loc, wq_h, wo_h, w_k, w_v, x_loc, gain, cos_t, sin_t)

    return jax.shard_map(device_step, mesh=mesh, in_specs=(act_spec, P(None), P(None, 'tp'), P(None, None), P(None, None), P('tp', None), act_spec), out_specs=(act_spec, act_spec, P('dp'), P('dp', 'tp'), P('dp', None), P('dp', None), P(('dp', 'tp'), None)), check_vma=False)
```
